32 devices in a mesh: fsdp: 4 (over x, core), ctx: 2 (over y), tp: 4 (over z).
Axes of the slice: x: 2, y: 2, z: 4, core: 2. Of those that a mesh axis runs over, the one named last changes fastest.
Arguments:
- features: bfloat16 [8, 24, 24, 768], P('fsdp', 'ctx'), may hold values from -6 to 6
- out_grad: float32 [8, 24, 24, 768], P('fsdp', 'ctx'), may hold values from -7 to 7
- regions: int32 [8, 24, 24], P('fsdp', 'ctx'), may hold values from 0 to 3
- rel_index: int32 [144, 144], replicated, may hold values from 0 to 528
- w_qkv: float32 [3, 768, 768], P(None, 'fsdp', 'tp'), may hold values from -0.21875 to 0.21875
- w_proj: float32 [768, 768], P('tp', 'fsdp'), may hold values from -0.875 to 0.875
- w_up: float32 [768, 3072], P('fsdp', 'tp'), may hold values from -0.21875 to 0.21875
- w_down: float32 [3072, 768], P('tp', 'fsdp'), may hold values from -0.109375 to 0.109375
- norm_vecs: float32 [6, 768], P(None, 'fsdp'), may hold values from -2.5 to 2.5
- head_bias: float32 [2, 24, 32], P(None, 'tp', 'fsdp'), may hold values from -3 to 3
- hidden_bias: float32 [96, 32], P('tp', 'fsdp'), may hold values from -3 to 3
- rel_table: float32 [529, 24], P(None, 'tp'), may hold values from -4 to 4
- row_qkv: float32 [3, 768], P(None, 'fsdp'), may hold values from 921.6 to 18432
- col_qkv: float32 [3, 768], P(None, 'tp'), may hold values from 921.6 to 18432
- row_proj: float32 [768], P('tp'), may hold values from 92.16 to 1843.2
- col_proj: float32 [768], P('fsdp'), may hold values from 92.16 to 1843.2
- row_up: float32 [768], P('fsdp'), may hold values from 138.24 to 2304
- col_up: float32 [3072], P('tp'), may hold values from 138.24 to 2304
- row_down: float32 [3072], P('tp'), may hold values from 460.8 to 6912
- col_down: float32 [768], P('fsdp'), may hold values from 460.8 to 6912
- state_norm: float32 [6, 768], P(None, 'fsdp'), may hold values from 230.4 to 23040
- state_heads: float32 [2, 24, 32], P(None, 'tp', 'fsdp'), may hold values from 921.6 to 18432
- state_hidden: float32 [96, 32], P('tp', 'fsdp'), may hold values from 138.24 to 2304
- state_table: float32 [529, 24], P(None, 'tp'), may hold values from 2.304 to 92.16
Outputs:
- block_out: float32 [8, 24, 24, 768], P('fsdp', 'ctx')
- grad_input: float32 [8, 24, 24, 768], P('fsdp', 'ctx')
- grad_qkv: float32 [3, 768, 768], P(None, 'fsdp', 'tp')
- grad_proj: float32 [768, 768], P('tp', 'fsdp')
- grad_up: float32 [768, 3072], P('fsdp', 'tp')
- grad_down: float32 [3072, 768], P('tp', 'fsdp')
- grad_norm: float32 [6, 768], P(None, 'fsdp')
- grad_heads: float32 [2, 24, 32], P(None, 'tp', 'fsdp')
- grad_hidden: float32 [96, 32], P('tp', 'fsdp')
- grad_table: float32 [529, 24], P(None, 'tp')
- new_qkv: float32 [3, 768, 768], P(None, 'fsdp', 'tp')
- new_proj: float32 [768, 768], P('tp', 'fsdp')
- new_up: float32 [768, 3072], P('fsdp', 'tp')
- new_down: float32 [3072, 768], P('tp', 'fsdp')
- new_norm: float32 [6, 768], P(None, 'fsdp')
- new_heads: float32 [2, 24, 32], P(None, 'tp', 'fsdp')
- new_hidden: float32 [96, 32], P('tp', 'fsdp')
- new_table: float32 [529, 24], P(None, 'tp')
- copy_qkv: bfloat16 [3, 768, 768], P(None, 'fsdp', 'tp')
- copy_proj: bfloat16 [768, 768], P('tp', 'fsdp')
- copy_up: bfloat16 [768, 3072], P('fsdp', 'tp')
- copy_down: bfloat16 [3072, 768], P('tp', 'fsdp')
- row_qkv_new: float32 [3, 768], P(None, 'fsdp')
- col_qkv_new: float32 [3, 768], P(None, 'tp')
- row_proj_new: float32 [768], P('tp')
- col_proj_new: float32 [768], P('fsdp')
- row_up_new: float32 [768], P('fsdp')
- col_up_new: float32 [3072], P('tp')
- row_down_new: float32 [3072], P('tp')
- col_down_new: float32 [768], P('fsdp')
- state_norm_new: float32 [6, 768], P(None, 'fsdp')
- state_heads_new: float32 [2, 24, 32], P(None, 'tp', 'fsdp')
- state_hidden_new: float32 [96, 32], P('tp', 'fsdp')
- state_table_new: float32 [529, 24], P(None, 'tp')
- clip_rms: float32 [], replicated
The draws below stay inside these ranges and needn't reach their ends.
All inputs are finite; a program needn't handle non-finite values.
Results may differ from the reference program's by a relative error of at most 0.012.
The reference program's roundings to bfloat16 on the way count: a program that leaves them out, or rounds other values in their place, can miss the bound.
Values may be sent and summed in bfloat16 or wider, within the bound.
A program may use at most 128 MiB of HBM per device.

```python
import math
import jax
import jax.numpy as jnp
from jax import lax

D = 768
HEADS = 24
HD = 32
FF = 3072
WIN = 12
SHIFT = 6
RELP = 529
HH = 24
WW = 24
IMG_DEV = 2
IMAGES = 8
N_FSDP = 4


def draw_out_grad(key, part):
    position = jnp.arange(D, dtype=jnp.float32) / (D - 1)
    feature_scale = jnp.exp(jnp.log(3.0) * (position - 0.5))
    base = jnp.clip(jax.random.normal(key, (IMAGES, HH, WW, D), jnp.float32), -4.0, 4.0)
    return base * feature_scale


def draw_norm_vecs(key, part):
    position = jnp.arange(D, dtype=jnp.float32) / (D - 1)
    feature_scale = jnp.exp(jnp.log(3.0) * (position - 0.5))
    picker = jnp.array([1.0, 0.0, 0.0, 1.0, 0.0, 0.0], jnp.float32)[:, None]
    noise = jnp.clip(jax.random.normal(key, (6, D), jnp.float32), -3.0, 3.0)
    gain_rows = feature_scale * (1.0 + 0.1 * noise)
    bias_rows = 0.5 * noise
    return picker * gain_rows + (1.0 - picker) * bias_rows


def touch_ends(drawn, rng, smallest, high):
    longest = drawn.shape.index(max(drawn.shape))
    spots = []
    for shift in (0, 1):
        where = [jax.random.randint(jax.random.fold_in(rng, axis), (), 0, length) for axis, length in enumerate(drawn.shape)]
        where[longest] = (where[longest] + shift) % drawn.shape[longest]
        spots.append(tuple(where))
    return drawn.at[spots[0]].set(smallest).at[spots[1]].set(high)


def level_of(own_key, shape, split, smallest, high):
    gain, own = 1.0, jax.random.fold_in(own_key, 6)
    for dim, shards_of in split:
        draws = jnp.exp(jax.random.uniform(jax.random.fold_in(own, dim), (shards_of,), jnp.float32, smallest / len(split), high / len(split)))
        gain = gain * jnp.repeat(draws, shape[dim] // shards_of).reshape([-1 if axis == dim else 1 for axis in range(len(shape))])
    return gain


def normal_values(stream_key, shape, deviation, reach, cuts=(), held_as=jnp.bfloat16):
    level = level_of(stream_key, shape, cuts, -0.22, 0.18) if cuts else 1.0
    values = jax.random.normal(stream_key, shape, jnp.float32) * deviation * level
    return jnp.minimum(jnp.maximum(values, -reach), reach).astype(held_as)


def setup_inputs(seed: int = 0) -> dict:
    key_of = jax.random.split(jax.random.key(seed), 25)
    return {
        "features": normal_values(key_of[0], (IMAGES, HH, WW, D), 1.0, 6.0, ((0, 4), (1, 2))),
        "out_grad": draw_out_grad(jax.random.fold_in(key_of[24], 71), 0),
        "regions": touch_ends(jax.random.randint(key_of[2], (IMAGES, HH, WW), 0, 4), jax.random.fold_in(key_of[2], 1), 0, 3).astype(jnp.int32),
        "rel_index": touch_ends(jax.random.randint(key_of[3], (WIN * WIN, WIN * WIN), 0, RELP), jax.random.fold_in(key_of[3], 1), 0, RELP - 1).astype(jnp.int32),
        "w_qkv": normal_values(key_of[4], (3, D, D), D ** -0.5, 0.21875, ((1, 4), (2, 4)), jnp.float32),
        "w_proj": normal_values(key_of[5], (D, D), (D // 16) ** -0.5, 0.875, ((0, 4), (1, 4)), jnp.float32),
        "w_up": normal_values(key_of[6], (D, FF), D ** -0.5, 0.21875, ((0, 4), (1, 4)), jnp.float32),
        "w_down": normal_values(key_of[7], (FF, D), FF ** -0.5, 0.109375, ((0, 4), (1, 4)), jnp.float32),
        "norm_vecs": draw_norm_vecs(jax.random.fold_in(key_of[24], 71), 0),
        "head_bias": normal_values(key_of[9], (2, HEADS, HD), 0.5, 3.0, ((1, 4), (2, 4)), jnp.float32),
        "hidden_bias": normal_values(key_of[10], (FF // HD, HD), 0.5, 3.0, ((0, 4), (1, 4)), jnp.float32),
        "rel_table": normal_values(key_of[11], (RELP, HEADS), 1.0, 4.0, ((1, 4),), jnp.float32),
        "row_qkv": jnp.clip(jnp.exp(math.log(18432.0) - 2.9957323 * jax.random.uniform(key_of[12], (3, D), jnp.float32) ** level_of(key_of[12], (3, D), ((1, 4),), -0.2, 0.2)), 921.6, 18432.0),
        "col_qkv": jnp.clip(jnp.exp(math.log(18432.0) - 2.9957323 * jax.random.uniform(key_of[13], (3, D), jnp.float32) ** level_of(key_of[13], (3, D), ((1, 4),), -0.2, 0.2)), 921.6, 18432.0),
        "row_proj": jnp.clip(jnp.exp(math.log(1843.2) - 2.9957322 * jax.random.uniform(key_of[14], (D,), jnp.float32) ** level_of(key_of[14], (D,), ((0, 4),), -0.2, 0.2)), 92.16, 1843.2),
        "col_proj": jnp.clip(jnp.exp(math.log(1843.2) - 2.9957322 * jax.random.uniform(key_of[15], (D,), jnp.float32) ** level_of(key_of[15], (D,), ((0, 4),), -0.2, 0.2)), 92.16, 1843.2),
        "row_up": jnp.clip(jnp.exp(math.log(2304.0) - 2.8134107 * jax.random.uniform(key_of[16], (D,), jnp.float32) ** level_of(key_of[16], (D,), ((0, 4),), -0.2, 0.2)), 138.24, 2304.0),
        "col_up": jnp.clip(jnp.exp(math.log(2304.0) - 2.8134107 * jax.random.uniform(key_of[17], (FF,), jnp.float32) ** level_of(key_of[17], (FF,), ((0, 4),), -0.2, 0.2)), 138.24, 2304.0),
        "row_down": jnp.clip(jnp.exp(math.log(6912.0) - 2.7080502 * jax.random.uniform(key_of[18], (FF,), jnp.float32) ** level_of(key_of[18], (FF,), ((0, 4),), -0.2, 0.2)), 460.8, 6912.0),
        "col_down": jnp.clip(jnp.exp(math.log(6912.0) - 2.7080502 * jax.random.uniform(key_of[19], (D,), jnp.float32) ** level_of(key_of[19], (D,), ((0, 4),), -0.2, 0.2)), 460.8, 6912.0),
        "state_norm": jnp.clip(jnp.exp(math.log(23040.0) - 4.6051702 * jax.random.uniform(key_of[20], (6, D), jnp.float32) ** level_of(key_of[20], (6, D), ((1, 4),), -0.2, 0.2)), 230.4, 23040.0),
        "state_heads": jnp.clip(jnp.exp(math.log(18432.0) - 2.9957323 * jax.random.uniform(key_of[21], (2, HEADS, HD), jnp.float32) ** level_of(key_of[21], (2, HEADS, HD), ((1, 4), (2, 4)), -0.2, 0.2)), 921.6, 18432.0),
        "state_hidden": jnp.clip(jnp.exp(math.log(2304.0) - 2.8134107 * jax.random.uniform(key_of[22], (FF // HD, HD), jnp.float32) ** level_of(key_of[22], (FF // HD, HD), ((0, 4), (1, 4)), -0.2, 0.2)), 138.24, 2304.0),
        "state_table": jnp.clip(jnp.exp(math.log(92.16) - 3.6888795 * jax.random.uniform(key_of[23], (RELP, HEADS), jnp.float32) ** level_of(key_of[23], (RELP, HEADS), ((1, 4),), -0.2, 0.2)), 2.304, 92.16),
    }


DECAY_RATE = 0.5
STAT_EPS = 1e-06
NORM_EPS = 1e-05
MASK_FILL = -100.0
STEP_RATE = 1.0
CLIP_LEVEL = 0.25
TOP_PRECISION = lax.Precision.HIGHEST

@jax.custom_vjp
def low(v):
    return lax.optimization_barrier(v.astype(jnp.bfloat16)).astype(jnp.float32)

@jax.custom_vjp
def low_back(v):
    return v

def low_keep(v):
    return (low(v), None)

def low_pass(kept, grad):
    return (grad,)

def back_keep(v):
    return (v, None)

def back_low(kept, grad):
    return (low(grad),)
low.defvjp(low_keep, low_pass)
low_back.defvjp(back_keep, back_low)

def layer_norm(values, gain_row, offset):
    mean_val = lax.optimization_barrier(jnp.mean(values, axis=-1, keepdims=True))
    centred = values - mean_val
    var_val = lax.optimization_barrier(jnp.mean(centred * centred, axis=-1, keepdims=True))
    return centred * lax.rsqrt(var_val + NORM_EPS) * gain_row + offset

def to_windows(values):
    image_count, row_count, col_count, channels = values.shape
    pieces = values.reshape(image_count, row_count // WIN, WIN, col_count // WIN, WIN, channels)
    return pieces.transpose(0, 1, 3, 2, 4, 5).reshape(-1, WIN * WIN, channels)

def from_windows(values, image_count, row_count, col_count):
    channels = values.shape[-1]
    pieces = values.reshape(image_count, row_count // WIN, col_count // WIN, WIN, WIN, channels)
    return pieces.transpose(0, 1, 3, 2, 4, 5).reshape(image_count, row_count, col_count, channels)

def forward(image_in, region_ids, rel_index, params):
    qkv_low, proj_low, up_low, down_low, vec_low, head_low, hidden_low, table_low = [low(member) for member in params]
    image_count = image_in.shape[0]
    rolled = jnp.roll(image_in, (-SHIFT, -SHIFT), axis=(1, 2))
    windows = to_windows(rolled)
    win_count = windows.shape[0]
    flat_one = windows.reshape(-1, D)
    normed_one = low(layer_norm(flat_one, vec_low[0], vec_low[1]))
    head_shape = (win_count, WIN * WIN, HEADS, HD)
    queries = low_back(low(jnp.dot(normed_one, qkv_low[0], precision=TOP_PRECISION) + head_low[0].reshape(D)))
    key_rows = low_back(low(jnp.dot(normed_one, qkv_low[1], precision=TOP_PRECISION)))
    value_rows = low_back(low(jnp.dot(normed_one, qkv_low[2], precision=TOP_PRECISION) + head_low[1].reshape(D)))
    queries = queries.reshape(head_shape)
    key_rows = key_rows.reshape(head_shape)
    value_rows = value_rows.reshape(head_shape)
    pos_bias = jnp.take(table_low, rel_index, axis=0).transpose(2, 0, 1)
    region_win = to_windows(region_ids[..., None])[..., 0]
    mask_add = jnp.where(region_win[:, :, None] == region_win[:, None, :], 0.0, MASK_FILL)
    products = jnp.einsum('wihc,wjhc->whij', queries, key_rows, precision=TOP_PRECISION)
    scores = low_back(products) * HD ** (-0.5) + pos_bias[None] + mask_add[:, None]
    prob_rows = low(jax.nn.softmax(scores, axis=-1))
    context = jnp.einsum('whij,wjhc->wihc', prob_rows, value_rows, precision=TOP_PRECISION)
    context = low_back(low(context)).reshape(-1, D)
    branch = low_back(jnp.dot(context, proj_low, precision=TOP_PRECISION))
    branch = from_windows(branch.reshape(win_count, WIN * WIN, D), image_count, HH, WW) + vec_low[2]
    resid = image_in + jnp.roll(branch, (SHIFT, SHIFT), axis=(1, 2))
    flat_two = resid.reshape(-1, D)
    normed_two = low(layer_norm(flat_two, vec_low[3], vec_low[4]))
    pre_act = low_back(jnp.dot(normed_two, up_low, precision=TOP_PRECISION)) + hidden_low.reshape(FF)
    hidden = low(jax.nn.gelu(pre_act, approximate=False))
    mixed = low_back(jnp.dot(hidden, down_low, precision=TOP_PRECISION)) + vec_low[5]
    return resid + mixed.reshape(resid.shape)

def factor_stats(grad, row_old, col_old):
    squares = grad * grad
    row_new = DECAY_RATE * row_old + (1.0 - DECAY_RATE) * (lax.optimization_barrier(jnp.mean(squares, axis=-1)) + STAT_EPS)
    col_new = DECAY_RATE * col_old + (1.0 - DECAY_RATE) * (lax.optimization_barrier(jnp.mean(squares, axis=-2)) + STAT_EPS)
    row_mean = lax.optimization_barrier(jnp.mean(row_new, axis=-1))[..., None, None]
    update = grad * lax.rsqrt(row_new[..., :, None] * col_new[..., None, :] / row_mean)
    return (row_new, col_new, update)

def plain_stats(grad, state_old):
    state_new = DECAY_RATE * state_old + (1.0 - DECAY_RATE) * (grad * grad + STAT_EPS)
    return (state_new, grad * lax.rsqrt(state_new))

def rel_scale(master, axes):
    return jnp.sqrt(lax.optimization_barrier(jnp.mean(master * master, axis=axes, keepdims=True)) + STAT_EPS)

def reference(features, out_grad, regions, rel_index, w_qkv, w_proj, w_up, w_down, norm_vecs, head_bias, hidden_bias, rel_table, row_qkv, col_qkv, row_proj, col_proj, row_up, col_up, row_down, col_down, state_norm, state_heads, state_hidden, state_table):
    params = (w_qkv, w_proj, w_up, w_down, norm_vecs, head_bias, hidden_bias, rel_table)
    image_all = features.astype(jnp.float32).reshape(N_FSDP, IMG_DEV, HH, WW, D)
    grad_all = out_grad.reshape(N_FSDP, IMG_DEV, HH, WW, D)
    region_all = regions.reshape(N_FSDP, IMG_DEV, HH, WW)

    def one_group(totals, member):
        image_in, grad_in, region_ids = member

        def run(image_val, param_vals):
            return forward(image_val, region_ids, rel_index, param_vals)
        result, pull = jax.vjp(run, image_in, params)
        grad_image, grad_params = pull(grad_in)
        totals = jax.tree.map(lambda left_val, right_val: left_val + right_val, totals, grad_params)
        return (totals, (result, grad_image))
    start = jax.tree.map(jnp.zeros_like, params)
    grad_list, (outputs, grad_images) = lax.scan(one_group, start, (image_all, grad_all, region_all))
    block_out = outputs.reshape(IMAGES, HH, WW, D)
    grad_input = grad_images.reshape(IMAGES, HH, WW, D)
    g_qkv, g_proj, g_up, g_down, g_norm, g_heads, g_hidden, g_table = grad_list
    row_qkv_new, col_qkv_new, u_qkv = factor_stats(g_qkv, row_qkv, col_qkv)
    row_proj_new, col_proj_new, u_proj = factor_stats(g_proj, row_proj, col_proj)
    row_up_new, col_up_new, u_up = factor_stats(g_up, row_up, col_up)
    row_down_new, col_down_new, u_down = factor_stats(g_down, row_down, col_down)
    state_norm_new, u_norm = plain_stats(g_norm, state_norm)
    state_heads_new, u_heads = plain_stats(g_heads, state_heads)
    state_hidden_new, u_hidden = plain_stats(g_hidden, state_hidden)
    state_table_new, u_table = plain_stats(g_table, state_table)
    updates = (u_qkv, u_proj, u_up, u_down, u_norm, u_heads, u_hidden, u_table)
    total_sq = sum((jnp.sum(member * member) for member in updates))
    count_all = 4 * D * D + 2 * D * FF + 8 * D + FF + RELP * HEADS
    clip_rms = jnp.sqrt(total_sq / count_all)
    factor = 1.0 / jnp.maximum(1.0, clip_rms / CLIP_LEVEL)
    new_qkv = w_qkv - STEP_RATE * rel_scale(w_qkv, (0, 1, 2)) * factor * u_qkv
    new_proj = w_proj - STEP_RATE * rel_scale(w_proj, (0, 1)) * factor * u_proj
    new_up = w_up - STEP_RATE * rel_scale(w_up, (0, 1)) * factor * u_up
    new_down = w_down - STEP_RATE * rel_scale(w_down, (0, 1)) * factor * u_down
    new_norm = norm_vecs - STEP_RATE * rel_scale(norm_vecs, (1,)) * factor * u_norm
    new_heads = head_bias - STEP_RATE * rel_scale(head_bias, (1, 2)) * factor * u_heads
    new_hidden = hidden_bias - STEP_RATE * rel_scale(hidden_bias, (0, 1)) * factor * u_hidden
    new_table = rel_table - STEP_RATE * rel_scale(rel_table, (0, 1)) * factor * u_table
    return (block_out, grad_input, g_qkv, g_proj, g_up, g_down, g_norm, g_heads, g_hidden, g_table, new_qkv, new_proj, new_up, new_down, new_norm, new_heads, new_hidden, new_table, new_qkv.astype(jnp.bfloat16), new_proj.astype(jnp.bfloat16), new_up.astype(jnp.bfloat16), new_down.astype(jnp.bfloat16), row_qkv_new, col_qkv_new, row_proj_new, col_proj_new, row_up_new, col_up_new, row_down_new, col_down_new, state_norm_new, state_heads_new, state_hidden_new, state_table_new, clip_rms)
```

```python
import jax
import jax.numpy as jnp
from jax import lax
from jax.sharding import PartitionSpec as P

D = 768
HEADS = 24
HD = 32
FF = 3072
WIN = 12
SHIFT = 6
RELP = 529


DECAY_RATE = 0.5
STAT_EPS = 1e-06
NORM_EPS = 1e-05
MASK_FILL = -100.0
STEP_RATE = 1.0
CLIP_LEVEL = 0.25


def passed_along(x, axis, by):
    count = lax.axis_size(axis)
    return lax.ppermute(x, axis, [(i, (i + by) % count) for i in range(count)])


def layer_norm(values, gain_row, offset):
    mean_val = jnp.mean(values, axis=-1, keepdims=True)
    centred = values - mean_val
    var_val = jnp.mean(centred * centred, axis=-1, keepdims=True)
    return centred * lax.rsqrt(var_val + NORM_EPS) * gain_row + offset


def exact_gelu(values):
    return jax.nn.gelu(values, approximate=False)


def to_windows(values):
    image_count, row_count, col_count, channels = values.shape
    pieces = values.reshape(image_count, row_count // WIN, WIN, col_count // WIN, WIN, channels)
    return pieces.transpose(0, 1, 3, 2, 4, 5).reshape(-1, WIN * WIN, channels)


def from_windows(values, image_count, row_count, col_count):
    channels = values.shape[-1]
    pieces = values.reshape(image_count, row_count // WIN, col_count // WIN, WIN, WIN, channels)
    return pieces.transpose(0, 1, 3, 2, 4, 5).reshape(image_count, row_count, col_count, channels)


def enter_frame(own_rows, received):
    joined = jnp.concatenate([own_rows[:, SHIFT:], received], axis=1)
    return jnp.roll(joined, -SHIFT, axis=2)


def project_heads(normed_low, weights_qkv, bias_query, bias_value, head_shape):
    query_full = (
        jnp.dot(normed_low, weights_qkv[0], preferred_element_type=jnp.float32) + bias_query
    )
    key_full = jnp.dot(normed_low, weights_qkv[1], preferred_element_type=jnp.float32)
    value_full = (
        jnp.dot(normed_low, weights_qkv[2], preferred_element_type=jnp.float32) + bias_value
    )
    return tuple(
        (
            member.astype(jnp.bfloat16).reshape(head_shape)
            for member in (query_full, key_full, value_full)
        )
    )


def attention_scores(query_low, key_low, pos_bias, mask_add):
    products = jnp.einsum("wihc,wjhc->whij", query_low, key_low, preferred_element_type=jnp.float32)
    return products * query_low.shape[-1] ** (-0.5) + pos_bias[None] + mask_add[:, None]


def table_lookup(table_low, rel_index):
    win_tokens = rel_index.shape[0]
    code_ids = jnp.arange(table_low.shape[0], dtype=jnp.int32)
    index_blocks = rel_index.reshape(WIN, -1)

    def lookup(index_block):
        one_hot = (index_block[:, None] == code_ids[None, :]).astype(jnp.bfloat16)
        return jnp.dot(one_hot, table_low, preferred_element_type=jnp.float32)

    looked = lax.map(lookup, index_blocks)
    return looked.reshape(win_tokens, win_tokens, -1).transpose(2, 0, 1)


def table_grad(d_pos, rel_index, table_rows):
    heads_here = d_pos.shape[0]
    code_ids = jnp.arange(table_rows, dtype=jnp.int32)
    index_blocks = rel_index.reshape(WIN, -1)
    grad_blocks = d_pos.transpose(1, 2, 0).reshape(WIN, -1, heads_here)

    def accumulate(running, member):
        index_block, grad_block = member
        one_hot = (index_block[:, None] == code_ids[None, :]).astype(jnp.float32)
        added = lax.dot_general(
            one_hot,
            grad_block,
            (((0,), (0,)), ((), ())),
            precision=lax.Precision.HIGHEST,
            preferred_element_type=jnp.float32,
        )
        return (running + added, None)

    result_pair = lax.scan(
        accumulate, jnp.zeros((table_rows, heads_here), jnp.float32), (index_blocks, grad_blocks)
    )
    return result_pair[0]


def place(part_vec, index_at, whole_len):
    size_of = part_vec.shape[-1]
    base = jnp.zeros(part_vec.shape[:-1] + (whole_len,), jnp.float32)
    return lax.dynamic_update_slice_in_dim(base, part_vec, index_at * size_of, part_vec.ndim - 1)


def own_part(whole_vec, index_at, size_of):
    return lax.dynamic_slice_in_dim(whole_vec, index_at * size_of, size_of, whole_vec.ndim - 1)


def factored(grad, row_local, col_local, row_mean):
    return grad * lax.rsqrt(row_local[..., :, None] * col_local[..., None, :] / row_mean)


def plain_stats(grad, state_old):
    state_new = DECAY_RATE * state_old + (1.0 - DECAY_RATE) * (grad * grad + STAT_EPS)
    return (state_new, grad * lax.rsqrt(state_new))


def shard_sum(grad_list):
    return (
        lax.psum_scatter(grad_list[0], "fsdp", scatter_dimension=1, tiled=True),
        lax.psum_scatter(grad_list[1], "fsdp", scatter_dimension=1, tiled=True),
        lax.psum_scatter(grad_list[2], "fsdp", scatter_dimension=0, tiled=True),
        lax.psum_scatter(grad_list[3], "fsdp", scatter_dimension=1, tiled=True),
        lax.psum_scatter(grad_list[4], "fsdp", scatter_dimension=1, tiled=True),
        lax.psum_scatter(grad_list[5], "fsdp", scatter_dimension=2, tiled=True),
        lax.psum_scatter(grad_list[6], "fsdp", scatter_dimension=1, tiled=True),
    )


def band_sum(grad_list):
    return lax.psum(
        (
            grad_list[0],
            grad_list[1],
            grad_list[2],
            grad_list[3],
            grad_list[4],
            grad_list[5],
            grad_list[6],
        ),
        "ctx",
    )


def per_device(
    features,
    out_grad,
    regions,
    rel_index,
    w_qkv,
    w_proj,
    w_up,
    w_down,
    norm_vecs,
    head_bias,
    hidden_bias,
    rel_table,
    row_qkv,
    col_qkv,
    row_proj,
    col_proj,
    row_up,
    col_up,
    row_down,
    col_down,
    state_norm,
    state_heads,
    state_hidden,
    state_table,
):
    images, band_rows, across, model_width = features.shape
    win_tokens = WIN * WIN
    fsdp_at = lax.axis_index("fsdp")
    ctx_at = lax.axis_index("ctx")
    tp_at = lax.axis_index("tp")
    first_fsdp = (fsdp_at == 0).astype(jnp.float32)
    first_ctx = (ctx_at == 0).astype(jnp.float32)
    first_tp = (tp_at == 0).astype(jnp.float32)
    weights_qkv, weights_proj, weights_up, weights_down, vec_copy, head_copy, hidden_copy = (
        lax.all_gather(w_qkv.astype(jnp.bfloat16), "fsdp", axis=1, tiled=True),
        lax.all_gather(w_proj.astype(jnp.bfloat16), "fsdp", axis=1, tiled=True),
        lax.all_gather(w_up.astype(jnp.bfloat16), "fsdp", axis=0, tiled=True),
        lax.all_gather(w_down.astype(jnp.bfloat16), "fsdp", axis=1, tiled=True),
        lax.all_gather(norm_vecs.astype(jnp.bfloat16), "fsdp", axis=1, tiled=True),
        lax.all_gather(head_bias.astype(jnp.bfloat16), "fsdp", axis=2, tiled=True),
        lax.all_gather(hidden_bias.astype(jnp.bfloat16), "fsdp", axis=1, tiled=True),
    )
    norm_rows = vec_copy.astype(jnp.float32)
    bias_query = head_copy[0].reshape(-1).astype(jnp.float32)
    bias_value = head_copy[1].reshape(-1).astype(jnp.float32)
    bias_hidden = hidden_copy.reshape(-1).astype(jnp.float32)
    table_copy = rel_table.astype(jnp.bfloat16)
    local_width = weights_qkv.shape[2]
    heads_here = local_width // HD

    def roll_in(home):
        received = passed_along(home[:, :SHIFT], "ctx", -1)
        return to_windows(enter_frame(home, received)).reshape(-1, model_width)

    def roll_out(rolled_flat):
        band = jnp.roll(
            from_windows(
                rolled_flat.reshape(-1, win_tokens, model_width), images, band_rows, across
            ),
            SHIFT,
            axis=2,
        )
        lower = passed_along(band[:, band_rows - SHIFT :], "ctx", 1)
        return jnp.concatenate([lower, band[:, : band_rows - SHIFT]], axis=1)

    flat_one = roll_in(features).astype(jnp.float32)
    grad_flat = roll_in(out_grad)
    win_count = flat_one.shape[0] // win_tokens
    normed_one, pull_one = jax.vjp(layer_norm, flat_one, norm_rows[0], norm_rows[1])
    normed_one_low = normed_one.astype(jnp.bfloat16)
    head_shape = (win_count, win_tokens, heads_here, HD)
    query_low, key_low, value_low = project_heads(
        normed_one_low, weights_qkv, bias_query, bias_value, head_shape
    )
    pos_bias = table_lookup(table_copy, rel_index)
    region_win = to_windows(regions[..., None])[..., 0]
    mask_add = jnp.where(region_win[:, :, None] == region_win[:, None, :], 0.0, MASK_FILL).astype(
        jnp.float32
    )
    scores = attention_scores(query_low, key_low, pos_bias, mask_add)
    top_score = jnp.max(scores, axis=-1, keepdims=True)
    lifted = jnp.exp(scores - top_score)
    prob_rows = lifted / jnp.sum(lifted, axis=-1, keepdims=True)
    prob_low = prob_rows.astype(jnp.bfloat16)
    context = jnp.einsum("whij,wjhc->wihc", prob_low, value_low, preferred_element_type=jnp.float32)
    context_low = context.astype(jnp.bfloat16).reshape(-1, local_width)
    branch_part = jnp.dot(context_low, weights_proj, preferred_element_type=jnp.float32)
    branch = lax.psum(branch_part.astype(jnp.bfloat16), "tp").astype(jnp.float32) + norm_rows[2]
    flat_two = flat_one + branch
    normed_two, pull_two = jax.vjp(layer_norm, flat_two, norm_rows[3], norm_rows[4])
    normed_two_low = normed_two.astype(jnp.bfloat16)
    pre_act = jnp.dot(normed_two_low, weights_up, preferred_element_type=jnp.float32) + bias_hidden
    hidden, pull_gelu = jax.vjp(exact_gelu, pre_act)
    hidden_low = hidden.astype(jnp.bfloat16)
    mixed_part = jnp.dot(hidden_low, weights_down, preferred_element_type=jnp.float32)
    mixed_whole = lax.psum(mixed_part.astype(jnp.bfloat16), "tp").astype(jnp.float32)
    block_out = features.astype(jnp.float32) + roll_out(
        (branch + mixed_whole + norm_rows[5]).astype(jnp.bfloat16)
    ).astype(jnp.float32)
    grad_low = grad_flat.astype(jnp.bfloat16)
    grad_down_full = jnp.einsum(
        "tf,td->fd", hidden_low, grad_low, preferred_element_type=jnp.float32
    )
    grad_down_bias = jnp.sum(grad_flat, axis=0)
    d_hidden = jnp.einsum("td,fd->tf", grad_low, weights_down, preferred_element_type=jnp.float32)
    d_pre = pull_gelu(d_hidden)[0]
    d_pre_low = d_pre.astype(jnp.bfloat16)
    grad_hidden_bias = jnp.sum(d_pre, axis=0)
    grad_up_full = jnp.einsum(
        "td,tf->df", normed_two_low, d_pre_low, preferred_element_type=jnp.float32
    )
    d_two_part = jnp.einsum("tf,df->td", d_pre_low, weights_up, preferred_element_type=jnp.float32)
    d_two = lax.psum(d_two_part.astype(jnp.bfloat16), "tp").astype(jnp.float32)
    d_flat_two, grad_gain_two, grad_offset_two = pull_two(d_two)
    d_resid = grad_flat + d_flat_two
    grad_proj_bias = jnp.sum(d_resid, axis=0)
    d_branch = d_resid.astype(jnp.bfloat16)
    grad_proj_full = jnp.einsum(
        "tc,td->cd", context_low, d_branch, preferred_element_type=jnp.float32
    )
    d_context = (
        jnp.einsum("td,cd->tc", d_branch, weights_proj, preferred_element_type=jnp.float32)
        .astype(jnp.bfloat16)
        .reshape(head_shape)
    )
    d_probs = jnp.einsum(
        "wihc,wjhc->whij", d_context, value_low, preferred_element_type=jnp.float32
    )
    d_value_low = jnp.einsum(
        "whij,wihc->wjhc", prob_low, d_context, preferred_element_type=jnp.float32
    ).astype(jnp.bfloat16)
    d_scores = prob_rows * (d_probs - jnp.sum(prob_rows * d_probs, axis=-1, keepdims=True))
    d_pos = jnp.sum(d_scores, axis=0)
    d_scaled = (d_scores * HD ** (-0.5)).astype(jnp.bfloat16)
    d_query_low = jnp.einsum(
        "whij,wjhc->wihc", d_scaled, key_low, preferred_element_type=jnp.float32
    ).astype(jnp.bfloat16)
    d_key_low = jnp.einsum(
        "whij,wihc->wjhc", d_scaled, query_low, preferred_element_type=jnp.float32
    ).astype(jnp.bfloat16)
    d_heads = jnp.stack([d_query_low, d_key_low, d_value_low]).reshape(3, -1, local_width)
    grad_qkv_full = jnp.einsum(
        "td,ktc->kdc", normed_one_low, d_heads, preferred_element_type=jnp.float32
    )
    grad_head_bias = jnp.stack(
        [
            jnp.sum(d_heads[0].astype(jnp.float32), axis=0),
            jnp.sum(d_heads[2].astype(jnp.float32), axis=0),
        ]
    ).reshape(2, heads_here, HD)
    d_one_part = jnp.einsum("ktc,kdc->td", d_heads, weights_qkv, preferred_element_type=jnp.float32)
    d_one = lax.psum(d_one_part.astype(jnp.bfloat16), "tp").astype(jnp.float32)
    d_flat_one, grad_gain_one, grad_offset_one = pull_one(d_one)
    grad_input = out_grad + roll_out((d_flat_two + d_flat_one).astype(jnp.bfloat16)).astype(
        jnp.float32
    )
    table_part = table_grad(d_pos, rel_index, rel_table.shape[0])
    grad_norm_full = jnp.stack(
        [
            grad_gain_one,
            grad_offset_one,
            grad_proj_bias,
            grad_gain_two,
            grad_offset_two,
            grad_down_bias,
        ]
    )
    grad_list = (
        grad_qkv_full,
        grad_proj_full,
        grad_up_full,
        grad_down_full,
        grad_norm_full,
        grad_head_bias,
        grad_hidden_bias.reshape(-1, HD),
    )
    g_qkv, g_proj, g_up, g_down, g_norm, g_heads, g_hidden = shard_sum(band_sum(grad_list))
    d_shard = w_qkv.shape[1]
    hidden_here = w_up.shape[1]
    keep = 1.0 - DECAY_RATE
    sq_qkv = g_qkv * g_qkv
    sq_proj = g_proj * g_proj
    sq_up = g_up * g_up
    sq_down = g_down * g_down
    stat_rq = place(
        (keep * jnp.sum(sq_qkv, axis=2) / D + first_tp * (DECAY_RATE * row_qkv + keep * STAT_EPS))
        * first_ctx,
        fsdp_at,
        D,
    )
    stat_cq = place(
        (keep * jnp.sum(sq_qkv, axis=1) / D + first_fsdp * (DECAY_RATE * col_qkv + keep * STAT_EPS))
        * first_ctx,
        tp_at,
        D,
    )
    stat_rp = place(
        (
            keep * jnp.sum(sq_proj, axis=1) / D
            + first_fsdp * (DECAY_RATE * row_proj + keep * STAT_EPS)
        )
        * first_ctx,
        tp_at,
        D,
    )
    stat_cp = place(
        (keep * jnp.sum(sq_proj, axis=0) / D + first_tp * (DECAY_RATE * col_proj + keep * STAT_EPS))
        * first_ctx,
        fsdp_at,
        D,
    )
    stat_ru = place(
        (keep * jnp.sum(sq_up, axis=1) / FF + first_tp * (DECAY_RATE * row_up + keep * STAT_EPS))
        * first_ctx,
        fsdp_at,
        D,
    )
    stat_cu = place(
        (keep * jnp.sum(sq_up, axis=0) / D + first_fsdp * (DECAY_RATE * col_up + keep * STAT_EPS))
        * first_ctx,
        tp_at,
        FF,
    )
    stat_rd = place(
        (
            keep * jnp.sum(sq_down, axis=1) / D
            + first_fsdp * (DECAY_RATE * row_down + keep * STAT_EPS)
        )
        * first_ctx,
        tp_at,
        FF,
    )
    stat_cd = place(
        (
            keep * jnp.sum(sq_down, axis=0) / FF
            + first_tp * (DECAY_RATE * col_down + keep * STAT_EPS)
        )
        * first_ctx,
        fsdp_at,
        D,
    )
    table_whole = place(table_part, tp_at, HEADS)
    master_sq = jnp.concatenate(
        [
            jnp.stack(
                [
                    jnp.sum(w_qkv * w_qkv),
                    jnp.sum(w_proj * w_proj),
                    jnp.sum(w_up * w_up),
                    jnp.sum(w_down * w_down),
                ]
            )
            * first_ctx,
            jnp.sum(norm_vecs * norm_vecs, axis=1) * first_ctx * first_tp,
            jnp.sum(head_bias * head_bias, axis=(1, 2)) * first_ctx,
            jnp.sum(hidden_bias * hidden_bias)[None] * first_ctx,
            jnp.sum(rel_table * rel_table)[None] * first_ctx * first_fsdp,
        ]
    )
    (
        full_rq,
        full_cq,
        full_rp,
        full_cp,
        full_ru,
        full_cu,
        full_rd,
        full_cd,
        table_sum,
        master_total,
    ) = lax.psum(
        (
            stat_rq,
            stat_cq,
            stat_rp,
            stat_cp,
            stat_ru,
            stat_cu,
            stat_rd,
            stat_cd,
            table_whole,
            master_sq,
        ),
        ("fsdp", "ctx", "tp"),
    )
    u_qkv = factored(
        g_qkv,
        own_part(full_rq, fsdp_at, d_shard),
        own_part(full_cq, tp_at, local_width),
        jnp.mean(full_rq, axis=1)[:, None, None],
    )
    u_proj = factored(
        g_proj,
        own_part(full_rp, tp_at, local_width),
        own_part(full_cp, fsdp_at, d_shard),
        jnp.mean(full_rp),
    )
    u_up = factored(
        g_up,
        own_part(full_ru, fsdp_at, d_shard),
        own_part(full_cu, tp_at, hidden_here),
        jnp.mean(full_ru),
    )
    u_down = factored(
        g_down,
        own_part(full_rd, tp_at, hidden_here),
        own_part(full_cd, fsdp_at, d_shard),
        jnp.mean(full_rd),
    )
    g_table = own_part(table_sum, tp_at, heads_here)
    state_norm_new, u_norm = plain_stats(g_norm, state_norm)
    state_heads_new, u_heads = plain_stats(g_heads, state_heads)
    state_hidden_new, u_hidden = plain_stats(g_hidden, state_hidden)
    state_table_new, u_table = plain_stats(g_table, state_table)
    local_sq = (
        jnp.sum(u_qkv * u_qkv)
        + jnp.sum(u_proj * u_proj)
        + jnp.sum(u_up * u_up)
        + jnp.sum(u_down * u_down)
        + jnp.sum(u_heads * u_heads)
        + jnp.sum(u_hidden * u_hidden)
        + first_tp * jnp.sum(u_norm * u_norm)
        + first_fsdp * jnp.sum(u_table * u_table)
    )
    total_sq = lax.psum(local_sq, ("fsdp", "tp"))
    count_all = 4 * D * D + 2 * D * FF + 8 * D + FF + RELP * HEADS
    clip_rms = jnp.sqrt(total_sq / count_all)
    factor = 1.0 / jnp.maximum(1.0, clip_rms / CLIP_LEVEL)
    counts = jnp.array(
        [3 * D * D, D * D, D * FF, FF * D, D, D, D, D, D, D, D, D, FF, RELP * HEADS], jnp.float32
    )
    scales = jnp.sqrt(master_total / counts + STAT_EPS)
    new_qkv = w_qkv - STEP_RATE * scales[0] * factor * u_qkv
    new_proj = w_proj - STEP_RATE * scales[1] * factor * u_proj
    new_up = w_up - STEP_RATE * scales[2] * factor * u_up
    new_down = w_down - STEP_RATE * scales[3] * factor * u_down
    new_norm = norm_vecs - STEP_RATE * scales[4:10][:, None] * factor * u_norm
    new_heads = head_bias - STEP_RATE * scales[10:12][:, None, None] * factor * u_heads
    new_hidden = hidden_bias - STEP_RATE * scales[12] * factor * u_hidden
    new_table = rel_table - STEP_RATE * scales[13] * factor * u_table
    return (
        block_out,
        grad_input,
        g_qkv,
        g_proj,
        g_up,
        g_down,
        g_norm,
        g_heads,
        g_hidden,
        g_table,
        new_qkv,
        new_proj,
        new_up,
        new_down,
        new_norm,
        new_heads,
        new_hidden,
        new_table,
        new_qkv.astype(jnp.bfloat16),
        new_proj.astype(jnp.bfloat16),
        new_up.astype(jnp.bfloat16),
        new_down.astype(jnp.bfloat16),
        own_part(full_rq, fsdp_at, d_shard),
        own_part(full_cq, tp_at, local_width),
        own_part(full_rp, tp_at, local_width),
        own_part(full_cp, fsdp_at, d_shard),
        own_part(full_ru, fsdp_at, d_shard),
        own_part(full_cu, tp_at, hidden_here),
        own_part(full_rd, tp_at, hidden_here),
        own_part(full_cd, fsdp_at, d_shard),
        state_norm_new,
        state_heads_new,
        state_hidden_new,
        state_table_new,
        clip_rms,
    )


def solution(mesh):
    return jax.shard_map(
        per_device,
        mesh=mesh,
        in_specs=(
            P("fsdp", "ctx", None, None),
            P("fsdp", "ctx", None, None),
            P("fsdp", "ctx", None),
            P(),
            P(None, "fsdp", "tp"),
            P("tp", "fsdp"),
            P("fsdp", "tp"),
            P("tp", "fsdp"),
            P(None, "fsdp"),
            P(None, "tp", "fsdp"),
            P("tp", "fsdp"),
            P(None, "tp"),
            P(None, "fsdp"),
            P(None, "tp"),
            P("tp"),
            P("fsdp"),
            P("fsdp"),
            P("tp"),
            P("tp"),
            P("fsdp"),
            P(None, "fsdp"),
            P(None, "tp", "fsdp"),
            P("tp", "fsdp"),
            P(None, "tp"),
        ),
        out_specs=(
            P("fsdp", "ctx", None, None),
            P("fsdp", "ctx", None, None),
            P(None, "fsdp", "tp"),
            P("tp", "fsdp"),
            P("fsdp", "tp"),
            P("tp", "fsdp"),
            P(None, "fsdp"),
            P(None, "tp", "fsdp"),
            P("tp", "fsdp"),
            P(None, "tp"),
            P(None, "fsdp", "tp"),
            P("tp", "fsdp"),
            P("fsdp", "tp"),
            P("tp", "fsdp"),
            P(None, "fsdp"),
            P(None, "tp", "fsdp"),
            P("tp", "fsdp"),
            P(None, "tp"),
            P(None, "fsdp", "tp"),
            P("tp", "fsdp"),
            P("fsdp", "tp"),
            P("tp", "fsdp"),
            P(None, "fsdp"),
            P(None, "tp"),
            P("tp"),
            P("fsdp"),
            P("fsdp"),
            P("tp"),
            P("tp"),
            P("fsdp"),
            P(None, "fsdp"),
            P(None, "tp", "fsdp"),
            P("tp", "fsdp"),
            P(None, "tp"),
            P(),
        ),
        check_vma=False,
    )
```

```python
import functools

import jax
import jax.numpy as jnp
from jax import lax
from jax.experimental import pallas as pl
from jax.experimental.pallas import tpu as pltpu
from jax.sharding import PartitionSpec as P


D = 768
HEADS = 24
HD = 32
FF = 3072
WIN = 12
SHIFT = 6
RELP = 529


DECAY_RATE = 0.5
STAT_EPS = 1e-06
NORM_EPS = 1e-05
MASK_FILL = -100.0
STEP_RATE = 1.0
CLIP_LEVEL = 0.25


def passed_along(x, axis, by):
    count = lax.axis_size(axis)
    return lax.ppermute(x, axis, [(i, (i + by) % count) for i in range(count)])


def layer_norm(values, gain_row, offset):
    mean_val = jnp.mean(values, axis=-1, keepdims=True)
    centred = values - mean_val
    var_val = jnp.mean(centred * centred, axis=-1, keepdims=True)
    return centred * lax.rsqrt(var_val + NORM_EPS) * gain_row + offset


def exact_gelu(values):
    return jax.nn.gelu(values, approximate=False)


def to_windows(values):
    image_count, row_count, col_count, channels = values.shape
    pieces = values.reshape(image_count, row_count // WIN, WIN, col_count // WIN, WIN, channels)
    return pieces.transpose(0, 1, 3, 2, 4, 5).reshape(-1, WIN * WIN, channels)


def from_windows(values, image_count, row_count, col_count):
    channels = values.shape[-1]
    pieces = values.reshape(image_count, row_count // WIN, col_count // WIN, WIN, WIN, channels)
    return pieces.transpose(0, 1, 3, 2, 4, 5).reshape(image_count, row_count, col_count, channels)


def enter_frame(own_rows, received):
    joined = jnp.concatenate([own_rows[:, SHIFT:], received], axis=1)
    return jnp.roll(joined, -SHIFT, axis=2)


def project_heads(normed_low, weights_qkv, bias_query, bias_value, head_shape):
    query_full = (
        jnp.dot(normed_low, weights_qkv[0], preferred_element_type=jnp.float32) + bias_query
    )
    key_full = jnp.dot(normed_low, weights_qkv[1], preferred_element_type=jnp.float32)
    value_full = (
        jnp.dot(normed_low, weights_qkv[2], preferred_element_type=jnp.float32) + bias_value
    )
    return tuple(
        (
            member.astype(jnp.bfloat16).reshape(head_shape)
            for member in (query_full, key_full, value_full)
        )
    )


def attention_scores(query_low, key_low, pos_bias, mask_add):
    products = jnp.einsum("wihc,wjhc->whij", query_low, key_low, preferred_element_type=jnp.float32)
    return products * query_low.shape[-1] ** (-0.5) + pos_bias[None] + mask_add[:, None]


def table_lookup(table_low, rel_index):
    win_tokens = rel_index.shape[0]
    code_ids = jnp.arange(table_low.shape[0], dtype=jnp.int32)
    index_blocks = rel_index.reshape(WIN, -1)

    def lookup(index_block):
        one_hot = (index_block[:, None] == code_ids[None, :]).astype(jnp.bfloat16)
        return jnp.dot(one_hot, table_low, preferred_element_type=jnp.float32)

    looked = lax.map(lookup, index_blocks)
    return looked.reshape(win_tokens, win_tokens, -1).transpose(2, 0, 1)


def table_grad(d_pos, rel_index, table_rows):
    heads_here = d_pos.shape[0]
    code_ids = jnp.arange(table_rows, dtype=jnp.int32)
    index_blocks = rel_index.reshape(WIN, -1)
    grad_blocks = d_pos.transpose(1, 2, 0).reshape(WIN, -1, heads_here)

    def accumulate(running, member):
        index_block, grad_block = member
        one_hot = (index_block[:, None] == code_ids[None, :]).astype(jnp.float32)
        added = lax.dot_general(
            one_hot,
            grad_block,
            (((0,), (0,)), ((), ())),
            precision=lax.Precision.HIGHEST,
            preferred_element_type=jnp.float32,
        )
        return (running + added, None)

    result_pair = lax.scan(
        accumulate, jnp.zeros((table_rows, heads_here), jnp.float32), (index_blocks, grad_blocks)
    )
    return result_pair[0]


def place(part_vec, index_at, whole_len):
    size_of = part_vec.shape[-1]
    base = jnp.zeros(part_vec.shape[:-1] + (whole_len,), jnp.float32)
    return lax.dynamic_update_slice_in_dim(base, part_vec, index_at * size_of, part_vec.ndim - 1)


def own_part(whole_vec, index_at, size_of):
    return lax.dynamic_slice_in_dim(whole_vec, index_at * size_of, size_of, whole_vec.ndim - 1)


def factored(grad, row_local, col_local, row_mean):
    return grad * lax.rsqrt(row_local[..., :, None] * col_local[..., None, :] / row_mean)


def plain_stats(grad, state_old):
    state_new = DECAY_RATE * state_old + (1.0 - DECAY_RATE) * (grad * grad + STAT_EPS)
    return (state_new, grad * lax.rsqrt(state_new))


def shard_sum(grad_list):
    return (
        lax.psum_scatter(grad_list[0], "fsdp", scatter_dimension=1, tiled=True),
        lax.psum_scatter(grad_list[1], "fsdp", scatter_dimension=1, tiled=True),
        lax.psum_scatter(grad_list[2], "fsdp", scatter_dimension=0, tiled=True),
        lax.psum_scatter(grad_list[3], "fsdp", scatter_dimension=1, tiled=True),
        lax.psum_scatter(grad_list[4], "fsdp", scatter_dimension=1, tiled=True),
        lax.psum_scatter(grad_list[5], "fsdp", scatter_dimension=2, tiled=True),
        lax.psum_scatter(grad_list[6], "fsdp", scatter_dimension=1, tiled=True),
    )


def band_sum(grad_list):
    return lax.psum(
        (
            grad_list[0],
            grad_list[1],
            grad_list[2],
            grad_list[3],
            grad_list[4],
            grad_list[5],
            grad_list[6],
        ),
        "ctx",
    )


BF = jnp.bfloat16
F32 = jnp.float32
MESH = pl.DeviceIdType.MESH
TOK = WIN * WIN
HALF = D // 2
VMEM_LIMIT = 66_000_000


def dot(a, b):
    return lax.dot_general(a, b, (((1,), (0,)), ((), ())), preferred_element_type=F32)


def dot_t(a, b):
    return lax.dot_general(a, b, (((1,), (1,)), ((), ())), preferred_element_type=F32)


def t_dot(a, b):
    return lax.dot_general(a, b, (((0,), (0,)), ((), ())), preferred_element_type=F32)


def row_mean(x):
    return jnp.sum(x, axis=-1, keepdims=True) * (1.0 / x.shape[-1])


def remote(src, dst, send, recv, where):
    return pltpu.make_async_remote_copy(
        src_ref=src, dst_ref=dst, send_sem=send, recv_sem=recv, device_id=where, device_id_type=MESH
    )


def greet(barrier, places):
    for place_of in places:
        pl.semaphore_signal(barrier, inc=1, device_id=place_of, device_id_type=MESH)


class LineSum:
    def __init__(self, part, send, from_outer, from_mid, total, sems):
        self.part, self.send, self.from_outer, self.from_mid, self.total = (
            part, send, from_outer, from_mid, total,
        )
        self.s_out, self.r_out, self.s_mid, self.r_mid, self.s_tot, self.r_tot, self.s_cross = sems
        z = lax.axis_index("tp")
        self.is_mid = jnp.logical_and(z > 0, z < 3)
        self.is_outer = jnp.logical_not(self.is_mid)
        self.outer = jnp.where(z < 2, 0, 3)
        self.mid = jnp.where(z < 2, 1, 2)
        self.other_mid = 3 - self.mid
        self.own = self.mid - 1
        self.other = 1 - self.own

    @staticmethod
    def scratch(count):
        return [
            pltpu.VMEM((count, 2, TOK, HALF), F32),
            pltpu.VMEM((count, 2, TOK, HALF), BF),
            pltpu.VMEM((count, 2, TOK, HALF), BF),
            pltpu.VMEM((count, TOK, HALF), BF),
            pltpu.SemaphoreType.DMA((count, 2)),
            pltpu.SemaphoreType.DMA((count, 2)),
            pltpu.SemaphoreType.DMA((count,)),
            pltpu.SemaphoreType.DMA((count,)),
            pltpu.SemaphoreType.DMA((count, 2)),
            pltpu.SemaphoreType.DMA((count, 2)),
            pltpu.SemaphoreType.DMA((count,)),
        ]

    @staticmethod
    def build(refs, total):
        return LineSum(refs[0], refs[1], refs[2], refs[3], total, refs[4:11])

    @staticmethod
    def peers():
        return 2

    def greet(self, barrier):
        pl.semaphore_signal(
            barrier, inc=1, device_id={"tp": jnp.where(self.is_mid, self.outer, self.mid)},
            device_id_type=MESH,
        )

        @pl.when(self.is_mid)
        def _():
            pl.semaphore_signal(
                barrier, inc=1, device_id={"tp": self.other_mid}, device_id_type=MESH
            )

    def greet_count(self):
        return jnp.where(self.is_mid, 2, 1)

    def _to_mid(self, w, h):
        return remote(self.send.at[w, h], self.from_outer.at[w, h], self.s_out.at[w, h],
                      self.r_out.at[w, h], {"tp": self.mid})

    def _across(self, w):
        return remote(self.send.at[w, self.other], self.from_mid.at[w], self.s_mid.at[w],
                      self.r_mid.at[w], {"tp": self.other_mid})

    def _total_across(self, w, h):
        return remote(self.total.at[w, h], self.total.at[w, h], self.s_cross.at[w],
                      self.r_tot.at[w, h], {"tp": self.other_mid})

    def _total_out(self, w, h):
        return remote(self.total.at[w, h], self.total.at[w, h], self.s_tot.at[w, h],
                      self.r_tot.at[w, h], {"tp": self.outer})

    def put(self, w, value):
        self.part[w, 0] = value[:, :HALF]
        self.part[w, 1] = value[:, HALF:]

    def start(self, w):
        @pl.when(self.is_outer)
        def _():
            self.send[w, self.other] = self.part[w, self.other].astype(BF)
            self._to_mid(w, self.other).start()
            self.send[w, self.own] = self.part[w, self.own].astype(BF)
            self._to_mid(w, self.own).start()

    def cross(self, w):
        @pl.when(self.is_mid)
        def _():
            self._to_mid(w, self.other).wait_recv()
            self.send[w, self.other] = (
                self.part[w, self.other] + self.from_outer[w, self.other].astype(F32)
            ).astype(BF)
            self._across(w).start()

    def settle(self, w):
        @pl.when(self.is_mid)
        def _():
            self._to_mid(w, self.own).wait_recv()
            self._across(w).wait_recv()
            self.total[w, self.own] = (
                self.part[w, self.own]
                + self.from_outer[w, self.own].astype(F32)
                + self.from_mid[w].astype(F32)
            ).astype(BF)
            self._total_across(w, self.own).start()
            self._total_out(w, self.own).start()

    def hand(self, w):
        @pl.when(self.is_mid)
        def _():
            self._total_across(w, self.other).wait_recv()
            self._total_out(w, self.other).start()

    def arrive(self, w):
        @pl.when(self.is_outer)
        def _():
            self._total_out(w, 0).wait_recv()
            self._total_out(w, 1).wait_recv()

    def drain(self, w):
        @pl.when(self.is_outer)
        def _():
            self._to_mid(w, 0).wait_send()
            self._to_mid(w, 1).wait_send()

        @pl.when(self.is_mid)
        def _():
            self._across(w).wait_send()
            self._total_across(w, self.own).wait_send()
            self._total_out(w, 0).wait_send()
            self._total_out(w, 1).wait_send()


def window_rows(row_of, row_tmp, image, dst):
    for r in range(WIN):
        row_tmp[...] = row_of(image, r).astype(F32)
        dst[2 * image, r * WIN : (r + 1) * WIN, :] = row_tmp[SHIFT : SHIFT + WIN, :]
        dst[2 * image + 1, r * WIN : r * WIN + SHIFT, :] = row_tmp[SHIFT + WIN :, :]
        dst[2 * image + 1, r * WIN + SHIFT : (r + 1) * WIN, :] = row_tmp[:SHIFT, :]


def attention_forward_body(
    feat, og, wq, wp, wu, wd, small, table_t, ridx, regr, regc,
    wq_o, wp_o, wu_o, wd_o, rows_o, xw_o, ogw_o, n1_o, q_o, k_o, v_o, probs_o, ctx_o, br_o,
    sm_g, wp_g, wd_g, fh, gh, bias_s, row_tmp,
    ls_a, ls_b, ls_c, ls_d, ls_e, ls_f, ls_g, ls_h, ls_i, ls_j, ls_k,
    w_send, w_recv, h_send, h_recv,
):
    windows = xw_o.shape[0]
    images = windows // 2
    f = lax.axis_index("fsdp")
    c = lax.axis_index("ctx")
    near, far = f + 1 - 2 * lax.rem(f, 2), lax.rem(f + 2, 4)
    line = LineSum.build((ls_a, ls_b, ls_c, ls_d, ls_e, ls_f, ls_g, ls_h, ls_i, ls_j, ls_k), br_o)
    barrier = pltpu.get_barrier_semaphore()
    greet(barrier, [{"fsdp": near}, {"fsdp": far}, {"ctx": 1 - c}])
    line.greet(barrier)

    shard = wq.shape[1]

    def block(at):
        return pl.ds(pl.multiple_of(at * shard, shard), shard)

    wq_o[:, block(f), :] = wq[...].astype(BF)
    sm_g[f] = small[...].astype(BF)
    wp_g[f] = wp[...].astype(BF)
    wu_o[block(f), :] = wu[...].astype(BF)
    wd_g[f] = wd[...].astype(BF)
    pl.semaphore_wait(barrier, 3 + line.greet_count())

    items = [
        lambda at: sm_g.at[at],
        lambda at: wq_o.at[:, block(at), :],
        lambda at: wp_g.at[at],
        lambda at: wu_o.at[block(at), :],
        lambda at: wd_g.at[at],
    ]

    def copy_of(n, kind, at, where):
        ref = items[n](at)
        return remote(ref, ref, w_send.at[n, kind], w_recv.at[n, kind], {"fsdp": where})

    halo_f = [
        remote(feat.at[i, 0:SHIFT], fh.at[i], h_send.at[i], h_recv.at[i], {"ctx": 1 - c})
        for i in range(images)
    ]
    halo_g = [
        remote(og.at[i, 0:SHIFT], gh.at[i], h_send.at[images + i], h_recv.at[images + i], {"ctx": 1 - c})
        for i in range(images)
    ]
    for copy in halo_f:
        copy.start()
    for n in range(len(items)):
        copy_of(n, 0, f, far).start()
        copy_of(n, 1, f, near).start()
    for copy in halo_g:
        copy.start()

    def relay(n):
        copy_of(n, 0, f, far).wait_recv()
        copy_of(n, 2, far, near).start()

    def gathered(n):
        copy_of(n, 1, f, near).wait_recv()
        copy_of(n, 2, far, near).wait_recv()

    relay(0)

    def bias_rows(step, carry):
        rows = pl.ds(pl.multiple_of(step * 8, 8), 8)
        for part in range(2):
            idx = ridx[rows, part * 128 : (part + 1) * 128]
            low = jnp.bitwise_and(idx, 127)
            high = jnp.right_shift(idx, 7)
            picks = [high == n for n in range(5)]
            for h in range(bias_s.shape[0]):
                found = jnp.zeros((8, 128), F32)
                for n in range(5):
                    tab = jnp.broadcast_to(table_t[h : h + 1, n * 128 : (n + 1) * 128], (8, 128))
                    got = jnp.take_along_axis(tab, low, axis=1, mode="promise_in_bounds")
                    found = jnp.where(picks[n], got, found)
                bias_s[h, rows, part * 128 : (part + 1) * 128] = found
        return carry

    lax.fori_loop(0, TOK // 8, bias_rows, 0)
    gathered(0)
    relay(1)
    lanes = rows_o.shape[1]
    rows_o[...] = jnp.concatenate([sm_g[n].astype(F32) for n in range(4)], axis=1)
    unit = lax.broadcasted_iota(jnp.int32, (shard, lanes), 0)
    lane = lax.broadcasted_iota(jnp.int32, (shard, lanes), 1)
    biases = jnp.zeros((16, lanes), F32)
    for n in range(4):
        same = jnp.logical_and(
            jnp.right_shift(lane, 5) == jnp.right_shift(unit, 3),
            jnp.bitwise_and(lane, 31) == jnp.bitwise_and(unit, 7) + n * 8,
        )
        biases = biases + dot(sm_g[n], jnp.where(same, 1.0, 0.0).astype(BF))
    rows_o[8:16, :] = biases[8:16, :]

    for i in range(images):
        halo_f[i].wait_recv()
        window_rows(
            lambda im, r: feat[im, SHIFT + r] if r < SHIFT else fh[im, r - SHIFT], row_tmp, i, xw_o
        )
    gain, offset = rows_o[0:1, :], rows_o[1:2, :]
    width = q_o.shape[2]
    bias_q, bias_v = rows_o[9:10, :width], rows_o[10:11, :width]
    head_of = jnp.right_shift(lax.broadcasted_iota(jnp.int32, (1, width), 1), 5)
    heads = width // HD
    gathered(1)

    def window(w, carry):
        x = xw_o[w]
        mean_val = row_mean(x)
        centred = x - mean_val
        var_val = row_mean(centred * centred)
        n1 = (centred * lax.rsqrt(var_val + NORM_EPS) * gain + offset).astype(BF)
        n1_o[w] = n1
        q = (dot(n1, wq_o[0]) + bias_q).astype(BF)
        k = dot(n1, wq_o[1]).astype(BF)
        v = (dot(n1, wq_o[2]) + bias_v).astype(BF)
        q_o[w] = q
        k_o[w] = k
        v_o[w] = v
        mask = jnp.where(regc[w] == regr[w], 0.0, MASK_FILL)

        @pl.when(w >= 1)
        def _():
            line.cross(w - 1)

        @pl.when(w == 0)
        def _():
            relay(2)
            gathered(2)
            wp_o[...] = jnp.concatenate([wp_g[n] for n in range(4)], axis=1)

        context = jnp.zeros((TOK, width), F32)
        for h in range(heads):
            pick = jnp.where(head_of == h, 1.0, 0.0).astype(BF)
            scores = dot_t(q * pick, k) * HD ** (-0.5) + bias_s[h, :, :TOK] + mask
            lifted = jnp.exp(scores - jnp.max(scores, axis=-1, keepdims=True))
            probs = lifted / jnp.sum(lifted, axis=-1, keepdims=True)
            probs_o[w, h] = probs
            context = context + dot(probs.astype(BF), v * pick)
        ctx = context.astype(BF)
        ctx_o[w] = ctx
        line.put(w, dot(ctx, wp_o[...]))
        line.start(w)

        @pl.when(w >= 1)
        def _():
            line.settle(w - 1)

        @pl.when(w >= 2)
        def _():
            line.hand(w - 2)

        return carry

    lax.fori_loop(0, windows, window, 0)
    line.cross(windows - 1)
    line.hand(windows - 2)
    relay(3)
    line.settle(windows - 1)
    relay(4)
    line.hand(windows - 1)
    gathered(3)
    gathered(4)
    wd_o[...] = jnp.concatenate([wd_g[n] for n in range(4)], axis=1)
    for i in range(images):
        halo_g[i].wait_recv()
        window_rows(
            lambda im, r: og[im, SHIFT + r] if r < SHIFT else gh[im, r - SHIFT], row_tmp, i, ogw_o
        )
    for w in range(windows):
        line.arrive(w)
        line.drain(w)
    for copy in halo_f + halo_g:
        copy.wait_send()
    for n in range(len(items)):
        copy_of(n, 0, f, far).wait_send()
        copy_of(n, 1, f, near).wait_send()
        copy_of(n, 2, far, near).wait_send()


def vmem_call(body, outs, scratch, name, collective_id):
    def call(*args):
        return pl.pallas_call(
            body,
            out_shape=[jax.ShapeDtypeStruct(s, t) for s, t in outs],
            in_specs=[pl.BlockSpec(memory_space=pltpu.VMEM)] * len(args),
            out_specs=[pl.BlockSpec(memory_space=pltpu.VMEM)] * len(outs),
            scratch_shapes=scratch,
            compiler_params=pltpu.CompilerParams(
                collective_id=collective_id, has_side_effects=True, vmem_limit_bytes=VMEM_LIMIT
            ),
            name=name,
        )(*args)

    return call


def attention_forward(features, out_grad, regions, rel_index, w_qkv, w_proj, w_up, w_down,
                      norm_vecs, head_bias, hidden_bias, rel_table):
    images = features.shape[0]
    windows = 2 * images
    shard, width = w_qkv.shape[1], w_qkv.shape[2]
    hidden = w_up.shape[1]
    heads = width // HD
    small = jnp.concatenate(
        [
            norm_vecs,
            jnp.zeros((2, shard), F32),
            hidden_bias.reshape(1, shard),
            jnp.pad(head_bias.reshape(2, -1), ((0, 5), (0, shard - head_bias[0].size))),
        ],
        axis=0,
    )
    table_t = jnp.pad(
        rel_table.astype(BF).astype(F32).T, ((0, 8 - heads), (0, 640 - rel_table.shape[0]))
    )
    ridx = jnp.pad(rel_index, ((0, 0), (0, 256 - TOK)))
    region_win = to_windows(regions[..., None])[..., 0]
    outs = [
        ((3, D, width), BF), ((width, D), BF), ((D, hidden), BF), ((hidden, D), BF), ((16, D), F32),
        ((windows, TOK, D), F32), ((windows, TOK, D), F32), ((windows, TOK, D), BF),
        ((windows, TOK, width), BF), ((windows, TOK, width), BF), ((windows, TOK, width), BF),
        ((windows, heads, TOK, TOK), F32), ((windows, TOK, width), BF),
        ((windows, 2, TOK, HALF), BF),
    ]
    scratch = [
        pltpu.VMEM((4, 16, shard), BF),
        pltpu.VMEM((4, width, shard), BF),
        pltpu.VMEM((4, hidden, shard), BF),
        pltpu.VMEM((images, SHIFT, 24, D), BF),
        pltpu.VMEM((images, SHIFT, 24, D), F32),
        pltpu.VMEM((heads, TOK, 256), F32),
        pltpu.VMEM((24, D), F32),
        *LineSum.scratch(windows),
        pltpu.SemaphoreType.DMA((5, 3)),
        pltpu.SemaphoreType.DMA((5, 3)),
        pltpu.SemaphoreType.DMA((2 * images,)),
        pltpu.SemaphoreType.DMA((2 * images,)),
    ]
    call = vmem_call(attention_forward_body, outs, scratch, "attention_forward", 1)
    return call(features, out_grad, w_qkv, w_proj, w_up, w_down, small, table_t, ridx,
                region_win[:, None, :], region_win[:, :, None])


def per_device_plain(
    features,
    out_grad,
    regions,
    rel_index,
    w_qkv,
    w_proj,
    w_up,
    w_down,
    norm_vecs,
    head_bias,
    hidden_bias,
    rel_table,
    row_qkv,
    col_qkv,
    row_proj,
    col_proj,
    row_up,
    col_up,
    row_down,
    col_down,
    state_norm,
    state_heads,
    state_hidden,
    state_table,
):
    images, band_rows, across, model_width = features.shape
    win_tokens = WIN * WIN
    fsdp_at = lax.axis_index("fsdp")
    ctx_at = lax.axis_index("ctx")
    tp_at = lax.axis_index("tp")
    first_fsdp = (fsdp_at == 0).astype(jnp.float32)
    first_ctx = (ctx_at == 0).astype(jnp.float32)
    first_tp = (tp_at == 0).astype(jnp.float32)
    weights_qkv, weights_proj, weights_up, weights_down, vec_copy, head_copy, hidden_copy = (
        lax.all_gather(w_qkv.astype(jnp.bfloat16), "fsdp", axis=1, tiled=True),
        lax.all_gather(w_proj.astype(jnp.bfloat16), "fsdp", axis=1, tiled=True),
        lax.all_gather(w_up.astype(jnp.bfloat16), "fsdp", axis=0, tiled=True),
        lax.all_gather(w_down.astype(jnp.bfloat16), "fsdp", axis=1, tiled=True),
        lax.all_gather(norm_vecs.astype(jnp.bfloat16), "fsdp", axis=1, tiled=True),
        lax.all_gather(head_bias.astype(jnp.bfloat16), "fsdp", axis=2, tiled=True),
        lax.all_gather(hidden_bias.astype(jnp.bfloat16), "fsdp", axis=1, tiled=True),
    )
    norm_rows = vec_copy.astype(jnp.float32)
    bias_query = head_copy[0].reshape(-1).astype(jnp.float32)
    bias_value = head_copy[1].reshape(-1).astype(jnp.float32)
    bias_hidden = hidden_copy.reshape(-1).astype(jnp.float32)
    table_copy = rel_table.astype(jnp.bfloat16)
    local_width = weights_qkv.shape[2]
    heads_here = local_width // HD

    def roll_in(home):
        received = passed_along(home[:, :SHIFT], "ctx", -1)
        return to_windows(enter_frame(home, received)).reshape(-1, model_width)

    def roll_out(rolled_flat):
        band = jnp.roll(
            from_windows(
                rolled_flat.reshape(-1, win_tokens, model_width), images, band_rows, across
            ),
            SHIFT,
            axis=2,
        )
        lower = passed_along(band[:, band_rows - SHIFT :], "ctx", 1)
        return jnp.concatenate([lower, band[:, : band_rows - SHIFT]], axis=1)

    flat_one = roll_in(features).astype(jnp.float32)
    grad_flat = roll_in(out_grad)
    win_count = flat_one.shape[0] // win_tokens
    normed_one, pull_one = jax.vjp(layer_norm, flat_one, norm_rows[0], norm_rows[1])
    normed_one_low = normed_one.astype(jnp.bfloat16)
    head_shape = (win_count, win_tokens, heads_here, HD)
    query_low, key_low, value_low = project_heads(
        normed_one_low, weights_qkv, bias_query, bias_value, head_shape
    )
    pos_bias = table_lookup(table_copy, rel_index)
    region_win = to_windows(regions[..., None])[..., 0]
    mask_add = jnp.where(region_win[:, :, None] == region_win[:, None, :], 0.0, MASK_FILL).astype(
        jnp.float32
    )
    scores = attention_scores(query_low, key_low, pos_bias, mask_add)
    top_score = jnp.max(scores, axis=-1, keepdims=True)
    lifted = jnp.exp(scores - top_score)
    prob_rows = lifted / jnp.sum(lifted, axis=-1, keepdims=True)
    prob_low = prob_rows.astype(jnp.bfloat16)
    context = jnp.einsum("whij,wjhc->wihc", prob_low, value_low, preferred_element_type=jnp.float32)
    context_low = context.astype(jnp.bfloat16).reshape(-1, local_width)
    branch_part = jnp.dot(context_low, weights_proj, preferred_element_type=jnp.float32)
    branch = lax.psum(branch_part.astype(jnp.bfloat16), "tp").astype(jnp.float32) + norm_rows[2]
    flat_two = flat_one + branch
    normed_two, pull_two = jax.vjp(layer_norm, flat_two, norm_rows[3], norm_rows[4])
    normed_two_low = normed_two.astype(jnp.bfloat16)
    pre_act = jnp.dot(normed_two_low, weights_up, preferred_element_type=jnp.float32) + bias_hidden
    hidden, pull_gelu = jax.vjp(exact_gelu, pre_act)
    hidden_low = hidden.astype(jnp.bfloat16)
    mixed_part = jnp.dot(hidden_low, weights_down, preferred_element_type=jnp.float32)
    mixed_whole = lax.psum(mixed_part.astype(jnp.bfloat16), "tp").astype(jnp.float32)
    block_out = features.astype(jnp.float32) + roll_out(
        (branch + mixed_whole + norm_rows[5]).astype(jnp.bfloat16)
    ).astype(jnp.float32)
    grad_low = grad_flat.astype(jnp.bfloat16)
    grad_down_full = jnp.einsum(
        "tf,td->fd", hidden_low, grad_low, preferred_element_type=jnp.float32
    )
    grad_down_bias = jnp.sum(grad_flat, axis=0)
    d_hidden = jnp.einsum("td,fd->tf", grad_low, weights_down, preferred_element_type=jnp.float32)
    d_pre = pull_gelu(d_hidden)[0]
    d_pre_low = d_pre.astype(jnp.bfloat16)
    grad_hidden_bias = jnp.sum(d_pre, axis=0)
    grad_up_full = jnp.einsum(
        "td,tf->df", normed_two_low, d_pre_low, preferred_element_type=jnp.float32
    )
    d_two_part = jnp.einsum("tf,df->td", d_pre_low, weights_up, preferred_element_type=jnp.float32)
    d_two = lax.psum(d_two_part.astype(jnp.bfloat16), "tp").astype(jnp.float32)
    d_flat_two, grad_gain_two, grad_offset_two = pull_two(d_two)
    d_resid = grad_flat + d_flat_two
    grad_proj_bias = jnp.sum(d_resid, axis=0)
    d_branch = d_resid.astype(jnp.bfloat16)
    grad_proj_full = jnp.einsum(
        "tc,td->cd", context_low, d_branch, preferred_element_type=jnp.float32
    )
    d_context = (
        jnp.einsum("td,cd->tc", d_branch, weights_proj, preferred_element_type=jnp.float32)
        .astype(jnp.bfloat16)
        .reshape(head_shape)
    )
    d_probs = jnp.einsum(
        "wihc,wjhc->whij", d_context, value_low, preferred_element_type=jnp.float32
    )
    d_value_low = jnp.einsum(
        "whij,wihc->wjhc", prob_low, d_context, preferred_element_type=jnp.float32
    ).astype(jnp.bfloat16)
    d_scores = prob_rows * (d_probs - jnp.sum(prob_rows * d_probs, axis=-1, keepdims=True))
    d_pos = jnp.sum(d_scores, axis=0)
    d_scaled = (d_scores * HD ** (-0.5)).astype(jnp.bfloat16)
    d_query_low = jnp.einsum(
        "whij,wjhc->wihc", d_scaled, key_low, preferred_element_type=jnp.float32
    ).astype(jnp.bfloat16)
    d_key_low = jnp.einsum(
        "whij,wihc->wjhc", d_scaled, query_low, preferred_element_type=jnp.float32
    ).astype(jnp.bfloat16)
    d_heads = jnp.stack([d_query_low, d_key_low, d_value_low]).reshape(3, -1, local_width)
    grad_qkv_full = jnp.einsum(
        "td,ktc->kdc", normed_one_low, d_heads, preferred_element_type=jnp.float32
    )
    grad_head_bias = jnp.stack(
        [
            jnp.sum(d_heads[0].astype(jnp.float32), axis=0),
            jnp.sum(d_heads[2].astype(jnp.float32), axis=0),
        ]
    ).reshape(2, heads_here, HD)
    d_one_part = jnp.einsum("ktc,kdc->td", d_heads, weights_qkv, preferred_element_type=jnp.float32)
    d_one = lax.psum(d_one_part.astype(jnp.bfloat16), "tp").astype(jnp.float32)
    d_flat_one, grad_gain_one, grad_offset_one = pull_one(d_one)
    grad_input = out_grad + roll_out((d_flat_two + d_flat_one).astype(jnp.bfloat16)).astype(
        jnp.float32
    )
    table_part = table_grad(d_pos, rel_index, rel_table.shape[0])
    grad_norm_full = jnp.stack(
        [
            grad_gain_one,
            grad_offset_one,
            grad_proj_bias,
            grad_gain_two,
            grad_offset_two,
            grad_down_bias,
        ]
    )
    grad_list = (
        grad_qkv_full,
        grad_proj_full,
        grad_up_full,
        grad_down_full,
        grad_norm_full,
        grad_head_bias,
        grad_hidden_bias.reshape(-1, HD),
    )
    g_qkv, g_proj, g_up, g_down, g_norm, g_heads, g_hidden = shard_sum(band_sum(grad_list))
    d_shard = w_qkv.shape[1]
    hidden_here = w_up.shape[1]
    keep = 1.0 - DECAY_RATE
    sq_qkv = g_qkv * g_qkv
    sq_proj = g_proj * g_proj
    sq_up = g_up * g_up
    sq_down = g_down * g_down
    stat_rq = place(
        (keep * jnp.sum(sq_qkv, axis=2) / D + first_tp * (DECAY_RATE * row_qkv + keep * STAT_EPS))
        * first_ctx,
        fsdp_at,
        D,
    )
    stat_cq = place(
        (keep * jnp.sum(sq_qkv, axis=1) / D + first_fsdp * (DECAY_RATE * col_qkv + keep * STAT_EPS))
        * first_ctx,
        tp_at,
        D,
    )
    stat_rp = place(
        (
            keep * jnp.sum(sq_proj, axis=1) / D
            + first_fsdp * (DECAY_RATE * row_proj + keep * STAT_EPS)
        )
        * first_ctx,
        tp_at,
        D,
    )
    stat_cp = place(
        (keep * jnp.sum(sq_proj, axis=0) / D + first_tp * (DECAY_RATE * col_proj + keep * STAT_EPS))
        * first_ctx,
        fsdp_at,
        D,
    )
    stat_ru = place(
        (keep * jnp.sum(sq_up, axis=1) / FF + first_tp * (DECAY_RATE * row_up + keep * STAT_EPS))
        * first_ctx,
        fsdp_at,
        D,
    )
    stat_cu = place(
        (keep * jnp.sum(sq_up, axis=0) / D + first_fsdp * (DECAY_RATE * col_up + keep * STAT_EPS))
        * first_ctx,
        tp_at,
        FF,
    )
    stat_rd = place(
        (
            keep * jnp.sum(sq_down, axis=1) / D
            + first_fsdp * (DECAY_RATE * row_down + keep * STAT_EPS)
        )
        * first_ctx,
        tp_at,
        FF,
    )
    stat_cd = place(
        (
            keep * jnp.sum(sq_down, axis=0) / FF
            + first_tp * (DECAY_RATE * col_down + keep * STAT_EPS)
        )
        * first_ctx,
        fsdp_at,
        D,
    )
    table_whole = place(table_part, tp_at, HEADS)
    master_sq = jnp.concatenate(
        [
            jnp.stack(
                [
                    jnp.sum(w_qkv * w_qkv),
                    jnp.sum(w_proj * w_proj),
                    jnp.sum(w_up * w_up),
                    jnp.sum(w_down * w_down),
                ]
            )
            * first_ctx,
            jnp.sum(norm_vecs * norm_vecs, axis=1) * first_ctx * first_tp,
            jnp.sum(head_bias * head_bias, axis=(1, 2)) * first_ctx,
            jnp.sum(hidden_bias * hidden_bias)[None] * first_ctx,
            jnp.sum(rel_table * rel_table)[None] * first_ctx * first_fsdp,
        ]
    )
    (
        full_rq,
        full_cq,
        full_rp,
        full_cp,
        full_ru,
        full_cu,
        full_rd,
        full_cd,
        table_sum,
        master_total,
    ) = lax.psum(
        (
            stat_rq,
            stat_cq,
            stat_rp,
            stat_cp,
            stat_ru,
            stat_cu,
            stat_rd,
            stat_cd,
            table_whole,
            master_sq,
        ),
        ("fsdp", "ctx", "tp"),
    )
    u_qkv = factored(
        g_qkv,
        own_part(full_rq, fsdp_at, d_shard),
        own_part(full_cq, tp_at, local_width),
        jnp.mean(full_rq, axis=1)[:, None, None],
    )
    u_proj = factored(
        g_proj,
        own_part(full_rp, tp_at, local_width),
        own_part(full_cp, fsdp_at, d_shard),
        jnp.mean(full_rp),
    )
    u_up = factored(
        g_up,
        own_part(full_ru, fsdp_at, d_shard),
        own_part(full_cu, tp_at, hidden_here),
        jnp.mean(full_ru),
    )
    u_down = factored(
        g_down,
        own_part(full_rd, tp_at, hidden_here),
        own_part(full_cd, fsdp_at, d_shard),
        jnp.mean(full_rd),
    )
    g_table = own_part(table_sum, tp_at, heads_here)
    state_norm_new, u_norm = plain_stats(g_norm, state_norm)
    state_heads_new, u_heads = plain_stats(g_heads, state_heads)
    state_hidden_new, u_hidden = plain_stats(g_hidden, state_hidden)
    state_table_new, u_table = plain_stats(g_table, state_table)
    local_sq = (
        jnp.sum(u_qkv * u_qkv)
        + jnp.sum(u_proj * u_proj)
        + jnp.sum(u_up * u_up)
        + jnp.sum(u_down * u_down)
        + jnp.sum(u_heads * u_heads)
        + jnp.sum(u_hidden * u_hidden)
        + first_tp * jnp.sum(u_norm * u_norm)
        + first_fsdp * jnp.sum(u_table * u_table)
    )
    total_sq = lax.psum(local_sq, ("fsdp", "tp"))
    count_all = 4 * D * D + 2 * D * FF + 8 * D + FF + RELP * HEADS
    clip_rms = jnp.sqrt(total_sq / count_all)
    factor = 1.0 / jnp.maximum(1.0, clip_rms / CLIP_LEVEL)
    counts = jnp.array(
        [3 * D * D, D * D, D * FF, FF * D, D, D, D, D, D, D, D, D, FF, RELP * HEADS], jnp.float32
    )
    scales = jnp.sqrt(master_total / counts + STAT_EPS)
    new_qkv = w_qkv - STEP_RATE * scales[0] * factor * u_qkv
    new_proj = w_proj - STEP_RATE * scales[1] * factor * u_proj
    new_up = w_up - STEP_RATE * scales[2] * factor * u_up
    new_down = w_down - STEP_RATE * scales[3] * factor * u_down
    new_norm = norm_vecs - STEP_RATE * scales[4:10][:, None] * factor * u_norm
    new_heads = head_bias - STEP_RATE * scales[10:12][:, None, None] * factor * u_heads
    new_hidden = hidden_bias - STEP_RATE * scales[12] * factor * u_hidden
    new_table = rel_table - STEP_RATE * scales[13] * factor * u_table
    return (
        block_out,
        grad_input,
        g_qkv,
        g_proj,
        g_up,
        g_down,
        g_norm,
        g_heads,
        g_hidden,
        g_table,
        new_qkv,
        new_proj,
        new_up,
        new_down,
        new_norm,
        new_heads,
        new_hidden,
        new_table,
        new_qkv.astype(jnp.bfloat16),
        new_proj.astype(jnp.bfloat16),
        new_up.astype(jnp.bfloat16),
        new_down.astype(jnp.bfloat16),
        own_part(full_rq, fsdp_at, d_shard),
        own_part(full_cq, tp_at, local_width),
        own_part(full_rp, tp_at, local_width),
        own_part(full_cp, fsdp_at, d_shard),
        own_part(full_ru, fsdp_at, d_shard),
        own_part(full_cu, tp_at, hidden_here),
        own_part(full_rd, tp_at, hidden_here),
        own_part(full_cd, fsdp_at, d_shard),
        state_norm_new,
        state_heads_new,
        state_hidden_new,
        state_table_new,
        clip_rms,
    )


def per_device(
    features,
    out_grad,
    regions,
    rel_index,
    w_qkv,
    w_proj,
    w_up,
    w_down,
    norm_vecs,
    head_bias,
    hidden_bias,
    rel_table,
    row_qkv,
    col_qkv,
    row_proj,
    col_proj,
    row_up,
    col_up,
    row_down,
    col_down,
    state_norm,
    state_heads,
    state_hidden,
    state_table,
):
    images, band_rows, across, model_width = features.shape
    win_tokens = WIN * WIN
    fsdp_at = lax.axis_index("fsdp")
    ctx_at = lax.axis_index("ctx")
    tp_at = lax.axis_index("tp")
    first_fsdp = (fsdp_at == 0).astype(jnp.float32)
    first_ctx = (ctx_at == 0).astype(jnp.float32)
    first_tp = (tp_at == 0).astype(jnp.float32)
    (weights_qkv, weights_proj, weights_up, weights_down, rows, xw, ogw, n1, query_low, key_low, value_low,
     prob_rows, context_low, br) = attention_forward(
        features, out_grad, regions, rel_index, w_qkv, w_proj, w_up, w_down,
        norm_vecs, head_bias, hidden_bias, rel_table)
    norm_rows = rows[:6]
    bias_hidden = rows[8]
    local_width = weights_qkv.shape[2]
    heads_here = local_width // HD
    win_count = xw.shape[0]
    head_shape = (win_count, win_tokens, heads_here, HD)
    flat_one = xw.reshape(-1, model_width)
    grad_flat = ogw.reshape(-1, model_width)
    normed_one_low = n1.reshape(-1, model_width)
    _, pull_one = jax.vjp(layer_norm, flat_one, norm_rows[0], norm_rows[1])
    query_low, key_low, value_low = (u.reshape(head_shape) for u in (query_low, key_low, value_low))
    prob_low = prob_rows.astype(jnp.bfloat16)
    context_low = context_low.reshape(-1, local_width)
    branch = br.transpose(0, 2, 1, 3).reshape(-1, model_width).astype(jnp.float32) + norm_rows[2]
    def roll_out(rolled_flat):
        band = jnp.roll(
            from_windows(
                rolled_flat.reshape(-1, win_tokens, model_width), images, band_rows, across
            ),
            SHIFT,
            axis=2,
        )
        lower = passed_along(band[:, band_rows - SHIFT :], "ctx", 1)
        return jnp.concatenate([lower, band[:, : band_rows - SHIFT]], axis=1)

    flat_two = flat_one + branch
    normed_two, pull_two = jax.vjp(layer_norm, flat_two, norm_rows[3], norm_rows[4])
    normed_two_low = normed_two.astype(jnp.bfloat16)
    pre_act = jnp.dot(normed_two_low, weights_up, preferred_element_type=jnp.float32) + bias_hidden
    hidden, pull_gelu = jax.vjp(exact_gelu, pre_act)
    hidden_low = hidden.astype(jnp.bfloat16)
    mixed_part = jnp.dot(hidden_low, weights_down, preferred_element_type=jnp.float32)
    mixed_whole = lax.psum(mixed_part.astype(jnp.bfloat16), "tp").astype(jnp.float32)
    block_out = features.astype(jnp.float32) + roll_out(
        (branch + mixed_whole + norm_rows[5]).astype(jnp.bfloat16)
    ).astype(jnp.float32)
    grad_low = grad_flat.astype(jnp.bfloat16)
    grad_down_full = jnp.einsum(
        "tf,td->fd", hidden_low, grad_low, preferred_element_type=jnp.float32
    )
    grad_down_bias = jnp.sum(grad_flat, axis=0)
    d_hidden = jnp.einsum("td,fd->tf", grad_low, weights_down, preferred_element_type=jnp.float32)
    d_pre = pull_gelu(d_hidden)[0]
    d_pre_low = d_pre.astype(jnp.bfloat16)
    grad_hidden_bias = jnp.sum(d_pre, axis=0)
    grad_up_full = jnp.einsum(
        "td,tf->df", normed_two_low, d_pre_low, preferred_element_type=jnp.float32
    )
    d_two_part = jnp.einsum("tf,df->td", d_pre_low, weights_up, preferred_element_type=jnp.float32)
    d_two = lax.psum(d_two_part.astype(jnp.bfloat16), "tp").astype(jnp.float32)
    d_flat_two, grad_gain_two, grad_offset_two = pull_two(d_two)
    d_resid = grad_flat + d_flat_two
    grad_proj_bias = jnp.sum(d_resid, axis=0)
    d_branch = d_resid.astype(jnp.bfloat16)
    grad_proj_full = jnp.einsum(
        "tc,td->cd", context_low, d_branch, preferred_element_type=jnp.float32
    )
    d_context = (
        jnp.einsum("td,cd->tc", d_branch, weights_proj, preferred_element_type=jnp.float32)
        .astype(jnp.bfloat16)
        .reshape(head_shape)
    )
    d_probs = jnp.einsum(
        "wihc,wjhc->whij", d_context, value_low, preferred_element_type=jnp.float32
    )
    d_value_low = jnp.einsum(
        "whij,wihc->wjhc", prob_low, d_context, preferred_element_type=jnp.float32
    ).astype(jnp.bfloat16)
    d_scores = prob_rows * (d_probs - jnp.sum(prob_rows * d_probs, axis=-1, keepdims=True))
    d_pos = jnp.sum(d_scores, axis=0)
    d_scaled = (d_scores * HD ** (-0.5)).astype(jnp.bfloat16)
    d_query_low = jnp.einsum(
        "whij,wjhc->wihc", d_scaled, key_low, preferred_element_type=jnp.float32
    ).astype(jnp.bfloat16)
    d_key_low = jnp.einsum(
        "whij,wihc->wjhc", d_scaled, query_low, preferred_element_type=jnp.float32
    ).astype(jnp.bfloat16)
    d_heads = jnp.stack([d_query_low, d_key_low, d_value_low]).reshape(3, -1, local_width)
    grad_qkv_full = jnp.einsum(
        "td,ktc->kdc", normed_one_low, d_heads, preferred_element_type=jnp.float32
    )
    grad_head_bias = jnp.stack(
        [
            jnp.sum(d_heads[0].astype(jnp.float32), axis=0),
            jnp.sum(d_heads[2].astype(jnp.float32), axis=0),
        ]
    ).reshape(2, heads_here, HD)
    d_one_part = jnp.einsum("ktc,kdc->td", d_heads, weights_qkv, preferred_element_type=jnp.float32)
    d_one = lax.psum(d_one_part.astype(jnp.bfloat16), "tp").astype(jnp.float32)
    d_flat_one, grad_gain_one, grad_offset_one = pull_one(d_one)
    grad_input = out_grad + roll_out((d_flat_two + d_flat_one).astype(jnp.bfloat16)).astype(
        jnp.float32
    )
    table_part = table_grad(d_pos, rel_index, rel_table.shape[0])
    grad_norm_full = jnp.stack(
        [
            grad_gain_one,
            grad_offset_one,
            grad_proj_bias,
            grad_gain_two,
            grad_offset_two,
            grad_down_bias,
        ]
    )
    grad_list = (
        grad_qkv_full,
        grad_proj_full,
        grad_up_full,
        grad_down_full,
        grad_norm_full,
        grad_head_bias,
        grad_hidden_bias.reshape(-1, HD),
    )
    g_qkv, g_proj, g_up, g_down, g_norm, g_heads, g_hidden = shard_sum(band_sum(grad_list))
    d_shard = w_qkv.shape[1]
    hidden_here = w_up.shape[1]
    keep = 1.0 - DECAY_RATE
    sq_qkv = g_qkv * g_qkv
    sq_proj = g_proj * g_proj
    sq_up = g_up * g_up
    sq_down = g_down * g_down
    stat_rq = place(
        (keep * jnp.sum(sq_qkv, axis=2) / D + first_tp * (DECAY_RATE * row_qkv + keep * STAT_EPS))
        * first_ctx,
        fsdp_at,
        D,
    )
    stat_cq = place(
        (keep * jnp.sum(sq_qkv, axis=1) / D + first_fsdp * (DECAY_RATE * col_qkv + keep * STAT_EPS))
        * first_ctx,
        tp_at,
        D,
    )
    stat_rp = place(
        (
            keep * jnp.sum(sq_proj, axis=1) / D
            + first_fsdp * (DECAY_RATE * row_proj + keep * STAT_EPS)
        )
        * first_ctx,
        tp_at,
        D,
    )
    stat_cp = place(
        (keep * jnp.sum(sq_proj, axis=0) / D + first_tp * (DECAY_RATE * col_proj + keep * STAT_EPS))
        * first_ctx,
        fsdp_at,
        D,
    )
    stat_ru = place(
        (keep * jnp.sum(sq_up, axis=1) / FF + first_tp * (DECAY_RATE * row_up + keep * STAT_EPS))
        * first_ctx,
        fsdp_at,
        D,
    )
    stat_cu = place(
        (keep * jnp.sum(sq_up, axis=0) / D + first_fsdp * (DECAY_RATE * col_up + keep * STAT_EPS))
        * first_ctx,
        tp_at,
        FF,
    )
    stat_rd = place(
        (
            keep * jnp.sum(sq_down, axis=1) / D
            + first_fsdp * (DECAY_RATE * row_down + keep * STAT_EPS)
        )
        * first_ctx,
        tp_at,
        FF,
    )
    stat_cd = place(
        (
            keep * jnp.sum(sq_down, axis=0) / FF
            + first_tp * (DECAY_RATE * col_down + keep * STAT_EPS)
        )
        * first_ctx,
        fsdp_at,
        D,
    )
    table_whole = place(table_part, tp_at, HEADS)
    master_sq = jnp.concatenate(
        [
            jnp.stack(
                [
                    jnp.sum(w_qkv * w_qkv),
                    jnp.sum(w_proj * w_proj),
                    jnp.sum(w_up * w_up),
                    jnp.sum(w_down * w_down),
                ]
            )
            * first_ctx,
            jnp.sum(norm_vecs * norm_vecs, axis=1) * first_ctx * first_tp,
            jnp.sum(head_bias * head_bias, axis=(1, 2)) * first_ctx,
            jnp.sum(hidden_bias * hidden_bias)[None] * first_ctx,
            jnp.sum(rel_table * rel_table)[None] * first_ctx * first_fsdp,
        ]
    )
    (
        full_rq,
        full_cq,
        full_rp,
        full_cp,
        full_ru,
        full_cu,
        full_rd,
        full_cd,
        table_sum,
        master_total,
    ) = lax.psum(
        (
            stat_rq,
            stat_cq,
            stat_rp,
            stat_cp,
            stat_ru,
            stat_cu,
            stat_rd,
            stat_cd,
            table_whole,
            master_sq,
        ),
        ("fsdp", "ctx", "tp"),
    )
    u_qkv = factored(
        g_qkv,
        own_part(full_rq, fsdp_at, d_shard),
        own_part(full_cq, tp_at, local_width),
        jnp.mean(full_rq, axis=1)[:, None, None],
    )
    u_proj = factored(
        g_proj,
        own_part(full_rp, tp_at, local_width),
        own_part(full_cp, fsdp_at, d_shard),
        jnp.mean(full_rp),
    )
    u_up = factored(
        g_up,
        own_part(full_ru, fsdp_at, d_shard),
        own_part(full_cu, tp_at, hidden_here),
        jnp.mean(full_ru),
    )
    u_down = factored(
        g_down,
        own_part(full_rd, tp_at, hidden_here),
        own_part(full_cd, fsdp_at, d_shard),
        jnp.mean(full_rd),
    )
    g_table = own_part(table_sum, tp_at, heads_here)
    state_norm_new, u_norm = plain_stats(g_norm, state_norm)
    state_heads_new, u_heads = plain_stats(g_heads, state_heads)
    state_hidden_new, u_hidden = plain_stats(g_hidden, state_hidden)
    state_table_new, u_table = plain_stats(g_table, state_table)
    local_sq = (
        jnp.sum(u_qkv * u_qkv)
        + jnp.sum(u_proj * u_proj)
        + jnp.sum(u_up * u_up)
        + jnp.sum(u_down * u_down)
        + jnp.sum(u_heads * u_heads)
        + jnp.sum(u_hidden * u_hidden)
        + first_tp * jnp.sum(u_norm * u_norm)
        + first_fsdp * jnp.sum(u_table * u_table)
    )
    total_sq = lax.psum(local_sq, ("fsdp", "tp"))
    count_all = 4 * D * D + 2 * D * FF + 8 * D + FF + RELP * HEADS
    clip_rms = jnp.sqrt(total_sq / count_all)
    factor = 1.0 / jnp.maximum(1.0, clip_rms / CLIP_LEVEL)
    counts = jnp.array(
        [3 * D * D, D * D, D * FF, FF * D, D, D, D, D, D, D, D, D, FF, RELP * HEADS], jnp.float32
    )
    scales = jnp.sqrt(master_total / counts + STAT_EPS)
    new_qkv = w_qkv - STEP_RATE * scales[0] * factor * u_qkv
    new_proj = w_proj - STEP_RATE * scales[1] * factor * u_proj
    new_up = w_up - STEP_RATE * scales[2] * factor * u_up
    new_down = w_down - STEP_RATE * scales[3] * factor * u_down
    new_norm = norm_vecs - STEP_RATE * scales[4:10][:, None] * factor * u_norm
    new_heads = head_bias - STEP_RATE * scales[10:12][:, None, None] * factor * u_heads
    new_hidden = hidden_bias - STEP_RATE * scales[12] * factor * u_hidden
    new_table = rel_table - STEP_RATE * scales[13] * factor * u_table
    return (
        block_out,
        grad_input,
        g_qkv,
        g_proj,
        g_up,
        g_down,
        g_norm,
        g_heads,
        g_hidden,
        g_table,
        new_qkv,
        new_proj,
        new_up,
        new_down,
        new_norm,
        new_heads,
        new_hidden,
        new_table,
        new_qkv.astype(jnp.bfloat16),
        new_proj.astype(jnp.bfloat16),
        new_up.astype(jnp.bfloat16),
        new_down.astype(jnp.bfloat16),
        own_part(full_rq, fsdp_at, d_shard),
        own_part(full_cq, tp_at, local_width),
        own_part(full_rp, tp_at, local_width),
        own_part(full_cp, fsdp_at, d_shard),
        own_part(full_ru, fsdp_at, d_shard),
        own_part(full_cu, tp_at, hidden_here),
        own_part(full_rd, tp_at, hidden_here),
        own_part(full_cd, fsdp_at, d_shard),
        state_norm_new,
        state_heads_new,
        state_hidden_new,
        state_table_new,
        clip_rms,
    )


def solution(mesh):
    line_of_four = mesh.shape["fsdp"] == 4 and mesh.shape["tp"] == 4 and mesh.shape["ctx"] == 2
    return jax.shard_map(
        per_device if line_of_four else per_device_plain,
        mesh=mesh,
        in_specs=(
            P("fsdp", "ctx", None, None),
            P("fsdp", "ctx", None, None),
            P("fsdp", "ctx", None),
            P(),
            P(None, "fsdp", "tp"),
            P("tp", "fsdp"),
            P("fsdp", "tp"),
            P("tp", "fsdp"),
            P(None, "fsdp"),
            P(None, "tp", "fsdp"),
            P("tp", "fsdp"),
            P(None, "tp"),
            P(None, "fsdp"),
            P(None, "tp"),
            P("tp"),
            P("fsdp"),
            P("fsdp"),
            P("tp"),
            P("tp"),
            P("fsdp"),
            P(None, "fsdp"),
            P(None, "tp", "fsdp"),
            P("tp", "fsdp"),
            P(None, "tp"),
        ),
        out_specs=(
            P("fsdp", "ctx", None, None),
            P("fsdp", "ctx", None, None),
            P(None, "fsdp", "tp"),
            P("tp", "fsdp"),
            P("fsdp", "tp"),
            P("tp", "fsdp"),
            P(None, "fsdp"),
            P(None, "tp", "fsdp"),
            P("tp", "fsdp"),
            P(None, "tp"),
            P(None, "fsdp", "tp"),
            P("tp", "fsdp"),
            P("fsdp", "tp"),
            P("tp", "fsdp"),
            P(None, "fsdp"),
            P(None, "tp", "fsdp"),
            P("tp", "fsdp"),
            P(None, "tp"),
            P(None, "fsdp", "tp"),
            P("tp", "fsdp"),
            P("fsdp", "tp"),
            P("tp", "fsdp"),
            P(None, "fsdp"),
            P(None, "tp"),
            P("tp"),
            P("fsdp"),
            P("fsdp"),
            P("tp"),
            P("tp"),
            P("fsdp"),
            P(None, "fsdp"),
            P(None, "tp", "fsdp"),
            P("tp", "fsdp"),
            P(None, "tp"),
            P(),
        ),
        check_vma=False,
    )
```

```python
import functools

import jax
import jax.numpy as jnp
from jax import lax
from jax.experimental import pallas as pl
from jax.experimental.pallas import tpu as pltpu
from jax.sharding import PartitionSpec as P


D = 768
HEADS = 24
HD = 32
FF = 3072
WIN = 12
SHIFT = 6
RELP = 529


DECAY_RATE = 0.5
STAT_EPS = 1e-06
NORM_EPS = 1e-05
MASK_FILL = -100.0
STEP_RATE = 1.0
CLIP_LEVEL = 0.25


def passed_along(x, axis, by):
    count = lax.axis_size(axis)
    return lax.ppermute(x, axis, [(i, (i + by) % count) for i in range(count)])


def layer_norm(values, gain_row, offset):
    mean_val = jnp.mean(values, axis=-1, keepdims=True)
    centred = values - mean_val
    var_val = jnp.mean(centred * centred, axis=-1, keepdims=True)
    return centred * lax.rsqrt(var_val + NORM_EPS) * gain_row + offset


def exact_gelu(values):
    return jax.nn.gelu(values, approximate=False)


def to_windows(values):
    image_count, row_count, col_count, channels = values.shape
    pieces = values.reshape(image_count, row_count // WIN, WIN, col_count // WIN, WIN, channels)
    return pieces.transpose(0, 1, 3, 2, 4, 5).reshape(-1, WIN * WIN, channels)


def from_windows(values, image_count, row_count, col_count):
    channels = values.shape[-1]
    pieces = values.reshape(image_count, row_count // WIN, col_count // WIN, WIN, WIN, channels)
    return pieces.transpose(0, 1, 3, 2, 4, 5).reshape(image_count, row_count, col_count, channels)


def enter_frame(own_rows, received):
    joined = jnp.concatenate([own_rows[:, SHIFT:], received], axis=1)
    return jnp.roll(joined, -SHIFT, axis=2)


def project_heads(normed_low, weights_qkv, bias_query, bias_value, head_shape):
    query_full = (
        jnp.dot(normed_low, weights_qkv[0], preferred_element_type=jnp.float32) + bias_query
    )
    key_full = jnp.dot(normed_low, weights_qkv[1], preferred_element_type=jnp.float32)
    value_full = (
        jnp.dot(normed_low, weights_qkv[2], preferred_element_type=jnp.float32) + bias_value
    )
    return tuple(
        (
            member.astype(jnp.bfloat16).reshape(head_shape)
            for member in (query_full, key_full, value_full)
        )
    )


def attention_scores(query_low, key_low, pos_bias, mask_add):
    products = jnp.einsum("wihc,wjhc->whij", query_low, key_low, preferred_element_type=jnp.float32)
    return products * query_low.shape[-1] ** (-0.5) + pos_bias[None] + mask_add[:, None]


def table_lookup(table_low, rel_index):
    win_tokens = rel_index.shape[0]
    code_ids = jnp.arange(table_low.shape[0], dtype=jnp.int32)
    index_blocks = rel_index.reshape(WIN, -1)

    def lookup(index_block):
        one_hot = (index_block[:, None] == code_ids[None, :]).astype(jnp.bfloat16)
        return jnp.dot(one_hot, table_low, preferred_element_type=jnp.float32)

    looked = lax.map(lookup, index_blocks)
    return looked.reshape(win_tokens, win_tokens, -1).transpose(2, 0, 1)


def table_grad(d_pos, rel_index, table_rows):
    heads_here = d_pos.shape[0]
    code_ids = jnp.arange(table_rows, dtype=jnp.int32)
    index_blocks = rel_index.reshape(WIN, -1)
    grad_blocks = d_pos.transpose(1, 2, 0).reshape(WIN, -1, heads_here)

    def accumulate(running, member):
        index_block, grad_block = member
        one_hot = (index_block[:, None] == code_ids[None, :]).astype(jnp.float32)
        added = lax.dot_general(
            one_hot,
            grad_block,
            (((0,), (0,)), ((), ())),
            precision=lax.Precision.HIGHEST,
            preferred_element_type=jnp.float32,
        )
        return (running + added, None)

    result_pair = lax.scan(
        accumulate, jnp.zeros((table_rows, heads_here), jnp.float32), (index_blocks, grad_blocks)
    )
    return result_pair[0]


def place(part_vec, index_at, whole_len):
    size_of = part_vec.shape[-1]
    base = jnp.zeros(part_vec.shape[:-1] + (whole_len,), jnp.float32)
    return lax.dynamic_update_slice_in_dim(base, part_vec, index_at * size_of, part_vec.ndim - 1)


def own_part(whole_vec, index_at, size_of):
    return lax.dynamic_slice_in_dim(whole_vec, index_at * size_of, size_of, whole_vec.ndim - 1)


def factored(grad, row_local, col_local, row_mean):
    return grad * lax.rsqrt(row_local[..., :, None] * col_local[..., None, :] / row_mean)


def plain_stats(grad, state_old):
    state_new = DECAY_RATE * state_old + (1.0 - DECAY_RATE) * (grad * grad + STAT_EPS)
    return (state_new, grad * lax.rsqrt(state_new))


def shard_sum(grad_list):
    return (
        lax.psum_scatter(grad_list[0], "fsdp", scatter_dimension=1, tiled=True),
        lax.psum_scatter(grad_list[1], "fsdp", scatter_dimension=1, tiled=True),
        lax.psum_scatter(grad_list[2], "fsdp", scatter_dimension=0, tiled=True),
        lax.psum_scatter(grad_list[3], "fsdp", scatter_dimension=1, tiled=True),
        lax.psum_scatter(grad_list[4], "fsdp", scatter_dimension=1, tiled=True),
        lax.psum_scatter(grad_list[5], "fsdp", scatter_dimension=2, tiled=True),
        lax.psum_scatter(grad_list[6], "fsdp", scatter_dimension=1, tiled=True),
    )


def band_sum(grad_list):
    return lax.psum(
        (
            grad_list[0],
            grad_list[1],
            grad_list[2],
            grad_list[3],
            grad_list[4],
            grad_list[5],
            grad_list[6],
        ),
        "ctx",
    )


BF = jnp.bfloat16
F32 = jnp.float32
MESH = pl.DeviceIdType.MESH
TOK = WIN * WIN
HALF = D // 2
VMEM_LIMIT = 66_000_000


def dot(a, b):
    return lax.dot_general(a, b, (((1,), (0,)), ((), ())), preferred_element_type=F32)


def dot_t(a, b):
    return lax.dot_general(a, b, (((1,), (1,)), ((), ())), preferred_element_type=F32)


def t_dot(a, b):
    return lax.dot_general(a, b, (((0,), (0,)), ((), ())), preferred_element_type=F32)


def row_mean(x):
    return jnp.sum(x, axis=-1, keepdims=True) * (1.0 / x.shape[-1])


def remote(src, dst, send, recv, where):
    return pltpu.make_async_remote_copy(
        src_ref=src, dst_ref=dst, send_sem=send, recv_sem=recv, device_id=where, device_id_type=MESH
    )


def greet(barrier, places):
    for place_of in places:
        pl.semaphore_signal(barrier, inc=1, device_id=place_of, device_id_type=MESH)


class LineSum:
    def __init__(self, part, send, from_outer, from_mid, total, sems):
        self.part, self.send, self.from_outer, self.from_mid, self.total = (
            part, send, from_outer, from_mid, total,
        )
        self.s_out, self.r_out, self.s_mid, self.r_mid, self.s_tot, self.r_tot, self.s_cross = sems
        z = lax.axis_index("tp")
        self.is_mid = jnp.logical_and(z > 0, z < 3)
        self.is_outer = jnp.logical_not(self.is_mid)
        self.outer = jnp.where(z < 2, 0, 3)
        self.mid = jnp.where(z < 2, 1, 2)
        self.other_mid = 3 - self.mid
        self.own = self.mid - 1
        self.other = 1 - self.own

    @staticmethod
    def scratch(count):
        return [
            pltpu.VMEM((count, 2, TOK, HALF), F32),
            pltpu.VMEM((count, 2, TOK, HALF), BF),
            pltpu.VMEM((count, 2, TOK, HALF), BF),
            pltpu.VMEM((count, TOK, HALF), BF),
            pltpu.SemaphoreType.DMA((count, 2)),
            pltpu.SemaphoreType.DMA((count, 2)),
            pltpu.SemaphoreType.DMA((count,)),
            pltpu.SemaphoreType.DMA((count,)),
            pltpu.SemaphoreType.DMA((count, 2)),
            pltpu.SemaphoreType.DMA((count, 2)),
            pltpu.SemaphoreType.DMA((count,)),
        ]

    @staticmethod
    def build(refs, total):
        return LineSum(refs[0], refs[1], refs[2], refs[3], total, refs[4:11])

    @staticmethod
    def peers():
        return 2

    def greet(self, barrier):
        pl.semaphore_signal(
            barrier, inc=1, device_id={"tp": jnp.where(self.is_mid, self.outer, self.mid)},
            device_id_type=MESH,
        )

        @pl.when(self.is_mid)
        def _():
            pl.semaphore_signal(
                barrier, inc=1, device_id={"tp": self.other_mid}, device_id_type=MESH
            )

    def greet_count(self):
        return jnp.where(self.is_mid, 2, 1)

    def _to_mid(self, w, h):
        return remote(self.send.at[w, h], self.from_outer.at[w, h], self.s_out.at[w, h],
                      self.r_out.at[w, h], {"tp": self.mid})

    def _across(self, w):
        return remote(self.send.at[w, self.other], self.from_mid.at[w], self.s_mid.at[w],
                      self.r_mid.at[w], {"tp": self.other_mid})

    def _total_across(self, w, h):
        return remote(self.total.at[w, h], self.total.at[w, h], self.s_cross.at[w],
                      self.r_tot.at[w, h], {"tp": self.other_mid})

    def _total_out(self, w, h):
        return remote(self.total.at[w, h], self.total.at[w, h], self.s_tot.at[w, h],
                      self.r_tot.at[w, h], {"tp": self.outer})

    def put(self, w, value):
        self.part[w, 0] = value[:, :HALF]
        self.part[w, 1] = value[:, HALF:]

    def start(self, w):
        @pl.when(self.is_outer)
        def _():
            self.send[w, self.other] = self.part[w, self.other].astype(BF)
            self._to_mid(w, self.other).start()
            self.send[w, self.own] = self.part[w, self.own].astype(BF)
            self._to_mid(w, self.own).start()

    def cross(self, w):
        @pl.when(self.is_mid)
        def _():
            self._to_mid(w, self.other).wait_recv()
            self.send[w, self.other] = (
                self.part[w, self.other] + self.from_outer[w, self.other].astype(F32)
            ).astype(BF)
            self._across(w).start()

    def settle(self, w):
        @pl.when(self.is_mid)
        def _():
            self._to_mid(w, self.own).wait_recv()
            self._across(w).wait_recv()
            self.total[w, self.own] = (
                self.part[w, self.own]
                + self.from_outer[w, self.own].astype(F32)
                + self.from_mid[w].astype(F32)
            ).astype(BF)
            self._total_across(w, self.own).start()
            self._total_out(w, self.own).start()

    def hand(self, w):
        @pl.when(self.is_mid)
        def _():
            self._total_across(w, self.other).wait_recv()
            self._total_out(w, self.other).start()

    def arrive(self, w):
        @pl.when(self.is_outer)
        def _():
            self._total_out(w, 0).wait_recv()
            self._total_out(w, 1).wait_recv()

    def drain(self, w):
        @pl.when(self.is_outer)
        def _():
            self._to_mid(w, 0).wait_send()
            self._to_mid(w, 1).wait_send()

        @pl.when(self.is_mid)
        def _():
            self._across(w).wait_send()
            self._total_across(w, self.own).wait_send()
            self._total_out(w, 0).wait_send()
            self._total_out(w, 1).wait_send()


def window_rows(row_of, row_tmp, image, dst):
    for r in range(WIN):
        row_tmp[...] = row_of(image, r).astype(F32)
        dst[2 * image, r * WIN : (r + 1) * WIN, :] = row_tmp[SHIFT : SHIFT + WIN, :]
        dst[2 * image + 1, r * WIN : r * WIN + SHIFT, :] = row_tmp[SHIFT + WIN :, :]
        dst[2 * image + 1, r * WIN + SHIFT : (r + 1) * WIN, :] = row_tmp[:SHIFT, :]


def attention_forward_body(
    feat, og, wq, wp, wu, wd, small, table_t, ridx, regr, regc,
    wq_o, wp_o, wu_o, wd_o, rows_o, xw_o, ogw_o, n1_o, q_o, k_o, v_o, probs_o, ctx_o, br_o,
    sm_g, wp_g, fh, gh, bias_s, row_tmp,
    ls_a, ls_b, ls_c, ls_d, ls_e, ls_f, ls_g, ls_h, ls_i, ls_j, ls_k,
    w_send, w_recv, h_send, h_recv,
):
    windows = xw_o.shape[0]
    images = windows // 2
    f = lax.axis_index("fsdp")
    c = lax.axis_index("ctx")
    near, far = f + 1 - 2 * lax.rem(f, 2), lax.rem(f + 2, 4)
    line = LineSum.build((ls_a, ls_b, ls_c, ls_d, ls_e, ls_f, ls_g, ls_h, ls_i, ls_j, ls_k), br_o)
    barrier = pltpu.get_barrier_semaphore()
    greet(barrier, [{"fsdp": near}, {"fsdp": far}, {"ctx": 1 - c}])
    line.greet(barrier)

    shard = wq.shape[1]

    def block(at):
        return pl.ds(pl.multiple_of(at * shard, shard), shard)

    wq_o[:, block(f), :] = wq[...].astype(BF)
    sm_g[f] = small[...].astype(BF)
    wp_g[f] = wp[...].astype(BF)
    wu_o[block(f), :] = wu[...].astype(BF)
    wd_o[block(f), :] = wd[...].astype(BF)
    pl.semaphore_wait(barrier, 3 + line.greet_count())

    items = [
        lambda at: sm_g.at[at],
        lambda at: wq_o.at[:, block(at), :],
        lambda at: wp_g.at[at],
        lambda at: wu_o.at[block(at), :],
        lambda at: wd_o.at[block(at), :],
    ]

    def copy_of(n, kind, at, where):
        ref = items[n](at)
        return remote(ref, ref, w_send.at[n, kind], w_recv.at[n, kind], {"fsdp": where})

    halo_f = [
        remote(feat.at[i, 0:SHIFT], fh.at[i], h_send.at[i], h_recv.at[i], {"ctx": 1 - c})
        for i in range(images)
    ]
    halo_g = [
        remote(og.at[i, 0:SHIFT], gh.at[i], h_send.at[images + i], h_recv.at[images + i], {"ctx": 1 - c})
        for i in range(images)
    ]
    for copy in halo_f:
        copy.start()
    for n in range(len(items)):
        copy_of(n, 0, f, far).start()
        copy_of(n, 1, f, near).start()
    for copy in halo_g:
        copy.start()

    def relay(n):
        copy_of(n, 0, f, far).wait_recv()
        copy_of(n, 2, far, near).start()

    def gathered(n):
        copy_of(n, 1, f, near).wait_recv()
        copy_of(n, 2, far, near).wait_recv()

    relay(0)

    def bias_rows(step, carry):
        rows = pl.ds(pl.multiple_of(step * 8, 8), 8)
        for part in range(2):
            idx = ridx[rows, part * 128 : (part + 1) * 128]
            low = jnp.bitwise_and(idx, 127)
            high = jnp.right_shift(idx, 7)
            picks = [high == n for n in range(5)]
            for h in range(bias_s.shape[0]):
                found = jnp.zeros((8, 128), F32)
                for n in range(5):
                    tab = jnp.broadcast_to(table_t[h : h + 1, n * 128 : (n + 1) * 128], (8, 128))
                    got = jnp.take_along_axis(tab, low, axis=1, mode="promise_in_bounds")
                    found = jnp.where(picks[n], got, found)
                bias_s[h, rows, part * 128 : (part + 1) * 128] = found
        return carry

    lax.fori_loop(0, TOK // 8, bias_rows, 0)
    gathered(0)
    relay(1)
    lanes = rows_o.shape[1]
    rows_o[...] = jnp.concatenate([sm_g[n].astype(F32) for n in range(4)], axis=1)
    unit = lax.broadcasted_iota(jnp.int32, (shard, lanes), 0)
    lane = lax.broadcasted_iota(jnp.int32, (shard, lanes), 1)
    biases = jnp.zeros((16, lanes), F32)
    for n in range(4):
        same = jnp.logical_and(
            jnp.right_shift(lane, 5) == jnp.right_shift(unit, 3),
            jnp.bitwise_and(lane, 31) == jnp.bitwise_and(unit, 7) + n * 8,
        )
        biases = biases + dot(sm_g[n], jnp.where(same, 1.0, 0.0).astype(BF))
    rows_o[8:16, :] = biases[8:16, :]

    for i in range(images):
        halo_f[i].wait_recv()
        window_rows(
            lambda im, r: feat[im, SHIFT + r] if r < SHIFT else fh[im, r - SHIFT], row_tmp, i, xw_o
        )
    gain, offset = rows_o[0:1, :], rows_o[1:2, :]
    width = q_o.shape[2]
    bias_q, bias_v = rows_o[9:10, :width], rows_o[10:11, :width]
    head_of = jnp.right_shift(lax.broadcasted_iota(jnp.int32, (1, width), 1), 5)
    heads = width // HD
    gathered(1)

    def window(w, carry):
        x = xw_o[w]
        mean_val = row_mean(x)
        centred = x - mean_val
        var_val = row_mean(centred * centred)
        n1 = (centred * lax.rsqrt(var_val + NORM_EPS) * gain + offset).astype(BF)
        n1_o[w] = n1
        q = (dot(n1, wq_o[0]) + bias_q).astype(BF)
        k = dot(n1, wq_o[1]).astype(BF)
        v = (dot(n1, wq_o[2]) + bias_v).astype(BF)
        q_o[w] = q
        k_o[w] = k
        v_o[w] = v
        mask = jnp.where(regc[w] == regr[w], 0.0, MASK_FILL)

        @pl.when(w >= 1)
        def _():
            line.cross(w - 1)

        @pl.when(w == 0)
        def _():
            relay(2)
            gathered(2)
            wp_o[...] = jnp.concatenate([wp_g[n] for n in range(4)], axis=1)

        context = jnp.zeros((TOK, width), F32)
        for h in range(heads):
            pick = jnp.where(head_of == h, 1.0, 0.0).astype(BF)
            scores = dot_t(q * pick, k) * HD ** (-0.5) + bias_s[h, :, :TOK] + mask
            lifted = jnp.exp(scores - jnp.max(scores, axis=-1, keepdims=True))
            probs = lifted / jnp.sum(lifted, axis=-1, keepdims=True)
            probs_o[w, h] = probs
            context = context + dot(probs.astype(BF), v * pick)
        ctx = context.astype(BF)
        ctx_o[w] = ctx
        line.put(w, dot(ctx, wp_o[...]))
        line.start(w)

        @pl.when(w >= 1)
        def _():
            line.settle(w - 1)

        @pl.when(w >= 2)
        def _():
            line.hand(w - 2)

        return carry

    lax.fori_loop(0, windows, window, 0)
    line.cross(windows - 1)
    line.hand(windows - 2)
    relay(3)
    line.settle(windows - 1)
    relay(4)
    line.hand(windows - 1)
    gathered(3)
    gathered(4)
    for i in range(images):
        halo_g[i].wait_recv()
        window_rows(
            lambda im, r: og[im, SHIFT + r] if r < SHIFT else gh[im, r - SHIFT], row_tmp, i, ogw_o
        )
    for w in range(windows):
        line.arrive(w)
        line.drain(w)
    for copy in halo_f + halo_g:
        copy.wait_send()
    for n in range(len(items)):
        copy_of(n, 0, f, far).wait_send()
        copy_of(n, 1, f, near).wait_send()
        copy_of(n, 2, far, near).wait_send()


def vmem_call(body, outs, scratch, name, collective_id):
    def call(*args):
        return pl.pallas_call(
            body,
            out_shape=[jax.ShapeDtypeStruct(s, t) for s, t in outs],
            in_specs=[pl.BlockSpec(memory_space=pltpu.VMEM)] * len(args),
            out_specs=[pl.BlockSpec(memory_space=pltpu.VMEM)] * len(outs),
            scratch_shapes=scratch,
            compiler_params=pltpu.CompilerParams(
                collective_id=collective_id, has_side_effects=True, vmem_limit_bytes=VMEM_LIMIT
            ),
            name=name,
        )(*args)

    return call


def attention_forward(features, out_grad, regions, rel_index, w_qkv, w_proj, w_up, w_down,
                      norm_vecs, head_bias, hidden_bias, rel_table):
    images = features.shape[0]
    windows = 2 * images
    shard, width = w_qkv.shape[1], w_qkv.shape[2]
    hidden = w_up.shape[1]
    heads = width // HD
    small = jnp.concatenate(
        [
            norm_vecs,
            jnp.zeros((2, shard), F32),
            hidden_bias.reshape(1, shard),
            jnp.pad(head_bias.reshape(2, -1), ((0, 5), (0, shard - head_bias[0].size))),
        ],
        axis=0,
    )
    table_t = jnp.pad(
        rel_table.astype(BF).astype(F32).T, ((0, 8 - heads), (0, 640 - rel_table.shape[0]))
    )
    ridx = jnp.pad(rel_index, ((0, 0), (0, 256 - TOK)))
    region_win = to_windows(regions[..., None])[..., 0]
    outs = [
        ((3, D, width), BF), ((width, D), BF), ((D, hidden), BF), ((D, hidden), BF), ((16, D), F32),
        ((windows, TOK, D), F32), ((windows, TOK, D), F32), ((windows, TOK, D), BF),
        ((windows, TOK, width), BF), ((windows, TOK, width), BF), ((windows, TOK, width), BF),
        ((windows, heads, TOK, TOK), F32), ((windows, TOK, width), BF),
        ((windows, 2, TOK, HALF), BF),
    ]
    scratch = [
        pltpu.VMEM((4, 16, shard), BF),
        pltpu.VMEM((4, width, shard), BF),
        pltpu.VMEM((images, SHIFT, 24, D), BF),
        pltpu.VMEM((images, SHIFT, 24, D), F32),
        pltpu.VMEM((heads, TOK, 256), F32),
        pltpu.VMEM((24, D), F32),
        *LineSum.scratch(windows),
        pltpu.SemaphoreType.DMA((5, 3)),
        pltpu.SemaphoreType.DMA((5, 3)),
        pltpu.SemaphoreType.DMA((2 * images,)),
        pltpu.SemaphoreType.DMA((2 * images,)),
    ]
    call = vmem_call(attention_forward_body, outs, scratch, "attention_forward", 1)
    return call(features, out_grad, w_qkv, w_proj, w_up, w_down.T, small, table_t, ridx,
                region_win[:, None, :], region_win[:, :, None])


def feed_forward_body(
    rows, wu, wd, xw, ogw, br,
    gu_o, gd_o, dft_o, dbr_o, mix_o, sums_o,
    n2_s, hid_s, dpl_s, ol_s, xhat_s, rstd_s, tot,
    ls_a, ls_b, ls_c, ls_d, ls_e, ls_f, ls_g, ls_h, ls_i, ls_j, ls_k,
):
    windows = xw.shape[0]
    line = LineSum.build((ls_a, ls_b, ls_c, ls_d, ls_e, ls_f, ls_g, ls_h, ls_i, ls_j, ls_k), tot)
    barrier = pltpu.get_barrier_semaphore()
    line.greet(barrier)
    pl.semaphore_wait(barrier, line.greet_count())
    sums_o[...] = jnp.zeros_like(sums_o)
    bias_proj, gain, offset = rows[2:3, :], rows[3:4, :], rows[4:5, :]
    bias_hidden = rows[8:9, :]

    def spot(w):
        return pl.ds(pl.multiple_of(w * TOK, TOK), TOK)

    def window(w, carry):
        resid = xw[w] + (jnp.concatenate([br[w, 0], br[w, 1]], axis=1).astype(F32) + bias_proj)
        centred = resid - row_mean(resid)
        rstd = lax.rsqrt(row_mean(centred * centred) + NORM_EPS)
        xhat = centred * rstd
        xhat_s[w] = xhat
        rstd_s[w] = jnp.broadcast_to(rstd, (TOK, 128))
        n2 = (xhat * gain + offset).astype(BF)
        n2_s[spot(w), :] = n2
        pre = dot(n2, wu[...]) + bias_hidden
        cdf = 0.5 * (1.0 + lax.erf(pre * 0.7071067811865476))
        slope = cdf + pre * (jnp.exp(-0.5 * (pre * pre)) * 0.3989422804014327)
        hid_s[spot(w), :] = (pre * cdf).astype(BF)
        ol = ogw[w].astype(BF)
        ol_s[spot(w), :] = ol
        d_pre = dot(ol, wd[...]) * slope
        sums_o[6:7, :] = sums_o[6:7, :] + jnp.sum(d_pre, axis=0, keepdims=True)
        dpl = d_pre.astype(BF)
        dpl_s[spot(w), :] = dpl

        @pl.when(w >= 1)
        def _():
            line.cross(w - 1)

        line.put(w, dot_t(dpl, wu[...]))
        line.start(w)
        mixed = dot_t(hid_s[spot(w), :], wd[...])
        mix_o[w, 0] = mixed[:, :HALF]
        mix_o[w, 1] = mixed[:, HALF:]

        @pl.when(w >= 1)
        def _():
            line.settle(w - 1)

        @pl.when(w >= 2)
        def _():
            line.hand(w - 2)

        return carry

    def back(w):
        line.arrive(w)
        d_two = jnp.concatenate([tot[w, 0], tot[w, 1]], axis=1).astype(F32)
        xhat = xhat_s[w]
        e = d_two * gain
        d_flat = (e - row_mean(e) - xhat * row_mean(e * xhat)) * rstd_s[w, :, 0:1]
        og = ogw[w]
        d_resid = og + d_flat
        dft_o[w] = d_flat
        dbr_o[w] = d_resid.astype(BF)
        for n, term in ((2, d_resid), (3, d_two * xhat), (4, d_two), (5, og)):
            sums_o[n : n + 1, :] = sums_o[n : n + 1, :] + jnp.sum(term, axis=0, keepdims=True)

    def grad_chunk(m, carry):
        part = pl.ds(pl.multiple_of(m * 256, 256), 256)
        gd_o[part, :] = t_dot(ol_s[:, part], hid_s[...])
        gu_o[part, :] = t_dot(n2_s[:, part], dpl_s[...])
        return carry

    lax.fori_loop(0, windows, window, 0)
    chunks = hid_s.shape[1] // 256
    line.cross(windows - 1)
    line.hand(windows - 2)
    lax.fori_loop(0, 1, grad_chunk, 0)
    line.settle(windows - 1)
    lax.fori_loop(1, 2, grad_chunk, 0)
    line.hand(windows - 1)
    lax.fori_loop(2, chunks, grad_chunk, 0)
    for w in range(windows):
        back(w)
    for w in range(windows):
        line.drain(w)


def feed_forward(rows, wu, wd, xw, ogw, br):
    windows, hidden = xw.shape[0], wu.shape[1]
    outs = [
        ((D, hidden), F32), ((D, hidden), F32), ((windows, TOK, D), F32),
        ((windows, TOK, D), BF), ((windows, 2, TOK, HALF), F32), ((8, D), F32),
    ]
    scratch = [
        pltpu.VMEM((windows * TOK, D), BF),
        pltpu.VMEM((windows * TOK, hidden), BF),
        pltpu.VMEM((windows * TOK, hidden), BF),
        pltpu.VMEM((windows * TOK, D), BF),
        pltpu.VMEM((windows, TOK, D), F32),
        pltpu.VMEM((windows, TOK, 128), F32),
        pltpu.VMEM((windows, 2, TOK, HALF), BF),
        *LineSum.scratch(windows),
    ]
    return vmem_call(feed_forward_body, outs, scratch, "feed_forward", 2)(
        rows, wu, wd, xw, ogw, br
    )


class ShardSum:
    def __init__(self, block_of, out, refs):
        self.block_of, self.out = block_of, out
        self.snd1, self.rcv1, self.snd2, self.rcv2, self.snd3, self.rcv3, self.s, self.r = refs
        f = lax.axis_index("fsdp")
        core = lax.rem(f, 2)
        self.f, self.core = f, core
        self.near, self.far = f + 1 - 2 * core, lax.rem(f + 2, 4)
        self.ctx = 1 - lax.axis_index("ctx")

    @staticmethod
    def scratch(shape):
        return [
            pltpu.VMEM((2, *shape), BF), pltpu.VMEM((2, *shape), BF),
            pltpu.VMEM(shape, BF), pltpu.VMEM(shape, BF),
            pltpu.VMEM(shape, BF), pltpu.VMEM(shape, BF),
            pltpu.SemaphoreType.DMA((4,)), pltpu.SemaphoreType.DMA((4,)),
        ]

    def _near(self, x):
        return remote(self.snd1.at[x], self.rcv1.at[x], self.s.at[x], self.r.at[x], {"fsdp": self.near})

    def _far(self):
        return remote(self.snd2, self.rcv2, self.s.at[2], self.r.at[2], {"fsdp": self.far})

    def _ctx(self):
        return remote(self.snd3, self.rcv3, self.s.at[3], self.r.at[3], {"ctx": self.ctx})

    def start(self):
        for x in range(2):
            self.snd1[x] = self.block_of(2 * x + 1 - self.core).astype(BF)
            self._near(x).start()

    def pair(self):
        for x in range(2):
            self._near(x).wait_recv()
        other = lax.div(self.far, 2)
        self.snd2[...] = (self.block_of(self.far) + self.rcv1[other].astype(F32)).astype(BF)
        self._far().start()

    def cross(self):
        self._far().wait_recv()
        mine = lax.div(self.f, 2)
        self.snd3[...] = (
            self.block_of(self.f) + self.rcv1[mine].astype(F32) + self.rcv2[...].astype(F32)
        ).astype(BF)
        self._ctx().start()

    def finish(self):
        self._ctx().wait_recv()
        self.out[...] = self.snd3[...].astype(F32) + self.rcv3[...].astype(F32)

    def drain(self):
        for x in range(2):
            self._near(x).wait_send()
        self._far().wait_send()
        self._ctx().wait_send()


def home_row(delta, row_tmp, image, r):
    row_tmp[SHIFT : SHIFT + WIN, :] = delta[2 * image, r * WIN : (r + 1) * WIN, :]
    row_tmp[SHIFT + WIN :, :] = delta[2 * image + 1, r * WIN : r * WIN + SHIFT, :]
    row_tmp[:SHIFT, :] = delta[2 * image + 1, r * WIN + SHIFT : (r + 1) * WIN, :]
    return row_tmp[...]


def attention_backward_body(
    rows, wq, wp, n1, q, k, v, probs, ctx, dbr, dft, xw, og, gu, gd, ridx_t, sums, mix,
    gin_o, gq_o, gp_o, small_o, gu_o, gd_o, mixed_o,
    dh_s, dpos_s, delta, row_tmp, halo_s, halo_r, tot, hist_s,
    ls_a, ls_b, ls_c, ls_d, ls_e, ls_f, ls_g, ls_h, ls_i, ls_j, ls_k,
    ua, ub, uc, ud, ue, uf, ug, uh,
    da, db, dc, dd, de, df, dg, dh,
    ms_b, ms_c, ms_d, ms_e, ms_f, ms_g, ms_h, ms_i, ms_j, ms_k,
    h_send, h_recv,
):
    windows, heads = probs.shape[0], probs.shape[1]
    images = windows // 2
    width = q.shape[2]
    c = lax.axis_index("ctx")
    line = LineSum.build((ls_a, ls_b, ls_c, ls_d, ls_e, ls_f, ls_g, ls_h, ls_i, ls_j, ls_k), tot)
    mix_line = LineSum.build((mix, ms_b, ms_c, ms_d, ms_e, ms_f, ms_g, ms_h, ms_i, ms_j, ms_k), mixed_o)
    shard = gu_o.shape[0]
    up = ShardSum(
        lambda at: gu[pl.ds(pl.multiple_of(at * shard, shard), shard), :], gu_o,
        (ua, ub, uc, ud, ue, uf, ug, uh),
    )
    down = ShardSum(
        lambda at: gd[pl.ds(pl.multiple_of(at * shard, shard), shard), :], gd_o,
        (da, db, dc, dd, de, df, dg, dh),
    )
    barrier = pltpu.get_barrier_semaphore()
    greet(barrier, [{"fsdp": up.near}, {"fsdp": up.far}, {"ctx": 1 - c}])
    line.greet(barrier)
    dpos_s[...] = jnp.zeros_like(dpos_s)
    small_o[...] = jnp.zeros_like(small_o)
    small_o[0:8, :] = sums[...]
    pl.semaphore_wait(barrier, 3 + line.greet_count())
    down.start()
    up.start()
    gain = rows[0:1, :]
    head_of = jnp.right_shift(lax.broadcasted_iota(jnp.int32, (1, width), 1), 5)

    def window(w, carry):
        d_branch = dbr[w]
        d_ctx = dot_t(d_branch, wp[...]).astype(BF)
        q_w, k_w, v_w = q[w], k[w], v[w]
        d_q = jnp.zeros((TOK, width), F32)
        d_k = jnp.zeros((TOK, width), F32)
        d_v = jnp.zeros((TOK, width), F32)
        for h in range(heads):
            pick = jnp.where(head_of == h, 1.0, 0.0).astype(BF)
            d_ctx_h = d_ctx * pick
            p = probs[w, h]
            d_p = dot_t(d_ctx_h, v_w)
            d_v = d_v + t_dot(p.astype(BF), d_ctx_h)
            d_s = p * (d_p - jnp.sum(p * d_p, axis=-1, keepdims=True))
            dpos_s[h, :, :TOK] = dpos_s[h, :, :TOK] + d_s
            d_l = (d_s * HD ** (-0.5)).astype(BF)
            d_q = d_q + dot(d_l, k_w * pick)
            d_k = d_k + t_dot(d_l, q_w * pick)
            if h == heads // 2 - 1:

                @pl.when(w >= 1)
                def _():
                    line.cross(w - 1)

        part = jnp.zeros((TOK, D), F32)
        for n, d_n in enumerate((d_q, d_k, d_v)):
            low = d_n.astype(BF)
            dh_s[n, pl.ds(pl.multiple_of(w * TOK, TOK), TOK), :] = low
            part = part + dot_t(low, wq[n])
            if n != 1:
                at = 8 + n // 2
                small_o[at : at + 1, :width] = small_o[at : at + 1, :width] + jnp.sum(
                    low.astype(F32), axis=0, keepdims=True
                )
        line.put(w, part)
        line.start(w)
        mix_line.start(w)

        @pl.when(w == 0)
        def _():
            down.pair()
            up.pair()

        @pl.when(w == 1)
        def _():
            down.cross()

        @pl.when(w == 2)
        def _():
            up.cross()

        @pl.when(w >= 1)
        def _():
            line.settle(w - 1)
            mix_line.cross(w - 1)

        @pl.when(w >= 2)
        def _():
            line.hand(w - 2)
            mix_line.settle(w - 2)

        return carry

    def back(w):
        line.arrive(w)
        x = xw[w]
        centred = x - row_mean(x)
        rstd = lax.rsqrt(row_mean(centred * centred) + NORM_EPS)
        xhat = centred * rstd
        d_one = jnp.concatenate([tot[w, 0], tot[w, 1]], axis=1).astype(F32)
        e = d_one * gain
        delta[w] = dft[w] + (e - row_mean(e) - xhat * row_mean(e * xhat)) * rstd
        for n, term in ((0, d_one * xhat), (1, d_one)):
            small_o[n : n + 1, :] = small_o[n : n + 1, :] + jnp.sum(term, axis=0, keepdims=True)

    halo = [
        remote(halo_s.at[i], halo_r.at[i], h_send.at[i], h_recv.at[i], {"ctx": 1 - c})
        for i in range(images)
    ]

    def go_home(i):
        for r in range(SHIFT, WIN):
            halo_s[i, r - SHIFT] = home_row(delta, row_tmp, i, r).astype(BF)
        halo[i].start()
        for r in range(SHIFT):
            gin_o[i, SHIFT + r] = og[i, SHIFT + r] + home_row(delta, row_tmp, i, r)

    ident = lax.broadcasted_iota(jnp.int32, (TOK, 640), 1)

    def bin_row(i, acc):
        col = ridx_t[i]
        hot = jnp.where(jnp.broadcast_to(col, (TOK, 640)) == ident, 1.0, 0.0).astype(BF)
        vals = jnp.concatenate([dpos_s[h, pl.ds(i, 1), :TOK] for h in range(heads)]
                               + [jnp.zeros((8 - heads, TOK), F32)], axis=0)
        high = vals.astype(BF)
        rest = vals - high.astype(F32)
        mid = rest.astype(BF)
        return acc + dot(high, hot) + dot(mid, hot)

    lax.fori_loop(0, windows, window, 0)
    hist = jnp.zeros((8, 640), F32)
    line.cross(windows - 1)
    line.hand(windows - 2)
    for n in range(3):
        gq_o[n] = t_dot(n1[...], dh_s[n])
    down.finish()
    up.finish()
    line.settle(windows - 1)
    hist = lax.fori_loop(0, TOK // 2, bin_row, hist)
    line.hand(windows - 1)
    mix_line.cross(windows - 1)
    mix_line.hand(0)
    mix_line.settle(windows - 2)
    back(0)
    back(1)
    go_home(0)
    gp = t_dot(ctx[...], dbr[...].reshape(windows * TOK, D))
    for n in range(4):
        gp_o[n] = gp[:, n * shard : (n + 1) * shard]
    mix_line.settle(windows - 1)
    mix_line.hand(1)
    mix_line.hand(2)
    back(2)
    back(3)
    mix_line.hand(windows - 1)
    go_home(1)
    hist = lax.fori_loop(TOK // 2, TOK, bin_row, hist)
    small_o[16:24, :640] = hist
    for i in range(images):
        halo[i].wait_recv()
        for r in range(SHIFT):
            gin_o[i, r] = og[i, r] + halo_r[i, r].astype(F32)
    for w in range(windows):
        line.drain(w)
        mix_line.arrive(w)
        mix_line.drain(w)
    for copy in halo:
        copy.wait_send()
    up.drain()
    down.drain()


def attention_backward(rows, wq, wp, n1, q, k, v, probs, ctx, dbr, dft, xw, og, gu, gd, rel_index, sums, mix):
    windows, heads = probs.shape[0], probs.shape[1]
    images, width, shard = windows // 2, q.shape[2], gd.shape[0] // 4
    hidden = gu.shape[1]
    outs = [
        (og.shape, F32), ((3, D, width), F32), ((4, width, shard), F32), ((24, D), F32),
        ((shard, hidden), F32), ((shard, hidden), F32),
        ((windows, 2, TOK, HALF), BF),
    ]
    scratch = [
        pltpu.VMEM((3, windows * TOK, width), BF),
        pltpu.VMEM((heads, TOK, 256), F32),
        pltpu.VMEM((windows, TOK, D), F32),
        pltpu.VMEM((24, D), F32),
        pltpu.VMEM((images, SHIFT, 24, D), BF),
        pltpu.VMEM((images, SHIFT, 24, D), BF),
        pltpu.VMEM((windows, 2, TOK, HALF), BF),
        pltpu.VMEM((8, 640), F32),
        *LineSum.scratch(windows),
        *ShardSum.scratch((shard, hidden)),
        *ShardSum.scratch((shard, hidden)),
        *LineSum.scratch(windows)[1:],
        pltpu.SemaphoreType.DMA((images,)),
        pltpu.SemaphoreType.DMA((images,)),
    ]
    return vmem_call(attention_backward_body, outs, scratch, "attention_backward", 3)(
        rows, wq, wp, n1.reshape(-1, D), q, k, v, probs, ctx.reshape(-1, width), dbr, dft, xw, og,
        gu, gd, rel_index[:, :, None], sums, mix,
    )


def total_of(x):
    return jnp.sum(jnp.sum(x, axis=1, keepdims=True), axis=0, keepdims=True)


def exact(a, b, dims):
    return lax.dot_general(
        a, b, (dims, ((), ())), precision=lax.Precision.HIGHEST, preferred_element_type=F32
    )


def lane_sums(squares):
    return exact(jnp.ones((8, squares.shape[1]), F32), squares, ((1,), (1,)))[0:1]


def as_column(row):
    n = row.shape[1]
    step = 64
    eye = lax.broadcasted_iota(jnp.int32, (step, step), 0) == lax.broadcasted_iota(
        jnp.int32, (step, step), 1
    )
    return jnp.concatenate(
        [
            jnp.sum(
                jnp.where(eye, jnp.broadcast_to(row[:, at : at + step], (step, step)), 0.0),
                axis=1, keepdims=True,
            )
            for at in range(0, n, step)
        ],
        axis=0,
    )


def lane_pack(values):
    lane = lax.broadcasted_iota(jnp.int32, (8, 128), 1)
    packed = jnp.zeros((8, 128), F32)
    for n, value in enumerate(values):
        packed = packed + jnp.where(lane == n, jnp.broadcast_to(value, (8, 128)), 0.0)
    return packed


def optimizer_body(
    gq, gp, g_up, g_down, small, rows, feat, br, mixed,
    w_qkv, w_proj, w_up, w_down, w_norm, w_heads, w_hidden, w_table,
    row_qkv, col_qkv, row_proj, col_proj, row_up, col_up, row_down, col_down,
    s_norm, s_heads, s_hidden, s_table,
    out_o, gq_o, gp_o, gn_o, gh_o, gu_o, gt_o,
    nq_o, np_o, nu_o, nd_o, nn_o, nh_o, nx_o, nt_o,
    cq_o, cp_o, cu_o, cd_o,
    rq_o, kq_o, rp_o, kp_o, ru_o, ku_o, rd_o, kd_o,
    sn_o, sh_o, sx_o, st_o, clip_o,
    qa, qb, qc, qd, qe, qf, qg, qh,
    pa, pb, pc, pd, pe, pf, pg, ph,
    sm_s, sm_r, t_s, f_s, z_s, c_s, delta, row_tmp, halo_s, halo_r,
    sm_send, sm_recv, t_send, t_recv, f_send, f_recv, z_send, z_recv, c_send, c_recv, h_send, h_recv,
):
    f, c, t = lax.axis_index("fsdp"), lax.axis_index("ctx"), lax.axis_index("tp")
    images = feat.shape[0]
    windows = 2 * images
    shard, width = w_qkv.shape[1], w_qkv.shape[2]
    me = f * 4 + t
    first_f = jnp.where(f == 0, 1.0, 0.0)
    first_t = jnp.where(t == 0, 1.0, 0.0)

    def other(n):
        at = lax.rem(me + n, 16)
        return {"fsdp": lax.div(at, 4), "tp": lax.rem(at, 4)}

    barrier = pltpu.get_barrier_semaphore()
    greet(barrier, [{"ctx": 1 - c}] + [other(n) for n in range(1, 16)])
    qkv = ShardSum(
        lambda at: gq[:, pl.ds(pl.multiple_of(at * shard, shard), shard), :], gq_o,
        (qa, qb, qc, qd, qe, qf, qg, qh),
    )
    proj = ShardSum(lambda at: gp[at], gp_o, (pa, pb, pc, pd, pe, pf, pg, ph))
    sm_s[0] = small[...]

    def swap(n):
        where = ({"fsdp": qkv.near}, {"fsdp": qkv.far}, {"ctx": 1 - c})[n]
        return remote(sm_s.at[n], sm_r.at[n], sm_send.at[n], sm_recv.at[n], where)

    pl.semaphore_wait(barrier, 16)
    swap(0).start()
    qkv.start()
    proj.start()

    keep = 1.0 - DECAY_RATE
    t_s[t] = jnp.zeros((8, shard), F32)
    f_s[f] = jnp.zeros((8, f_s.shape[2]), F32)
    sq_up = g_up[...] * g_up[...]
    sq_down = g_down[...] * g_down[...]
    t_s[t, 4:5, :] = lane_sums(sq_up)
    t_s[t, 5:6, :] = lane_sums(sq_down)
    f_s[f, 4:5, :] = jnp.sum(sq_up, axis=0, keepdims=True)
    f_s[f, 5:6, :] = jnp.sum(sq_down, axis=0, keepdims=True)
    tot_up, tot_down = total_of(sq_up), total_of(sq_down)
    old_rows = [
        first_t * jnp.sum(row_qkv[0:1, :], axis=1, keepdims=True),
        first_t * jnp.sum(row_qkv[1:2, :], axis=1, keepdims=True),
        first_t * jnp.sum(row_qkv[2:3, :], axis=1, keepdims=True),
        first_f * jnp.sum(row_proj[...], axis=1, keepdims=True),
        first_t * jnp.sum(row_up[...], axis=1, keepdims=True),
        first_f * jnp.sum(row_down[...], axis=1, keepdims=True),
    ]
    masters = [
        sum(total_of(w_qkv[n] * w_qkv[n]) for n in range(3)),
        total_of(w_proj[...] * w_proj[...]),
        total_of(w_up[...] * w_up[...]),
        total_of(w_down[...] * w_down[...]),
        *[
            first_t * jnp.sum(w_norm[n : n + 1, :] * w_norm[n : n + 1, :], axis=1, keepdims=True)
            for n in range(6)
        ],
        *[total_of(w_heads[n] * w_heads[n]) for n in range(2)],
        total_of(w_hidden[...] * w_hidden[...]),
        first_f * total_of(w_table[...] * w_table[...]),
    ]

    qkv.pair()
    proj.pair()
    swap(0).wait_recv()
    sm_s[1] = sm_s[0] + sm_r[0]
    swap(1).start()

    bias_two, bias_five = rows[2:3, :], rows[5:6, :]
    for w in range(windows):
        delta[w] = (
            jnp.concatenate([br[w, 0], br[w, 1]], axis=1).astype(F32) + bias_two
            + jnp.concatenate([mixed[w, 0], mixed[w, 1]], axis=1).astype(F32) + bias_five
        )
    halo = [
        remote(halo_s.at[i], halo_r.at[i], h_send.at[i], h_recv.at[i], {"ctx": 1 - c})
        for i in range(images)
    ]
    qkv.cross()
    proj.cross()
    swap(1).wait_recv()
    sm_s[2] = sm_s[1] + sm_r[1]
    swap(2).start()
    for i in range(images):
        for r in range(SHIFT, WIN):
            halo_s[i, r - SHIFT] = home_row(delta, row_tmp, i, r).astype(BF)
        for r in range(SHIFT):
            out_o[i, SHIFT + r] = feat[i, SHIFT + r].astype(F32) + home_row(delta, row_tmp, i, r)
    qkv.finish()
    proj.finish()

    tot_q = []
    for n in range(3):
        sq = gq_o[n] * gq_o[n]
        t_s[t, n : n + 1, :] = lane_sums(sq)
        f_s[f, n : n + 1, :width] = jnp.sum(sq, axis=0, keepdims=True)
        tot_q.append(total_of(sq))
    sq = gp_o[...] * gp_o[...]
    f_s[f, 3:4, :shard] = lane_sums(sq)
    t_s[t, 3:4, :] = jnp.sum(sq, axis=0, keepdims=True)
    z_s[me] = lane_pack([*tot_q, total_of(sq), tot_up, tot_down, *old_rows, *masters])

    def t_copy(n):
        return remote(t_s.at[t], t_s.at[t], t_send.at[n], t_recv.at[n], {"tp": lax.rem(t + n, 4)})

    def f_copy(n):
        return remote(f_s.at[f], f_s.at[f], f_send.at[n], f_recv.at[n], {"fsdp": lax.rem(f + n, 4)})

    def z_copy(n):
        return remote(z_s.at[me], z_s.at[me], z_send.at[n], z_recv.at[n], other(n))

    def c_copy(n):
        return remote(c_s.at[me], c_s.at[me], c_send.at[n], c_recv.at[n], other(n))

    for n in range(1, 4):
        t_copy(n).start()
        f_copy(n).start()
    for n in range(1, 16):
        z_copy(n).start()
    for i in range(images):
        halo[i].start()

    swap(2).wait_recv()
    sm = sm_s[2] + sm_r[2]

    def own_lanes(x, size):
        out = x[:, :size]
        for n in range(1, 4):
            out = jnp.where(f == n, x[:, n * size : (n + 1) * size], out)
        return out

    gn = own_lanes(sm[0:6, :], shard)
    gn_o[...] = gn
    part = HD // 4

    def spread(row, count):
        lanes = count * HD
        lane = lax.broadcasted_iota(jnp.int32, (count, lanes), 1)
        unit = lax.broadcasted_iota(jnp.int32, (count, lanes), 0)
        only = jnp.where(
            jnp.right_shift(lane, 5) == unit, jnp.broadcast_to(row, (count, lanes)), 0.0
        )
        at = lax.broadcasted_iota(jnp.int32, (lanes, part), 0)
        k = lax.broadcasted_iota(jnp.int32, (lanes, part), 1)
        pick = jnp.where(jnp.bitwise_and(at, HD - 1) == f * part + k, 1.0, 0.0)
        return exact(only, pick, ((1,), (0,)))

    heads = width // HD
    gh = [spread(sm[8 + n : 9 + n, :width], heads) for n in range(2)]
    gx = spread(sm[6:7, :], nx_o.shape[0])
    gu_o[...] = gx
    eye = jnp.where(
        lax.broadcasted_iota(jnp.int32, (8, 8), 0) == lax.broadcasted_iota(jnp.int32, (8, 8), 1),
        1.0, 0.0,
    )
    gt = exact(sm[16:24, :640], eye, ((0,), (0,)))[: w_table.shape[0], :heads]
    gt_o[...] = gt

    def plain(grad, state):
        new = DECAY_RATE * state + keep * (grad * grad + STAT_EPS)
        return new, grad * lax.rsqrt(new)

    sn, un = plain(gn, s_norm[...])
    sn_o[...] = sn
    uh = []
    for n in range(2):
        gh_o[n] = gh[n]
        sh, u = plain(gh[n], s_heads[n])
        sh_o[n] = sh
        uh.append(u)
    sx, ux = plain(gx, s_hidden[...])
    sx_o[...] = sx
    st, ut = plain(gt, s_table[...])
    st_o[...] = st
    small_sq = (
        first_t * total_of(un * un) + total_of(uh[0] * uh[0]) + total_of(uh[1] * uh[1])
        + total_of(ux * ux) + first_f * total_of(ut * ut)
    )

    for n in range(1, 4):
        t_copy(n).wait_recv()
        f_copy(n).wait_recv()
    t_sum = t_s[0] + t_s[1] + t_s[2] + t_s[3]
    f_sum = f_s[0] + f_s[1] + f_s[2] + f_s[3]
    for n in range(1, 16):
        z_copy(n).wait_recv()
    z_sum = z_s[0]
    for n in range(1, 16):
        z_sum = z_sum + z_s[n]
    lane8 = lax.broadcasted_iota(jnp.int32, (8, 128), 1)

    def scalar(n):
        return jnp.sum(jnp.where(lane8 == n, z_sum, 0.0)[0:1], axis=1, keepdims=True)

    def fresh(old, summed, count):
        return DECAY_RATE * old + keep * (summed / count + STAT_EPS)

    hidden = f_s.shape[2]
    ff = 4 * hidden
    rq = fresh(row_qkv[...], t_sum[0:3, :], D)
    kq = fresh(col_qkv[...], f_sum[0:3, :width], D)
    rp = fresh(row_proj[...], f_sum[3:4, :width], D)
    kp = fresh(col_proj[...], t_sum[3:4, :], D)
    ru = fresh(row_up[...], t_sum[4:5, :], ff)
    ku = fresh(col_up[...], f_sum[4:5, :], D)
    rd = fresh(row_down[...], f_sum[5:6, :], D)
    kd = fresh(col_down[...], t_sum[5:6, :], ff)
    for ref, val in (
        (rq_o, rq), (kq_o, kq), (rp_o, rp), (kp_o, kp), (ru_o, ru), (ku_o, ku), (rd_o, rd), (kd_o, kd)
    ):
        ref[...] = val

    def mean_row(n, rows_all, cols_all):
        return (DECAY_RATE * scalar(6 + n) + keep * (scalar(n) / cols_all + rows_all * STAT_EPS)) / rows_all

    scale_q = [
        as_column(lax.rsqrt(rq[n : n + 1, :] / mean_row(n, D, D))) * lax.rsqrt(kq[n : n + 1, :])
        for n in range(3)
    ]
    scale_p = as_column(lax.rsqrt(rp / mean_row(3, D, D))) * lax.rsqrt(kp)
    scale_u = as_column(lax.rsqrt(ru / mean_row(4, D, ff))) * lax.rsqrt(ku)
    scale_d = as_column(lax.rsqrt(kd)) * lax.rsqrt(rd / mean_row(5, ff, D))
    big_sq = small_sq
    for n in range(3):
        u = gq_o[n] * scale_q[n]
        nq_o[n] = u
        big_sq = big_sq + total_of(u * u)
    for grad, scale, ref in ((gp_o, scale_p, np_o), (g_up, scale_u, nu_o), (g_down, scale_d, nd_o)):
        u = grad[...] * scale
        ref[...] = u
        big_sq = big_sq + total_of(u * u)
    c_s[me] = jnp.broadcast_to(big_sq, (8, 128))
    for n in range(1, 16):
        c_copy(n).start()
    for i in range(images):
        halo[i].wait_recv()
        for r in range(SHIFT):
            out_o[i, r] = feat[i, r].astype(F32) + halo_r[i, r].astype(F32)
    counts = [3 * D * D, D * D, D * ff, ff * D] + [D] * 8 + [ff, RELP * HEADS]
    sizes = [jnp.sqrt(scalar(12 + n) / counts[n] + STAT_EPS) for n in range(14)]
    for n in range(1, 16):
        c_copy(n).wait_recv()
    all_sq = c_s[0]
    for n in range(1, 16):
        all_sq = all_sq + c_s[n]
    count_all = 4 * D * D + 2 * D * ff + 8 * D + ff + RELP * HEADS
    clip = jnp.sqrt(all_sq[0:1, 0:1] / count_all)
    clip_o[...] = clip
    factor = STEP_RATE / jnp.maximum(1.0, clip / CLIP_LEVEL)

    for n in range(3):
        new = w_qkv[n] - sizes[0] * factor * nq_o[n]
        nq_o[n] = new
        cq_o[n] = new.astype(BF)
    for master, size, ref, low in (
        (w_proj, sizes[1], np_o, cp_o), (w_up, sizes[2], nu_o, cu_o), (w_down, sizes[3], nd_o, cd_o)
    ):
        new = master[...] - size * factor * ref[...]
        ref[...] = new
        low[...] = new.astype(BF)
    for n in range(6):
        nn_o[n : n + 1, :] = w_norm[n : n + 1, :] - sizes[4 + n] * factor * un[n : n + 1, :]
    for n in range(2):
        nh_o[n] = w_heads[n] - sizes[10 + n] * factor * uh[n]
    nx_o[...] = w_hidden[...] - sizes[12] * factor * ux
    nt_o[...] = w_table[...] - sizes[13] * factor * ut

    for n in range(3):
        swap(n).wait_send()
    for n in range(1, 4):
        t_copy(n).wait_send()
        f_copy(n).wait_send()
    for n in range(1, 16):
        z_copy(n).wait_send()
        c_copy(n).wait_send()
    for copy in halo:
        copy.wait_send()
    qkv.drain()
    proj.drain()


def optimizer(gq, gp, g_up, g_down, small, rows, feat, br, mixed, masters, stats, states):
    w_qkv, w_proj, w_up, w_down, w_norm, w_heads, w_hidden, w_table = masters
    images = feat.shape[0]
    windows = 2 * images
    shard, width = w_qkv.shape[1], w_qkv.shape[2]
    hidden = w_up.shape[1]
    stats = [u if u.ndim == 2 else u[None] for u in stats]
    like = lambda u: (u.shape, F32)
    mats = (w_qkv, w_proj, w_up, w_down)
    small_ps = (w_norm, w_heads, w_hidden, w_table)
    outs = [
        (feat.shape, F32), like(w_qkv), like(w_proj), like(w_norm), like(w_heads), like(w_hidden),
        like(w_table), *map(like, masters), *[(u.shape, BF) for u in mats], *map(like, stats),
        *map(like, small_ps), ((1, 1), F32),
    ]
    scratch = [
        *ShardSum.scratch((3, shard, width)),
        *ShardSum.scratch((width, shard)),
        pltpu.VMEM((3, 24, D), F32), pltpu.VMEM((3, 24, D), F32),
        pltpu.VMEM((4, 8, shard), F32), pltpu.VMEM((4, 8, hidden), F32),
        pltpu.VMEM((16, 8, 128), F32), pltpu.VMEM((16, 8, 128), F32),
        pltpu.VMEM((windows, TOK, D), F32), pltpu.VMEM((24, D), F32),
        pltpu.VMEM((images, SHIFT, 24, D), BF), pltpu.VMEM((images, SHIFT, 24, D), BF),
        pltpu.SemaphoreType.DMA((3,)), pltpu.SemaphoreType.DMA((3,)),
        *[pltpu.SemaphoreType.DMA((4,)) for _ in range(4)],
        *[pltpu.SemaphoreType.DMA((16,)) for _ in range(4)],
        pltpu.SemaphoreType.DMA((images,)), pltpu.SemaphoreType.DMA((images,)),
    ]
    return vmem_call(optimizer_body, outs, scratch, "optimizer", 4)(
        gq, gp, g_up, g_down, small, rows, feat, br, mixed, *masters, *stats, *states
    )


def per_device_plain(
    features,
    out_grad,
    regions,
    rel_index,
    w_qkv,
    w_proj,
    w_up,
    w_down,
    norm_vecs,
    head_bias,
    hidden_bias,
    rel_table,
    row_qkv,
    col_qkv,
    row_proj,
    col_proj,
    row_up,
    col_up,
    row_down,
    col_down,
    state_norm,
    state_heads,
    state_hidden,
    state_table,
):
    images, band_rows, across, model_width = features.shape
    win_tokens = WIN * WIN
    fsdp_at = lax.axis_index("fsdp")
    ctx_at = lax.axis_index("ctx")
    tp_at = lax.axis_index("tp")
    first_fsdp = (fsdp_at == 0).astype(jnp.float32)
    first_ctx = (ctx_at == 0).astype(jnp.float32)
    first_tp = (tp_at == 0).astype(jnp.float32)
    weights_qkv, weights_proj, weights_up, weights_down, vec_copy, head_copy, hidden_copy = (
        lax.all_gather(w_qkv.astype(jnp.bfloat16), "fsdp", axis=1, tiled=True),
        lax.all_gather(w_proj.astype(jnp.bfloat16), "fsdp", axis=1, tiled=True),
        lax.all_gather(w_up.astype(jnp.bfloat16), "fsdp", axis=0, tiled=True),
        lax.all_gather(w_down.astype(jnp.bfloat16), "fsdp", axis=1, tiled=True),
        lax.all_gather(norm_vecs.astype(jnp.bfloat16), "fsdp", axis=1, tiled=True),
        lax.all_gather(head_bias.astype(jnp.bfloat16), "fsdp", axis=2, tiled=True),
        lax.all_gather(hidden_bias.astype(jnp.bfloat16), "fsdp", axis=1, tiled=True),
    )
    norm_rows = vec_copy.astype(jnp.float32)
    bias_query = head_copy[0].reshape(-1).astype(jnp.float32)
    bias_value = head_copy[1].reshape(-1).astype(jnp.float32)
    bias_hidden = hidden_copy.reshape(-1).astype(jnp.float32)
    table_copy = rel_table.astype(jnp.bfloat16)
    local_width = weights_qkv.shape[2]
    heads_here = local_width // HD

    def roll_in(home):
        received = passed_along(home[:, :SHIFT], "ctx", -1)
        return to_windows(enter_frame(home, received)).reshape(-1, model_width)

    def roll_out(rolled_flat):
        band = jnp.roll(
            from_windows(
                rolled_flat.reshape(-1, win_tokens, model_width), images, band_rows, across
            ),
            SHIFT,
            axis=2,
        )
        lower = passed_along(band[:, band_rows - SHIFT :], "ctx", 1)
        return jnp.concatenate([lower, band[:, : band_rows - SHIFT]], axis=1)

    flat_one = roll_in(features).astype(jnp.float32)
    grad_flat = roll_in(out_grad)
    win_count = flat_one.shape[0] // win_tokens
    normed_one, pull_one = jax.vjp(layer_norm, flat_one, norm_rows[0], norm_rows[1])
    normed_one_low = normed_one.astype(jnp.bfloat16)
    head_shape = (win_count, win_tokens, heads_here, HD)
    query_low, key_low, value_low = project_heads(
        normed_one_low, weights_qkv, bias_query, bias_value, head_shape
    )
    pos_bias = table_lookup(table_copy, rel_index)
    region_win = to_windows(regions[..., None])[..., 0]
    mask_add = jnp.where(region_win[:, :, None] == region_win[:, None, :], 0.0, MASK_FILL).astype(
        jnp.float32
    )
    scores = attention_scores(query_low, key_low, pos_bias, mask_add)
    top_score = jnp.max(scores, axis=-1, keepdims=True)
    lifted = jnp.exp(scores - top_score)
    prob_rows = lifted / jnp.sum(lifted, axis=-1, keepdims=True)
    prob_low = prob_rows.astype(jnp.bfloat16)
    context = jnp.einsum("whij,wjhc->wihc", prob_low, value_low, preferred_element_type=jnp.float32)
    context_low = context.astype(jnp.bfloat16).reshape(-1, local_width)
    branch_part = jnp.dot(context_low, weights_proj, preferred_element_type=jnp.float32)
    branch = lax.psum(branch_part.astype(jnp.bfloat16), "tp").astype(jnp.float32) + norm_rows[2]
    flat_two = flat_one + branch
    normed_two, pull_two = jax.vjp(layer_norm, flat_two, norm_rows[3], norm_rows[4])
    normed_two_low = normed_two.astype(jnp.bfloat16)
    pre_act = jnp.dot(normed_two_low, weights_up, preferred_element_type=jnp.float32) + bias_hidden
    hidden, pull_gelu = jax.vjp(exact_gelu, pre_act)
    hidden_low = hidden.astype(jnp.bfloat16)
    mixed_part = jnp.dot(hidden_low, weights_down, preferred_element_type=jnp.float32)
    mixed_whole = lax.psum(mixed_part.astype(jnp.bfloat16), "tp").astype(jnp.float32)
    block_out = features.astype(jnp.float32) + roll_out(
        (branch + mixed_whole + norm_rows[5]).astype(jnp.bfloat16)
    ).astype(jnp.float32)
    grad_low = grad_flat.astype(jnp.bfloat16)
    grad_down_full = jnp.einsum(
        "tf,td->fd", hidden_low, grad_low, preferred_element_type=jnp.float32
    )
    grad_down_bias = jnp.sum(grad_flat, axis=0)
    d_hidden = jnp.einsum("td,fd->tf", grad_low, weights_down, preferred_element_type=jnp.float32)
    d_pre = pull_gelu(d_hidden)[0]
    d_pre_low = d_pre.astype(jnp.bfloat16)
    grad_hidden_bias = jnp.sum(d_pre, axis=0)
    grad_up_full = jnp.einsum(
        "td,tf->df", normed_two_low, d_pre_low, preferred_element_type=jnp.float32
    )
    d_two_part = jnp.einsum("tf,df->td", d_pre_low, weights_up, preferred_element_type=jnp.float32)
    d_two = lax.psum(d_two_part.astype(jnp.bfloat16), "tp").astype(jnp.float32)
    d_flat_two, grad_gain_two, grad_offset_two = pull_two(d_two)
    d_resid = grad_flat + d_flat_two
    grad_proj_bias = jnp.sum(d_resid, axis=0)
    d_branch = d_resid.astype(jnp.bfloat16)
    grad_proj_full = jnp.einsum(
        "tc,td->cd", context_low, d_branch, preferred_element_type=jnp.float32
    )
    d_context = (
        jnp.einsum("td,cd->tc", d_branch, weights_proj, preferred_element_type=jnp.float32)
        .astype(jnp.bfloat16)
        .reshape(head_shape)
    )
    d_probs = jnp.einsum(
        "wihc,wjhc->whij", d_context, value_low, preferred_element_type=jnp.float32
    )
    d_value_low = jnp.einsum(
        "whij,wihc->wjhc", prob_low, d_context, preferred_element_type=jnp.float32
    ).astype(jnp.bfloat16)
    d_scores = prob_rows * (d_probs - jnp.sum(prob_rows * d_probs, axis=-1, keepdims=True))
    d_pos = jnp.sum(d_scores, axis=0)
    d_scaled = (d_scores * HD ** (-0.5)).astype(jnp.bfloat16)
    d_query_low = jnp.einsum(
        "whij,wjhc->wihc", d_scaled, key_low, preferred_element_type=jnp.float32
    ).astype(jnp.bfloat16)
    d_key_low = jnp.einsum(
        "whij,wihc->wjhc", d_scaled, query_low, preferred_element_type=jnp.float32
    ).astype(jnp.bfloat16)
    d_heads = jnp.stack([d_query_low, d_key_low, d_value_low]).reshape(3, -1, local_width)
    grad_qkv_full = jnp.einsum(
        "td,ktc->kdc", normed_one_low, d_heads, preferred_element_type=jnp.float32
    )
    grad_head_bias = jnp.stack(
        [
            jnp.sum(d_heads[0].astype(jnp.float32), axis=0),
            jnp.sum(d_heads[2].astype(jnp.float32), axis=0),
        ]
    ).reshape(2, heads_here, HD)
    d_one_part = jnp.einsum("ktc,kdc->td", d_heads, weights_qkv, preferred_element_type=jnp.float32)
    d_one = lax.psum(d_one_part.astype(jnp.bfloat16), "tp").astype(jnp.float32)
    d_flat_one, grad_gain_one, grad_offset_one = pull_one(d_one)
    grad_input = out_grad + roll_out((d_flat_two + d_flat_one).astype(jnp.bfloat16)).astype(
        jnp.float32
    )
    table_part = table_grad(d_pos, rel_index, rel_table.shape[0])
    grad_norm_full = jnp.stack(
        [
            grad_gain_one,
            grad_offset_one,
            grad_proj_bias,
            grad_gain_two,
            grad_offset_two,
            grad_down_bias,
        ]
    )
    grad_list = (
        grad_qkv_full,
        grad_proj_full,
        grad_up_full,
        grad_down_full,
        grad_norm_full,
        grad_head_bias,
        grad_hidden_bias.reshape(-1, HD),
    )
    g_qkv, g_proj, g_up, g_down, g_norm, g_heads, g_hidden = shard_sum(band_sum(grad_list))
    d_shard = w_qkv.shape[1]
    hidden_here = w_up.shape[1]
    keep = 1.0 - DECAY_RATE
    sq_qkv = g_qkv * g_qkv
    sq_proj = g_proj * g_proj
    sq_up = g_up * g_up
    sq_down = g_down * g_down
    stat_rq = place(
        (keep * jnp.sum(sq_qkv, axis=2) / D + first_tp * (DECAY_RATE * row_qkv + keep * STAT_EPS))
        * first_ctx,
        fsdp_at,
        D,
    )
    stat_cq = place(
        (keep * jnp.sum(sq_qkv, axis=1) / D + first_fsdp * (DECAY_RATE * col_qkv + keep * STAT_EPS))
        * first_ctx,
        tp_at,
        D,
    )
    stat_rp = place(
        (
            keep * jnp.sum(sq_proj, axis=1) / D
            + first_fsdp * (DECAY_RATE * row_proj + keep * STAT_EPS)
        )
        * first_ctx,
        tp_at,
        D,
    )
    stat_cp = place(
        (keep * jnp.sum(sq_proj, axis=0) / D + first_tp * (DECAY_RATE * col_proj + keep * STAT_EPS))
        * first_ctx,
        fsdp_at,
        D,
    )
    stat_ru = place(
        (keep * jnp.sum(sq_up, axis=1) / FF + first_tp * (DECAY_RATE * row_up + keep * STAT_EPS))
        * first_ctx,
        fsdp_at,
        D,
    )
    stat_cu = place(
        (keep * jnp.sum(sq_up, axis=0) / D + first_fsdp * (DECAY_RATE * col_up + keep * STAT_EPS))
        * first_ctx,
        tp_at,
        FF,
    )
    stat_rd = place(
        (
            keep * jnp.sum(sq_down, axis=1) / D
            + first_fsdp * (DECAY_RATE * row_down + keep * STAT_EPS)
        )
        * first_ctx,
        tp_at,
        FF,
    )
    stat_cd = place(
        (
            keep * jnp.sum(sq_down, axis=0) / FF
            + first_tp * (DECAY_RATE * col_down + keep * STAT_EPS)
        )
        * first_ctx,
        fsdp_at,
        D,
    )
    table_whole = place(table_part, tp_at, HEADS)
    master_sq = jnp.concatenate(
        [
            jnp.stack(
                [
                    jnp.sum(w_qkv * w_qkv),
                    jnp.sum(w_proj * w_proj),
                    jnp.sum(w_up * w_up),
                    jnp.sum(w_down * w_down),
                ]
            )
            * first_ctx,
            jnp.sum(norm_vecs * norm_vecs, axis=1) * first_ctx * first_tp,
            jnp.sum(head_bias * head_bias, axis=(1, 2)) * first_ctx,
            jnp.sum(hidden_bias * hidden_bias)[None] * first_ctx,
            jnp.sum(rel_table * rel_table)[None] * first_ctx * first_fsdp,
        ]
    )
    (
        full_rq,
        full_cq,
        full_rp,
        full_cp,
        full_ru,
        full_cu,
        full_rd,
        full_cd,
        table_sum,
        master_total,
    ) = lax.psum(
        (
            stat_rq,
            stat_cq,
            stat_rp,
            stat_cp,
            stat_ru,
            stat_cu,
            stat_rd,
            stat_cd,
            table_whole,
            master_sq,
        ),
        ("fsdp", "ctx", "tp"),
    )
    u_qkv = factored(
        g_qkv,
        own_part(full_rq, fsdp_at, d_shard),
        own_part(full_cq, tp_at, local_width),
        jnp.mean(full_rq, axis=1)[:, None, None],
    )
    u_proj = factored(
        g_proj,
        own_part(full_rp, tp_at, local_width),
        own_part(full_cp, fsdp_at, d_shard),
        jnp.mean(full_rp),
    )
    u_up = factored(
        g_up,
        own_part(full_ru, fsdp_at, d_shard),
        own_part(full_cu, tp_at, hidden_here),
        jnp.mean(full_ru),
    )
    u_down = factored(
        g_down,
        own_part(full_rd, tp_at, hidden_here),
        own_part(full_cd, fsdp_at, d_shard),
        jnp.mean(full_rd),
    )
    g_table = own_part(table_sum, tp_at, heads_here)
    state_norm_new, u_norm = plain_stats(g_norm, state_norm)
    state_heads_new, u_heads = plain_stats(g_heads, state_heads)
    state_hidden_new, u_hidden = plain_stats(g_hidden, state_hidden)
    state_table_new, u_table = plain_stats(g_table, state_table)
    local_sq = (
        jnp.sum(u_qkv * u_qkv)
        + jnp.sum(u_proj * u_proj)
        + jnp.sum(u_up * u_up)
        + jnp.sum(u_down * u_down)
        + jnp.sum(u_heads * u_heads)
        + jnp.sum(u_hidden * u_hidden)
        + first_tp * jnp.sum(u_norm * u_norm)
        + first_fsdp * jnp.sum(u_table * u_table)
    )
    total_sq = lax.psum(local_sq, ("fsdp", "tp"))
    count_all = 4 * D * D + 2 * D * FF + 8 * D + FF + RELP * HEADS
    clip_rms = jnp.sqrt(total_sq / count_all)
    factor = 1.0 / jnp.maximum(1.0, clip_rms / CLIP_LEVEL)
    counts = jnp.array(
        [3 * D * D, D * D, D * FF, FF * D, D, D, D, D, D, D, D, D, FF, RELP * HEADS], jnp.float32
    )
    scales = jnp.sqrt(master_total / counts + STAT_EPS)
    new_qkv = w_qkv - STEP_RATE * scales[0] * factor * u_qkv
    new_proj = w_proj - STEP_RATE * scales[1] * factor * u_proj
    new_up = w_up - STEP_RATE * scales[2] * factor * u_up
    new_down = w_down - STEP_RATE * scales[3] * factor * u_down
    new_norm = norm_vecs - STEP_RATE * scales[4:10][:, None] * factor * u_norm
    new_heads = head_bias - STEP_RATE * scales[10:12][:, None, None] * factor * u_heads
    new_hidden = hidden_bias - STEP_RATE * scales[12] * factor * u_hidden
    new_table = rel_table - STEP_RATE * scales[13] * factor * u_table
    return (
        block_out,
        grad_input,
        g_qkv,
        g_proj,
        g_up,
        g_down,
        g_norm,
        g_heads,
        g_hidden,
        g_table,
        new_qkv,
        new_proj,
        new_up,
        new_down,
        new_norm,
        new_heads,
        new_hidden,
        new_table,
        new_qkv.astype(jnp.bfloat16),
        new_proj.astype(jnp.bfloat16),
        new_up.astype(jnp.bfloat16),
        new_down.astype(jnp.bfloat16),
        own_part(full_rq, fsdp_at, d_shard),
        own_part(full_cq, tp_at, local_width),
        own_part(full_rp, tp_at, local_width),
        own_part(full_cp, fsdp_at, d_shard),
        own_part(full_ru, fsdp_at, d_shard),
        own_part(full_cu, tp_at, hidden_here),
        own_part(full_rd, tp_at, hidden_here),
        own_part(full_cd, fsdp_at, d_shard),
        state_norm_new,
        state_heads_new,
        state_hidden_new,
        state_table_new,
        clip_rms,
    )


def per_device(
    features,
    out_grad,
    regions,
    rel_index,
    w_qkv,
    w_proj,
    w_up,
    w_down,
    norm_vecs,
    head_bias,
    hidden_bias,
    rel_table,
    row_qkv,
    col_qkv,
    row_proj,
    col_proj,
    row_up,
    col_up,
    row_down,
    col_down,
    state_norm,
    state_heads,
    state_hidden,
    state_table,
):
    (weights_qkv, weights_proj, weights_up, weights_down, rows, xw, ogw, n1, query_low, key_low, value_low,
     prob_rows, ctx, br) = attention_forward(
        features, out_grad, regions, rel_index, w_qkv, w_proj, w_up, w_down,
        norm_vecs, head_bias, hidden_bias, rel_table)
    gu, gd, dft, dbr, mix, sums = feed_forward(rows, weights_up, weights_down, xw, ogw, br)
    grad_input, gq, gp, small, g_up, g_down, mixed = attention_backward(
        rows, weights_qkv, weights_proj, n1, query_low, key_low, value_low, prob_rows, ctx, dbr, dft,
        xw, out_grad, gu, gd, rel_index, sums, mix)
    (block_out, g_qkv, g_proj, g_norm, g_heads, g_hidden, g_table,
     new_qkv, new_proj, new_up, new_down, new_norm, new_heads, new_hidden, new_table,
     copy_qkv, copy_proj, copy_up, copy_down, *stats, clip_rms) = optimizer(
        gq, gp, g_up, g_down, small, rows, features, br, mixed,
        (w_qkv, w_proj, w_up, w_down.T, norm_vecs, head_bias, hidden_bias, rel_table),
        (row_qkv, col_qkv, row_proj, col_proj, row_up, col_up, row_down, col_down),
        (state_norm, state_heads, state_hidden, state_table))
    factors, states = stats[:8], stats[8:]
    factors = factors[:2] + [u[0] for u in factors[2:]]
    return (
        block_out, grad_input, g_qkv, g_proj, g_up, g_down.T, g_norm, g_heads, g_hidden, g_table,
        new_qkv, new_proj, new_up, new_down.T, new_norm, new_heads, new_hidden, new_table,
        copy_qkv, copy_proj, copy_up, copy_down.T, *factors, *states, clip_rms[0, 0],
    )


def solution(mesh):
    line_of_four = mesh.shape["fsdp"] == 4 and mesh.shape["tp"] == 4 and mesh.shape["ctx"] == 2
    return jax.shard_map(
        per_device if line_of_four else per_device_plain,
        mesh=mesh,
        in_specs=(
            P("fsdp", "ctx", None, None),
            P("fsdp", "ctx", None, None),
            P("fsdp", "ctx", None),
            P(),
            P(None, "fsdp", "tp"),
            P("tp", "fsdp"),
            P("fsdp", "tp"),
            P("tp", "fsdp"),
            P(None, "fsdp"),
            P(None, "tp", "fsdp"),
            P("tp", "fsdp"),
            P(None, "tp"),
            P(None, "fsdp"),
            P(None, "tp"),
            P("tp"),
            P("fsdp"),
            P("fsdp"),
            P("tp"),
            P("tp"),
            P("fsdp"),
            P(None, "fsdp"),
            P(None, "tp", "fsdp"),
            P("tp", "fsdp"),
            P(None, "tp"),
        ),
        out_specs=(
            P("fsdp", "ctx", None, None),
            P("fsdp", "ctx", None, None),
            P(None, "fsdp", "tp"),
            P("tp", "fsdp"),
            P("fsdp", "tp"),
            P("tp", "fsdp"),
            P(None, "fsdp"),
            P(None, "tp", "fsdp"),
            P("tp", "fsdp"),
            P(None, "tp"),
            P(None, "fsdp", "tp"),
            P("tp", "fsdp"),
            P("fsdp", "tp"),
            P("tp", "fsdp"),
            P(None, "fsdp"),
            P(None, "tp", "fsdp"),
            P("tp", "fsdp"),
            P(None, "tp"),
            P(None, "fsdp", "tp"),
            P("tp", "fsdp"),
            P("fsdp", "tp"),
            P("tp", "fsdp"),
            P(None, "fsdp"),
            P(None, "tp"),
            P("tp"),
            P("fsdp"),
            P("fsdp"),
            P("tp"),
            P("tp"),
            P("fsdp"),
            P(None, "fsdp"),
            P(None, "tp", "fsdp"),
            P("tp", "fsdp"),
            P(None, "tp"),
            P(),
        ),
        check_vma=False,
    )
```

```python
import functools

import jax
import jax.numpy as jnp
from jax import lax
from jax.experimental import pallas as pl
from jax.experimental.pallas import tpu as pltpu
from jax.sharding import PartitionSpec as P


D = 768
HEADS = 24
HD = 32
FF = 3072
WIN = 12
SHIFT = 6
RELP = 529


DECAY_RATE = 0.5
STAT_EPS = 1e-06
NORM_EPS = 1e-05
MASK_FILL = -100.0
STEP_RATE = 1.0
CLIP_LEVEL = 0.25


def passed_along(x, axis, by):
    count = lax.axis_size(axis)
    return lax.ppermute(x, axis, [(i, (i + by) % count) for i in range(count)])


def layer_norm(values, gain_row, offset):
    mean_val = jnp.mean(values, axis=-1, keepdims=True)
    centred = values - mean_val
    var_val = jnp.mean(centred * centred, axis=-1, keepdims=True)
    return centred * lax.rsqrt(var_val + NORM_EPS) * gain_row + offset


def exact_gelu(values):
    return jax.nn.gelu(values, approximate=False)


def to_windows(values):
    image_count, row_count, col_count, channels = values.shape
    pieces = values.reshape(image_count, row_count // WIN, WIN, col_count // WIN, WIN, channels)
    return pieces.transpose(0, 1, 3, 2, 4, 5).reshape(-1, WIN * WIN, channels)


def from_windows(values, image_count, row_count, col_count):
    channels = values.shape[-1]
    pieces = values.reshape(image_count, row_count // WIN, col_count // WIN, WIN, WIN, channels)
    return pieces.transpose(0, 1, 3, 2, 4, 5).reshape(image_count, row_count, col_count, channels)


def enter_frame(own_rows, received):
    joined = jnp.concatenate([own_rows[:, SHIFT:], received], axis=1)
    return jnp.roll(joined, -SHIFT, axis=2)


def project_heads(normed_low, weights_qkv, bias_query, bias_value, head_shape):
    query_full = (
        jnp.dot(normed_low, weights_qkv[0], preferred_element_type=jnp.float32) + bias_query
    )
    key_full = jnp.dot(normed_low, weights_qkv[1], preferred_element_type=jnp.float32)
    value_full = (
        jnp.dot(normed_low, weights_qkv[2], preferred_element_type=jnp.float32) + bias_value
    )
    return tuple(
        (
            member.astype(jnp.bfloat16).reshape(head_shape)
            for member in (query_full, key_full, value_full)
        )
    )


def attention_scores(query_low, key_low, pos_bias, mask_add):
    products = jnp.einsum("wihc,wjhc->whij", query_low, key_low, preferred_element_type=jnp.float32)
    return products * query_low.shape[-1] ** (-0.5) + pos_bias[None] + mask_add[:, None]


def table_lookup(table_low, rel_index):
    win_tokens = rel_index.shape[0]
    code_ids = jnp.arange(table_low.shape[0], dtype=jnp.int32)
    index_blocks = rel_index.reshape(WIN, -1)

    def lookup(index_block):
        one_hot = (index_block[:, None] == code_ids[None, :]).astype(jnp.bfloat16)
        return jnp.dot(one_hot, table_low, preferred_element_type=jnp.float32)

    looked = lax.map(lookup, index_blocks)
    return looked.reshape(win_tokens, win_tokens, -1).transpose(2, 0, 1)


def table_grad(d_pos, rel_index, table_rows):
    heads_here = d_pos.shape[0]
    code_ids = jnp.arange(table_rows, dtype=jnp.int32)
    index_blocks = rel_index.reshape(WIN, -1)
    grad_blocks = d_pos.transpose(1, 2, 0).reshape(WIN, -1, heads_here)

    def accumulate(running, member):
        index_block, grad_block = member
        one_hot = (index_block[:, None] == code_ids[None, :]).astype(jnp.float32)
        added = lax.dot_general(
            one_hot,
            grad_block,
            (((0,), (0,)), ((), ())),
            precision=lax.Precision.HIGHEST,
            preferred_element_type=jnp.float32,
        )
        return (running + added, None)

    result_pair = lax.scan(
        accumulate, jnp.zeros((table_rows, heads_here), jnp.float32), (index_blocks, grad_blocks)
    )
    return result_pair[0]


def place(part_vec, index_at, whole_len):
    size_of = part_vec.shape[-1]
    base = jnp.zeros(part_vec.shape[:-1] + (whole_len,), jnp.float32)
    return lax.dynamic_update_slice_in_dim(base, part_vec, index_at * size_of, part_vec.ndim - 1)


def own_part(whole_vec, index_at, size_of):
    return lax.dynamic_slice_in_dim(whole_vec, index_at * size_of, size_of, whole_vec.ndim - 1)


def factored(grad, row_local, col_local, row_mean):
    return grad * lax.rsqrt(row_local[..., :, None] * col_local[..., None, :] / row_mean)


def plain_stats(grad, state_old):
    state_new = DECAY_RATE * state_old + (1.0 - DECAY_RATE) * (grad * grad + STAT_EPS)
    return (state_new, grad * lax.rsqrt(state_new))


def shard_sum(grad_list):
    return (
        lax.psum_scatter(grad_list[0], "fsdp", scatter_dimension=1, tiled=True),
        lax.psum_scatter(grad_list[1], "fsdp", scatter_dimension=1, tiled=True),
        lax.psum_scatter(grad_list[2], "fsdp", scatter_dimension=0, tiled=True),
        lax.psum_scatter(grad_list[3], "fsdp", scatter_dimension=1, tiled=True),
        lax.psum_scatter(grad_list[4], "fsdp", scatter_dimension=1, tiled=True),
        lax.psum_scatter(grad_list[5], "fsdp", scatter_dimension=2, tiled=True),
        lax.psum_scatter(grad_list[6], "fsdp", scatter_dimension=1, tiled=True),
    )


def band_sum(grad_list):
    return lax.psum(
        (
            grad_list[0],
            grad_list[1],
            grad_list[2],
            grad_list[3],
            grad_list[4],
            grad_list[5],
            grad_list[6],
        ),
        "ctx",
    )


BF = jnp.bfloat16
F32 = jnp.float32
MESH = pl.DeviceIdType.MESH
TOK = WIN * WIN
HALF = D // 2
VMEM_LIMIT = 66_000_000


def dot(a, b):
    return lax.dot_general(a, b, (((1,), (0,)), ((), ())), preferred_element_type=F32)


def dot_t(a, b):
    return lax.dot_general(a, b, (((1,), (1,)), ((), ())), preferred_element_type=F32)


def t_dot(a, b):
    return lax.dot_general(a, b, (((0,), (0,)), ((), ())), preferred_element_type=F32)


def row_mean(x):
    return jnp.sum(x, axis=-1, keepdims=True) * (1.0 / x.shape[-1])


def remote(src, dst, send, recv, where):
    return pltpu.make_async_remote_copy(
        src_ref=src, dst_ref=dst, send_sem=send, recv_sem=recv, device_id=where, device_id_type=MESH
    )


def greet(barrier, places):
    for place_of in places:
        pl.semaphore_signal(barrier, inc=1, device_id=place_of, device_id_type=MESH)


class LineSum:
    def __init__(self, part, send, from_outer, from_mid, total, sems):
        self.part, self.send, self.from_outer, self.from_mid, self.total = (
            part, send, from_outer, from_mid, total,
        )
        self.s_out, self.r_out, self.s_mid, self.r_mid, self.s_tot, self.r_tot, self.s_cross = sems
        z = lax.axis_index("tp")
        self.is_mid = jnp.logical_and(z > 0, z < 3)
        self.is_outer = jnp.logical_not(self.is_mid)
        self.outer = jnp.where(z < 2, 0, 3)
        self.mid = jnp.where(z < 2, 1, 2)
        self.other_mid = 3 - self.mid
        self.own = self.mid - 1
        self.other = 1 - self.own

    @staticmethod
    def scratch(count):
        return [
            pltpu.VMEM((count, 2, TOK, HALF), BF),
            pltpu.VMEM((count, 2, TOK, HALF), BF),
            pltpu.VMEM((count, TOK, HALF), BF),
            pltpu.SemaphoreType.DMA((count, 2)),
            pltpu.SemaphoreType.DMA((count, 2)),
            pltpu.SemaphoreType.DMA((count,)),
            pltpu.SemaphoreType.DMA((count,)),
            pltpu.SemaphoreType.DMA((count, 2)),
            pltpu.SemaphoreType.DMA((count, 2)),
            pltpu.SemaphoreType.DMA((count,)),
        ]

    @staticmethod
    def build(part, refs, total):
        return LineSum(part, refs[0], refs[1], refs[2], total, refs[3:10])

    @staticmethod
    def peers():
        return 2

    def greet(self, barrier):
        pl.semaphore_signal(
            barrier, inc=1, device_id={"tp": jnp.where(self.is_mid, self.outer, self.mid)},
            device_id_type=MESH,
        )

        @pl.when(self.is_mid)
        def _():
            pl.semaphore_signal(
                barrier, inc=1, device_id={"tp": self.other_mid}, device_id_type=MESH
            )

    def greet_count(self):
        return jnp.where(self.is_mid, 2, 1)

    def _to_mid(self, w, h):
        return remote(self.send.at[w, h], self.from_outer.at[w, h], self.s_out.at[w, h],
                      self.r_out.at[w, h], {"tp": self.mid})

    def _across(self, w):
        return remote(self.send.at[w, self.other], self.from_mid.at[w], self.s_mid.at[w],
                      self.r_mid.at[w], {"tp": self.other_mid})

    def _total_across(self, w, h):
        return remote(self.total.at[w, h], self.total.at[w, h], self.s_cross.at[w],
                      self.r_tot.at[w, h], {"tp": self.other_mid})

    def _total_out(self, w, h):
        return remote(self.total.at[w, h], self.total.at[w, h], self.s_tot.at[w, h],
                      self.r_tot.at[w, h], {"tp": self.outer})

    def put(self, w, value):
        self.part[w, 0] = value[:, :HALF]
        self.part[w, 1] = value[:, HALF:]

    def start(self, w):
        @pl.when(self.is_outer)
        def _():
            self.send[w, self.other] = self.part[w, self.other].astype(BF)
            self._to_mid(w, self.other).start()
            self.send[w, self.own] = self.part[w, self.own].astype(BF)
            self._to_mid(w, self.own).start()

    def cross(self, w):
        @pl.when(self.is_mid)
        def _():
            self._to_mid(w, self.other).wait_recv()
            self.send[w, self.other] = (
                self.part[w, self.other] + self.from_outer[w, self.other].astype(F32)
            ).astype(BF)
            self._across(w).start()

    def settle(self, w):
        @pl.when(self.is_mid)
        def _():
            self._to_mid(w, self.own).wait_recv()
            self._across(w).wait_recv()
            self.total[w, self.own] = (
                self.part[w, self.own]
                + self.from_outer[w, self.own].astype(F32)
                + self.from_mid[w].astype(F32)
            ).astype(BF)
            self._total_across(w, self.own).start()
            self._total_out(w, self.own).start()

    def hand(self, w):
        @pl.when(self.is_mid)
        def _():
            self._total_across(w, self.other).wait_recv()
            self._total_out(w, self.other).start()

    def arrive(self, w):
        @pl.when(self.is_outer)
        def _():
            self._total_out(w, 0).wait_recv()
            self._total_out(w, 1).wait_recv()

    def drain(self, w):
        @pl.when(self.is_outer)
        def _():
            self._to_mid(w, 0).wait_send()
            self._to_mid(w, 1).wait_send()

        @pl.when(self.is_mid)
        def _():
            self._across(w).wait_send()
            self._total_across(w, self.own).wait_send()
            self._total_out(w, 0).wait_send()
            self._total_out(w, 1).wait_send()


class ShardSum:
    def __init__(self, block_of, out, refs):
        self.block_of, self.out = block_of, out
        self.snd1, self.rcv1, self.snd2, self.rcv2, self.snd3, self.rcv3, self.s, self.r = refs
        f = lax.axis_index("fsdp")
        core = lax.rem(f, 2)
        self.f, self.core = f, core
        self.near, self.far = f + 1 - 2 * core, lax.rem(f + 2, 4)
        self.ctx = 1 - lax.axis_index("ctx")

    @staticmethod
    def scratch(shape):
        return [
            pltpu.VMEM((2, *shape), BF), pltpu.VMEM((2, *shape), BF),
            pltpu.VMEM(shape, BF), pltpu.VMEM(shape, BF),
            pltpu.VMEM(shape, BF), pltpu.VMEM(shape, BF),
            pltpu.SemaphoreType.DMA((4,)), pltpu.SemaphoreType.DMA((4,)),
        ]

    def _near(self, x):
        return remote(self.snd1.at[x], self.rcv1.at[x], self.s.at[x], self.r.at[x], {"fsdp": self.near})

    def _far(self):
        return remote(self.snd2, self.rcv2, self.s.at[2], self.r.at[2], {"fsdp": self.far})

    def _ctx(self):
        return remote(self.snd3, self.rcv3, self.s.at[3], self.r.at[3], {"ctx": self.ctx})

    def start(self):
        for x in range(2):
            self.snd1[x] = self.block_of(2 * x + 1 - self.core).astype(BF)
            self._near(x).start()

    def pair(self):
        for x in range(2):
            self._near(x).wait_recv()
        other = lax.div(self.far, 2)
        self.snd2[...] = (self.block_of(self.far) + self.rcv1[other].astype(F32)).astype(BF)
        self._far().start()

    def cross(self):
        self._far().wait_recv()
        mine = lax.div(self.f, 2)
        self.snd3[...] = (
            self.block_of(self.f) + self.rcv1[mine].astype(F32) + self.rcv2[...].astype(F32)
        ).astype(BF)
        self._ctx().start()

    def finish(self):
        self._ctx().wait_recv()
        self.out[...] = self.snd3[...].astype(F32) + self.rcv3[...].astype(F32)

    def drain(self):
        for x in range(2):
            self._near(x).wait_send()
        self._far().wait_send()
        self._ctx().wait_send()


def vmem_call(body, outs, scratch, name, collective_id):
    remote_kernel = {} if collective_id is None else dict(
        collective_id=collective_id, has_side_effects=True
    )

    def call(*args):
        return pl.pallas_call(
            body,
            out_shape=[jax.ShapeDtypeStruct(s, t) for s, t in outs],
            in_specs=[pl.BlockSpec(memory_space=pltpu.VMEM)] * len(args),
            out_specs=[pl.BlockSpec(memory_space=pltpu.VMEM)] * len(outs),
            scratch_shapes=scratch,
            compiler_params=pltpu.CompilerParams(vmem_limit_bytes=VMEM_LIMIT, **remote_kernel),
            name=name,
        )(*args)

    return call


def take(refs, counts):
    groups, at = [], 0
    for n in counts:
        groups.append(refs[at : at + n])
        at += n
    return groups


def window_rows(row_of, row_tmp, image, dst):
    for r in range(WIN):
        row_tmp[...] = row_of(image, r).astype(F32)
        dst[2 * image, r * WIN : (r + 1) * WIN, :] = row_tmp[SHIFT : SHIFT + WIN, :]
        dst[2 * image + 1, r * WIN : r * WIN + SHIFT, :] = row_tmp[SHIFT + WIN :, :]
        dst[2 * image + 1, r * WIN + SHIFT : (r + 1) * WIN, :] = row_tmp[:SHIFT, :]


def home_row(delta, row_tmp, image, r):
    row_tmp[SHIFT : SHIFT + WIN, :] = delta[2 * image, r * WIN : (r + 1) * WIN, :]
    row_tmp[SHIFT + WIN :, :] = delta[2 * image + 1, r * WIN : r * WIN + SHIFT, :]
    row_tmp[:SHIFT, :] = delta[2 * image + 1, r * WIN + SHIFT : (r + 1) * WIN, :]
    return row_tmp[...].astype(BF)


class HomeRows:
    def __init__(self, delta, row_tmp, out, halo, send, recv):
        self.delta, self.row_tmp, self.out, self.halo, self.s, self.r = (
            delta, row_tmp, out, halo, send, recv,
        )

    def _copy(self, i):
        return remote(self.halo.at[i], self.out.at[i, 0:SHIFT], self.s.at[i], self.r.at[i],
                      {"ctx": 1 - lax.axis_index("ctx")})

    def go(self, i):
        for r in range(SHIFT, WIN):
            self.halo[i, r - SHIFT] = home_row(self.delta, self.row_tmp, i, r)
        self._copy(i).start()
        for r in range(SHIFT):
            self.out[i, SHIFT + r] = home_row(self.delta, self.row_tmp, i, r)

    def wait(self, i):
        self._copy(i).wait_recv()
        self._copy(i).wait_send()


class TableSum:
    def __init__(self, part, refs):
        self.part = part
        self.snd1, self.rcv1, self.snd2, self.rcv2, self.snd3, self.rcv3, self.s, self.r = refs
        f = lax.axis_index("fsdp")
        self.core, self.x, self.c = lax.rem(f, 2), lax.div(f, 2), lax.axis_index("ctx")
        self.near, self.far = f + 1 - 2 * self.core, lax.rem(f + 2, 4)

    @staticmethod
    def scratch(heads):
        shapes = [(heads, 2, 2, 24, 256)] * 2 + [(heads, 2, 24, 256)] * 2 + [(heads, 24, 256)] * 2
        return [*[pltpu.VMEM(s, BF) for s in shapes], pltpu.SemaphoreType.DMA((3,)),
                pltpu.SemaphoreType.DMA((3,))]

    def _copy(self, n):
        src, dst = ((self.snd1, self.rcv1), (self.snd2, self.rcv2), (self.snd3, self.rcv3))[n]
        where = ({"fsdp": self.near}, {"fsdp": self.far}, {"ctx": 1 - self.c})[n]
        return remote(src, dst, self.s.at[n], self.r.at[n], where)

    def rows(self, core, x, c):
        return pl.ds(pl.multiple_of(core * 96 + x * 48 + c * 24, 8), 24)

    def start(self):
        for x in range(2):
            for c in range(2):
                self.snd1[:, x, c] = self.part[:, self.rows(1 - self.core, x, c), :].astype(BF)
        self._copy(0).start()

    def pair(self):
        self._copy(0).wait_recv()
        x = 1 - self.x
        for c in range(2):
            self.snd2[:, c] = (
                self.part[:, self.rows(self.core, x, c), :] + self.rcv1[:, x, c].astype(F32)
            ).astype(BF)
        self._copy(1).start()

    def cross(self):
        self._copy(1).wait_recv()
        c = 1 - self.c
        self.snd3[...] = (
            self.part[:, self.rows(self.core, self.x, c), :] + self.rcv1[:, self.x, c].astype(F32)
            + self.rcv2[:, c].astype(F32)
        ).astype(BF)
        self._copy(2).start()

    def finish(self, out):
        self._copy(2).wait_recv()
        out[...] = (
            self.part[:, self.rows(self.core, self.x, self.c), :]
            + self.rcv1[:, self.x, self.c].astype(F32)
            + self.rcv2[:, self.c].astype(F32) + self.rcv3[...].astype(F32)
        )

    def first_row(self):
        return self.core * 96 + self.x * 48 + self.c * 24

    def drain(self):
        for n in range(3):
            self._copy(n).wait_send()


def main_body(*refs):
    (
        (feat, og, wq_m, wp_m, wu_m, wd_m, small_m, table_t, ridx, regr, regc),
        (gin_o, gq_o, gp_o, small_o, gu_o, gd_o, rows, br, mix_o),
        (sm_g, wq, wp_g, wp, wu, wd, fh, gh, bias_s, row_tmp, xw, ogw, n1, q, k, v, probs, ctx, part),
        (n2_s, hid_s, dpl_s, ol_s, xhat_s, rstd_s, tot_two, gu, gd, dft, dbr),
        (dh_s, dpos_s, chunk_s, halo_s, tot_one),
        ls_one, ls_two, ls_four, up_refs, down_refs, table_refs,
        (w_send, w_recv, h_send, h_recv, o_send, o_recv),
    ) = take(refs, (11, 9, 19, 11, 5, 10, 10, 10, 8, 8, 8, 6))
    windows, heads = probs.shape[0], probs.shape[1]
    images = windows // 2
    width = q.shape[2]
    shard = wq_m.shape[1]
    f, c = lax.axis_index("fsdp"), lax.axis_index("ctx")
    near, far = f + 1 - 2 * lax.rem(f, 2), lax.rem(f + 2, 4)
    one = LineSum.build(part, ls_one, br)
    two = LineSum.build(part, ls_two, tot_two)
    four = LineSum.build(part, ls_four, tot_one)

    def block(at):
        return pl.ds(pl.multiple_of(at * shard, shard), shard)

    up = ShardSum(lambda at: gu[block(at), :], gu_o, up_refs)
    down = ShardSum(lambda at: gd[block(at), :], gd_o, down_refs)
    table = TableSum(dpos_s, table_refs)
    barrier = pltpu.get_barrier_semaphore()
    greet(barrier, [{"fsdp": near}, {"fsdp": far}, {"ctx": 1 - c}])
    one.greet(barrier)
    wq[:, block(f), :] = wq_m[...].astype(BF)
    sm_g[f] = small_m[...].astype(BF)
    wp_g[f] = wp_m[...].astype(BF)
    wu[block(f), :] = wu_m[...].astype(BF)
    wd[block(f), :] = wd_m[...].astype(BF)
    pl.semaphore_wait(barrier, 3 + one.greet_count())

    items = [
        lambda at: sm_g.at[at],
        lambda at: wq.at[:, block(at), :],
        lambda at: wp_g.at[at],
        lambda at: wu.at[block(at), :],
        lambda at: wd.at[block(at), :],
    ]

    def copy_of(n, kind, at, where):
        ref = items[n](at)
        return remote(ref, ref, w_send.at[n, kind], w_recv.at[n, kind], {"fsdp": where})

    halo_f = [
        remote(feat.at[i, 0:SHIFT], fh.at[i], h_send.at[i], h_recv.at[i], {"ctx": 1 - c})
        for i in range(images)
    ]
    halo_g = [
        remote(og.at[i, 0:SHIFT], gh.at[i], h_send.at[images + i], h_recv.at[images + i], {"ctx": 1 - c})
        for i in range(images)
    ]
    for copy in halo_f:
        copy.start()
    for n in range(len(items)):
        copy_of(n, 0, f, far).start()
        copy_of(n, 1, f, near).start()
    for copy in halo_g:
        copy.start()

    def relay(n):
        copy_of(n, 0, f, far).wait_recv()
        copy_of(n, 2, far, near).start()

    def gathered(n):
        copy_of(n, 1, f, near).wait_recv()
        copy_of(n, 2, far, near).wait_recv()

    relay(0)

    table_low = table_t[...].astype(BF).astype(F32)

    def bias_rows(step, carry):
        rows_at = pl.ds(pl.multiple_of(step * 8, 8), 8)
        for half in range(2):
            lanes_at = slice(half * 128, (half + 1) * 128)
            idx = ridx[rows_at, lanes_at]
            low = jnp.bitwise_and(idx, 127)
            high = jnp.right_shift(idx, 7)
            picks = [high == n for n in range(5)]
            for h in range(heads):
                found = jnp.zeros((8, 128), F32)
                for n in range(5):
                    tab = jnp.broadcast_to(
                        table_low[h : h + 1, n * 128 : (n + 1) * 128], (8, 128)
                    )
                    got = jnp.take_along_axis(tab, low, axis=1, mode="promise_in_bounds")
                    found = jnp.where(picks[n], got, found)
                bias_s[h, rows_at, lanes_at] = found
        return carry

    lax.fori_loop(0, TOK // 8, bias_rows, 0)
    gathered(0)
    lanes = rows.shape[1]
    rows[...] = jnp.concatenate([sm_g[n].astype(F32) for n in range(4)], axis=1)
    unit = lax.broadcasted_iota(jnp.int32, (shard, lanes), 0)
    lane = lax.broadcasted_iota(jnp.int32, (shard, lanes), 1)
    biases = jnp.zeros((16, lanes), F32)
    for n in range(4):
        same = jnp.logical_and(
            jnp.right_shift(lane, 5) == jnp.right_shift(unit, 3),
            jnp.bitwise_and(lane, 31) == jnp.bitwise_and(unit, 7) + n * 8,
        )
        biases = biases + dot(sm_g[n], jnp.where(same, 1.0, 0.0).astype(BF))
    rows[8:16, :] = biases[8:16, :]
    dpos_s[...] = jnp.zeros_like(dpos_s)
    small_o[...] = jnp.zeros_like(small_o)
    for i in range(images):
        halo_f[i].wait_recv()
        window_rows(
            lambda im, r: feat[im, SHIFT + r] if r < SHIFT else fh[im, r - SHIFT], row_tmp, i, xw
        )
    relay(1)
    gain_one, offset_one = rows[0:1, :], rows[1:2, :]
    bias_proj, gain_two, offset_two = rows[2:3, :], rows[3:4, :], rows[4:5, :]
    bias_hidden = rows[8:9, :]
    bias_q, bias_v = rows[9:10, :width], rows[10:11, :width]
    head_of = jnp.right_shift(lax.broadcasted_iota(jnp.int32, (1, width), 1), 5)
    picks_of = [jnp.where(head_of == h, 1.0, 0.0).astype(BF) for h in range(heads)]
    gathered(1)
    relay(2)
    gathered(2)
    wp[...] = jnp.concatenate([wp_g[n] for n in range(4)], axis=1)

    def spot(w):
        return pl.ds(pl.multiple_of(w * TOK, TOK), TOK)

    def add_rows(n, term):
        small_o[n : n + 1, : term.shape[1]] = small_o[n : n + 1, : term.shape[1]] + jnp.sum(
            term, axis=0, keepdims=True
        )

    def serve(w, line, before):
        @pl.when(w == 0)
        def _():
            if before is not None:
                before.cross(windows - 1)
                before.settle(windows - 1)
                before.hand(windows - 2)

        @pl.when(w == 1)
        def _():
            if before is not None:
                before.hand(windows - 1)

        @pl.when(w >= 1)
        def _():
            line.cross(w - 1)
            line.settle(w - 1)

        @pl.when(w >= 2)
        def _():
            line.hand(w - 2)

    def forward(w, carry):
        x = xw[w]
        centred = x - row_mean(x)
        xhat = centred * lax.rsqrt(row_mean(centred * centred) + NORM_EPS)
        normed = (xhat * gain_one + offset_one).astype(BF)
        n1[spot(w), :] = normed
        q_w = (dot(normed, wq[0]) + bias_q).astype(BF)
        k_w = dot(normed, wq[1]).astype(BF)
        v_w = (dot(normed, wq[2]) + bias_v).astype(BF)
        q[w] = q_w
        k[w] = k_w
        v[w] = v_w
        mask = jnp.where(regc[w] == regr[w], 0.0, MASK_FILL)
        context = jnp.zeros((TOK, width), F32)
        for h in range(heads):
            scores = dot_t(q_w * picks_of[h], k_w) * HD ** (-0.5) + bias_s[h, :, :TOK] + mask
            lifted = jnp.exp(scores - jnp.max(scores, axis=-1, keepdims=True))
            p = lifted / jnp.sum(lifted, axis=-1, keepdims=True)
            probs[w, h] = p
            context = context + dot(p.astype(BF), v_w * picks_of[h])
        low = context.astype(BF)
        ctx[spot(w), :] = low
        one.put(w, dot(low, wp[...]))
        one.start(w)
        serve(w, one, None)
        return carry

    lax.fori_loop(0, windows, forward, 0)
    relay(3)
    relay(4)
    gathered(3)
    gathered(4)

    def middle(w, carry):
        one.arrive(w)
        resid = xw[w] + (jnp.concatenate([br[w, 0], br[w, 1]], axis=1).astype(F32) + bias_proj)
        centred = resid - row_mean(resid)
        rstd = lax.rsqrt(row_mean(centred * centred) + NORM_EPS)
        xhat = centred * rstd
        xhat_s[w] = xhat
        rstd_s[w] = jnp.broadcast_to(rstd, (TOK, 128))
        normed = (xhat * gain_two + offset_two).astype(BF)
        n2_s[spot(w), :] = normed
        pre = dot(normed, wu[...]) + bias_hidden
        cdf = 0.5 * (1.0 + lax.erf(pre * 0.7071067811865476))
        slope = cdf + pre * (jnp.exp(-0.5 * (pre * pre)) * 0.3989422804014327)
        hid = (pre * cdf).astype(BF)
        hid_s[spot(w), :] = hid

        @pl.when(w % 2 == 0)
        def _():
            i = w // 2
            for n in range(images):

                @pl.when(i == n)
                def _():
                    halo_g[n].wait_recv()
                    window_rows(
                        lambda im, r: og[im, SHIFT + r] if r < SHIFT else gh[im, r - SHIFT],
                        row_tmp, n, ogw,
                    )

        low = ogw[w].astype(BF)
        ol_s[spot(w), :] = low
        d_pre = dot(low, wd[...]) * slope
        add_rows(6, d_pre)
        dpl = d_pre.astype(BF)
        dpl_s[spot(w), :] = dpl
        two.put(w, dot_t(dpl, wu[...]))
        two.start(w)
        mixed = dot_t(hid, wd[...])
        mix_o[w, 0] = mixed[:, :HALF]
        mix_o[w, 1] = mixed[:, HALF:]
        serve(w, two, one)
        return carry

    lax.fori_loop(0, windows, middle, 0)

    def grad_chunk(m, carry):
        chunk = pl.ds(pl.multiple_of(m * 256, 256), 256)
        gd[chunk, :] = t_dot(ol_s[:, chunk], hid_s[...])
        gu[chunk, :] = t_dot(n2_s[:, chunk], dpl_s[...])
        return carry

    lax.fori_loop(0, D // 256, grad_chunk, 0)
    down.start()
    up.start()

    def backward(w, carry):
        two.arrive(w)
        d_two = jnp.concatenate([tot_two[w, 0], tot_two[w, 1]], axis=1).astype(F32)
        xhat = xhat_s[w]
        e = d_two * gain_two
        d_flat = (e - row_mean(e) - xhat * row_mean(e * xhat)) * rstd_s[w, :, 0:1]
        og_w = ogw[w]
        d_resid = og_w + d_flat
        dft[w] = d_flat
        d_branch = d_resid.astype(BF)
        dbr[spot(w), :] = d_branch
        for n, term in ((2, d_resid), (3, d_two * xhat), (4, d_two), (5, og_w)):
            add_rows(n, term)
        d_ctx = dot_t(d_branch, wp[...]).astype(BF)
        q_w, k_w, v_w = q[w], k[w], v[w]
        d_q = jnp.zeros((TOK, width), F32)
        d_k = jnp.zeros((TOK, width), F32)
        d_v = jnp.zeros((TOK, width), F32)
        for h in range(heads):
            d_ctx_h = d_ctx * picks_of[h]
            p = probs[w, h]
            d_p = dot_t(d_ctx_h, v_w)
            d_v = d_v + t_dot(p.astype(BF), d_ctx_h)
            d_s = p * (d_p - jnp.sum(p * d_p, axis=-1, keepdims=True))
            dpos_s[h, :TOK, :TOK] = dpos_s[h, :TOK, :TOK] + d_s
            d_l = (d_s * HD ** (-0.5)).astype(BF)
            d_q = d_q + dot(d_l, k_w * picks_of[h])
            d_k = d_k + t_dot(d_l, q_w * picks_of[h])
        partial = jnp.zeros((TOK, D), F32)
        for n, d_n in enumerate((d_q, d_k, d_v)):
            low = d_n.astype(BF)
            dh_s[n, spot(w), :] = low
            partial = partial + dot_t(low, wq[n])
            if n != 1:
                add_rows(8 + n // 2, low.astype(F32))
        four.put(w, partial)
        four.start(w)
        serve(w, four, two)

        @pl.when(w == 1)
        def _():
            down.pair()
            up.pair()

        @pl.when(w == windows - 1)
        def _():
            down.cross()
            up.cross()

        return carry

    lax.fori_loop(0, windows, backward, 0)
    table.start()
    for n in range(3):
        gq_o[n] = t_dot(n1[...], dh_s[n])
    four.cross(windows - 1)
    table.pair()
    gp = t_dot(ctx[...], dbr[...])
    for n in range(4):
        gp_o[n] = gp[:, n * shard : (n + 1) * shard]
    four.hand(windows - 2)
    four.settle(windows - 1)
    table.cross()

    home = HomeRows(xhat_s, row_tmp, gin_o, halo_s, o_send, o_recv)

    def back(w):
        four.arrive(w)
        x = xw[w]
        centred = x - row_mean(x)
        rstd = lax.rsqrt(row_mean(centred * centred) + NORM_EPS)
        xhat = centred * rstd
        d_one = jnp.concatenate([tot_one[w, 0], tot_one[w, 1]], axis=1).astype(F32)
        e = d_one * gain_one
        xhat_s[w] = dft[w] + (e - row_mean(e) - xhat * row_mean(e * xhat)) * rstd
        for n, term in ((0, d_one * xhat), (1, d_one)):
            add_rows(n, term)

    back(0)
    back(1)
    home.go(0)
    table.finish(chunk_s)
    first = table.first_row()
    ident = lax.broadcasted_iota(jnp.int32, (640, TOK), 0)

    def bin_row(i, acc):
        hot = jnp.where(ident == ridx[pl.ds(first + i, 1), :TOK], 1.0, 0.0).astype(BF)
        vals = jnp.concatenate(
            [chunk_s[h, pl.ds(i, 1), :TOK] for h in range(heads)] + [jnp.zeros((8 - heads, TOK), F32)],
            axis=0,
        )
        high = vals.astype(BF)
        low = (vals - high.astype(F32)).astype(BF)
        return acc + dot_t(jnp.concatenate([high, low], axis=0), hot)

    hist = lax.fori_loop(0, 24, bin_row, jnp.zeros((16, 640), F32))
    small_o[16:24, :640] = hist[0:8] + hist[8:16]
    four.hand(windows - 1)
    down.finish()
    up.finish()
    back(2)
    back(3)
    home.go(1)
    for i in range(images):
        home.wait(i)
    for w in range(windows):
        for line in (one, two, four):
            line.drain(w)
    for copy in halo_f + halo_g:
        copy.wait_send()
    for n in range(len(items)):
        copy_of(n, 0, f, far).wait_send()
        copy_of(n, 1, f, near).wait_send()
        copy_of(n, 2, far, near).wait_send()
    up.drain()
    down.drain()
    table.drain()


def forward_backward(features, out_grad, regions, rel_index, w_qkv, w_proj, w_up, w_down_t,
                     norm_vecs, head_bias, hidden_bias, rel_table):
    images = features.shape[0]
    windows = 2 * images
    shard, width = w_qkv.shape[1], w_qkv.shape[2]
    hidden = w_up.shape[1]
    heads = width // HD
    small = jnp.concatenate(
        [
            norm_vecs,
            jnp.zeros((2, shard), F32),
            hidden_bias.reshape(1, shard),
            jnp.pad(head_bias.reshape(2, -1), ((0, 5), (0, shard - head_bias[0].size))),
        ],
        axis=0,
    )
    table_t = jnp.pad(
        rel_table.T, ((0, 8 - heads), (0, 640 - rel_table.shape[0]))
    )
    ridx = jnp.pad(rel_index, ((0, 192 - TOK), (0, 256 - TOK)))
    region_win = to_windows(regions[..., None])[..., 0]
    halves = (windows, 2, TOK, HALF)
    outs = [
        (features.shape, BF), ((3, D, width), F32), ((4, width, shard), F32), ((24, D), F32),
        ((shard, hidden), F32), ((shard, hidden), F32), ((16, D), F32), (halves, BF), (halves, F32),
    ]
    vm = pltpu.VMEM
    flat = windows * TOK
    scratch = [
        vm((4, 16, shard), BF), vm((3, D, width), BF), vm((4, width, shard), BF), vm((width, D), BF),
        vm((D, hidden), BF), vm((D, hidden), BF), vm((images, SHIFT, 24, D), BF),
        vm((images, SHIFT, 24, D), F32), vm((heads, TOK, 256), F32), vm((24, D), F32),
        vm((windows, TOK, D), F32), vm((windows, TOK, D), F32), vm((flat, D), BF),
        vm((windows, TOK, width), BF), vm((windows, TOK, width), BF), vm((windows, TOK, width), BF),
        vm((windows, heads, TOK, TOK), F32), vm((flat, width), BF), vm(halves, F32),
        vm((flat, D), BF), vm((flat, hidden), BF), vm((flat, hidden), BF), vm((flat, D), BF),
        vm((windows, TOK, D), F32), vm((windows, TOK, 128), F32), vm(halves, BF),
        vm((D, hidden), F32), vm((D, hidden), F32), vm((windows, TOK, D), F32), vm((flat, D), BF),
        vm((3, flat, width), BF), vm((heads, 192, 256), F32), vm((heads, 24, 256), F32),
        vm((images, SHIFT, 24, D), BF), vm(halves, BF),
        *LineSum.scratch(windows), *LineSum.scratch(windows), *LineSum.scratch(windows),
        *ShardSum.scratch((shard, hidden)), *ShardSum.scratch((shard, hidden)),
        *TableSum.scratch(heads),
        *[pltpu.SemaphoreType.DMA((5, 3))] * 2,
        *[pltpu.SemaphoreType.DMA((2 * images,))] * 2,
        *[pltpu.SemaphoreType.DMA((images,))] * 2,
    ]
    return vmem_call(main_body, outs, scratch, "forward_backward", 1)(
        features, out_grad, w_qkv, w_proj, w_up, w_down_t, small, table_t, ridx,
        region_win[:, None, :], region_win[:, :, None],
    )


def total_of(x):
    return jnp.sum(jnp.sum(x, axis=1, keepdims=True), axis=0, keepdims=True)


def exact(a, b, dims):
    return lax.dot_general(
        a, b, (dims, ((), ())), precision=lax.Precision.HIGHEST, preferred_element_type=F32
    )


def lane_sums(squares):
    return exact(jnp.ones((8, squares.shape[1]), F32), squares, ((1,), (1,)))[0:1]


def as_column(row):
    n = row.shape[1]
    step = 64
    eye = lax.broadcasted_iota(jnp.int32, (step, step), 0) == lax.broadcasted_iota(
        jnp.int32, (step, step), 1
    )
    return jnp.concatenate(
        [
            jnp.sum(
                jnp.where(eye, jnp.broadcast_to(row[:, at : at + step], (step, step)), 0.0),
                axis=1, keepdims=True,
            )
            for at in range(0, n, step)
        ],
        axis=0,
    )


def lane_pack(values):
    lane = lax.broadcasted_iota(jnp.int32, (8, 128), 1)
    packed = jnp.zeros((8, 128), F32)
    for n, value in enumerate(values):
        packed = packed + jnp.where(lane == n, jnp.broadcast_to(value, (8, 128)), 0.0)
    return packed


def wide(ref):
    if ref.shape[1] != 128:
        return ref[...]
    return jnp.concatenate([ref[n : n + 1, :] for n in range(ref.shape[0])], axis=1)


def put_wide(ref, row):
    if ref.shape[1] != 128:
        ref[...] = row
    else:
        for n in range(ref.shape[0]):
            ref[n : n + 1, :] = row[:, n * 128 : (n + 1) * 128]


def plain(grad, state):
    new = DECAY_RATE * state + (1.0 - DECAY_RATE) * (grad * grad + STAT_EPS)
    return new, grad * lax.rsqrt(new)


def optimizer_body(*refs):
    (
        (gq, gp, g_up, g_down, small, rows, br, mix),
        (w_qkv, w_proj, w_up, w_down, w_norm, w_heads, w_hidden, w_table),
        (row_qkv, col_qkv, row_proj, col_proj, row_up, col_up, row_down, col_down),
        (s_norm, s_heads, s_hidden, s_table),
        (home_o, gq_o, gp_o, gn_o, gh_o, gx_o, gt_o, uq_o, up_o, uu_o, ud_o),
        (rq_o, kq_o, rp_o, kp_o, ru_o, ku_o, rd_o, kd_o, size_o),
        qkv_refs, proj_refs, line_refs,
        (mixed, sm_s, sm_r, t_s, f_s, z_s, c_s, delta, row_tmp, halo_s),
        (sm_send, sm_recv, t_send, t_recv, f_send, f_recv, z_send, z_recv, c_send, c_recv,
         o_send, o_recv),
    ) = take(refs, (8, 8, 8, 4, 11, 9, 8, 8, 10, 10, 12))
    f, c, t = lax.axis_index("fsdp"), lax.axis_index("ctx"), lax.axis_index("tp")
    windows = br.shape[0]
    images = windows // 2
    shard, width = w_qkv.shape[1], w_qkv.shape[2]
    hidden = f_s.shape[2]
    ff = 4 * hidden
    heads = width // HD
    me = f * 4 + t
    first_f = jnp.where(f == 0, 1.0, 0.0)
    first_t = jnp.where(t == 0, 1.0, 0.0)

    def other(n):
        at = lax.rem(me + n, 16)
        return {"fsdp": lax.div(at, 4), "tp": lax.rem(at, 4)}

    barrier = pltpu.get_barrier_semaphore()
    greet(barrier, [{"ctx": 1 - c}] + [other(n) for n in range(1, 16)])
    qkv = ShardSum(
        lambda at: gq[:, pl.ds(pl.multiple_of(at * shard, shard), shard), :], gq_o, qkv_refs
    )
    proj = ShardSum(lambda at: gp[at], gp_o, proj_refs)
    line = LineSum.build(mix, line_refs, mixed)
    sm_s[0] = small[...]

    def swap(n):
        where = ({"fsdp": qkv.near}, {"fsdp": qkv.far}, {"ctx": 1 - c})[n]
        return remote(sm_s.at[n], sm_r.at[n], sm_send.at[n], sm_recv.at[n], where)

    pl.semaphore_wait(barrier, 16)
    swap(0).start()
    qkv.start()
    proj.start()
    for w in range(windows):
        line.start(w)

    keep = 1.0 - DECAY_RATE
    t_s[t] = jnp.zeros((8, shard), F32)
    f_s[f] = jnp.zeros((8, hidden), F32)
    sq_up = g_up[...] * g_up[...]
    sq_down = g_down[...] * g_down[...]
    t_s[t, 4:5, :] = lane_sums(sq_up)
    t_s[t, 5:6, :] = lane_sums(sq_down)
    f_s[f, 4:5, :] = jnp.sum(sq_up, axis=0, keepdims=True)
    f_s[f, 5:6, :] = jnp.sum(sq_down, axis=0, keepdims=True)
    tot_up, tot_down = total_of(sq_up), total_of(sq_down)

    qkv.pair()
    proj.pair()
    swap(0).wait_recv()
    sm_s[1] = sm_s[0] + sm_r[0]
    swap(1).start()
    line.cross(0)

    old_rows = [
        first_t * jnp.sum(row_qkv[0:1, :], axis=1, keepdims=True),
        first_t * jnp.sum(row_qkv[1:2, :], axis=1, keepdims=True),
        first_t * jnp.sum(row_qkv[2:3, :], axis=1, keepdims=True),
        first_f * total_of(row_proj[...]),
        first_t * total_of(row_up[...]),
        first_f * total_of(row_down[...]),
    ]
    masters = [
        sum(total_of(w_qkv[n] * w_qkv[n]) for n in range(3)),
        total_of(w_proj[...] * w_proj[...]),
        total_of(w_up[...] * w_up[...]),
        total_of(w_down[...] * w_down[...]),
        *[
            first_t * jnp.sum(w_norm[n : n + 1, :] * w_norm[n : n + 1, :], axis=1, keepdims=True)
            for n in range(6)
        ],
        *[total_of(w_heads[:, n, :] * w_heads[:, n, :]) for n in range(2)],
        total_of(w_hidden[...] * w_hidden[...]),
        first_f * total_of(w_table[...] * w_table[...]),
    ]
    line.settle(0)
    line.cross(1)
    qkv.cross()
    proj.cross()
    swap(1).wait_recv()
    sm_s[2] = sm_s[1] + sm_r[1]
    swap(2).start()
    line.hand(0)
    line.settle(1)
    line.cross(2)
    qkv.finish()
    proj.finish()

    tot_q = []
    for n in range(3):
        sq = gq_o[n] * gq_o[n]
        t_s[t, n : n + 1, :] = lane_sums(sq)
        f_s[f, n : n + 1, :width] = jnp.sum(sq, axis=0, keepdims=True)
        tot_q.append(total_of(sq))
    sq = gp_o[...] * gp_o[...]
    f_s[f, 3:4, :shard] = lane_sums(sq)
    t_s[t, 3:4, :] = jnp.sum(sq, axis=0, keepdims=True)
    z_s[me] = lane_pack([*tot_q, total_of(sq), tot_up, tot_down, *old_rows, *masters])

    def t_copy(n):
        return remote(t_s.at[t], t_s.at[t], t_send.at[n], t_recv.at[n], {"tp": lax.rem(t + n, 4)})

    def f_copy(n):
        return remote(f_s.at[f], f_s.at[f], f_send.at[n], f_recv.at[n], {"fsdp": lax.rem(f + n, 4)})

    def z_copy(n):
        return remote(z_s.at[me], z_s.at[me], z_send.at[n], z_recv.at[n], other(n))

    def c_copy(n):
        return remote(c_s.at[me], c_s.at[me], c_send.at[n], c_recv.at[n], other(n))

    for n in range(1, 4):
        t_copy(n).start()
        f_copy(n).start()
    for n in range(1, 16):
        z_copy(n).start()
    line.hand(1)
    line.settle(2)
    line.cross(3)

    swap(2).wait_recv()
    sm = sm_s[2] + sm_r[2]

    def own_lanes(x, size):
        out = x[:, :size]
        for n in range(1, 4):
            out = jnp.where(f == n, x[:, n * size : (n + 1) * size], out)
        return out

    part = HD // 4

    def own_units(row, count):
        lanes = count * HD
        lane = lax.broadcasted_iota(jnp.int32, (count, lanes), 1)
        unit = lax.broadcasted_iota(jnp.int32, (count, lanes), 0)
        only = jnp.where(
            jnp.right_shift(lane, 5) == unit, jnp.broadcast_to(row, (count, lanes)), 0.0
        )
        at = lax.broadcasted_iota(jnp.int32, (lanes, part), 0)
        k = lax.broadcasted_iota(jnp.int32, (lanes, part), 1)
        pick = jnp.where(jnp.bitwise_and(at, HD - 1) == f * part + k, 1.0, 0.0)
        return only, pick

    gn = own_lanes(sm[0:6, :], shard)
    gh = [exact(*own_units(sm[8 + n : 9 + n, :width], heads), ((1,), (0,))) for n in range(2)]
    only, pick = own_units(sm[6:7, :], hidden // HD)
    gx = exact(pick, only, ((0,), (1,)))
    gt = sm[16 : 16 + heads, : w_table.shape[1]]
    gn_o[...] = gn
    gx_o[...] = gx
    gt_o[...] = gt
    small_sq = first_t * total_of(plain(gn, s_norm[...])[1] ** 2)
    for n in range(2):
        gh_o[:, n, :] = gh[n]
        small_sq = small_sq + total_of(plain(gh[n], s_heads[:, n, :])[1] ** 2)
    small_sq = small_sq + total_of(plain(gx, s_hidden[...])[1] ** 2)
    small_sq = small_sq + first_f * total_of(plain(gt, s_table[...])[1] ** 2)

    for n in range(1, 4):
        t_copy(n).wait_recv()
        f_copy(n).wait_recv()
    t_sum = t_s[0] + t_s[1] + t_s[2] + t_s[3]
    f_sum = f_s[0] + f_s[1] + f_s[2] + f_s[3]
    for n in range(1, 16):
        z_copy(n).wait_recv()
    z_sum = z_s[0]
    for n in range(1, 16):
        z_sum = z_sum + z_s[n]
    lane8 = lax.broadcasted_iota(jnp.int32, (8, 128), 1)

    def scalar(n):
        return jnp.sum(jnp.where(lane8 == n, z_sum, 0.0)[0:1], axis=1, keepdims=True)

    def fresh(old, summed, count):
        return DECAY_RATE * old + keep * (summed / count + STAT_EPS)

    rq = fresh(row_qkv[...], t_sum[0:3, :], D)
    kq = fresh(col_qkv[...], f_sum[0:3, :width], D)
    rp = fresh(wide(row_proj), f_sum[3:4, :width], D)
    kp = fresh(wide(col_proj), t_sum[3:4, :], D)
    ru = fresh(wide(row_up), t_sum[4:5, :], ff)
    ku = fresh(wide(col_up), f_sum[4:5, :], D)
    rd = fresh(wide(row_down), f_sum[5:6, :], D)
    kd = fresh(wide(col_down), t_sum[5:6, :], ff)

    def mean_row(n, rows_all, cols_all):
        return (
            DECAY_RATE * scalar(6 + n) + keep * (scalar(n) / cols_all + rows_all * STAT_EPS)
        ) / rows_all

    scale_q = [
        as_column(lax.rsqrt(rq[n : n + 1, :] / mean_row(n, D, D))) * lax.rsqrt(kq[n : n + 1, :])
        for n in range(3)
    ]
    scale_p = as_column(lax.rsqrt(rp / mean_row(3, D, D))) * lax.rsqrt(kp)
    scale_u = as_column(lax.rsqrt(ru / mean_row(4, D, ff))) * lax.rsqrt(ku)
    scale_d = as_column(lax.rsqrt(kd)) * lax.rsqrt(rd / mean_row(5, ff, D))
    big_sq = small_sq
    for n in range(3):
        u = gq_o[n] * scale_q[n]
        uq_o[n] = u
        big_sq = big_sq + total_of(u * u)
    for grad, scale, ref in ((gp_o, scale_p, up_o), (g_up, scale_u, uu_o), (g_down, scale_d, ud_o)):
        u = grad[...] * scale
        ref[...] = u
        big_sq = big_sq + total_of(u * u)
    c_s[me] = jnp.broadcast_to(big_sq, (8, 128))
    for n in range(1, 16):
        c_copy(n).start()
    line.hand(2)
    line.settle(3)
    rq_o[...] = rq
    kq_o[...] = kq
    for ref, row in ((rp_o, rp), (kp_o, kp), (ru_o, ru), (ku_o, ku), (rd_o, rd), (kd_o, kd)):
        put_wide(ref, row)

    home = HomeRows(delta, row_tmp, home_o, halo_s, o_send, o_recv)
    both_bias = rows[2:3, :] + rows[5:6, :]

    def lift(w):
        line.arrive(w)
        delta[w] = (
            jnp.concatenate([br[w, 0], br[w, 1]], axis=1).astype(F32)
            + jnp.concatenate([mixed[w, 0], mixed[w, 1]], axis=1).astype(F32) + both_bias
        )

    lift(0)
    lift(1)
    home.go(0)
    line.hand(3)
    lift(2)
    lift(3)
    home.go(1)

    counts = [3 * D * D, D * D, D * ff, ff * D] + [D] * 8 + [ff, RELP * HEADS]
    sizes = [jnp.sqrt(scalar(12 + n) / counts[n] + STAT_EPS) for n in range(14)]
    for n in range(1, 16):
        c_copy(n).wait_recv()
    all_sq = c_s[0]
    for n in range(1, 16):
        all_sq = all_sq + c_s[n]
    count_all = 4 * D * D + 2 * D * ff + 8 * D + ff + RELP * HEADS
    clip = jnp.sqrt(all_sq[0:1, 0:1] / count_all)
    factor = STEP_RATE / jnp.maximum(1.0, clip / CLIP_LEVEL)
    size_o[...] = lane_pack([size * factor for size in sizes] + [clip])
    for i in range(images):
        home.wait(i)
    for n in range(3):
        swap(n).wait_send()
    for n in range(1, 4):
        t_copy(n).wait_send()
        f_copy(n).wait_send()
    for n in range(1, 16):
        z_copy(n).wait_send()
        c_copy(n).wait_send()
    for w in range(windows):
        line.drain(w)
    qkv.drain()
    proj.drain()


def finish_body(*refs):
    (
        (home_out, feat, home_in, og, gq, gp, g_up, g_down, gn, gh, gx, gt, uq, up, uu, ud),
        (w_qkv, w_proj, w_up, w_down, w_norm, w_heads, w_hidden, w_table),
        (s_norm, s_heads, s_hidden, s_table),
        stats, (size,),
        (out_o, gin_o, gq_o, gp_o, gu_o, gd_o, gn_o, gh_o, gx_o, gt_o),
        (nq_o, np_o, nu_o, nd_o, nn_o, nh_o, nx_o, nt_o),
        (cq_o, cp_o, cu_o, cd_o),
        stats_o, (sn_o, sh_o, sx_o, st_o), (clip_o,),
    ) = take(refs, (16, 8, 4, 8, 1, 10, 8, 4, 8, 4, 1))
    lane8 = lax.broadcasted_iota(jnp.int32, (8, 128), 1)
    table = size[...]

    def step(n):
        return jnp.sum(jnp.where(lane8 == n, table, 0.0)[0:1], axis=1, keepdims=True)

    out_o[...] = feat[...].astype(F32) + home_out[...].astype(F32)
    gin_o[...] = og[...] + home_in[...].astype(F32)
    for src, dst in (
        (gq, gq_o), (gp, gp_o), (g_up, gu_o), (g_down, gd_o), (gn, gn_o), (gh, gh_o), (gx, gx_o),
        (gt, gt_o), *zip(stats, stats_o),
    ):
        dst[...] = src[...]
    for n, (master, u, new_o, low_o) in enumerate(
        ((w_qkv, uq, nq_o, cq_o), (w_proj, up, np_o, cp_o), (w_up, uu, nu_o, cu_o), (w_down, ud, nd_o, cd_o))
    ):
        new = master[...] - step(n) * u[...]
        new_o[...] = new
        low_o[...] = new.astype(BF)
    sn, un = plain(gn[...], s_norm[...])
    sn_o[...] = sn
    for n in range(6):
        nn_o[n : n + 1, :] = w_norm[n : n + 1, :] - step(4 + n) * un[n : n + 1, :]
    for n in range(2):
        sh, uh = plain(gh[:, n, :], s_heads[:, n, :])
        sh_o[:, n, :] = sh
        nh_o[:, n, :] = w_heads[:, n, :] - step(10 + n) * uh
    sx, ux = plain(gx[...], s_hidden[...])
    sx_o[...] = sx
    nx_o[...] = w_hidden[...] - step(12) * ux
    st, ut = plain(gt[...], s_table[...])
    st_o[...] = st
    nt_o[...] = w_table[...] - step(13) * ut
    clip_o[...] = step(14)


def optimizer(gq, gp, g_up, g_down, small, rows, br, mix, home_in, feat, og, masters, stats, states):
    w_qkv, w_proj, w_up, w_down, w_norm, w_heads, w_hidden, w_table = masters
    windows = br.shape[0]
    images = windows // 2
    shard, width = w_qkv.shape[1], w_qkv.shape[2]
    hidden = w_up.shape[1]
    stats = [
        u if u.ndim == 2 else (u.reshape(-1, 128) if u.shape[0] % 512 == 0 or u.shape[0] == hidden
                               else u[None])
        for u in stats
    ]
    like = lambda u: (u.shape, F32)
    mats = (w_qkv, w_proj, w_up, w_down)
    smalls = (w_norm, w_heads, w_hidden, w_table)
    vm, dma = pltpu.VMEM, pltpu.SemaphoreType.DMA
    outs = [
        (feat.shape, BF), like(w_qkv), like(w_proj), *map(like, smalls), *map(like, mats),
        *map(like, stats), ((8, 128), F32),
    ]
    halves = (windows, 2, TOK, HALF)
    scratch = [
        *ShardSum.scratch((3, shard, width)), *ShardSum.scratch((width, shard)),
        *LineSum.scratch(windows),
        vm(halves, BF), vm((3, 24, D), F32), vm((3, 24, D), F32), vm((4, 8, shard), F32),
        vm((4, 8, hidden), F32), vm((16, 8, 128), F32), vm((16, 8, 128), F32),
        vm((windows, TOK, D), F32), vm((24, D), F32), vm((images, SHIFT, 24, D), BF),
        dma((3,)), dma((3,)), *[dma((4,))] * 4, *[dma((16,))] * 4, *[dma((images,))] * 2,
    ]
    got = vmem_call(optimizer_body, outs, scratch, "optimizer", 4)(
        gq, gp, g_up, g_down, small, rows, br, mix, *masters, *stats, *states
    )
    home_out, g_qkv, g_proj, gn, gh, gx, gt, uq, up, uu, ud, *new_stats, size = got
    outs = [
        like(og), like(og), *map(like, mats), *map(like, smalls), *map(like, masters),
        *[(u.shape, BF) for u in mats], *map(like, stats), *map(like, smalls), ((1, 1), F32),
    ]
    return vmem_call(finish_body, outs, [], "finish", None)(
        home_out, feat, home_in, og, g_qkv, g_proj, g_up, g_down, gn, gh, gx, gt, uq, up, uu, ud,
        *masters, *states, *new_stats, size,
    )


def per_device_plain(
    features,
    out_grad,
    regions,
    rel_index,
    w_qkv,
    w_proj,
    w_up,
    w_down,
    norm_vecs,
    head_bias,
    hidden_bias,
    rel_table,
    row_qkv,
    col_qkv,
    row_proj,
    col_proj,
    row_up,
    col_up,
    row_down,
    col_down,
    state_norm,
    state_heads,
    state_hidden,
    state_table,
):
    images, band_rows, across, model_width = features.shape
    win_tokens = WIN * WIN
    fsdp_at = lax.axis_index("fsdp")
    ctx_at = lax.axis_index("ctx")
    tp_at = lax.axis_index("tp")
    first_fsdp = (fsdp_at == 0).astype(jnp.float32)
    first_ctx = (ctx_at == 0).astype(jnp.float32)
    first_tp = (tp_at == 0).astype(jnp.float32)
    weights_qkv, weights_proj, weights_up, weights_down, vec_copy, head_copy, hidden_copy = (
        lax.all_gather(w_qkv.astype(jnp.bfloat16), "fsdp", axis=1, tiled=True),
        lax.all_gather(w_proj.astype(jnp.bfloat16), "fsdp", axis=1, tiled=True),
        lax.all_gather(w_up.astype(jnp.bfloat16), "fsdp", axis=0, tiled=True),
        lax.all_gather(w_down.astype(jnp.bfloat16), "fsdp", axis=1, tiled=True),
        lax.all_gather(norm_vecs.astype(jnp.bfloat16), "fsdp", axis=1, tiled=True),
        lax.all_gather(head_bias.astype(jnp.bfloat16), "fsdp", axis=2, tiled=True),
        lax.all_gather(hidden_bias.astype(jnp.bfloat16), "fsdp", axis=1, tiled=True),
    )
    norm_rows = vec_copy.astype(jnp.float32)
    bias_query = head_copy[0].reshape(-1).astype(jnp.float32)
    bias_value = head_copy[1].reshape(-1).astype(jnp.float32)
    bias_hidden = hidden_copy.reshape(-1).astype(jnp.float32)
    table_copy = rel_table.astype(jnp.bfloat16)
    local_width = weights_qkv.shape[2]
    heads_here = local_width // HD

    def roll_in(home):
        received = passed_along(home[:, :SHIFT], "ctx", -1)
        return to_windows(enter_frame(home, received)).reshape(-1, model_width)

    def roll_out(rolled_flat):
        band = jnp.roll(
            from_windows(
                rolled_flat.reshape(-1, win_tokens, model_width), images, band_rows, across
            ),
            SHIFT,
            axis=2,
        )
        lower = passed_along(band[:, band_rows - SHIFT :], "ctx", 1)
        return jnp.concatenate([lower, band[:, : band_rows - SHIFT]], axis=1)

    flat_one = roll_in(features).astype(jnp.float32)
    grad_flat = roll_in(out_grad)
    win_count = flat_one.shape[0] // win_tokens
    normed_one, pull_one = jax.vjp(layer_norm, flat_one, norm_rows[0], norm_rows[1])
    normed_one_low = normed_one.astype(jnp.bfloat16)
    head_shape = (win_count, win_tokens, heads_here, HD)
    query_low, key_low, value_low = project_heads(
        normed_one_low, weights_qkv, bias_query, bias_value, head_shape
    )
    pos_bias = table_lookup(table_copy, rel_index)
    region_win = to_windows(regions[..., None])[..., 0]
    mask_add = jnp.where(region_win[:, :, None] == region_win[:, None, :], 0.0, MASK_FILL).astype(
        jnp.float32
    )
    scores = attention_scores(query_low, key_low, pos_bias, mask_add)
    top_score = jnp.max(scores, axis=-1, keepdims=True)
    lifted = jnp.exp(scores - top_score)
    prob_rows = lifted / jnp.sum(lifted, axis=-1, keepdims=True)
    prob_low = prob_rows.astype(jnp.bfloat16)
    context = jnp.einsum("whij,wjhc->wihc", prob_low, value_low, preferred_element_type=jnp.float32)
    context_low = context.astype(jnp.bfloat16).reshape(-1, local_width)
    branch_part = jnp.dot(context_low, weights_proj, preferred_element_type=jnp.float32)
    branch = lax.psum(branch_part.astype(jnp.bfloat16), "tp").astype(jnp.float32) + norm_rows[2]
    flat_two = flat_one + branch
    normed_two, pull_two = jax.vjp(layer_norm, flat_two, norm_rows[3], norm_rows[4])
    normed_two_low = normed_two.astype(jnp.bfloat16)
    pre_act = jnp.dot(normed_two_low, weights_up, preferred_element_type=jnp.float32) + bias_hidden
    hidden, pull_gelu = jax.vjp(exact_gelu, pre_act)
    hidden_low = hidden.astype(jnp.bfloat16)
    mixed_part = jnp.dot(hidden_low, weights_down, preferred_element_type=jnp.float32)
    mixed_whole = lax.psum(mixed_part.astype(jnp.bfloat16), "tp").astype(jnp.float32)
    block_out = features.astype(jnp.float32) + roll_out(
        (branch + mixed_whole + norm_rows[5]).astype(jnp.bfloat16)
    ).astype(jnp.float32)
    grad_low = grad_flat.astype(jnp.bfloat16)
    grad_down_full = jnp.einsum(
        "tf,td->fd", hidden_low, grad_low, preferred_element_type=jnp.float32
    )
    grad_down_bias = jnp.sum(grad_flat, axis=0)
    d_hidden = jnp.einsum("td,fd->tf", grad_low, weights_down, preferred_element_type=jnp.float32)
    d_pre = pull_gelu(d_hidden)[0]
    d_pre_low = d_pre.astype(jnp.bfloat16)
    grad_hidden_bias = jnp.sum(d_pre, axis=0)
    grad_up_full = jnp.einsum(
        "td,tf->df", normed_two_low, d_pre_low, preferred_element_type=jnp.float32
    )
    d_two_part = jnp.einsum("tf,df->td", d_pre_low, weights_up, preferred_element_type=jnp.float32)
    d_two = lax.psum(d_two_part.astype(jnp.bfloat16), "tp").astype(jnp.float32)
    d_flat_two, grad_gain_two, grad_offset_two = pull_two(d_two)
    d_resid = grad_flat + d_flat_two
    grad_proj_bias = jnp.sum(d_resid, axis=0)
    d_branch = d_resid.astype(jnp.bfloat16)
    grad_proj_full = jnp.einsum(
        "tc,td->cd", context_low, d_branch, preferred_element_type=jnp.float32
    )
    d_context = (
        jnp.einsum("td,cd->tc", d_branch, weights_proj, preferred_element_type=jnp.float32)
        .astype(jnp.bfloat16)
        .reshape(head_shape)
    )
    d_probs = jnp.einsum(
        "wihc,wjhc->whij", d_context, value_low, preferred_element_type=jnp.float32
    )
    d_value_low = jnp.einsum(
        "whij,wihc->wjhc", prob_low, d_context, preferred_element_type=jnp.float32
    ).astype(jnp.bfloat16)
    d_scores = prob_rows * (d_probs - jnp.sum(prob_rows * d_probs, axis=-1, keepdims=True))
    d_pos = jnp.sum(d_scores, axis=0)
    d_scaled = (d_scores * HD ** (-0.5)).astype(jnp.bfloat16)
    d_query_low = jnp.einsum(
        "whij,wjhc->wihc", d_scaled, key_low, preferred_element_type=jnp.float32
    ).astype(jnp.bfloat16)
    d_key_low = jnp.einsum(
        "whij,wihc->wjhc", d_scaled, query_low, preferred_element_type=jnp.float32
    ).astype(jnp.bfloat16)
    d_heads = jnp.stack([d_query_low, d_key_low, d_value_low]).reshape(3, -1, local_width)
    grad_qkv_full = jnp.einsum(
        "td,ktc->kdc", normed_one_low, d_heads, preferred_element_type=jnp.float32
    )
    grad_head_bias = jnp.stack(
        [
            jnp.sum(d_heads[0].astype(jnp.float32), axis=0),
            jnp.sum(d_heads[2].astype(jnp.float32), axis=0),
        ]
    ).reshape(2, heads_here, HD)
    d_one_part = jnp.einsum("ktc,kdc->td", d_heads, weights_qkv, preferred_element_type=jnp.float32)
    d_one = lax.psum(d_one_part.astype(jnp.bfloat16), "tp").astype(jnp.float32)
    d_flat_one, grad_gain_one, grad_offset_one = pull_one(d_one)
    grad_input = out_grad + roll_out((d_flat_two + d_flat_one).astype(jnp.bfloat16)).astype(
        jnp.float32
    )
    table_part = table_grad(d_pos, rel_index, rel_table.shape[0])
    grad_norm_full = jnp.stack(
        [
            grad_gain_one,
            grad_offset_one,
            grad_proj_bias,
            grad_gain_two,
            grad_offset_two,
            grad_down_bias,
        ]
    )
    grad_list = (
        grad_qkv_full,
        grad_proj_full,
        grad_up_full,
        grad_down_full,
        grad_norm_full,
        grad_head_bias,
        grad_hidden_bias.reshape(-1, HD),
    )
    g_qkv, g_proj, g_up, g_down, g_norm, g_heads, g_hidden = shard_sum(band_sum(grad_list))
    d_shard = w_qkv.shape[1]
    hidden_here = w_up.shape[1]
    keep = 1.0 - DECAY_RATE
    sq_qkv = g_qkv * g_qkv
    sq_proj = g_proj * g_proj
    sq_up = g_up * g_up
    sq_down = g_down * g_down
    stat_rq = place(
        (keep * jnp.sum(sq_qkv, axis=2) / D + first_tp * (DECAY_RATE * row_qkv + keep * STAT_EPS))
        * first_ctx,
        fsdp_at,
        D,
    )
    stat_cq = place(
        (keep * jnp.sum(sq_qkv, axis=1) / D + first_fsdp * (DECAY_RATE * col_qkv + keep * STAT_EPS))
        * first_ctx,
        tp_at,
        D,
    )
    stat_rp = place(
        (
            keep * jnp.sum(sq_proj, axis=1) / D
            + first_fsdp * (DECAY_RATE * row_proj + keep * STAT_EPS)
        )
        * first_ctx,
        tp_at,
        D,
    )
    stat_cp = place(
        (keep * jnp.sum(sq_proj, axis=0) / D + first_tp * (DECAY_RATE * col_proj + keep * STAT_EPS))
        * first_ctx,
        fsdp_at,
        D,
    )
    stat_ru = place(
        (keep * jnp.sum(sq_up, axis=1) / FF + first_tp * (DECAY_RATE * row_up + keep * STAT_EPS))
        * first_ctx,
        fsdp_at,
        D,
    )
    stat_cu = place(
        (keep * jnp.sum(sq_up, axis=0) / D + first_fsdp * (DECAY_RATE * col_up + keep * STAT_EPS))
        * first_ctx,
        tp_at,
        FF,
    )
    stat_rd = place(
        (
            keep * jnp.sum(sq_down, axis=1) / D
            + first_fsdp * (DECAY_RATE * row_down + keep * STAT_EPS)
        )
        * first_ctx,
        tp_at,
        FF,
    )
    stat_cd = place(
        (
            keep * jnp.sum(sq_down, axis=0) / FF
            + first_tp * (DECAY_RATE * col_down + keep * STAT_EPS)
        )
        * first_ctx,
        fsdp_at,
        D,
    )
    table_whole = place(table_part, tp_at, HEADS)
    master_sq = jnp.concatenate(
        [
            jnp.stack(
                [
                    jnp.sum(w_qkv * w_qkv),
                    jnp.sum(w_proj * w_proj),
                    jnp.sum(w_up * w_up),
                    jnp.sum(w_down * w_down),
                ]
            )
            * first_ctx,
            jnp.sum(norm_vecs * norm_vecs, axis=1) * first_ctx * first_tp,
            jnp.sum(head_bias * head_bias, axis=(1, 2)) * first_ctx,
            jnp.sum(hidden_bias * hidden_bias)[None] * first_ctx,
            jnp.sum(rel_table * rel_table)[None] * first_ctx * first_fsdp,
        ]
    )
    (
        full_rq,
        full_cq,
        full_rp,
        full_cp,
        full_ru,
        full_cu,
        full_rd,
        full_cd,
        table_sum,
        master_total,
    ) = lax.psum(
        (
            stat_rq,
            stat_cq,
            stat_rp,
            stat_cp,
            stat_ru,
            stat_cu,
            stat_rd,
            stat_cd,
            table_whole,
            master_sq,
        ),
        ("fsdp", "ctx", "tp"),
    )
    u_qkv = factored(
        g_qkv,
        own_part(full_rq, fsdp_at, d_shard),
        own_part(full_cq, tp_at, local_width),
        jnp.mean(full_rq, axis=1)[:, None, None],
    )
    u_proj = factored(
        g_proj,
        own_part(full_rp, tp_at, local_width),
        own_part(full_cp, fsdp_at, d_shard),
        jnp.mean(full_rp),
    )
    u_up = factored(
        g_up,
        own_part(full_ru, fsdp_at, d_shard),
        own_part(full_cu, tp_at, hidden_here),
        jnp.mean(full_ru),
    )
    u_down = factored(
        g_down,
        own_part(full_rd, tp_at, hidden_here),
        own_part(full_cd, fsdp_at, d_shard),
        jnp.mean(full_rd),
    )
    g_table = own_part(table_sum, tp_at, heads_here)
    state_norm_new, u_norm = plain_stats(g_norm, state_norm)
    state_heads_new, u_heads = plain_stats(g_heads, state_heads)
    state_hidden_new, u_hidden = plain_stats(g_hidden, state_hidden)
    state_table_new, u_table = plain_stats(g_table, state_table)
    local_sq = (
        jnp.sum(u_qkv * u_qkv)
        + jnp.sum(u_proj * u_proj)
        + jnp.sum(u_up * u_up)
        + jnp.sum(u_down * u_down)
        + jnp.sum(u_heads * u_heads)
        + jnp.sum(u_hidden * u_hidden)
        + first_tp * jnp.sum(u_norm * u_norm)
        + first_fsdp * jnp.sum(u_table * u_table)
    )
    total_sq = lax.psum(local_sq, ("fsdp", "tp"))
    count_all = 4 * D * D + 2 * D * FF + 8 * D + FF + RELP * HEADS
    clip_rms = jnp.sqrt(total_sq / count_all)
    factor = 1.0 / jnp.maximum(1.0, clip_rms / CLIP_LEVEL)
    counts = jnp.array(
        [3 * D * D, D * D, D * FF, FF * D, D, D, D, D, D, D, D, D, FF, RELP * HEADS], jnp.float32
    )
    scales = jnp.sqrt(master_total / counts + STAT_EPS)
    new_qkv = w_qkv - STEP_RATE * scales[0] * factor * u_qkv
    new_proj = w_proj - STEP_RATE * scales[1] * factor * u_proj
    new_up = w_up - STEP_RATE * scales[2] * factor * u_up
    new_down = w_down - STEP_RATE * scales[3] * factor * u_down
    new_norm = norm_vecs - STEP_RATE * scales[4:10][:, None] * factor * u_norm
    new_heads = head_bias - STEP_RATE * scales[10:12][:, None, None] * factor * u_heads
    new_hidden = hidden_bias - STEP_RATE * scales[12] * factor * u_hidden
    new_table = rel_table - STEP_RATE * scales[13] * factor * u_table
    return (
        block_out,
        grad_input,
        g_qkv,
        g_proj,
        g_up,
        g_down,
        g_norm,
        g_heads,
        g_hidden,
        g_table,
        new_qkv,
        new_proj,
        new_up,
        new_down,
        new_norm,
        new_heads,
        new_hidden,
        new_table,
        new_qkv.astype(jnp.bfloat16),
        new_proj.astype(jnp.bfloat16),
        new_up.astype(jnp.bfloat16),
        new_down.astype(jnp.bfloat16),
        own_part(full_rq, fsdp_at, d_shard),
        own_part(full_cq, tp_at, local_width),
        own_part(full_rp, tp_at, local_width),
        own_part(full_cp, fsdp_at, d_shard),
        own_part(full_ru, fsdp_at, d_shard),
        own_part(full_cu, tp_at, hidden_here),
        own_part(full_rd, tp_at, hidden_here),
        own_part(full_cd, fsdp_at, d_shard),
        state_norm_new,
        state_heads_new,
        state_hidden_new,
        state_table_new,
        clip_rms,
    )


def per_device(
    features,
    out_grad,
    regions,
    rel_index,
    w_qkv,
    w_proj,
    w_up,
    w_down,
    norm_vecs,
    head_bias,
    hidden_bias,
    rel_table,
    row_qkv,
    col_qkv,
    row_proj,
    col_proj,
    row_up,
    col_up,
    row_down,
    col_down,
    state_norm,
    state_heads,
    state_hidden,
    state_table,
):
    home_in, gq, gp, small, g_up, g_down, rows, br, mix = forward_backward(
        features, out_grad, regions, rel_index, w_qkv, w_proj, w_up, w_down.T,
        norm_vecs, head_bias, hidden_bias, rel_table)
    flip = lambda u: u.transpose(1, 0, 2)
    (block_out, grad_input, g_qkv, g_proj, g_up, g_down, g_norm, g_heads, g_hidden, g_table,
     new_qkv, new_proj, new_up, new_down, new_norm, new_heads, new_hidden, new_table,
     copy_qkv, copy_proj, copy_up, copy_down, *rest) = optimizer(
        gq, gp, g_up, g_down, small, rows, br, mix, home_in, features, out_grad,
        (w_qkv, w_proj, w_up, w_down.T, norm_vecs, flip(head_bias), hidden_bias.T, rel_table.T),
        (row_qkv, col_qkv, row_proj, col_proj, row_up, col_up, row_down, col_down),
        (state_norm, flip(state_heads), state_hidden.T, state_table.T))
    factors, states, clip_rms = rest[:8], rest[8:12], rest[12]
    factors = list(factors[:2]) + [u.reshape(-1) for u in factors[2:]]
    return (
        block_out, grad_input, g_qkv, g_proj, g_up, g_down.T, g_norm, flip(g_heads), g_hidden.T,
        g_table.T, new_qkv, new_proj, new_up, new_down.T, new_norm, flip(new_heads), new_hidden.T,
        new_table.T, copy_qkv, copy_proj, copy_up, copy_down.T, *factors,
        states[0], flip(states[1]), states[2].T, states[3].T, clip_rms[0, 0],
    )


def solution(mesh):
    line_of_four = mesh.shape["fsdp"] == 4 and mesh.shape["tp"] == 4 and mesh.shape["ctx"] == 2
    return jax.shard_map(
        per_device if line_of_four else per_device_plain,
        mesh=mesh,
        in_specs=(
            P("fsdp", "ctx", None, None),
            P("fsdp", "ctx", None, None),
            P("fsdp", "ctx", None),
            P(),
            P(None, "fsdp", "tp"),
            P("tp", "fsdp"),
            P("fsdp", "tp"),
            P("tp", "fsdp"),
            P(None, "fsdp"),
            P(None, "tp", "fsdp"),
            P("tp", "fsdp"),
            P(None, "tp"),
            P(None, "fsdp"),
            P(None, "tp"),
            P("tp"),
            P("fsdp"),
            P("fsdp"),
            P("tp"),
            P("tp"),
            P("fsdp"),
            P(None, "fsdp"),
            P(None, "tp", "fsdp"),
            P("tp", "fsdp"),
            P(None, "tp"),
        ),
        out_specs=(
            P("fsdp", "ctx", None, None),
            P("fsdp", "ctx", None, None),
            P(None, "fsdp", "tp"),
            P("tp", "fsdp"),
            P("fsdp", "tp"),
            P("tp", "fsdp"),
            P(None, "fsdp"),
            P(None, "tp", "fsdp"),
            P("tp", "fsdp"),
            P(None, "tp"),
            P(None, "fsdp", "tp"),
            P("tp", "fsdp"),
            P("fsdp", "tp"),
            P("tp", "fsdp"),
            P(None, "fsdp"),
            P(None, "tp", "fsdp"),
            P("tp", "fsdp"),
            P(None, "tp"),
            P(None, "fsdp", "tp"),
            P("tp", "fsdp"),
            P("fsdp", "tp"),
            P("tp", "fsdp"),
            P(None, "fsdp"),
            P(None, "tp"),
            P("tp"),
            P("fsdp"),
            P("fsdp"),
            P("tp"),
            P("tp"),
            P("fsdp"),
            P(None, "fsdp"),
            P(None, "tp", "fsdp"),
            P("tp", "fsdp"),
            P(None, "tp"),
            P(),
        ),
        check_vma=False,
    )
```

```python
import functools

import jax
import jax.numpy as jnp
from jax import lax
from jax.experimental import pallas as pl
from jax.experimental.pallas import tpu as pltpu
from jax.sharding import PartitionSpec as P


D = 768
HEADS = 24
HD = 32
FF = 3072
WIN = 12
SHIFT = 6
RELP = 529


DECAY_RATE = 0.5
STAT_EPS = 1e-06
NORM_EPS = 1e-05
MASK_FILL = -100.0
STEP_RATE = 1.0
CLIP_LEVEL = 0.25


def passed_along(x, axis, by):
    count = lax.axis_size(axis)
    return lax.ppermute(x, axis, [(i, (i + by) % count) for i in range(count)])


def layer_norm(values, gain_row, offset):
    mean_val = jnp.mean(values, axis=-1, keepdims=True)
    centred = values - mean_val
    var_val = jnp.mean(centred * centred, axis=-1, keepdims=True)
    return centred * lax.rsqrt(var_val + NORM_EPS) * gain_row + offset


def exact_gelu(values):
    return jax.nn.gelu(values, approximate=False)


def to_windows(values):
    image_count, row_count, col_count, channels = values.shape
    pieces = values.reshape(image_count, row_count // WIN, WIN, col_count // WIN, WIN, channels)
    return pieces.transpose(0, 1, 3, 2, 4, 5).reshape(-1, WIN * WIN, channels)


def from_windows(values, image_count, row_count, col_count):
    channels = values.shape[-1]
    pieces = values.reshape(image_count, row_count // WIN, col_count // WIN, WIN, WIN, channels)
    return pieces.transpose(0, 1, 3, 2, 4, 5).reshape(image_count, row_count, col_count, channels)


def enter_frame(own_rows, received):
    joined = jnp.concatenate([own_rows[:, SHIFT:], received], axis=1)
    return jnp.roll(joined, -SHIFT, axis=2)


def project_heads(normed_low, weights_qkv, bias_query, bias_value, head_shape):
    query_full = (
        jnp.dot(normed_low, weights_qkv[0], preferred_element_type=jnp.float32) + bias_query
    )
    key_full = jnp.dot(normed_low, weights_qkv[1], preferred_element_type=jnp.float32)
    value_full = (
        jnp.dot(normed_low, weights_qkv[2], preferred_element_type=jnp.float32) + bias_value
    )
    return tuple(
        (
            member.astype(jnp.bfloat16).reshape(head_shape)
            for member in (query_full, key_full, value_full)
        )
    )


def attention_scores(query_low, key_low, pos_bias, mask_add):
    products = jnp.einsum("wihc,wjhc->whij", query_low, key_low, preferred_element_type=jnp.float32)
    return products * query_low.shape[-1] ** (-0.5) + pos_bias[None] + mask_add[:, None]


def table_lookup(table_low, rel_index):
    win_tokens = rel_index.shape[0]
    code_ids = jnp.arange(table_low.shape[0], dtype=jnp.int32)
    index_blocks = rel_index.reshape(WIN, -1)

    def lookup(index_block):
        one_hot = (index_block[:, None] == code_ids[None, :]).astype(jnp.bfloat16)
        return jnp.dot(one_hot, table_low, preferred_element_type=jnp.float32)

    looked = lax.map(lookup, index_blocks)
    return looked.reshape(win_tokens, win_tokens, -1).transpose(2, 0, 1)


def table_grad(d_pos, rel_index, table_rows):
    heads_here = d_pos.shape[0]
    code_ids = jnp.arange(table_rows, dtype=jnp.int32)
    index_blocks = rel_index.reshape(WIN, -1)
    grad_blocks = d_pos.transpose(1, 2, 0).reshape(WIN, -1, heads_here)

    def accumulate(running, member):
        index_block, grad_block = member
        one_hot = (index_block[:, None] == code_ids[None, :]).astype(jnp.float32)
        added = lax.dot_general(
            one_hot,
            grad_block,
            (((0,), (0,)), ((), ())),
            precision=lax.Precision.HIGHEST,
            preferred_element_type=jnp.float32,
        )
        return (running + added, None)

    result_pair = lax.scan(
        accumulate, jnp.zeros((table_rows, heads_here), jnp.float32), (index_blocks, grad_blocks)
    )
    return result_pair[0]


def place(part_vec, index_at, whole_len):
    size_of = part_vec.shape[-1]
    base = jnp.zeros(part_vec.shape[:-1] + (whole_len,), jnp.float32)
    return lax.dynamic_update_slice_in_dim(base, part_vec, index_at * size_of, part_vec.ndim - 1)


def own_part(whole_vec, index_at, size_of):
    return lax.dynamic_slice_in_dim(whole_vec, index_at * size_of, size_of, whole_vec.ndim - 1)


def factored(grad, row_local, col_local, row_mean):
    return grad * lax.rsqrt(row_local[..., :, None] * col_local[..., None, :] / row_mean)


def plain_stats(grad, state_old):
    state_new = DECAY_RATE * state_old + (1.0 - DECAY_RATE) * (grad * grad + STAT_EPS)
    return (state_new, grad * lax.rsqrt(state_new))


def shard_sum(grad_list):
    return (
        lax.psum_scatter(grad_list[0], "fsdp", scatter_dimension=1, tiled=True),
        lax.psum_scatter(grad_list[1], "fsdp", scatter_dimension=1, tiled=True),
        lax.psum_scatter(grad_list[2], "fsdp", scatter_dimension=0, tiled=True),
        lax.psum_scatter(grad_list[3], "fsdp", scatter_dimension=1, tiled=True),
        lax.psum_scatter(grad_list[4], "fsdp", scatter_dimension=1, tiled=True),
        lax.psum_scatter(grad_list[5], "fsdp", scatter_dimension=2, tiled=True),
        lax.psum_scatter(grad_list[6], "fsdp", scatter_dimension=1, tiled=True),
    )


def band_sum(grad_list):
    return lax.psum(
        (
            grad_list[0],
            grad_list[1],
            grad_list[2],
            grad_list[3],
            grad_list[4],
            grad_list[5],
            grad_list[6],
        ),
        "ctx",
    )


BF = jnp.bfloat16
F32 = jnp.float32
MESH = pl.DeviceIdType.MESH
TOK = WIN * WIN
HALF = D // 2
ROWS = TOK // 2
VMEM_LIMIT = 67_043_328


def dot(a, b):
    return lax.dot_general(a, b, (((1,), (0,)), ((), ())), preferred_element_type=F32)


def dot_t(a, b):
    return lax.dot_general(a, b, (((1,), (1,)), ((), ())), preferred_element_type=F32)


def t_dot(a, b):
    return lax.dot_general(a, b, (((0,), (0,)), ((), ())), preferred_element_type=F32)


def row_mean(x):
    return jnp.sum(x, axis=-1, keepdims=True) * (1.0 / x.shape[-1])


def remote(src, dst, send, recv, where):
    return pltpu.make_async_remote_copy(
        src_ref=src, dst_ref=dst, send_sem=send, recv_sem=recv, device_id=where, device_id_type=MESH
    )


def greet(barrier, places):
    for place_of in places:
        pl.semaphore_signal(barrier, inc=1, device_id=place_of, device_id_type=MESH)


class LineSum:
    def __init__(self, part, send, from_outer, from_mid, total, sems):
        self.part, self.send, self.from_outer, self.from_mid, self.total = (
            part, send, from_outer, from_mid, total,
        )
        self.s_out, self.r_out, self.s_mid, self.r_mid, self.s_tot, self.r_tot, self.s_cross = sems
        z = lax.axis_index("tp")
        self.is_mid = jnp.logical_and(z > 0, z < 3)
        self.is_outer = jnp.logical_not(self.is_mid)
        self.outer = jnp.where(z < 2, 0, 3)
        self.mid = jnp.where(z < 2, 1, 2)
        self.other_mid = 3 - self.mid
        self.own = self.mid - 1
        self.other = 1 - self.own

    @staticmethod
    def scratch(count):
        return [
            pltpu.VMEM((count, 2, ROWS, HALF), BF),
            pltpu.VMEM((count, 2, ROWS, HALF), BF),
            pltpu.VMEM((count, ROWS, HALF), BF),
            pltpu.SemaphoreType.DMA((count, 2)),
            pltpu.SemaphoreType.DMA((count, 2)),
            pltpu.SemaphoreType.DMA((count,)),
            pltpu.SemaphoreType.DMA((count,)),
            pltpu.SemaphoreType.DMA((count, 2)),
            pltpu.SemaphoreType.DMA((count, 2)),
            pltpu.SemaphoreType.DMA((count,)),
        ]

    @staticmethod
    def build(part, refs, total):
        return LineSum(part, refs[0], refs[1], refs[2], total, refs[3:10])

    @staticmethod
    def peers():
        return 2

    def greet(self, barrier):
        pl.semaphore_signal(
            barrier, inc=1, device_id={"tp": jnp.where(self.is_mid, self.outer, self.mid)},
            device_id_type=MESH,
        )

        @pl.when(self.is_mid)
        def _():
            pl.semaphore_signal(
                barrier, inc=1, device_id={"tp": self.other_mid}, device_id_type=MESH
            )

    def greet_count(self):
        return jnp.where(self.is_mid, 2, 1)

    def _to_mid(self, w, h):
        return remote(self.send.at[w, h], self.from_outer.at[w, h], self.s_out.at[w, h],
                      self.r_out.at[w, h], {"tp": self.mid})

    def _across(self, w):
        return remote(self.send.at[w, self.other], self.from_mid.at[w], self.s_mid.at[w],
                      self.r_mid.at[w], {"tp": self.other_mid})

    def _total_across(self, w, h):
        return remote(self.total.at[w, h], self.total.at[w, h], self.s_cross.at[w],
                      self.r_tot.at[w, h], {"tp": self.other_mid})

    def _total_out(self, w, h):
        return remote(self.total.at[w, h], self.total.at[w, h], self.s_tot.at[w, h],
                      self.r_tot.at[w, h], {"tp": self.outer})

    def put(self, w, value):
        for s in range(2):
            for h in range(2):
                self.part[2 * w + s, h] = value[s * ROWS : (s + 1) * ROWS, h * HALF : (h + 1) * HALF]

    def get(self, w):
        return jnp.concatenate(
            [
                jnp.concatenate([self.total[2 * w + s, h].astype(F32) for h in range(2)], axis=1)
                for s in range(2)
            ],
            axis=0,
        )

    def start(self, w):
        @pl.when(self.is_outer)
        def _():
            for j in (2 * w, 2 * w + 1):
                for h in (self.other, self.own):
                    self.send[j, h] = self.part[j, h].astype(BF)
                    self._to_mid(j, h).start()

    def cross(self, w):
        @pl.when(self.is_mid)
        def _():
            for j in (2 * w, 2 * w + 1):
                self._to_mid(j, self.other).wait_recv()
                self.send[j, self.other] = (
                    self.part[j, self.other] + self.from_outer[j, self.other].astype(F32)
                ).astype(BF)
                self._across(j).start()

    def settle(self, w):
        @pl.when(self.is_mid)
        def _():
            for j in (2 * w, 2 * w + 1):
                self._to_mid(j, self.own).wait_recv()
                self._across(j).wait_recv()
                self.total[j, self.own] = (
                    self.part[j, self.own]
                    + self.from_outer[j, self.own].astype(F32)
                    + self.from_mid[j].astype(F32)
                ).astype(BF)
                self._total_across(j, self.own).start()
                self._total_out(j, self.own).start()

    def hand(self, w):
        @pl.when(self.is_mid)
        def _():
            for j in (2 * w, 2 * w + 1):
                self._total_across(j, self.other).wait_recv()
                self._total_out(j, self.other).start()

    def arrive(self, w):
        @pl.when(self.is_outer)
        def _():
            for j in (2 * w, 2 * w + 1):
                self._total_out(j, 0).wait_recv()
                self._total_out(j, 1).wait_recv()

    def drain(self, w):
        @pl.when(self.is_outer)
        def _():
            for j in (2 * w, 2 * w + 1):
                self._to_mid(j, 0).wait_send()
                self._to_mid(j, 1).wait_send()

        @pl.when(self.is_mid)
        def _():
            for j in (2 * w, 2 * w + 1):
                self._across(j).wait_send()
                self._total_across(j, self.own).wait_send()
                self._total_out(j, 0).wait_send()
                self._total_out(j, 1).wait_send()


class ShardSum:
    def __init__(self, block_of, out, refs):
        self.block_of, self.out = block_of, out
        self.snd1, self.rcv1, self.snd2, self.rcv2, self.snd3, self.rcv3, self.s, self.r = refs
        f = lax.axis_index("fsdp")
        core = lax.rem(f, 2)
        self.f, self.core = f, core
        self.near, self.far = f + 1 - 2 * core, lax.rem(f + 2, 4)
        self.ctx = 1 - lax.axis_index("ctx")

    @staticmethod
    def scratch(shape):
        return [
            pltpu.VMEM((2, *shape), BF), pltpu.VMEM((2, *shape), BF),
            pltpu.VMEM(shape, BF), pltpu.VMEM(shape, BF),
            pltpu.VMEM(shape, BF), pltpu.VMEM(shape, BF),
            pltpu.SemaphoreType.DMA((4,)), pltpu.SemaphoreType.DMA((4,)),
        ]

    def _near(self, x):
        return remote(self.snd1.at[x], self.rcv1.at[x], self.s.at[x], self.r.at[x], {"fsdp": self.near})

    def _far(self):
        return remote(self.snd2, self.rcv2, self.s.at[2], self.r.at[2], {"fsdp": self.far})

    def _ctx(self):
        return remote(self.snd3, self.rcv3, self.s.at[3], self.r.at[3], {"ctx": self.ctx})

    def start(self):
        for x in range(2):
            self.snd1[x] = self.block_of(2 * x + 1 - self.core).astype(BF)
            self._near(x).start()

    def pair(self):
        for x in range(2):
            self._near(x).wait_recv()
        other = lax.div(self.far, 2)
        self.snd2[...] = (self.block_of(self.far) + self.rcv1[other].astype(F32)).astype(BF)
        self._far().start()

    def cross(self):
        self._far().wait_recv()
        mine = lax.div(self.f, 2)
        self.snd3[...] = (
            self.block_of(self.f) + self.rcv1[mine].astype(F32) + self.rcv2[...].astype(F32)
        ).astype(BF)
        self._ctx().start()

    def finish(self):
        self._ctx().wait_recv()
        self.out[...] = self.snd3[...].astype(F32) + self.rcv3[...].astype(F32)

    def drain(self):
        for x in range(2):
            self._near(x).wait_send()
        self._far().wait_send()
        self._ctx().wait_send()


def vmem_call(body, outs, scratch, name, collective_id):
    remote_kernel = {} if collective_id is None else dict(
        collective_id=collective_id, has_side_effects=True
    )

    def call(*args):
        return pl.pallas_call(
            body,
            out_shape=[jax.ShapeDtypeStruct(s, t) for s, t in outs],
            in_specs=[pl.BlockSpec(memory_space=pltpu.VMEM)] * len(args),
            out_specs=[pl.BlockSpec(memory_space=pltpu.VMEM)] * len(outs),
            scratch_shapes=scratch,
            compiler_params=pltpu.CompilerParams(vmem_limit_bytes=VMEM_LIMIT, **remote_kernel),
            name=name,
        )(*args)

    return call


def take(refs, counts):
    groups, at = [], 0
    for n in counts:
        groups.append(refs[at : at + n])
        at += n
    return groups


def window_rows(row_of, row_tmp, image, dst):
    for r in range(WIN):
        row_tmp[...] = row_of(image, r).astype(F32)
        dst[2 * image, r * WIN : (r + 1) * WIN, :] = row_tmp[SHIFT : SHIFT + WIN, :]
        dst[2 * image + 1, r * WIN : r * WIN + SHIFT, :] = row_tmp[SHIFT + WIN :, :]
        dst[2 * image + 1, r * WIN + SHIFT : (r + 1) * WIN, :] = row_tmp[:SHIFT, :]


def home_row(delta, row_tmp, image, r):
    row_tmp[SHIFT : SHIFT + WIN, :] = delta[2 * image, r * WIN : (r + 1) * WIN, :]
    row_tmp[SHIFT + WIN :, :] = delta[2 * image + 1, r * WIN : r * WIN + SHIFT, :]
    row_tmp[:SHIFT, :] = delta[2 * image + 1, r * WIN + SHIFT : (r + 1) * WIN, :]
    return row_tmp[...].astype(BF)


class HomeRows:
    def __init__(self, delta, row_tmp, out, halo, send, recv):
        self.delta, self.row_tmp, self.out, self.halo, self.s, self.r = (
            delta, row_tmp, out, halo, send, recv,
        )

    def _copy(self, i):
        return remote(self.halo.at[i], self.out.at[i, 0:SHIFT], self.s.at[i], self.r.at[i],
                      {"ctx": 1 - lax.axis_index("ctx")})

    def go(self, i):
        for r in range(SHIFT, WIN):
            self.halo[i, r - SHIFT] = home_row(self.delta, self.row_tmp, i, r)
        self._copy(i).start()
        for r in range(SHIFT):
            self.out[i, SHIFT + r] = home_row(self.delta, self.row_tmp, i, r)

    def wait(self, i):
        self._copy(i).wait_recv()
        self._copy(i).wait_send()


class TableSum:
    def __init__(self, part, refs):
        self.part = part
        self.snd1, self.rcv1, self.snd2, self.rcv2, self.snd3, self.rcv3, self.s, self.r = refs
        f = lax.axis_index("fsdp")
        self.core, self.x, self.c = lax.rem(f, 2), lax.div(f, 2), lax.axis_index("ctx")
        self.near, self.far = f + 1 - 2 * self.core, lax.rem(f + 2, 4)

    @staticmethod
    def scratch(heads):
        shapes = [(heads, 2, 2, 24, 256)] * 2 + [(heads, 2, 24, 256)] * 2 + [(heads, 24, 256)] * 2
        return [*[pltpu.VMEM(s, BF) for s in shapes], pltpu.SemaphoreType.DMA((3,)),
                pltpu.SemaphoreType.DMA((3,))]

    def _copy(self, n):
        src, dst = ((self.snd1, self.rcv1), (self.snd2, self.rcv2), (self.snd3, self.rcv3))[n]
        where = ({"fsdp": self.near}, {"fsdp": self.far}, {"ctx": 1 - self.c})[n]
        return remote(src, dst, self.s.at[n], self.r.at[n], where)

    def rows(self, core, x, c):
        return pl.ds(pl.multiple_of(core * 96 + x * 48 + c * 24, 8), 24)

    def start(self):
        for x in range(2):
            for c in range(2):
                self.snd1[:, x, c] = self.part[:, self.rows(1 - self.core, x, c), :].astype(BF)
        self._copy(0).start()

    def pair(self):
        self._copy(0).wait_recv()
        x = 1 - self.x
        for c in range(2):
            self.snd2[:, c] = (
                self.part[:, self.rows(self.core, x, c), :] + self.rcv1[:, x, c].astype(F32)
            ).astype(BF)
        self._copy(1).start()

    def cross(self):
        self._copy(1).wait_recv()
        c = 1 - self.c
        self.snd3[...] = (
            self.part[:, self.rows(self.core, self.x, c), :] + self.rcv1[:, self.x, c].astype(F32)
            + self.rcv2[:, c].astype(F32)
        ).astype(BF)
        self._copy(2).start()

    def finish(self, out):
        self._copy(2).wait_recv()
        out[...] = (
            self.part[:, self.rows(self.core, self.x, self.c), :]
            + self.rcv1[:, self.x, self.c].astype(F32)
            + self.rcv2[:, self.c].astype(F32) + self.rcv3[...].astype(F32)
        )

    def first_row(self):
        return self.core * 96 + self.x * 48 + self.c * 24

    def drain(self):
        for n in range(3):
            self._copy(n).wait_send()


def total_of(x):
    return jnp.sum(jnp.sum(x, axis=1, keepdims=True), axis=0, keepdims=True)


def exact(a, b, dims):
    return lax.dot_general(
        a, b, (dims, ((), ())), precision=lax.Precision.HIGHEST, preferred_element_type=F32
    )


def lane_sums(squares):
    return exact(jnp.ones((8, squares.shape[1]), F32), squares, ((1,), (1,)))[0:1]


def as_column(row):
    n = row.shape[1]
    step = 64
    eye = lax.broadcasted_iota(jnp.int32, (step, step), 0) == lax.broadcasted_iota(
        jnp.int32, (step, step), 1
    )
    return jnp.concatenate(
        [
            jnp.sum(
                jnp.where(eye, jnp.broadcast_to(row[:, at : at + step], (step, step)), 0.0),
                axis=1, keepdims=True,
            )
            for at in range(0, n, step)
        ],
        axis=0,
    )


def lane_pack(values):
    lane = lax.broadcasted_iota(jnp.int32, (8, 128), 1)
    packed = jnp.zeros((8, 128), F32)
    for n, value in enumerate(values):
        packed = packed + jnp.where(lane == n, jnp.broadcast_to(value, (8, 128)), 0.0)
    return packed


def wide(ref):
    if ref.shape[1] != 128:
        return ref[...]
    return jnp.concatenate([ref[n : n + 1, :] for n in range(ref.shape[0])], axis=1)


def put_wide(ref, row):
    if ref.shape[1] != 128:
        ref[...] = row
    else:
        for n in range(ref.shape[0]):
            ref[n : n + 1, :] = row[:, n * 128 : (n + 1) * 128]


def plain(grad, state):
    new = DECAY_RATE * state + (1.0 - DECAY_RATE) * (grad * grad + STAT_EPS)
    return new, grad * lax.rsqrt(new)


def step_body(*refs):
    (
        (feat, og, regions, ridx_m, w_qkv, w_proj, w_up, w_down, w_norm, w_heads, w_hidden, w_table),
        (row_qkv, col_qkv, row_proj, col_proj, row_up, col_up, row_down, col_down),
        (s_norm, s_heads, s_hidden, s_table),
        (home_o, gin_o, gq_o, gp_o, gu_o, gd_o, gn_o, gh_o, gx_o, gt_o, uq_o, up_o, uu_o, ud_o),
        (rq_o, kq_o, rp_o, kp_o, ru_o, ku_o, rd_o, kd_o, size_o),
        (sm_g, wq, wp_g, wp, wu, wd, fh, gh, og_low, bias_s, row_tmp, rows, ridx, table_t, small),
        (xw, ogw, n1, q, k, v, probs, ctx, part),
        (n2_s, hid_s, dpl_s, xhat_s, rstd_s, tot_two, gu, gd, dft, dbr, mix),
        (dh_s, dpos_s, chunk_s, tot_four),
        ls_two, ls_four, up_refs, down_refs, qkv_refs, proj_refs, table_refs,
        (sm_s, sm_r, t_s, f_s, z_s, c_s),
        (w_send, w_recv, p_send, p_recv, v_send, v_recv, h_send, h_recv, a_send, a_recv,
         b_send, b_recv, x_send, x_recv),
        (sm_send, sm_recv, t_send, t_recv, f_send, f_recv, z_send, z_recv, c_send, c_recv),
    ) = take(refs, (12, 8, 4, 14, 9, 15, 9, 11, 4, 10, 10, 8, 8, 8, 8, 8, 6, 14, 10))
    windows, heads = probs.shape[0], probs.shape[1]
    images = windows // 2
    width = q.shape[2]
    shard = w_qkv.shape[1]
    hidden = w_up.shape[1]
    ff = 4 * hidden
    f, c, t = lax.axis_index("fsdp"), lax.axis_index("ctx"), lax.axis_index("tp")
    near, far = f + 1 - 2 * lax.rem(f, 2), lax.rem(f + 2, 4)
    me = f * 4 + t
    two = LineSum.build(part, ls_two, tot_two)
    four = LineSum.build(part, ls_four, tot_four)
    mixl = LineSum.build(mix, ls_two, tot_two)

    def block(at):
        return pl.ds(pl.multiple_of(at * shard, shard), shard)

    def band(at):
        return pl.ds(pl.multiple_of(at * width, width), width)

    def other(n):
        at = lax.rem(me + n, 16)
        return {"fsdp": lax.div(at, 4), "tp": lax.rem(at, 4)}

    up = ShardSum(lambda at: gu[block(at), :], gu_o, up_refs)
    down = ShardSum(lambda at: gd[block(at), :], gd_o, down_refs)
    qkv = ShardSum(
        lambda at: jnp.stack([gu[block(at), n * 256 : n * 256 + width] for n in range(3)]),
        gq_o, qkv_refs,
    )
    proj = ShardSum(lambda at: gd[block(at), :shard], gp_o, proj_refs)
    table = TableSum(dpos_s, table_refs)
    barrier = pltpu.get_barrier_semaphore()
    greet(barrier, [{"ctx": 1 - c}] + [other(n) for n in range(1, 16)])

    part_of = HD // 4

    def ints(shape, axis):
        return lax.broadcasted_iota(jnp.int32, shape, axis)

    def ones_where(cond):
        return jnp.where(cond, 1.0, 0.0).astype(BF)

    def flat_units(values, count):
        lanes = count * part_of
        spread = dot(values, ones_where(jnp.bitwise_and(ints((part_of, lanes), 1), 7) == ints((part_of, lanes), 0)))
        return jnp.sum(
            jnp.where(jnp.right_shift(ints((count, lanes), 1), 3) == ints((count, lanes), 0), spread, 0.0),
            axis=0, keepdims=True,
        )

    wq[:, block(f), :] = w_qkv[...].astype(BF)
    wp_g[f, band(t), :] = w_proj[...].astype(BF)
    units = hidden // HD
    lanes = units * part_of
    spread = dot(
        w_hidden[...].astype(BF),
        ones_where(jnp.right_shift(ints((units, lanes), 1), 3) == ints((units, lanes), 0)),
    )
    hidden_row = jnp.sum(
        jnp.where(jnp.bitwise_and(ints((8, lanes), 1), 7) == ints((8, lanes), 0), spread, 0.0),
        axis=0, keepdims=True,
    )
    own = jnp.concatenate([w_norm[...], jnp.zeros((2, shard), F32), hidden_row, jnp.zeros((7, shard), F32)], axis=0)
    small[0:16, :shard] = own
    small[0:16, shard:] = jnp.zeros((16, D - shard), F32)
    for n in range(2):
        small[9 + n : 10 + n, : heads * part_of] = flat_units(w_heads[:, n, :].astype(BF), heads)
    sm_g[f] = small[0:16, :shard].astype(BF)
    wu[block(f), :] = w_up[...].astype(BF)
    wd[block(f), :] = w_down[...].astype(BF)
    for i in range(images):
        og_low[i] = og[i, 0:SHIFT].astype(BF)
    pl.semaphore_wait(barrier, 16)

    items = [
        lambda at: sm_g.at[at],
        lambda at: wq.at[:, block(at), :],
        lambda at: wu.at[block(at), :],
        lambda at: wd.at[block(at), :],
    ]

    def copy_of(n, kind, at, where):
        ref = items[n](at)
        return remote(ref, ref, w_send.at[n, kind], w_recv.at[n, kind], {"fsdp": where})

    def proj_copy(n, kind, at, where):
        ref = wp_g.at[at, band(lax.rem(t - n + 4, 4))]
        return remote(ref, ref, p_send.at[n, kind], p_recv.at[n, kind], {"fsdp": where})

    def proj_line(n):
        ref = wp_g.at[f, band(t)]
        return remote(ref, ref, v_send.at[n], v_recv.at[n], {"tp": lax.rem(t + n, 4)})

    halo_f = [
        remote(feat.at[i, 0:SHIFT], fh.at[i], h_send.at[i], h_recv.at[i], {"ctx": 1 - c})
        for i in range(images)
    ]
    halo_g = [
        remote(og_low.at[i], gh.at[i], h_send.at[images + i], h_recv.at[images + i], {"ctx": 1 - c})
        for i in range(images)
    ]

    def send_both(n):
        copy_of(n, 0, f, far).start()
        copy_of(n, 1, f, near).start()

    def proj_both(n):
        proj_copy(n, 0, f, far).start()
        proj_copy(n, 1, f, near).start()

    send_both(0)
    for copy in halo_f:
        copy.start()
    for n in range(1, 4):
        proj_line(n).start()
    send_both(1)
    proj_both(0)

    def relay(n):
        copy_of(n, 0, f, far).wait_recv()
        copy_of(n, 2, far, near).start()

    def gathered(n):
        copy_of(n, 1, f, near).wait_recv()
        copy_of(n, 2, far, near).wait_recv()

    ridx[...] = jnp.zeros_like(ridx)
    ridx[:TOK, :TOK] = ridx_m[...]
    table_t[...] = jnp.zeros_like(table_t)
    table_t[:heads, : w_table.shape[1]] = w_table[...].astype(BF).astype(F32)

    def bias_rows(step, carry):
        rows_at = pl.ds(pl.multiple_of(step * 8, 8), 8)
        for half in range(2):
            lanes_at = slice(half * 128, (half + 1) * 128)
            idx = ridx[rows_at, lanes_at]
            low = jnp.bitwise_and(idx, 127)
            high = jnp.right_shift(idx, 7)
            picks = [high == n for n in range(5)]
            for h in range(heads):
                found = jnp.zeros((8, 128), F32)
                for n in range(5):
                    tab = jnp.broadcast_to(table_t[h : h + 1, n * 128 : (n + 1) * 128], (8, 128))
                    got = jnp.take_along_axis(tab, low, axis=1, mode="promise_in_bounds")
                    found = jnp.where(picks[n], got, found)
                bias_s[h, rows_at, lanes_at] = found
        return carry

    lax.fori_loop(0, TOK // 8, bias_rows, 0)
    relay(0)
    dpos_s[...] = jnp.zeros_like(dpos_s)
    for n in range(1, 4):
        proj_line(n).wait_recv()
        proj_both(n)
    send_both(2)
    send_both(3)
    for copy in halo_g:
        copy.start()
    gathered(0)
    rows[...] = jnp.concatenate([sm_g[n].astype(F32) for n in range(4)], axis=1)
    unit = ints((shard, D), 0)
    lane = ints((shard, D), 1)
    biases = jnp.zeros((16, D), F32)
    for n in range(4):
        same = jnp.logical_and(
            jnp.right_shift(lane, 5) == jnp.right_shift(unit, 3),
            jnp.bitwise_and(lane, 31) == jnp.bitwise_and(unit, 7) + n * 8,
        )
        biases = biases + dot(sm_g[n], ones_where(same))
    rows[8:16, :] = biases[8:16, :]
    small[...] = jnp.zeros_like(small)
    relay(1)

    def enter(i):
        halo_f[i].wait_recv()
        window_rows(
            lambda im, r: feat[im, SHIFT + r] if r < SHIFT else fh[im, r - SHIFT], row_tmp, i, xw
        )

    enter(0)
    gain_one, offset_one = rows[0:1, :], rows[1:2, :]
    bias_proj, gain_two, offset_two = rows[2:3, :], rows[3:4, :], rows[4:5, :]
    bias_hidden = rows[8:9, :]
    bias_q, bias_v = rows[9:10, :width], rows[10:11, :width]
    head_of = jnp.right_shift(ints((1, width), 1), 5)
    picks_of = [ones_where(head_of == h) for h in range(heads)]

    def over(p):
        return jnp.right_shift(p * 171, 11)

    def region_forms(w):
        i, j = lax.div(w, 2), lax.rem(w, 2)
        both = regions[i].astype(F32)
        square = jnp.where(j == 0, both[:, :WIN], both[:, WIN:]).astype(BF)
        p_row, r_row = ints((WIN, TOK), 1), ints((WIN, TOK), 0)
        spread_row = dot(square, ones_where(p_row - WIN * over(p_row) == r_row))
        row = jnp.sum(jnp.where(over(p_row) == r_row, spread_row, 0.0), axis=0, keepdims=True)
        p_col, r_col = ints((TOK, WIN), 0), ints((TOK, WIN), 1)
        spread_col = dot(ones_where(over(p_col) == r_col), square)
        col = jnp.sum(
            jnp.where(p_col - WIN * over(p_col) == r_col, spread_col, 0.0), axis=1, keepdims=True
        )
        return row, col

    def spot(w):
        return pl.ds(pl.multiple_of(w * TOK, TOK), TOK)

    def add_rows(n, term):
        small[n : n + 1, : term.shape[1]] = small[n : n + 1, : term.shape[1]] + jnp.sum(
            term, axis=0, keepdims=True
        )

    def ctx_copy(w, n):
        ref = ctx.at[w, t]
        return remote(ref, ref, x_send.at[w, n], x_recv.at[w, n], {"tp": lax.rem(t + n, 4)})

    gathered(1)

    def forward(w, carry):
        @pl.when(w == 2)
        def _():
            enter(1)

        x = xw[w]
        centred = x - row_mean(x)
        xhat = centred * lax.rsqrt(row_mean(centred * centred) + NORM_EPS)
        normed = (xhat * gain_one + offset_one).astype(BF)
        n1[spot(w), :] = normed
        q_w = (dot(normed, wq[0]) + bias_q).astype(BF)
        k_w = dot(normed, wq[1]).astype(BF)
        v_w = (dot(normed, wq[2]) + bias_v).astype(BF)
        q[w] = q_w
        k[w] = k_w
        v[w] = v_w
        reg_row, reg_col = region_forms(w)
        mask = jnp.where(reg_col == reg_row, 0.0, MASK_FILL)
        context = jnp.zeros((TOK, width), F32)
        for h in range(heads):
            scores = dot_t(q_w * picks_of[h], k_w) * HD ** (-0.5) + bias_s[h, :, :TOK] + mask
            lifted = jnp.exp(scores - jnp.max(scores, axis=-1, keepdims=True))
            p = lifted / jnp.sum(lifted, axis=-1, keepdims=True)
            probs[w, h] = p
            context = context + dot(p.astype(BF), v_w * picks_of[h])
        ctx[w, t] = context.astype(BF)
        for n in (2, 1, 3):
            ctx_copy(w, n).start()
        return carry

    lax.fori_loop(0, windows, forward, 0)
    for n in range(4):
        proj_copy(n, 0, f, far).wait_recv()
        proj_copy(n, 2, far, near).start()
    relay(2)
    relay(3)
    for n in range(4):
        proj_copy(n, 1, f, near).wait_recv()
        proj_copy(n, 2, far, near).wait_recv()
    wp[...] = jnp.concatenate([wp_g[n] for n in range(4)], axis=1)
    gathered(2)
    gathered(3)

    def middle(w, carry):
        for n in range(1, 4):
            ctx_copy(w, n).wait_recv()
        branch = jnp.zeros((TOK, D), F32) + bias_proj
        for n in range(4):
            branch = branch + dot(ctx[w, n], wp[n * width : (n + 1) * width, :])
        resid = xw[w] + branch
        centred = resid - row_mean(resid)
        rstd = lax.rsqrt(row_mean(centred * centred) + NORM_EPS)
        xhat = centred * rstd
        xhat_s[w] = xhat
        rstd_s[w] = jnp.broadcast_to(rstd, (TOK, 128))
        normed = (xhat * gain_two + offset_two).astype(BF)
        n2_s[spot(w), :] = normed
        pre = dot(normed, wu[...]) + bias_hidden
        cdf = 0.5 * (1.0 + lax.erf(pre * 0.7071067811865476))
        slope = cdf + pre * (jnp.exp(-0.5 * (pre * pre)) * 0.3989422804014327)
        hid = (pre * cdf).astype(BF)
        hid_s[spot(w), :] = hid

        for n in range(images):

            @pl.when(w == 2 * n)
            def _():
                halo_g[n].wait_recv()
                window_rows(
                    lambda im, r: og[im, SHIFT + r] if r < SHIFT else gh[im, r - SHIFT],
                    row_tmp, n, ogw,
                )

        @pl.when(w >= 1)
        def _():
            two.cross(w - 1)

        low = ogw[w].astype(BF)
        d_pre = dot(low, wd[...]) * slope
        add_rows(6, d_pre)
        dpl = d_pre.astype(BF)
        dpl_s[spot(w), :] = dpl
        two.put(w, dot_t(dpl, wu[...]))
        two.start(w)
        mixl.put(w, dot_t(hid, wd[...]))

        @pl.when(two.is_mid)
        def _():
            whole = branch + rows[5:6, :]
            for s in range(2):
                for h in range(2):

                    @pl.when(two.own == h)
                    def _():
                        mix[2 * w + s, h] = (
                            mix[2 * w + s, h]
                            + whole[s * ROWS : (s + 1) * ROWS, h * HALF : (h + 1) * HALF]
                        )

        @pl.when(w >= 1)
        def _():
            two.settle(w - 1)

        @pl.when(w >= 2)
        def _():
            two.hand(w - 2)

        return carry

    lax.fori_loop(0, windows, middle, 0)
    two.cross(windows - 1)

    def grad_chunk(m, carry):
        chunk = pl.ds(pl.multiple_of(m * 256, 256), 256)
        low = jnp.concatenate([ogw[w, :, chunk] for w in range(windows)], axis=0).astype(BF)
        gd[chunk, :] = t_dot(low, hid_s[...])
        gu[chunk, :] = t_dot(n2_s[:, chunk], dpl_s[...])
        return carry

    lax.fori_loop(0, 1, grad_chunk, 0)
    two.hand(windows - 2)
    lax.fori_loop(1, 2, grad_chunk, 0)
    two.settle(windows - 1)
    lax.fori_loop(2, D // 256, grad_chunk, 0)
    down.start()
    up.start()

    def backward(w, carry):
        two.arrive(w)
        d_two = two.get(w)
        xhat = xhat_s[w]
        e = d_two * gain_two
        d_flat = (e - row_mean(e) - xhat * row_mean(e * xhat)) * rstd_s[w, :, 0:1]
        og_w = ogw[w]
        d_resid = og_w + d_flat
        dft[w] = d_flat
        d_branch = d_resid.astype(BF)
        dbr[spot(w), :] = d_branch
        for n, term in ((2, d_resid), (3, d_two * xhat), (4, d_two), (5, og_w)):
            add_rows(n, term)
        d_ctx = dot_t(d_branch, wp[band(t), :]).astype(BF)
        q_w, k_w, v_w = q[w], k[w], v[w]
        d_q = jnp.zeros((TOK, width), F32)
        d_k = jnp.zeros((TOK, width), F32)
        d_v = jnp.zeros((TOK, width), F32)
        for h in range(heads):
            if h == heads // 2:

                @pl.when(w >= 1)
                def _():
                    four.cross(w - 1)

                @pl.when(w == 0)
                def _():
                    two.hand(windows - 1)

            d_ctx_h = d_ctx * picks_of[h]
            p = probs[w, h]
            d_p = dot_t(d_ctx_h, v_w)
            d_v = d_v + t_dot(p.astype(BF), d_ctx_h)
            d_s = p * (d_p - jnp.sum(p * d_p, axis=-1, keepdims=True))
            dpos_s[h, :TOK, :TOK] = dpos_s[h, :TOK, :TOK] + d_s
            d_l = (d_s * HD ** (-0.5)).astype(BF)
            d_q = d_q + dot(d_l, k_w * picks_of[h])
            d_k = d_k + t_dot(d_l, q_w * picks_of[h])
        partial = jnp.zeros((TOK, D), F32)
        for n, d_n in enumerate((d_q, d_k, d_v)):
            low = d_n.astype(BF)
            dh_s[n, spot(w), :] = low
            partial = partial + dot_t(low, wq[n])
            if n != 1:
                add_rows(8 + n // 2, low.astype(F32))
        four.put(w, partial)
        four.start(w)

        @pl.when(w >= 1)
        def _():
            four.settle(w - 1)

        @pl.when(w >= 2)
        def _():
            four.hand(w - 2)

        @pl.when(w == 1)
        def _():
            down.pair()
            up.pair()

        @pl.when(w == windows - 1)
        def _():
            down.cross()
            up.cross()

        return carry

    lax.fori_loop(0, windows, backward, 0)
    for n in range(3):
        gu[:, n * 256 : n * 256 + width] = t_dot(n1[...], dh_s[n])
    qkv.start()
    ctx_own = jnp.concatenate([ctx[w, t] for w in range(windows)], axis=0)
    gp = t_dot(ctx_own, dbr[...])
    for n in range(4):
        gd[n * width : (n + 1) * width, :shard] = gp[:, n * shard : (n + 1) * shard]
    proj.start()
    four.cross(windows - 1)
    table.start()
    for w in range(windows):
        two.drain(w)
        mixl.start(w)
    four.hand(windows - 2)
    four.settle(windows - 1)

    keep = 1.0 - DECAY_RATE
    first_f = jnp.where(f == 0, 1.0, 0.0)
    first_t = jnp.where(t == 0, 1.0, 0.0)
    old_rows = [
        first_t * jnp.sum(row_qkv[0:1, :], axis=1, keepdims=True),
        first_t * jnp.sum(row_qkv[1:2, :], axis=1, keepdims=True),
        first_t * jnp.sum(row_qkv[2:3, :], axis=1, keepdims=True),
        first_f * total_of(row_proj[...]),
        first_t * total_of(row_up[...]),
        first_f * total_of(row_down[...]),
    ]
    masters = [
        sum(total_of(w_qkv[n] * w_qkv[n]) for n in range(3)),
        total_of(w_proj[...] * w_proj[...]),
        total_of(w_up[...] * w_up[...]),
        total_of(w_down[...] * w_down[...]),
        *[
            first_t * jnp.sum(w_norm[n : n + 1, :] * w_norm[n : n + 1, :], axis=1, keepdims=True)
            for n in range(6)
        ],
        *[total_of(w_heads[:, n, :] * w_heads[:, n, :]) for n in range(2)],
        total_of(w_hidden[...] * w_hidden[...]),
        first_f * total_of(w_table[...] * w_table[...]),
    ]
    qkv.pair()
    proj.pair()
    table.pair()
    down.finish()
    up.finish()
    t_s[t] = jnp.zeros((8, shard), F32)
    f_s[f] = jnp.zeros((8, hidden), F32)
    sq_up = gu_o[...] * gu_o[...]
    sq_down = gd_o[...] * gd_o[...]
    t_s[t, 4:5, :] = lane_sums(sq_up)
    t_s[t, 5:6, :] = lane_sums(sq_down)
    f_s[f, 4:5, :] = jnp.sum(sq_up, axis=0, keepdims=True)
    f_s[f, 5:6, :] = jnp.sum(sq_down, axis=0, keepdims=True)
    tot_up, tot_down = total_of(sq_up), total_of(sq_down)

    for copy in halo_g:
        copy.wait_send()
    home_in = HomeRows(xhat_s, row_tmp, gin_o, og_low, a_send, a_recv)

    def back(w):
        four.arrive(w)
        x = xw[w]
        centred = x - row_mean(x)
        rstd = lax.rsqrt(row_mean(centred * centred) + NORM_EPS)
        xhat = centred * rstd
        d_one = four.get(w)
        e = d_one * gain_one
        xhat_s[w] = dft[w] + (e - row_mean(e) - xhat * row_mean(e * xhat)) * rstd
        for n, term in ((0, d_one * xhat), (1, d_one)):
            add_rows(n, term)

    back(0)
    back(1)
    home_in.go(0)
    four.hand(windows - 1)
    table.cross()
    mixl.cross(0)
    qkv.cross()
    proj.cross()
    mixl.settle(0)
    mixl.cross(1)
    table.finish(chunk_s)
    first = table.first_row()
    ident = ints((640, TOK), 0)

    def bin_row(step, acc):
        for n in range(4):
            i = step * 4 + n
            hot = ones_where(ident == ridx[pl.ds(first + i, 1), :TOK])
            vals = jnp.concatenate(
                [chunk_s[h, pl.ds(i, 1), :TOK] for h in range(heads)]
                + [jnp.zeros((8 - heads, TOK), F32)],
                axis=0,
            )
            high = vals.astype(BF)
            low = (vals - high.astype(F32)).astype(BF)
            acc = acc + dot_t(jnp.concatenate([high, low], axis=0), hot)
        return acc

    hist = lax.fori_loop(0, 6, bin_row, jnp.zeros((16, 640), F32))
    small[16:24, :640] = hist[0:8] + hist[8:16]
    back(2)
    back(3)
    sm_s[0] = small[...]

    def swap(n):
        where = ({"fsdp": near}, {"fsdp": far}, {"ctx": 1 - c})[n]
        return remote(sm_s.at[n], sm_r.at[n], sm_send.at[n], sm_recv.at[n], where)

    swap(0).start()
    home_in.go(1)
    mixl.settle(1)
    mixl.hand(0)
    mixl.cross(2)
    swap(0).wait_recv()
    sm_s[1] = sm_s[0] + sm_r[0]
    swap(1).start()
    qkv.finish()
    proj.finish()

    tot_q = []
    for n in range(3):
        sq = gq_o[n] * gq_o[n]
        t_s[t, n : n + 1, :] = lane_sums(sq)
        f_s[f, n : n + 1, :width] = jnp.sum(sq, axis=0, keepdims=True)
        tot_q.append(total_of(sq))
    sq = gp_o[...] * gp_o[...]
    f_s[f, 3:4, :shard] = lane_sums(sq)
    t_s[t, 3:4, :] = jnp.sum(sq, axis=0, keepdims=True)
    z_s[me] = lane_pack([*tot_q, total_of(sq), tot_up, tot_down, *old_rows, *masters])

    def t_copy(n):
        return remote(t_s.at[t], t_s.at[t], t_send.at[n], t_recv.at[n], {"tp": lax.rem(t + n, 4)})

    def f_copy(n):
        return remote(f_s.at[f], f_s.at[f], f_send.at[n], f_recv.at[n], {"fsdp": lax.rem(f + n, 4)})

    def z_copy(n):
        return remote(z_s.at[me], z_s.at[me], z_send.at[n], z_recv.at[n], other(n))

    def c_copy(n):
        return remote(c_s.at[me], c_s.at[me], c_send.at[n], c_recv.at[n], other(n))

    for n in range(1, 4):
        t_copy(n).start()
        f_copy(n).start()
    for n in range(1, 16):
        z_copy(n).start()
    swap(1).wait_recv()
    sm_s[2] = sm_s[1] + sm_r[1]
    swap(2).start()
    mixl.settle(2)
    mixl.hand(1)
    mixl.cross(3)

    swap(2).wait_recv()
    sm = sm_s[2] + sm_r[2]

    def own_lanes(x, size):
        out = x[:, :size]
        for n in range(1, 4):
            out = jnp.where(f == n, x[:, n * size : (n + 1) * size], out)
        return out

    def own_units(row, count):
        all_lanes = count * HD
        at_lane = ints((count, all_lanes), 1)
        only = jnp.where(
            jnp.right_shift(at_lane, 5) == ints((count, all_lanes), 0),
            jnp.broadcast_to(row, (count, all_lanes)), 0.0,
        )
        pick = jnp.where(
            jnp.bitwise_and(ints((all_lanes, part_of), 0), HD - 1)
            == f * part_of + ints((all_lanes, part_of), 1),
            1.0, 0.0,
        )
        return only, pick

    gn = own_lanes(sm[0:6, :], shard)
    gh_new = [exact(*own_units(sm[8 + n : 9 + n, :width], heads), ((1,), (0,))) for n in range(2)]
    only, pick = own_units(sm[6:7, :], hidden // HD)
    gx = exact(pick, only, ((0,), (1,)))
    gt = sm[16 : 16 + heads, : w_table.shape[1]]
    gn_o[...] = gn
    gx_o[...] = gx
    gt_o[...] = gt
    small_sq = first_t * total_of(plain(gn, s_norm[...])[1] ** 2)
    for n in range(2):
        gh_o[:, n, :] = gh_new[n]
        small_sq = small_sq + total_of(plain(gh_new[n], s_heads[:, n, :])[1] ** 2)
    small_sq = small_sq + total_of(plain(gx, s_hidden[...])[1] ** 2)
    small_sq = small_sq + first_f * total_of(plain(gt, s_table[...])[1] ** 2)

    for n in range(1, 4):
        t_copy(n).wait_recv()
        f_copy(n).wait_recv()
    t_sum = t_s[0] + t_s[1] + t_s[2] + t_s[3]
    f_sum = f_s[0] + f_s[1] + f_s[2] + f_s[3]
    for n in range(1, 16):
        z_copy(n).wait_recv()
    z_sum = z_s[0]
    for n in range(1, 16):
        z_sum = z_sum + z_s[n]
    lane8 = ints((8, 128), 1)

    def scalar(n):
        return jnp.sum(jnp.where(lane8 == n, z_sum, 0.0)[0:1], axis=1, keepdims=True)

    def fresh(old, summed, count):
        return DECAY_RATE * old + keep * (summed / count + STAT_EPS)

    rq = fresh(row_qkv[...], t_sum[0:3, :], D)
    kq = fresh(col_qkv[...], f_sum[0:3, :width], D)
    rp = fresh(wide(row_proj), f_sum[3:4, :width], D)
    kp = fresh(wide(col_proj), t_sum[3:4, :], D)
    ru = fresh(wide(row_up), t_sum[4:5, :], ff)
    ku = fresh(wide(col_up), f_sum[4:5, :], D)
    rd = fresh(wide(row_down), f_sum[5:6, :], D)
    kd = fresh(wide(col_down), t_sum[5:6, :], ff)

    def mean_row(n, rows_all, cols_all):
        return (
            DECAY_RATE * scalar(6 + n) + keep * (scalar(n) / cols_all + rows_all * STAT_EPS)
        ) / rows_all

    scale_q = [
        as_column(lax.rsqrt(rq[n : n + 1, :] / mean_row(n, D, D))) * lax.rsqrt(kq[n : n + 1, :])
        for n in range(3)
    ]
    scale_p = as_column(lax.rsqrt(rp / mean_row(3, D, D))) * lax.rsqrt(kp)
    scale_u = as_column(lax.rsqrt(ru / mean_row(4, D, ff))) * lax.rsqrt(ku)
    scale_d = as_column(lax.rsqrt(kd)) * lax.rsqrt(rd / mean_row(5, ff, D))
    big_sq = small_sq
    for n in range(3):
        u = gq_o[n] * scale_q[n]
        uq_o[n] = u
        big_sq = big_sq + total_of(u * u)
    for grad, scale, ref in ((gp_o, scale_p, up_o), (gu_o, scale_u, uu_o), (gd_o, scale_d, ud_o)):
        u = grad[...] * scale
        ref[...] = u
        big_sq = big_sq + total_of(u * u)
    c_s[me] = jnp.broadcast_to(big_sq, (8, 128))
    for n in range(1, 16):
        c_copy(n).start()
    mixl.settle(3)
    mixl.hand(2)
    rq_o[...] = rq
    kq_o[...] = kq
    for ref, row in ((rp_o, rp), (kp_o, kp), (ru_o, ru), (ku_o, ku), (rd_o, rd), (kd_o, kd)):
        put_wide(ref, row)

    home_out = HomeRows(dft, row_tmp, home_o, fh, b_send, b_recv)

    def lift(w):
        mixl.arrive(w)
        dft[w] = mixl.get(w)

    lift(0)
    lift(1)
    home_out.go(0)
    mixl.hand(3)
    lift(2)
    lift(3)
    home_out.go(1)

    counts = [3 * D * D, D * D, D * ff, ff * D] + [D] * 8 + [ff, RELP * HEADS]
    sizes = [jnp.sqrt(scalar(12 + n) / counts[n] + STAT_EPS) for n in range(14)]
    for n in range(1, 16):
        c_copy(n).wait_recv()
    all_sq = c_s[0]
    for n in range(1, 16):
        all_sq = all_sq + c_s[n]
    count_all = 4 * D * D + 2 * D * ff + 8 * D + ff + RELP * HEADS
    clip = jnp.sqrt(all_sq[0:1, 0:1] / count_all)
    factor = STEP_RATE / jnp.maximum(1.0, clip / CLIP_LEVEL)
    size_o[...] = lane_pack([size * factor for size in sizes] + [clip])
    for i in range(images):
        home_in.wait(i)
        home_out.wait(i)
    for n in range(3):
        swap(n).wait_send()
    for n in range(1, 4):
        t_copy(n).wait_send()
        f_copy(n).wait_send()
        proj_line(n).wait_send()
        for w in range(windows):
            ctx_copy(w, n).wait_send()
    for n in range(1, 16):
        z_copy(n).wait_send()
        c_copy(n).wait_send()
    for w in range(windows):
        mixl.drain(w)
        four.drain(w)
    for copy in halo_f:
        copy.wait_send()
    for n in range(4):
        copy_of(n, 0, f, far).wait_send()
        copy_of(n, 1, f, near).wait_send()
        copy_of(n, 2, far, near).wait_send()
        proj_copy(n, 0, f, far).wait_send()
        proj_copy(n, 1, f, near).wait_send()
        proj_copy(n, 2, far, near).wait_send()
    for member in (up, down, qkv, proj, table):
        member.drain()
def finish_body(*refs):
    (
        (home_out, feat, home_in, og, gq, gp, g_up, g_down, gn, gh, gx, gt, uq, up, uu, ud),
        (w_qkv, w_proj, w_up, w_down, w_norm, w_heads, w_hidden, w_table),
        (s_norm, s_heads, s_hidden, s_table),
        stats, (size,),
        (out_o, gin_o, gq_o, gp_o, gu_o, gd_o, gn_o, gh_o, gx_o, gt_o),
        (nq_o, np_o, nu_o, nd_o, nn_o, nh_o, nx_o, nt_o),
        (cq_o, cp_o, cu_o, cd_o),
        stats_o, (sn_o, sh_o, sx_o, st_o), (clip_o,),
    ) = take(refs, (16, 8, 4, 8, 1, 10, 8, 4, 8, 4, 1))
    lane8 = lax.broadcasted_iota(jnp.int32, (8, 128), 1)
    table = size[...]

    def step(n):
        return jnp.sum(jnp.where(lane8 == n, table, 0.0)[0:1], axis=1, keepdims=True)

    out_o[...] = feat[...].astype(F32) + home_out[...].astype(F32)
    gin_o[...] = og[...] + home_in[...].astype(F32)
    for src, dst in (
        (gq, gq_o), (gp, gp_o), (g_up, gu_o), (g_down, gd_o), (gn, gn_o), (gh, gh_o), (gx, gx_o),
        (gt, gt_o), *zip(stats, stats_o),
    ):
        dst[...] = src[...]
    for n, (master, u, new_o, low_o) in enumerate(
        ((w_qkv, uq, nq_o, cq_o), (w_proj, up, np_o, cp_o), (w_up, uu, nu_o, cu_o), (w_down, ud, nd_o, cd_o))
    ):
        new = master[...] - step(n) * u[...]
        new_o[...] = new
        low_o[...] = new.astype(BF)
    sn, un = plain(gn[...], s_norm[...])
    sn_o[...] = sn
    for n in range(6):
        nn_o[n : n + 1, :] = w_norm[n : n + 1, :] - step(4 + n) * un[n : n + 1, :]
    for n in range(2):
        sh, uh = plain(gh[:, n, :], s_heads[:, n, :])
        sh_o[:, n, :] = sh
        nh_o[:, n, :] = w_heads[:, n, :] - step(10 + n) * uh
    sx, ux = plain(gx[...], s_hidden[...])
    sx_o[...] = sx
    nx_o[...] = w_hidden[...] - step(12) * ux
    st, ut = plain(gt[...], s_table[...])
    st_o[...] = st
    nt_o[...] = w_table[...] - step(13) * ut
    clip_o[...] = step(14)


def whole_step(feat, og, regions, rel_index, masters, stats, states):
    w_qkv, w_proj, w_up, w_down, w_norm, w_heads, w_hidden, w_table = masters
    images = feat.shape[0]
    windows = 2 * images
    shard, width = w_qkv.shape[1], w_qkv.shape[2]
    hidden = w_up.shape[1]
    heads = width // HD
    stats = [u if u.ndim == 2 else u.reshape(-1, 128) if u.shape[0] == D else u[None] for u in stats]
    like = lambda u: (u.shape, F32)
    mats = (w_qkv, w_proj, w_up, w_down)
    smalls = (w_norm, w_heads, w_hidden, w_table)
    vm, dma = pltpu.VMEM, pltpu.SemaphoreType.DMA
    flat = windows * TOK
    halves = (2 * windows, 2, ROWS, HALF)
    tokens = (windows, TOK, D)
    rows_of = (images, SHIFT, 24, D)
    outs = [
        (feat.shape, BF), (feat.shape, BF), *map(like, mats), *map(like, smalls), *map(like, mats),
        *map(like, stats), ((8, 128), F32),
    ]
    scratch = [
        vm((4, 16, shard), BF), vm((3, D, width), BF), vm((4, D, shard), BF), vm((D, D), BF),
        vm((D, hidden), BF), vm((D, hidden), BF), vm(rows_of, BF), vm(rows_of, BF), vm(rows_of, BF),
        vm((heads, TOK, 256), F32), vm((24, D), F32), vm((16, D), F32), vm((192, 256), jnp.int32),
        vm((8, 640), F32), vm((24, D), F32),
        vm(tokens, F32), vm(tokens, F32), vm((flat, D), BF), vm((windows, TOK, width), BF),
        vm((windows, TOK, width), BF), vm((windows, TOK, width), BF),
        vm((windows, heads, TOK, TOK), F32), vm((windows, 4, TOK, width), BF), vm(halves, F32),
        vm((flat, D), BF), vm((flat, hidden), BF), vm((flat, hidden), BF),
        vm(tokens, F32), vm((windows, TOK, 128), F32), vm(halves, BF), vm((D, hidden), F32),
        vm((D, hidden), F32), vm(tokens, F32), vm((flat, D), BF), vm(halves, F32),
        vm((3, flat, width), BF), vm((heads, 192, 256), F32), vm((heads, 24, 256), F32),
        vm(halves, BF),
        *LineSum.scratch(2 * windows), *LineSum.scratch(2 * windows),
        *ShardSum.scratch((shard, hidden)), *ShardSum.scratch((shard, hidden)),
        *ShardSum.scratch((3, shard, width)), *ShardSum.scratch((width, shard)),
        *TableSum.scratch(heads),
        vm((3, 24, D), F32), vm((3, 24, D), F32), vm((4, 8, shard), F32), vm((4, 8, hidden), F32),
        vm((16, 8, 128), F32), vm((16, 8, 128), F32),
        dma((4, 3)), dma((4, 3)), dma((4, 3)), dma((4, 3)), dma((4,)), dma((4,)),
        dma((2 * images,)), dma((2 * images,)), *[dma((images,))] * 4,
        dma((windows, 4)), dma((windows, 4)),
        dma((3,)), dma((3,)), *[dma((4,))] * 4, *[dma((16,))] * 4,
    ]
    got = vmem_call(step_body, outs, scratch, "whole_step", 1)(
        feat, og, regions, rel_index, *masters, *stats, *states
    )
    home_out, home_in, g_qkv, g_proj, g_up, g_down, gn, gh, gx, gt, uq, up, uu, ud, *rest = got
    new_stats, size = rest[:8], rest[8]
    outs = [
        like(og), like(og), *map(like, mats), *map(like, smalls), *map(like, masters),
        *[(u.shape, BF) for u in mats], *map(like, stats), *map(like, smalls), ((1, 1), F32),
    ]
    return vmem_call(finish_body, outs, [], "finish", None)(
        home_out, feat, home_in, og, g_qkv, g_proj, g_up, g_down, gn, gh, gx, gt, uq, up, uu, ud,
        *masters, *states, *new_stats, size,
    )


def per_device_plain(
    features,
    out_grad,
    regions,
    rel_index,
    w_qkv,
    w_proj,
    w_up,
    w_down,
    norm_vecs,
    head_bias,
    hidden_bias,
    rel_table,
    row_qkv,
    col_qkv,
    row_proj,
    col_proj,
    row_up,
    col_up,
    row_down,
    col_down,
    state_norm,
    state_heads,
    state_hidden,
    state_table,
):
    images, band_rows, across, model_width = features.shape
    win_tokens = WIN * WIN
    fsdp_at = lax.axis_index("fsdp")
    ctx_at = lax.axis_index("ctx")
    tp_at = lax.axis_index("tp")
    first_fsdp = (fsdp_at == 0).astype(jnp.float32)
    first_ctx = (ctx_at == 0).astype(jnp.float32)
    first_tp = (tp_at == 0).astype(jnp.float32)
    weights_qkv, weights_proj, weights_up, weights_down, vec_copy, head_copy, hidden_copy = (
        lax.all_gather(w_qkv.astype(jnp.bfloat16), "fsdp", axis=1, tiled=True),
        lax.all_gather(w_proj.astype(jnp.bfloat16), "fsdp", axis=1, tiled=True),
        lax.all_gather(w_up.astype(jnp.bfloat16), "fsdp", axis=0, tiled=True),
        lax.all_gather(w_down.astype(jnp.bfloat16), "fsdp", axis=1, tiled=True),
        lax.all_gather(norm_vecs.astype(jnp.bfloat16), "fsdp", axis=1, tiled=True),
        lax.all_gather(head_bias.astype(jnp.bfloat16), "fsdp", axis=2, tiled=True),
        lax.all_gather(hidden_bias.astype(jnp.bfloat16), "fsdp", axis=1, tiled=True),
    )
    norm_rows = vec_copy.astype(jnp.float32)
    bias_query = head_copy[0].reshape(-1).astype(jnp.float32)
    bias_value = head_copy[1].reshape(-1).astype(jnp.float32)
    bias_hidden = hidden_copy.reshape(-1).astype(jnp.float32)
    table_copy = rel_table.astype(jnp.bfloat16)
    local_width = weights_qkv.shape[2]
    heads_here = local_width // HD

    def roll_in(home):
        received = passed_along(home[:, :SHIFT], "ctx", -1)
        return to_windows(enter_frame(home, received)).reshape(-1, model_width)

    def roll_out(rolled_flat):
        band = jnp.roll(
            from_windows(
                rolled_flat.reshape(-1, win_tokens, model_width), images, band_rows, across
            ),
            SHIFT,
            axis=2,
        )
        lower = passed_along(band[:, band_rows - SHIFT :], "ctx", 1)
        return jnp.concatenate([lower, band[:, : band_rows - SHIFT]], axis=1)

    flat_one = roll_in(features).astype(jnp.float32)
    grad_flat = roll_in(out_grad)
    win_count = flat_one.shape[0] // win_tokens
    normed_one, pull_one = jax.vjp(layer_norm, flat_one, norm_rows[0], norm_rows[1])
    normed_one_low = normed_one.astype(jnp.bfloat16)
    head_shape = (win_count, win_tokens, heads_here, HD)
    query_low, key_low, value_low = project_heads(
        normed_one_low, weights_qkv, bias_query, bias_value, head_shape
    )
    pos_bias = table_lookup(table_copy, rel_index)
    region_win = to_windows(regions[..., None])[..., 0]
    mask_add = jnp.where(region_win[:, :, None] == region_win[:, None, :], 0.0, MASK_FILL).astype(
        jnp.float32
    )
    scores = attention_scores(query_low, key_low, pos_bias, mask_add)
    top_score = jnp.max(scores, axis=-1, keepdims=True)
    lifted = jnp.exp(scores - top_score)
    prob_rows = lifted / jnp.sum(lifted, axis=-1, keepdims=True)
    prob_low = prob_rows.astype(jnp.bfloat16)
    context = jnp.einsum("whij,wjhc->wihc", prob_low, value_low, preferred_element_type=jnp.float32)
    context_low = context.astype(jnp.bfloat16).reshape(-1, local_width)
    branch_part = jnp.dot(context_low, weights_proj, preferred_element_type=jnp.float32)
    branch = lax.psum(branch_part.astype(jnp.bfloat16), "tp").astype(jnp.float32) + norm_rows[2]
    flat_two = flat_one + branch
    normed_two, pull_two = jax.vjp(layer_norm, flat_two, norm_rows[3], norm_rows[4])
    normed_two_low = normed_two.astype(jnp.bfloat16)
    pre_act = jnp.dot(normed_two_low, weights_up, preferred_element_type=jnp.float32) + bias_hidden
    hidden, pull_gelu = jax.vjp(exact_gelu, pre_act)
    hidden_low = hidden.astype(jnp.bfloat16)
    mixed_part = jnp.dot(hidden_low, weights_down, preferred_element_type=jnp.float32)
    mixed_whole = lax.psum(mixed_part.astype(jnp.bfloat16), "tp").astype(jnp.float32)
    block_out = features.astype(jnp.float32) + roll_out(
        (branch + mixed_whole + norm_rows[5]).astype(jnp.bfloat16)
    ).astype(jnp.float32)
    grad_low = grad_flat.astype(jnp.bfloat16)
    grad_down_full = jnp.einsum(
        "tf,td->fd", hidden_low, grad_low, preferred_element_type=jnp.float32
    )
    grad_down_bias = jnp.sum(grad_flat, axis=0)
    d_hidden = jnp.einsum("td,fd->tf", grad_low, weights_down, preferred_element_type=jnp.float32)
    d_pre = pull_gelu(d_hidden)[0]
    d_pre_low = d_pre.astype(jnp.bfloat16)
    grad_hidden_bias = jnp.sum(d_pre, axis=0)
    grad_up_full = jnp.einsum(
        "td,tf->df", normed_two_low, d_pre_low, preferred_element_type=jnp.float32
    )
    d_two_part = jnp.einsum("tf,df->td", d_pre_low, weights_up, preferred_element_type=jnp.float32)
    d_two = lax.psum(d_two_part.astype(jnp.bfloat16), "tp").astype(jnp.float32)
    d_flat_two, grad_gain_two, grad_offset_two = pull_two(d_two)
    d_resid = grad_flat + d_flat_two
    grad_proj_bias = jnp.sum(d_resid, axis=0)
    d_branch = d_resid.astype(jnp.bfloat16)
    grad_proj_full = jnp.einsum(
        "tc,td->cd", context_low, d_branch, preferred_element_type=jnp.float32
    )
    d_context = (
        jnp.einsum("td,cd->tc", d_branch, weights_proj, preferred_element_type=jnp.float32)
        .astype(jnp.bfloat16)
        .reshape(head_shape)
    )
    d_probs = jnp.einsum(
        "wihc,wjhc->whij", d_context, value_low, preferred_element_type=jnp.float32
    )
    d_value_low = jnp.einsum(
        "whij,wihc->wjhc", prob_low, d_context, preferred_element_type=jnp.float32
    ).astype(jnp.bfloat16)
    d_scores = prob_rows * (d_probs - jnp.sum(prob_rows * d_probs, axis=-1, keepdims=True))
    d_pos = jnp.sum(d_scores, axis=0)
    d_scaled = (d_scores * HD ** (-0.5)).astype(jnp.bfloat16)
    d_query_low = jnp.einsum(
        "whij,wjhc->wihc", d_scaled, key_low, preferred_element_type=jnp.float32
    ).astype(jnp.bfloat16)
    d_key_low = jnp.einsum(
        "whij,wihc->wjhc", d_scaled, query_low, preferred_element_type=jnp.float32
    ).astype(jnp.bfloat16)
    d_heads = jnp.stack([d_query_low, d_key_low, d_value_low]).reshape(3, -1, local_width)
    grad_qkv_full = jnp.einsum(
        "td,ktc->kdc", normed_one_low, d_heads, preferred_element_type=jnp.float32
    )
    grad_head_bias = jnp.stack(
        [
            jnp.sum(d_heads[0].astype(jnp.float32), axis=0),
            jnp.sum(d_heads[2].astype(jnp.float32), axis=0),
        ]
    ).reshape(2, heads_here, HD)
    d_one_part = jnp.einsum("ktc,kdc->td", d_heads, weights_qkv, preferred_element_type=jnp.float32)
    d_one = lax.psum(d_one_part.astype(jnp.bfloat16), "tp").astype(jnp.float32)
    d_flat_one, grad_gain_one, grad_offset_one = pull_one(d_one)
    grad_input = out_grad + roll_out((d_flat_two + d_flat_one).astype(jnp.bfloat16)).astype(
        jnp.float32
    )
    table_part = table_grad(d_pos, rel_index, rel_table.shape[0])
    grad_norm_full = jnp.stack(
        [
            grad_gain_one,
            grad_offset_one,
            grad_proj_bias,
            grad_gain_two,
            grad_offset_two,
            grad_down_bias,
        ]
    )
    grad_list = (
        grad_qkv_full,
        grad_proj_full,
        grad_up_full,
        grad_down_full,
        grad_norm_full,
        grad_head_bias,
        grad_hidden_bias.reshape(-1, HD),
    )
    g_qkv, g_proj, g_up, g_down, g_norm, g_heads, g_hidden = shard_sum(band_sum(grad_list))
    d_shard = w_qkv.shape[1]
    hidden_here = w_up.shape[1]
    keep = 1.0 - DECAY_RATE
    sq_qkv = g_qkv * g_qkv
    sq_proj = g_proj * g_proj
    sq_up = g_up * g_up
    sq_down = g_down * g_down
    stat_rq = place(
        (keep * jnp.sum(sq_qkv, axis=2) / D + first_tp * (DECAY_RATE * row_qkv + keep * STAT_EPS))
        * first_ctx,
        fsdp_at,
        D,
    )
    stat_cq = place(
        (keep * jnp.sum(sq_qkv, axis=1) / D + first_fsdp * (DECAY_RATE * col_qkv + keep * STAT_EPS))
        * first_ctx,
        tp_at,
        D,
    )
    stat_rp = place(
        (
            keep * jnp.sum(sq_proj, axis=1) / D
            + first_fsdp * (DECAY_RATE * row_proj + keep * STAT_EPS)
        )
        * first_ctx,
        tp_at,
        D,
    )
    stat_cp = place(
        (keep * jnp.sum(sq_proj, axis=0) / D + first_tp * (DECAY_RATE * col_proj + keep * STAT_EPS))
        * first_ctx,
        fsdp_at,
        D,
    )
    stat_ru = place(
        (keep * jnp.sum(sq_up, axis=1) / FF + first_tp * (DECAY_RATE * row_up + keep * STAT_EPS))
        * first_ctx,
        fsdp_at,
        D,
    )
    stat_cu = place(
        (keep * jnp.sum(sq_up, axis=0) / D + first_fsdp * (DECAY_RATE * col_up + keep * STAT_EPS))
        * first_ctx,
        tp_at,
        FF,
    )
    stat_rd = place(
        (
            keep * jnp.sum(sq_down, axis=1) / D
            + first_fsdp * (DECAY_RATE * row_down + keep * STAT_EPS)
        )
        * first_ctx,
        tp_at,
        FF,
    )
    stat_cd = place(
        (
            keep * jnp.sum(sq_down, axis=0) / FF
            + first_tp * (DECAY_RATE * col_down + keep * STAT_EPS)
        )
        * first_ctx,
        fsdp_at,
        D,
    )
    table_whole = place(table_part, tp_at, HEADS)
    master_sq = jnp.concatenate(
        [
            jnp.stack(
                [
                    jnp.sum(w_qkv * w_qkv),
                    jnp.sum(w_proj * w_proj),
                    jnp.sum(w_up * w_up),
                    jnp.sum(w_down * w_down),
                ]
            )
            * first_ctx,
            jnp.sum(norm_vecs * norm_vecs, axis=1) * first_ctx * first_tp,
            jnp.sum(head_bias * head_bias, axis=(1, 2)) * first_ctx,
            jnp.sum(hidden_bias * hidden_bias)[None] * first_ctx,
            jnp.sum(rel_table * rel_table)[None] * first_ctx * first_fsdp,
        ]
    )
    (
        full_rq,
        full_cq,
        full_rp,
        full_cp,
        full_ru,
        full_cu,
        full_rd,
        full_cd,
        table_sum,
        master_total,
    ) = lax.psum(
        (
            stat_rq,
            stat_cq,
            stat_rp,
            stat_cp,
            stat_ru,
            stat_cu,
            stat_rd,
            stat_cd,
            table_whole,
            master_sq,
        ),
        ("fsdp", "ctx", "tp"),
    )
    u_qkv = factored(
        g_qkv,
        own_part(full_rq, fsdp_at, d_shard),
        own_part(full_cq, tp_at, local_width),
        jnp.mean(full_rq, axis=1)[:, None, None],
    )
    u_proj = factored(
        g_proj,
        own_part(full_rp, tp_at, local_width),
        own_part(full_cp, fsdp_at, d_shard),
        jnp.mean(full_rp),
    )
    u_up = factored(
        g_up,
        own_part(full_ru, fsdp_at, d_shard),
        own_part(full_cu, tp_at, hidden_here),
        jnp.mean(full_ru),
    )
    u_down = factored(
        g_down,
        own_part(full_rd, tp_at, hidden_here),
        own_part(full_cd, fsdp_at, d_shard),
        jnp.mean(full_rd),
    )
    g_table = own_part(table_sum, tp_at, heads_here)
    state_norm_new, u_norm = plain_stats(g_norm, state_norm)
    state_heads_new, u_heads = plain_stats(g_heads, state_heads)
    state_hidden_new, u_hidden = plain_stats(g_hidden, state_hidden)
    state_table_new, u_table = plain_stats(g_table, state_table)
    local_sq = (
        jnp.sum(u_qkv * u_qkv)
        + jnp.sum(u_proj * u_proj)
        + jnp.sum(u_up * u_up)
        + jnp.sum(u_down * u_down)
        + jnp.sum(u_heads * u_heads)
        + jnp.sum(u_hidden * u_hidden)
        + first_tp * jnp.sum(u_norm * u_norm)
        + first_fsdp * jnp.sum(u_table * u_table)
    )
    total_sq = lax.psum(local_sq, ("fsdp", "tp"))
    count_all = 4 * D * D + 2 * D * FF + 8 * D + FF + RELP * HEADS
    clip_rms = jnp.sqrt(total_sq / count_all)
    factor = 1.0 / jnp.maximum(1.0, clip_rms / CLIP_LEVEL)
    counts = jnp.array(
        [3 * D * D, D * D, D * FF, FF * D, D, D, D, D, D, D, D, D, FF, RELP * HEADS], jnp.float32
    )
    scales = jnp.sqrt(master_total / counts + STAT_EPS)
    new_qkv = w_qkv - STEP_RATE * scales[0] * factor * u_qkv
    new_proj = w_proj - STEP_RATE * scales[1] * factor * u_proj
    new_up = w_up - STEP_RATE * scales[2] * factor * u_up
    new_down = w_down - STEP_RATE * scales[3] * factor * u_down
    new_norm = norm_vecs - STEP_RATE * scales[4:10][:, None] * factor * u_norm
    new_heads = head_bias - STEP_RATE * scales[10:12][:, None, None] * factor * u_heads
    new_hidden = hidden_bias - STEP_RATE * scales[12] * factor * u_hidden
    new_table = rel_table - STEP_RATE * scales[13] * factor * u_table
    return (
        block_out,
        grad_input,
        g_qkv,
        g_proj,
        g_up,
        g_down,
        g_norm,
        g_heads,
        g_hidden,
        g_table,
        new_qkv,
        new_proj,
        new_up,
        new_down,
        new_norm,
        new_heads,
        new_hidden,
        new_table,
        new_qkv.astype(jnp.bfloat16),
        new_proj.astype(jnp.bfloat16),
        new_up.astype(jnp.bfloat16),
        new_down.astype(jnp.bfloat16),
        own_part(full_rq, fsdp_at, d_shard),
        own_part(full_cq, tp_at, local_width),
        own_part(full_rp, tp_at, local_width),
        own_part(full_cp, fsdp_at, d_shard),
        own_part(full_ru, fsdp_at, d_shard),
        own_part(full_cu, tp_at, hidden_here),
        own_part(full_rd, tp_at, hidden_here),
        own_part(full_cd, fsdp_at, d_shard),
        state_norm_new,
        state_heads_new,
        state_hidden_new,
        state_table_new,
        clip_rms,
    )


def per_device(
    features,
    out_grad,
    regions,
    rel_index,
    w_qkv,
    w_proj,
    w_up,
    w_down,
    norm_vecs,
    head_bias,
    hidden_bias,
    rel_table,
    row_qkv,
    col_qkv,
    row_proj,
    col_proj,
    row_up,
    col_up,
    row_down,
    col_down,
    state_norm,
    state_heads,
    state_hidden,
    state_table,
):
    flip = lambda u: u.transpose(1, 0, 2)
    (block_out, grad_input, g_qkv, g_proj, g_up, g_down, g_norm, g_heads, g_hidden, g_table,
     new_qkv, new_proj, new_up, new_down, new_norm, new_heads, new_hidden, new_table,
     copy_qkv, copy_proj, copy_up, copy_down, *rest) = whole_step(
        features, out_grad, regions, rel_index,
        (w_qkv, w_proj, w_up, w_down.T, norm_vecs, flip(head_bias), hidden_bias.T, rel_table.T),
        (row_qkv, col_qkv, row_proj, col_proj, row_up, col_up, row_down, col_down),
        (state_norm, flip(state_heads), state_hidden.T, state_table.T))
    factors, states, clip_rms = rest[:8], rest[8:12], rest[12]
    factors = list(factors[:2]) + [u.reshape(-1) for u in factors[2:]]
    return (
        block_out, grad_input, g_qkv, g_proj, g_up, g_down.T, g_norm, flip(g_heads), g_hidden.T,
        g_table.T, new_qkv, new_proj, new_up, new_down.T, new_norm, flip(new_heads), new_hidden.T,
        new_table.T, copy_qkv, copy_proj, copy_up, copy_down.T, *factors,
        states[0], flip(states[1]), states[2].T, states[3].T, clip_rms[0, 0],
    )


def solution(mesh):
    line_of_four = mesh.shape["fsdp"] == 4 and mesh.shape["tp"] == 4 and mesh.shape["ctx"] == 2
    return jax.shard_map(
        per_device if line_of_four else per_device_plain,
        mesh=mesh,
        in_specs=(
            P("fsdp", "ctx", None, None),
            P("fsdp", "ctx", None, None),
            P("fsdp", "ctx", None),
            P(),
            P(None, "fsdp", "tp"),
            P("tp", "fsdp"),
            P("fsdp", "tp"),
            P("tp", "fsdp"),
            P(None, "fsdp"),
            P(None, "tp", "fsdp"),
            P("tp", "fsdp"),
            P(None, "tp"),
            P(None, "fsdp"),
            P(None, "tp"),
            P("tp"),
            P("fsdp"),
            P("fsdp"),
            P("tp"),
            P("tp"),
            P("fsdp"),
            P(None, "fsdp"),
            P(None, "tp", "fsdp"),
            P("tp", "fsdp"),
            P(None, "tp"),
        ),
        out_specs=(
            P("fsdp", "ctx", None, None),
            P("fsdp", "ctx", None, None),
            P(None, "fsdp", "tp"),
            P("tp", "fsdp"),
            P("fsdp", "tp"),
            P("tp", "fsdp"),
            P(None, "fsdp"),
            P(None, "tp", "fsdp"),
            P("tp", "fsdp"),
            P(None, "tp"),
            P(None, "fsdp", "tp"),
            P("tp", "fsdp"),
            P("fsdp", "tp"),
            P("tp", "fsdp"),
            P(None, "fsdp"),
            P(None, "tp", "fsdp"),
            P("tp", "fsdp"),
            P(None, "tp"),
            P(None, "fsdp", "tp"),
            P("tp", "fsdp"),
            P("fsdp", "tp"),
            P("tp", "fsdp"),
            P(None, "fsdp"),
            P(None, "tp"),
            P("tp"),
            P("fsdp"),
            P("fsdp"),
            P("tp"),
            P("tp"),
            P("fsdp"),
            P(None, "fsdp"),
            P(None, "tp", "fsdp"),
            P("tp", "fsdp"),
            P(None, "tp"),
            P(),
        ),
        check_vma=False,
    )
```

```python
import functools

import jax
import jax.numpy as jnp
from jax import lax
from jax.experimental import pallas as pl
from jax.experimental.pallas import tpu as pltpu
from jax.sharding import PartitionSpec as P


D = 768
HEADS = 24
HD = 32
FF = 3072
WIN = 12
SHIFT = 6
RELP = 529


DECAY_RATE = 0.5
STAT_EPS = 1e-06
NORM_EPS = 1e-05
MASK_FILL = -100.0
STEP_RATE = 1.0
CLIP_LEVEL = 0.25


def passed_along(x, axis, by):
    count = lax.axis_size(axis)
    return lax.ppermute(x, axis, [(i, (i + by) % count) for i in range(count)])


def layer_norm(values, gain_row, offset):
    mean_val = jnp.mean(values, axis=-1, keepdims=True)
    centred = values - mean_val
    var_val = jnp.mean(centred * centred, axis=-1, keepdims=True)
    return centred * lax.rsqrt(var_val + NORM_EPS) * gain_row + offset


def exact_gelu(values):
    return jax.nn.gelu(values, approximate=False)


def to_windows(values):
    image_count, row_count, col_count, channels = values.shape
    pieces = values.reshape(image_count, row_count // WIN, WIN, col_count // WIN, WIN, channels)
    return pieces.transpose(0, 1, 3, 2, 4, 5).reshape(-1, WIN * WIN, channels)


def from_windows(values, image_count, row_count, col_count):
    channels = values.shape[-1]
    pieces = values.reshape(image_count, row_count // WIN, col_count // WIN, WIN, WIN, channels)
    return pieces.transpose(0, 1, 3, 2, 4, 5).reshape(image_count, row_count, col_count, channels)


def enter_frame(own_rows, received):
    joined = jnp.concatenate([own_rows[:, SHIFT:], received], axis=1)
    return jnp.roll(joined, -SHIFT, axis=2)


def project_heads(normed_low, weights_qkv, bias_query, bias_value, head_shape):
    query_full = (
        jnp.dot(normed_low, weights_qkv[0], preferred_element_type=jnp.float32) + bias_query
    )
    key_full = jnp.dot(normed_low, weights_qkv[1], preferred_element_type=jnp.float32)
    value_full = (
        jnp.dot(normed_low, weights_qkv[2], preferred_element_type=jnp.float32) + bias_value
    )
    return tuple(
        (
            member.astype(jnp.bfloat16).reshape(head_shape)
            for member in (query_full, key_full, value_full)
        )
    )


def attention_scores(query_low, key_low, pos_bias, mask_add):
    products = jnp.einsum("wihc,wjhc->whij", query_low, key_low, preferred_element_type=jnp.float32)
    return products * query_low.shape[-1] ** (-0.5) + pos_bias[None] + mask_add[:, None]


def table_lookup(table_low, rel_index):
    win_tokens = rel_index.shape[0]
    code_ids = jnp.arange(table_low.shape[0], dtype=jnp.int32)
    index_blocks = rel_index.reshape(WIN, -1)

    def lookup(index_block):
        one_hot = (index_block[:, None] == code_ids[None, :]).astype(jnp.bfloat16)
        return jnp.dot(one_hot, table_low, preferred_element_type=jnp.float32)

    looked = lax.map(lookup, index_blocks)
    return looked.reshape(win_tokens, win_tokens, -1).transpose(2, 0, 1)


def table_grad(d_pos, rel_index, table_rows):
    heads_here = d_pos.shape[0]
    code_ids = jnp.arange(table_rows, dtype=jnp.int32)
    index_blocks = rel_index.reshape(WIN, -1)
    grad_blocks = d_pos.transpose(1, 2, 0).reshape(WIN, -1, heads_here)

    def accumulate(running, member):
        index_block, grad_block = member
        one_hot = (index_block[:, None] == code_ids[None, :]).astype(jnp.float32)
        added = lax.dot_general(
            one_hot,
            grad_block,
            (((0,), (0,)), ((), ())),
            precision=lax.Precision.HIGHEST,
            preferred_element_type=jnp.float32,
        )
        return (running + added, None)

    result_pair = lax.scan(
        accumulate, jnp.zeros((table_rows, heads_here), jnp.float32), (index_blocks, grad_blocks)
    )
    return result_pair[0]


def place(part_vec, index_at, whole_len):
    size_of = part_vec.shape[-1]
    base = jnp.zeros(part_vec.shape[:-1] + (whole_len,), jnp.float32)
    return lax.dynamic_update_slice_in_dim(base, part_vec, index_at * size_of, part_vec.ndim - 1)


def own_part(whole_vec, index_at, size_of):
    return lax.dynamic_slice_in_dim(whole_vec, index_at * size_of, size_of, whole_vec.ndim - 1)


def factored(grad, row_local, col_local, row_mean):
    return grad * lax.rsqrt(row_local[..., :, None] * col_local[..., None, :] / row_mean)


def plain_stats(grad, state_old):
    state_new = DECAY_RATE * state_old + (1.0 - DECAY_RATE) * (grad * grad + STAT_EPS)
    return (state_new, grad * lax.rsqrt(state_new))


def shard_sum(grad_list):
    return (
        lax.psum_scatter(grad_list[0], "fsdp", scatter_dimension=1, tiled=True),
        lax.psum_scatter(grad_list[1], "fsdp", scatter_dimension=1, tiled=True),
        lax.psum_scatter(grad_list[2], "fsdp", scatter_dimension=0, tiled=True),
        lax.psum_scatter(grad_list[3], "fsdp", scatter_dimension=1, tiled=True),
        lax.psum_scatter(grad_list[4], "fsdp", scatter_dimension=1, tiled=True),
        lax.psum_scatter(grad_list[5], "fsdp", scatter_dimension=2, tiled=True),
        lax.psum_scatter(grad_list[6], "fsdp", scatter_dimension=1, tiled=True),
    )


def band_sum(grad_list):
    return lax.psum(
        (
            grad_list[0],
            grad_list[1],
            grad_list[2],
            grad_list[3],
            grad_list[4],
            grad_list[5],
            grad_list[6],
        ),
        "ctx",
    )


BF = jnp.bfloat16
F32 = jnp.float32
MESH = pl.DeviceIdType.MESH
TOK = WIN * WIN
HALF = D // 2
ROWS = TOK // 2
VMEM_LIMIT = 67_043_328


def dot(a, b):
    return lax.dot_general(a, b, (((1,), (0,)), ((), ())), preferred_element_type=F32)


def dot_t(a, b):
    return lax.dot_general(a, b, (((1,), (1,)), ((), ())), preferred_element_type=F32)


def t_dot(a, b):
    return lax.dot_general(a, b, (((0,), (0,)), ((), ())), preferred_element_type=F32)


def row_mean(x):
    return jnp.sum(x, axis=-1, keepdims=True) * (1.0 / x.shape[-1])


def remote(src, dst, send, recv, where):
    return pltpu.make_async_remote_copy(
        src_ref=src, dst_ref=dst, send_sem=send, recv_sem=recv, device_id=where, device_id_type=MESH
    )


def greet(barrier, places):
    for place_of in places:
        pl.semaphore_signal(barrier, inc=1, device_id=place_of, device_id_type=MESH)


class LineSum:
    def __init__(self, part, send, from_outer, from_mid, total, sems):
        self.part, self.send, self.from_outer, self.from_mid, self.total = (
            part, send, from_outer, from_mid, total,
        )
        self.s_out, self.r_out, self.s_mid, self.r_mid, self.s_tot, self.r_tot, self.s_cross = sems
        z = lax.axis_index("tp")
        self.is_mid = jnp.logical_and(z > 0, z < 3)
        self.is_outer = jnp.logical_not(self.is_mid)
        self.outer = jnp.where(z < 2, 0, 3)
        self.mid = jnp.where(z < 2, 1, 2)
        self.other_mid = 3 - self.mid
        self.own = self.mid - 1
        self.other = 1 - self.own

    @staticmethod
    def scratch(count):
        return [
            pltpu.VMEM((count, 2, ROWS, HALF), BF),
            pltpu.VMEM((count, 2, ROWS, HALF), BF),
            pltpu.VMEM((count, ROWS, HALF), BF),
            pltpu.SemaphoreType.DMA((count, 2)),
            pltpu.SemaphoreType.DMA((count, 2)),
            pltpu.SemaphoreType.DMA((count,)),
            pltpu.SemaphoreType.DMA((count,)),
            pltpu.SemaphoreType.DMA((count, 2)),
            pltpu.SemaphoreType.DMA((count, 2)),
            pltpu.SemaphoreType.DMA((count,)),
        ]

    @staticmethod
    def build(part, refs, total):
        return LineSum(part, refs[0], refs[1], refs[2], total, refs[3:10])

    @staticmethod
    def peers():
        return 2

    def greet(self, barrier):
        pl.semaphore_signal(
            barrier, inc=1, device_id={"tp": jnp.where(self.is_mid, self.outer, self.mid)},
            device_id_type=MESH,
        )

        @pl.when(self.is_mid)
        def _():
            pl.semaphore_signal(
                barrier, inc=1, device_id={"tp": self.other_mid}, device_id_type=MESH
            )

    def greet_count(self):
        return jnp.where(self.is_mid, 2, 1)

    def _to_mid(self, w, h):
        return remote(self.send.at[w, h], self.from_outer.at[w, h], self.s_out.at[w, h],
                      self.r_out.at[w, h], {"tp": self.mid})

    def _across(self, w):
        return remote(self.send.at[w, self.other], self.from_mid.at[w], self.s_mid.at[w],
                      self.r_mid.at[w], {"tp": self.other_mid})

    def _total_across(self, w, h):
        return remote(self.total.at[w, h], self.total.at[w, h], self.s_cross.at[w],
                      self.r_tot.at[w, h], {"tp": self.other_mid})

    def _total_out(self, w, h):
        return remote(self.total.at[w, h], self.total.at[w, h], self.s_tot.at[w, h],
                      self.r_tot.at[w, h], {"tp": self.outer})

    def order(self, w):
        return (2 * w, 2 * w + 1)

    def put(self, w, value):
        for s in range(2):
            for h in range(2):
                self.part[2 * w + s, h] = value[s * ROWS : (s + 1) * ROWS, h * HALF : (h + 1) * HALF]

    def get(self, w):
        return jnp.concatenate(
            [
                jnp.concatenate([self.total[2 * w + s, h].astype(F32) for h in range(2)], axis=1)
                for s in range(2)
            ],
            axis=0,
        )

    def start(self, w):
        @pl.when(self.is_outer)
        def _():
            for h in (self.other, self.own):
                for j in self.order(w):
                    self.send[j, h] = self.part[j, h].astype(BF)
                    self._to_mid(j, h).start()

    def cross(self, w):
        @pl.when(self.is_mid)
        def _():
            for j in self.order(w):
                self._to_mid(j, self.other).wait_recv()
                self.send[j, self.other] = (
                    self.part[j, self.other] + self.from_outer[j, self.other].astype(F32)
                ).astype(BF)
                self._across(j).start()

    def settle(self, w):
        @pl.when(self.is_mid)
        def _():
            for j in (2 * w, 2 * w + 1):
                self._to_mid(j, self.own).wait_recv()
                self._across(j).wait_recv()
                self.total[j, self.own] = (
                    self.part[j, self.own]
                    + self.from_outer[j, self.own].astype(F32)
                    + self.from_mid[j].astype(F32)
                ).astype(BF)
                self._total_across(j, self.own).start()
                self._total_out(j, self.own).start()

    def hand(self, w):
        @pl.when(self.is_mid)
        def _():
            for j in (2 * w, 2 * w + 1):
                self._total_across(j, self.other).wait_recv()
                self._total_out(j, self.other).start()

    def arrive(self, w):
        @pl.when(self.is_outer)
        def _():
            for j in (2 * w, 2 * w + 1):
                self._total_out(j, 0).wait_recv()
                self._total_out(j, 1).wait_recv()

    def drain(self, w):
        @pl.when(self.is_outer)
        def _():
            for j in (2 * w, 2 * w + 1):
                self._to_mid(j, 0).wait_send()
                self._to_mid(j, 1).wait_send()

        @pl.when(self.is_mid)
        def _():
            for j in (2 * w, 2 * w + 1):
                self._across(j).wait_send()
                self._total_across(j, self.own).wait_send()
                self._total_out(j, 0).wait_send()
                self._total_out(j, 1).wait_send()


class TradeSum(LineSum):
    def __init__(self, base, away, sems):
        self.__dict__.update(base.__dict__)
        self.away, (self.s_ctx, self.r_ctx) = away, sems
        self.ctx = 1 - lax.axis_index("ctx")

    def order(self, w):
        return (2 * w + 1, 2 * w)

    def _trade(self, w):
        return remote(self.away.at[w], self.total.at[2 * w + 1, self.own], self.s_ctx.at[w],
                      self.r_ctx.at[w], {"ctx": self.ctx})

    def settle(self, w):
        @pl.when(self.is_mid)
        def _():
            for s, j in ((1, 2 * w + 1), (0, 2 * w)):
                self._to_mid(j, self.own).wait_recv()
                self._across(j).wait_recv()
                whole = (
                    self.part[j, self.own]
                    + self.from_outer[j, self.own].astype(F32)
                    + self.from_mid[j].astype(F32)
                ).astype(BF)
                if s == 1:
                    self.away[w] = whole
                    self._trade(w).start()
                else:
                    self.total[j, self.own] = whole
                    self._total_across(j, self.own).start()
                    self._total_out(j, self.own).start()

    def trade(self, w):
        @pl.when(self.is_mid)
        def _():
            j = 2 * w + 1
            self._trade(w).wait_recv()
            self._total_across(j, self.own).start()
            self._total_out(j, self.own).start()

    def drain(self, w):
        LineSum.drain(self, w)

        @pl.when(self.is_mid)
        def _():
            self._trade(w).wait_send()


class ShardSum:
    def __init__(self, block_of, out, refs):
        self.block_of, self.out = block_of, out
        self.snd1, self.rcv1, self.snd2, self.rcv2, self.snd3, self.rcv3, self.s, self.r = refs
        f = lax.axis_index("fsdp")
        core = lax.rem(f, 2)
        self.f, self.core = f, core
        self.near, self.far = f + 1 - 2 * core, lax.rem(f + 2, 4)
        self.ctx = 1 - lax.axis_index("ctx")

    @staticmethod
    def scratch(shape):
        return [
            pltpu.VMEM((2, *shape), BF), pltpu.VMEM((2, *shape), BF),
            pltpu.VMEM(shape, BF), pltpu.VMEM(shape, BF),
            pltpu.VMEM(shape, BF), pltpu.VMEM(shape, BF),
            pltpu.SemaphoreType.DMA((4,)), pltpu.SemaphoreType.DMA((4,)),
        ]

    def _near(self, x):
        return remote(self.snd1.at[x], self.rcv1.at[x], self.s.at[x], self.r.at[x], {"fsdp": self.near})

    def _far(self):
        return remote(self.snd2, self.rcv2, self.s.at[2], self.r.at[2], {"fsdp": self.far})

    def _ctx(self):
        return remote(self.snd3, self.rcv3, self.s.at[3], self.r.at[3], {"ctx": self.ctx})

    def start(self):
        for x in range(2):
            self.snd1[x] = self.block_of(2 * x + 1 - self.core).astype(BF)
            self._near(x).start()

    def pair(self):
        for x in range(2):
            self._near(x).wait_recv()
        other = lax.div(self.far, 2)
        self.snd2[...] = (self.block_of(self.far) + self.rcv1[other].astype(F32)).astype(BF)
        self._far().start()
        mine = lax.div(self.f, 2)
        self.out[...] = self.block_of(self.f) + self.rcv1[mine].astype(F32)

    def cross(self):
        self._far().wait_recv()
        self.snd3[...] = (self.out[...] + self.rcv2[...].astype(F32)).astype(BF)
        self._ctx().start()

    def finish(self):
        self._ctx().wait_recv()
        self.out[...] = self.snd3[...].astype(F32) + self.rcv3[...].astype(F32)

    def drain(self):
        for x in range(2):
            self._near(x).wait_send()
        self._far().wait_send()
        self._ctx().wait_send()


class BandFirstSum:
    def __init__(self, block_of, out, refs):
        self.block_of, self.out = block_of, out
        self.snd1, self.rcv1, self.sndy, self.rcvy, self.sndx, self.rcvx, self.sndf, self.rcvf = refs[:8]
        self.s, self.r = refs[8:]
        f = lax.axis_index("fsdp")
        self.f, self.core, self.x = f, lax.rem(f, 2), lax.div(f, 2)
        self.near, self.far = f + 1 - 2 * self.core, lax.rem(f + 2, 4)
        self.c = lax.axis_index("ctx")
        self.half = out.shape[0] // 2

    @staticmethod
    def scratch(shape):
        two = (2, *shape)
        half = (shape[0] // 2, shape[1])
        shapes = [two, two, (2, *half), (2, *half), half, half, half, half]
        return [*[pltpu.VMEM(u, BF) for u in shapes], pltpu.SemaphoreType.DMA((5,)),
                pltpu.SemaphoreType.DMA((5,))]

    def _near(self, x):
        return remote(self.snd1.at[x], self.rcv1.at[x], self.s.at[x], self.r.at[x], {"fsdp": self.near})

    def _copy(self, n):
        src, dst = ((self.sndy, self.rcvy), (self.sndx, self.rcvx), (self.sndf, self.rcvf))[n]
        where = {"fsdp": self.far} if n == 1 else {"ctx": 1 - self.c}
        return remote(src, dst, self.s.at[2 + n], self.r.at[2 + n], where)

    def _rows(self, c):
        return pl.ds(pl.multiple_of(c * self.half, self.half), self.half)

    def _sum(self, x, c):
        return self.block_of(2 * x + self.core, c * self.half, self.half) + self.rcv1[
            x, self._rows(c), :
        ].astype(F32)

    def start(self):
        for x in range(2):
            self.snd1[x] = self.block_of(2 * x + 1 - self.core, 0, 2 * self.half).astype(BF)
            self._near(x).start()

    def pair(self):
        for x in range(2):
            self._near(x).wait_recv()
            self.sndy[x] = self._sum(x, 1 - self.c).astype(BF)
        self._copy(0).start()

    def cross(self):
        self._copy(0).wait_recv()
        other = 1 - self.x
        self.sndx[...] = (self._sum(other, self.c) + self.rcvy[other].astype(F32)).astype(BF)
        self._copy(1).start()
        self.out[self._rows(self.c), :] = self._sum(self.x, self.c) + self.rcvy[self.x].astype(F32)

    def share(self):
        self._copy(1).wait_recv()
        self.sndf[...] = (self.out[self._rows(self.c), :] + self.rcvx[...].astype(F32)).astype(BF)
        self._copy(2).start()

    def finish(self):
        self._copy(2).wait_recv()
        self.out[self._rows(self.c), :] = self.sndf[...].astype(F32)
        self.out[self._rows(1 - self.c), :] = self.rcvf[...].astype(F32)

    def drain(self):
        for x in range(2):
            self._near(x).wait_send()
        for n in range(3):
            self._copy(n).wait_send()


def vmem_call(body, outs, scratch, name, collective_id, in_place=0, out_place=0):
    remote_kernel = {} if collective_id is None else dict(
        collective_id=collective_id, has_side_effects=True
    )

    def call(*args):
        return pl.pallas_call(
            body,
            out_shape=[jax.ShapeDtypeStruct(s, t) for s, t in outs],
            in_specs=[
                pl.BlockSpec(memory_space=pl.ANY if n < in_place else pltpu.VMEM)
                for n in range(len(args))
            ],
            out_specs=[
                pl.BlockSpec(memory_space=pl.ANY if n < out_place else pltpu.VMEM)
                for n in range(len(outs))
            ],
            scratch_shapes=scratch,
            compiler_params=pltpu.CompilerParams(vmem_limit_bytes=VMEM_LIMIT, **remote_kernel),
            name=name,
        )(*args)

    return call


def take(refs, counts):
    groups, at = [], 0
    for n in counts:
        groups.append(refs[at : at + n])
        at += n
    return groups


def window_rows(row_of, row_tmp, image, dst):
    for r in range(WIN):
        row_tmp[...] = row_of(image, r).astype(F32)
        dst[2 * image, r * WIN : (r + 1) * WIN, :] = row_tmp[SHIFT : SHIFT + WIN, :]
        dst[2 * image + 1, r * WIN : r * WIN + SHIFT, :] = row_tmp[SHIFT + WIN :, :]
        dst[2 * image + 1, r * WIN + SHIFT : (r + 1) * WIN, :] = row_tmp[:SHIFT, :]


def home_row(delta, row_tmp, image, r):
    row_tmp[SHIFT : SHIFT + WIN, :] = delta[2 * image, r * WIN : (r + 1) * WIN, :]
    row_tmp[SHIFT + WIN :, :] = delta[2 * image + 1, r * WIN : r * WIN + SHIFT, :]
    row_tmp[:SHIFT, :] = delta[2 * image + 1, r * WIN + SHIFT : (r + 1) * WIN, :]
    return row_tmp[...].astype(BF)


class HomeRows:
    def __init__(self, delta, row_tmp, out, halo, send, recv):
        self.delta, self.row_tmp, self.out, self.halo, self.s, self.r = (
            delta, row_tmp, out, halo, send, recv,
        )

    def _copy(self, i):
        return remote(self.halo.at[i], self.out.at[i, 0:SHIFT], self.s.at[i], self.r.at[i],
                      {"ctx": 1 - lax.axis_index("ctx")})

    def go(self, i):
        for r in range(SHIFT, WIN):
            self.halo[i, r - SHIFT] = home_row(self.delta, self.row_tmp, i, r)
        self._copy(i).start()
        for r in range(SHIFT):
            self.out[i, SHIFT + r] = home_row(self.delta, self.row_tmp, i, r)

    def wait(self, i):
        self._copy(i).wait_recv()
        self._copy(i).wait_send()


class TableSum:
    def __init__(self, part, refs):
        self.part = part
        self.snd1, self.rcv1, self.snd2, self.rcv2, self.snd3, self.rcv3, self.s, self.r = refs
        f = lax.axis_index("fsdp")
        self.core, self.x, self.c = lax.rem(f, 2), lax.div(f, 2), lax.axis_index("ctx")
        self.near, self.far = f + 1 - 2 * self.core, lax.rem(f + 2, 4)

    @staticmethod
    def scratch(heads):
        shapes = [(heads, 2, 2, 24, 256)] * 2 + [(heads, 2, 24, 256)] * 2 + [(heads, 24, 256)] * 2
        return [*[pltpu.VMEM(s, BF) for s in shapes], pltpu.SemaphoreType.DMA((3,)),
                pltpu.SemaphoreType.DMA((3,))]

    def _copy(self, n):
        src, dst = ((self.snd1, self.rcv1), (self.snd2, self.rcv2), (self.snd3, self.rcv3))[n]
        where = ({"fsdp": self.near}, {"fsdp": self.far}, {"ctx": 1 - self.c})[n]
        return remote(src, dst, self.s.at[n], self.r.at[n], where)

    def rows(self, core, x, c):
        return pl.ds(pl.multiple_of(core * 96 + x * 48 + c * 24, 8), 24)

    def start(self):
        for x in range(2):
            for c in range(2):
                self.snd1[:, x, c] = self.part[:, self.rows(1 - self.core, x, c), :].astype(BF)
        self._copy(0).start()

    def pair(self):
        self._copy(0).wait_recv()
        x = 1 - self.x
        for c in range(2):
            self.snd2[:, c] = (
                self.part[:, self.rows(self.core, x, c), :] + self.rcv1[:, x, c].astype(F32)
            ).astype(BF)
        self._copy(1).start()

    def cross(self):
        self._copy(1).wait_recv()
        c = 1 - self.c
        self.snd3[...] = (
            self.part[:, self.rows(self.core, self.x, c), :] + self.rcv1[:, self.x, c].astype(F32)
            + self.rcv2[:, c].astype(F32)
        ).astype(BF)
        self._copy(2).start()

    def finish(self, out):
        self._copy(2).wait_recv()
        out[...] = (
            self.part[:, self.rows(self.core, self.x, self.c), :]
            + self.rcv1[:, self.x, self.c].astype(F32)
            + self.rcv2[:, self.c].astype(F32) + self.rcv3[...].astype(F32)
        )

    def first_row(self):
        return self.core * 96 + self.x * 48 + self.c * 24

    def drain(self):
        for n in range(3):
            self._copy(n).wait_send()


def total_of(x):
    return jnp.sum(jnp.sum(x, axis=1, keepdims=True), axis=0, keepdims=True)


def exact(a, b, dims):
    return lax.dot_general(
        a, b, (dims, ((), ())), precision=lax.Precision.HIGHEST, preferred_element_type=F32
    )


def lane_sums(squares):
    return exact(jnp.ones((8, squares.shape[1]), F32), squares, ((1,), (1,)))[0:1]


def as_column(row):
    n = row.shape[1]
    step = 64
    eye = lax.broadcasted_iota(jnp.int32, (step, step), 0) == lax.broadcasted_iota(
        jnp.int32, (step, step), 1
    )
    return jnp.concatenate(
        [
            jnp.sum(
                jnp.where(eye, jnp.broadcast_to(row[:, at : at + step], (step, step)), 0.0),
                axis=1, keepdims=True,
            )
            for at in range(0, n, step)
        ],
        axis=0,
    )


def lane_pack(values):
    lane = lax.broadcasted_iota(jnp.int32, (8, 128), 1)
    packed = jnp.zeros((8, 128), F32)
    for n, value in enumerate(values):
        packed = packed + jnp.where(lane == n, jnp.broadcast_to(value, (8, 128)), 0.0)
    return packed


def wide(ref):
    if ref.shape[1] != 128:
        return ref[...]
    return jnp.concatenate([ref[n : n + 1, :] for n in range(ref.shape[0])], axis=1)


def put_wide(ref, row):
    if ref.shape[1] != 128:
        ref[...] = row
    else:
        for n in range(ref.shape[0]):
            ref[n : n + 1, :] = row[:, n * 128 : (n + 1) * 128]


def plain(grad, state):
    new = DECAY_RATE * state + (1.0 - DECAY_RATE) * (grad * grad + STAT_EPS)
    return new, grad * lax.rsqrt(new)


def update_scales(rq, kq, rp, kp, ru, ku, rd, kd, means):
    def outer(first, second):
        return as_column(lax.rsqrt(first)) * lax.rsqrt(second)

    return [
        *[outer(rq[n : n + 1, :] / means[n], kq[n : n + 1, :]) for n in range(3)],
        outer(rp / means[3], kp), outer(ru / means[4], ku), outer(kd, rd / means[5]),
    ]


def step_body(*refs):
    (
        big_inputs,
        (regions, ridx_m, w_norm, w_heads, w_hidden, w_table),
        (row_qkv, col_qkv, row_proj, col_proj, row_up, col_up, row_down, col_down),
        (s_norm, s_heads, s_hidden, s_table),
        (home_o, gin_o, gq_o, gp_o, gu_o, gd_o, gn_o, gh_o, gx_o, gt_o),
        (rq_o, kq_o, rp_o, kp_o, ru_o, ku_o, rd_o, kd_o, size_o),
        (sm_g, wq, wp_g, wp, wu, wd, fh, gh, og_low, bias_s, row_tmp, rows, ridx, table_t, small),
        (xw, ogw, n1, q, k, v, probs, ctx, part),
        (n2_s, hid_s, dpl_s, xhat_s, rstd_s, tot_two, gu, gd, dft, dbr, mix),
        (dh_s, dpos_s, chunk_s, tot_four),
        ls_two, ls_four, up_refs, down_refs, qkv_refs, proj_refs, table_refs,
        (sm_s, sm_r, t_s, f_s, z_s, c_s),
        (feat, og, w_qkv, w_proj, w_up, w_down), (tot_mix, away, y_send, y_recv, i_sem, d_send, d_recv),
        (w_send, w_recv, p_send, p_recv, v_send, v_recv, h_send, h_recv, a_send, a_recv,
         x_send, x_recv),
        (sm_send, sm_recv, t_send, t_recv, f_send, f_recv, z_send, z_recv, c_send, c_recv),
    ) = take(refs, (6, 6, 8, 4, 10, 9, 15, 9, 11, 4, 10, 10, 8, 10, 24, 8, 8, 6, 6, 7, 12, 10))
    windows, heads = probs.shape[0], probs.shape[1]
    images = windows // 2
    width = q.shape[2]
    shard = w_qkv.shape[1]
    hidden = w_up.shape[1]
    ff = 4 * hidden
    f, c, t = lax.axis_index("fsdp"), lax.axis_index("ctx"), lax.axis_index("tp")
    near, far = f + 1 - 2 * lax.rem(f, 2), lax.rem(f + 2, 4)
    me = f * 4 + t
    two = LineSum.build(part, ls_two, tot_two)
    four = LineSum.build(part, ls_four, tot_four)
    mixl = TradeSum(LineSum.build(mix, ls_two, tot_mix), away, (y_send, y_recv))

    def block(at):
        return pl.ds(pl.multiple_of(at * shard, shard), shard)

    def band(at):
        return pl.ds(pl.multiple_of(at * width, width), width)

    def other(n):
        at = lax.rem(me + n, 16)
        return {"fsdp": lax.div(at, 4), "tp": lax.rem(at, 4)}

    up = ShardSum(lambda at: gu[block(at), :], gu_o, up_refs)
    down = BandFirstSum(
        lambda at, first, size: gd[pl.ds(pl.multiple_of(at * shard + first, 32), size), :], gd_o, down_refs
    )
    qkv = [
        ShardSum(
            lambda at, n=n: gu[block(at), n * 256 : n * 256 + width], gq_o.at[n], qkv_refs[8 * n : 8 * n + 8]
        )
        for n in range(3)
    ]
    proj = ShardSum(lambda at: gd[block(at), :shard], gp_o, proj_refs)
    table = TableSum(dpos_s, table_refs)
    barrier = pltpu.get_barrier_semaphore()
    greet(barrier, [{"ctx": 1 - c}] + [other(n) for n in range(1, 16)])
    fetch = [
        pltpu.make_async_copy(src, dst, i_sem.at[n])
        for n, (src, dst) in enumerate(zip(big_inputs, (feat, og, w_qkv, w_proj, w_up, w_down)))
    ]
    for n in (2, 3, 0, 4, 5, 1):
        fetch[n].start()

    part_of = HD // 4

    def ints(shape, axis):
        return lax.broadcasted_iota(jnp.int32, shape, axis)

    def ones_where(cond):
        return jnp.where(cond, 1.0, 0.0).astype(BF)

    def flat_units(values, count):
        lanes = count * part_of
        spread = dot(values, ones_where(jnp.bitwise_and(ints((part_of, lanes), 1), 7) == ints((part_of, lanes), 0)))
        return jnp.sum(
            jnp.where(jnp.right_shift(ints((count, lanes), 1), 3) == ints((count, lanes), 0), spread, 0.0),
            axis=0, keepdims=True,
        )

    units = hidden // HD
    lanes = units * part_of
    spread = dot(
        w_hidden[...].astype(BF),
        ones_where(jnp.right_shift(ints((units, lanes), 1), 3) == ints((units, lanes), 0)),
    )
    hidden_row = jnp.sum(
        jnp.where(jnp.bitwise_and(ints((8, lanes), 1), 7) == ints((8, lanes), 0), spread, 0.0),
        axis=0, keepdims=True,
    )
    own = jnp.concatenate([w_norm[...], jnp.zeros((2, shard), F32), hidden_row, jnp.zeros((7, shard), F32)], axis=0)
    small[0:16, :shard] = own
    small[0:16, shard:] = jnp.zeros((16, D - shard), F32)
    for n in range(2):
        small[9 + n : 10 + n, : heads * part_of] = flat_units(w_heads[:, n, :].astype(BF), heads)
    sm_g[f] = small[0:16, :shard].astype(BF)
    fetch[2].wait()
    wq[:, block(f), :] = w_qkv[...].astype(BF)
    fetch[3].wait()
    wp_g[f, band(t), :] = w_proj[...].astype(BF)
    fetch[0].wait()
    fetch[4].wait()
    wu[block(f), :] = w_up[...].astype(BF)
    fetch[5].wait()
    wd[block(f), :] = w_down[...].astype(BF)
    fetch[1].wait()
    for i in range(images):
        og_low[i] = og[i, 0:SHIFT].astype(BF)
    pl.semaphore_wait(barrier, 16)

    items = [
        lambda at: sm_g.at[at],
        lambda at: wq.at[:, block(at), :],
        lambda at: wu.at[block(at), :],
    ]
    half = shard // 2

    def down_copy(n, at, cc, where):
        ref = wd.at[block(at), :] if cc is None else wd.at[
            pl.ds(pl.multiple_of(at * shard + cc * half, half), half), :
        ]
        return remote(ref, ref, d_send.at[n], d_recv.at[n], where)

    down_copies = (
        down_copy(0, f, c, {"fsdp": far}), down_copy(1, f, None, {"fsdp": near}),
        down_copy(2, far, c, {"ctx": 1 - c}), down_copy(3, far, c, {"fsdp": near}),
        down_copy(4, far, 1 - c, {"fsdp": near}),
    )

    def copy_of(n, kind, at, where):
        ref = items[n](at)
        return remote(ref, ref, w_send.at[n, kind], w_recv.at[n, kind], {"fsdp": where})

    def proj_copy(n, kind, at, where):
        ref = wp_g.at[at, band(lax.rem(t - n + 4, 4))]
        return remote(ref, ref, p_send.at[n, kind], p_recv.at[n, kind], {"fsdp": where})

    def proj_line(n):
        ref = wp_g.at[f, band(t)]
        return remote(ref, ref, v_send.at[n], v_recv.at[n], {"tp": lax.rem(t + n, 4)})

    halo_f = [
        remote(feat.at[i, 0:SHIFT], fh.at[i], h_send.at[i], h_recv.at[i], {"ctx": 1 - c})
        for i in range(images)
    ]
    halo_g = [
        remote(og_low.at[i], gh.at[i], h_send.at[images + i], h_recv.at[images + i], {"ctx": 1 - c})
        for i in range(images)
    ]

    def send_both(n):
        copy_of(n, 0, f, far).start()
        copy_of(n, 1, f, near).start()

    def proj_both(n):
        proj_copy(n, 0, f, far).start()
        proj_copy(n, 1, f, near).start()

    send_both(0)
    for copy in halo_f:
        copy.start()
    for n in range(1, 4):
        proj_line(n).start()
    send_both(1)
    proj_both(0)
    down_copies[0].start()
    halo_g[0].start()

    def relay(n):
        copy_of(n, 0, f, far).wait_recv()
        copy_of(n, 2, far, near).start()

    def gathered(n):
        copy_of(n, 1, f, near).wait_recv()
        copy_of(n, 2, far, near).wait_recv()

    ridx[...] = jnp.zeros_like(ridx)
    ridx[:TOK, :TOK] = ridx_m[...]
    table_t[...] = jnp.zeros_like(table_t)
    table_t[:heads, : w_table.shape[1]] = w_table[...].astype(BF).astype(F32)

    def bias_rows(step, carry):
        rows_at = pl.ds(pl.multiple_of(step * 8, 8), 8)
        for half in range(2):
            lanes_at = slice(half * 128, (half + 1) * 128)
            idx = ridx[rows_at, lanes_at]
            low = jnp.bitwise_and(idx, 127)
            high = jnp.right_shift(idx, 7)
            picks = [high == n for n in range(5)]
            for h in range(heads):
                found = jnp.zeros((8, 128), F32)
                for n in range(5):
                    tab = jnp.broadcast_to(table_t[h : h + 1, n * 128 : (n + 1) * 128], (8, 128))
                    got = jnp.take_along_axis(tab, low, axis=1, mode="promise_in_bounds")
                    found = jnp.where(picks[n], got, found)
                bias_s[h, rows_at, lanes_at] = found
        return carry

    lax.fori_loop(0, TOK // 8, bias_rows, 0)
    relay(0)
    dpos_s[...] = jnp.zeros_like(dpos_s)
    for n in range(1, 4):
        proj_line(n).wait_recv()
        proj_both(n)
    send_both(2)
    down_copies[1].start()
    gathered(0)
    rows[...] = jnp.concatenate([sm_g[n].astype(F32) for n in range(4)], axis=1)
    unit = ints((shard, D), 0)
    lane = ints((shard, D), 1)
    biases = jnp.zeros((16, D), F32)
    for n in range(4):
        same = jnp.logical_and(
            jnp.right_shift(lane, 5) == jnp.right_shift(unit, 3),
            jnp.bitwise_and(lane, 31) == jnp.bitwise_and(unit, 7) + n * 8,
        )
        biases = biases + dot(sm_g[n], ones_where(same))
    rows[8:16, :] = biases[8:16, :]
    small[...] = jnp.zeros_like(small)
    relay(1)

    def enter(i):
        halo_f[i].wait_recv()
        window_rows(
            lambda im, r: feat[im, SHIFT + r] if r < SHIFT else fh[im, r - SHIFT], row_tmp, i, xw
        )

    enter(0)
    gain_one, offset_one = rows[0:1, :], rows[1:2, :]
    bias_proj, gain_two, offset_two = rows[2:3, :], rows[3:4, :], rows[4:5, :]
    bias_hidden = rows[8:9, :]
    bias_q, bias_v = rows[9:10, :width], rows[10:11, :width]
    head_of = jnp.right_shift(ints((1, width), 1), 5)
    picks_of = [ones_where(head_of == h) for h in range(heads)]

    def over(p):
        return jnp.right_shift(p * 171, 11)

    def region_forms(w):
        i, j = lax.div(w, 2), lax.rem(w, 2)
        both = regions[i].astype(F32)
        square = jnp.where(j == 0, both[:, :WIN], both[:, WIN:]).astype(BF)
        p_row, r_row = ints((WIN, TOK), 1), ints((WIN, TOK), 0)
        spread_row = dot(square, ones_where(p_row - WIN * over(p_row) == r_row))
        row = jnp.sum(jnp.where(over(p_row) == r_row, spread_row, 0.0), axis=0, keepdims=True)
        p_col, r_col = ints((TOK, WIN), 0), ints((TOK, WIN), 1)
        spread_col = dot(ones_where(over(p_col) == r_col), square)
        col = jnp.sum(
            jnp.where(p_col - WIN * over(p_col) == r_col, spread_col, 0.0), axis=1, keepdims=True
        )
        return row, col

    def spot(w):
        return pl.ds(pl.multiple_of(w * TOK, TOK), TOK)

    def add_rows(n, term):
        small[n : n + 1, : term.shape[1]] = small[n : n + 1, : term.shape[1]] + jnp.sum(
            term, axis=0, keepdims=True
        )

    def ctx_copy(w, n):
        ref = ctx.at[w, t]
        return remote(ref, ref, x_send.at[w, n], x_recv.at[w, n], {"tp": lax.rem(t + n, 4)})

    gathered(1)
    down_copies[0].wait_recv()
    down_copies[2].start()
    for copy in halo_g[1:]:
        copy.start()
    down_copies[3].start()

    def forward(w, carry):
        @pl.when(w == 2)
        def _():
            enter(1)

        x = xw[w]
        centred = x - row_mean(x)
        xhat = centred * lax.rsqrt(row_mean(centred * centred) + NORM_EPS)
        normed = (xhat * gain_one + offset_one).astype(BF)
        n1[spot(w), :] = normed
        q_w = (dot(normed, wq[0]) + bias_q).astype(BF)
        k_w = dot(normed, wq[1]).astype(BF)
        v_w = (dot(normed, wq[2]) + bias_v).astype(BF)
        q[w] = q_w
        k[w] = k_w
        v[w] = v_w
        reg_row, reg_col = region_forms(w)
        mask = jnp.where(reg_col == reg_row, 0.0, MASK_FILL)
        context = jnp.zeros((TOK, width), F32)
        for h in range(heads):
            scores = dot_t(q_w * picks_of[h], k_w) * HD ** (-0.5) + bias_s[h, :, :TOK] + mask
            lifted = jnp.exp(scores - jnp.max(scores, axis=-1, keepdims=True))
            p = lifted / jnp.sum(lifted, axis=-1, keepdims=True)
            probs[w, h] = p
            context = context + dot(p.astype(BF), v_w * picks_of[h])
        ctx[w, t] = context.astype(BF)
        for n in (2, 1, 3):
            ctx_copy(w, n).start()
        return carry

    lax.fori_loop(0, windows, forward, 0)
    for n in range(4):
        proj_copy(n, 0, f, far).wait_recv()
        proj_copy(n, 2, far, near).start()
    down_copies[2].wait_recv()
    down_copies[4].start()
    relay(2)
    for n in range(4):
        proj_copy(n, 1, f, near).wait_recv()
        proj_copy(n, 2, far, near).wait_recv()
    wp[...] = jnp.concatenate([wp_g[n] for n in range(4)], axis=1)
    gathered(2)
    for n in (1, 3, 4):
        down_copies[n].wait_recv()

    def middle(w, carry):
        for n in range(1, 4):
            ctx_copy(w, n).wait_recv()
        branch = jnp.zeros((TOK, D), F32) + bias_proj
        for n in range(4):
            branch = branch + dot(ctx[w, n], wp[n * width : (n + 1) * width, :])
        resid = xw[w] + branch
        centred = resid - row_mean(resid)
        rstd = lax.rsqrt(row_mean(centred * centred) + NORM_EPS)
        xhat = centred * rstd
        xhat_s[w] = xhat
        rstd_s[w] = jnp.broadcast_to(rstd, (TOK, 128))
        normed = (xhat * gain_two + offset_two).astype(BF)
        n2_s[spot(w), :] = normed
        pre = dot(normed, wu[...]) + bias_hidden
        cdf = 0.5 * (1.0 + lax.erf(pre * 0.7071067811865476))
        slope = cdf + pre * (jnp.exp(-0.5 * (pre * pre)) * 0.3989422804014327)
        hid = (pre * cdf).astype(BF)
        hid_s[spot(w), :] = hid

        for n in range(images):

            @pl.when(w == 2 * n)
            def _():
                halo_g[n].wait_recv()
                window_rows(
                    lambda im, r: og[im, SHIFT + r] if r < SHIFT else gh[im, r - SHIFT],
                    row_tmp, n, ogw,
                )

        @pl.when(w >= 3)
        def _():
            two.hand(w - 3)

        @pl.when(w >= 2)
        def _():
            two.settle(w - 2)

        @pl.when(w >= 1)
        def _():
            two.cross(w - 1)

        low = ogw[w].astype(BF)
        d_pre = dot(low, wd[...]) * slope
        add_rows(6, d_pre)
        dpl = d_pre.astype(BF)
        dpl_s[spot(w), :] = dpl
        two.put(w, dot_t(dpl, wu[...]))
        two.start(w)
        mixl.put(w, dot_t(hid, wd[...]))

        @pl.when(two.is_mid)
        def _():
            whole = branch + rows[5:6, :]
            for s in range(2):
                for h in range(2):

                    @pl.when(two.own == h)
                    def _():
                        mix[2 * w + s, h] = (
                            mix[2 * w + s, h]
                            + whole[s * ROWS : (s + 1) * ROWS, h * HALF : (h + 1) * HALF]
                        )

        return carry

    lax.fori_loop(0, windows, middle, 0)
    two.cross(windows - 1)

    def grad_chunk(m, carry):
        chunk = pl.ds(pl.multiple_of(m * 256, 256), 256)
        low = jnp.concatenate([ogw[w, :, chunk] for w in range(windows)], axis=0).astype(BF)
        gd[chunk, :] = t_dot(low, hid_s[...])
        gu[chunk, :] = t_dot(n2_s[:, chunk], dpl_s[...])
        return carry

    lax.fori_loop(0, D // 256, grad_chunk, 0)
    down.start()
    up.start()
    two.hand(windows - 3)
    two.settle(windows - 2)

    def backward(w, carry):
        two.arrive(w)
        d_two = two.get(w)
        xhat = xhat_s[w]
        e = d_two * gain_two
        d_flat = (e - row_mean(e) - xhat * row_mean(e * xhat)) * rstd_s[w, :, 0:1]
        og_w = ogw[w]
        d_resid = og_w + d_flat
        dft[w] = d_flat
        d_branch = d_resid.astype(BF)
        dbr[spot(w), :] = d_branch
        for n, term in ((2, d_resid), (3, d_two * xhat), (4, d_two), (5, og_w)):
            add_rows(n, term)
        d_ctx = dot_t(d_branch, wp[band(t), :]).astype(BF)
        q_w, k_w, v_w = q[w], k[w], v[w]
        d_q = jnp.zeros((TOK, width), F32)
        d_k = jnp.zeros((TOK, width), F32)
        d_v = jnp.zeros((TOK, width), F32)
        for h in range(heads):
            d_ctx_h = d_ctx * picks_of[h]
            p = probs[w, h]
            d_p = dot_t(d_ctx_h, v_w)
            d_v = d_v + t_dot(p.astype(BF), d_ctx_h)
            d_s = p * (d_p - jnp.sum(p * d_p, axis=-1, keepdims=True))
            dpos_s[h, :TOK, :TOK] = dpos_s[h, :TOK, :TOK] + d_s
            d_l = (d_s * HD ** (-0.5)).astype(BF)
            d_q = d_q + dot(d_l, k_w * picks_of[h])
            d_k = d_k + t_dot(d_l, q_w * picks_of[h])
        partial = jnp.zeros((TOK, D), F32)
        for n, d_n in enumerate((d_q, d_k, d_v)):
            low = d_n.astype(BF)
            dh_s[n, spot(w), :] = low
            partial = partial + dot_t(low, wq[n])
            if n != 1:
                add_rows(8 + n // 2, low.astype(F32))
        four.put(w, partial)
        four.start(w)

        @pl.when(w == 0)
        def _():
            down.pair()
            up.pair()
            two.settle(windows - 1)
            two.hand(windows - 2)

        @pl.when(w == 1)
        def _():
            two.hand(windows - 1)

        @pl.when(w >= 2)
        def _():
            four.cross(w - 2)

        @pl.when(w == 2)
        def _():
            down.cross()

        @pl.when(w == 3)
        def _():
            up.cross()

        return carry

    lax.fori_loop(0, windows, backward, 0)
    table.start()
    for n in range(3):
        gu[:, n * 256 : n * 256 + width] = t_dot(n1[...], dh_s[n])
        qkv[n].start()
    four.settle(0)
    ctx_own = jnp.concatenate([ctx[w, t] for w in range(windows)], axis=0)
    gp = t_dot(ctx_own, dbr[...])
    for n in range(4):
        gd[n * width : (n + 1) * width, :shard] = gp[:, n * shard : (n + 1) * shard]
    proj.start()
    for w in range(windows):
        two.drain(w)
        mixl.start(w)
    table.pair()
    down.share()
    four.cross(2)
    four.settle(1)
    for member in (*qkv, proj):
        member.pair()
    four.hand(0)
    four.cross(3)
    table.cross()
    four.hand(1)
    four.settle(2)
    qkv[0].cross()

    keep = 1.0 - DECAY_RATE
    first_f = jnp.where(f == 0, 1.0, 0.0)
    first_t = jnp.where(t == 0, 1.0, 0.0)
    old_rows = [
        first_t * jnp.sum(row_qkv[0:1, :], axis=1, keepdims=True),
        first_t * jnp.sum(row_qkv[1:2, :], axis=1, keepdims=True),
        first_t * jnp.sum(row_qkv[2:3, :], axis=1, keepdims=True),
        first_f * total_of(row_proj[...]),
        first_t * total_of(row_up[...]),
        first_f * total_of(row_down[...]),
    ]
    masters = [
        sum(total_of(w_qkv[n] * w_qkv[n]) for n in range(3)),
        total_of(w_proj[...] * w_proj[...]),
        total_of(w_up[...] * w_up[...]),
        total_of(w_down[...] * w_down[...]),
        *[
            first_t * jnp.sum(w_norm[n : n + 1, :] * w_norm[n : n + 1, :], axis=1, keepdims=True)
            for n in range(6)
        ],
        *[total_of(w_heads[:, n, :] * w_heads[:, n, :]) for n in range(2)],
        total_of(w_hidden[...] * w_hidden[...]),
        first_f * total_of(w_table[...] * w_table[...]),
    ]
    four.settle(3)

    for copy in halo_g:
        copy.wait_send()
    home_in = HomeRows(xhat_s, row_tmp, gin_o, og_low, a_send, a_recv)

    def back(w):
        four.arrive(w)
        x = xw[w]
        centred = x - row_mean(x)
        rstd = lax.rsqrt(row_mean(centred * centred) + NORM_EPS)
        xhat = centred * rstd
        d_one = four.get(w)
        e = d_one * gain_one
        xhat_s[w] = dft[w] + (e - row_mean(e) - xhat * row_mean(e * xhat)) * rstd
        for n, term in ((0, d_one * xhat), (1, d_one)):
            add_rows(n, term)

    back(0)
    mixl.cross(0)
    four.hand(2)
    qkv[1].cross()
    qkv[2].cross()
    back(1)
    four.hand(3)
    proj.cross()
    mixl.settle(0)
    mixl.cross(1)
    down.finish()
    up.finish()
    t_s[t] = jnp.zeros((8, shard), F32)
    f_s[f] = jnp.zeros((8, hidden), F32)
    sq_up = gu_o[...] * gu_o[...]
    sq_down = gd_o[...] * gd_o[...]
    t_s[t, 4:5, :] = lane_sums(sq_up)
    t_s[t, 5:6, :] = lane_sums(sq_down)
    f_s[f, 4:5, :] = jnp.sum(sq_up, axis=0, keepdims=True)
    f_s[f, 5:6, :] = jnp.sum(sq_down, axis=0, keepdims=True)
    tot_up, tot_down = total_of(sq_up), total_of(sq_down)
    table.finish(chunk_s)
    first = table.first_row()
    ident = ints((640, TOK), 0)

    def bin_row(step, acc):
        for n in range(4):
            i = step * 4 + n
            hot = ones_where(ident == ridx[pl.ds(first + i, 1), :TOK])
            vals = jnp.concatenate(
                [chunk_s[h, pl.ds(i, 1), :TOK] for h in range(heads)]
                + [jnp.zeros((8 - heads, TOK), F32)],
                axis=0,
            )
            high = vals.astype(BF)
            low = (vals - high.astype(F32)).astype(BF)
            acc = acc + dot_t(jnp.concatenate([high, low], axis=0), hot)
        return acc

    hist = lax.fori_loop(0, 3, bin_row, jnp.zeros((16, 640), F32))
    mixl.settle(1)
    back(2)
    mixl.trade(0)
    hist = lax.fori_loop(3, 6, bin_row, hist)
    small[16:24, :640] = hist[0:8] + hist[8:16]
    mixl.cross(2)
    home_in.go(0)
    back(3)
    sm_s[0] = small[...]

    def swap(n):
        where = ({"fsdp": near}, {"fsdp": far}, {"ctx": 1 - c})[n]
        return remote(sm_s.at[n], sm_r.at[n], sm_send.at[n], sm_recv.at[n], where)

    swap(0).start()
    mixl.hand(0)
    for member in (*qkv, proj):
        member.finish()

    tot_q = []
    for n in range(3):
        sq = gq_o[n] * gq_o[n]
        t_s[t, n : n + 1, :] = lane_sums(sq)
        f_s[f, n : n + 1, :width] = jnp.sum(sq, axis=0, keepdims=True)
        tot_q.append(total_of(sq))
    sq = gp_o[...] * gp_o[...]
    f_s[f, 3:4, :shard] = lane_sums(sq)
    t_s[t, 3:4, :] = jnp.sum(sq, axis=0, keepdims=True)
    z_s[me] = lane_pack([*tot_q, total_of(sq), tot_up, tot_down, *old_rows, *masters])

    def t_copy(n):
        return remote(t_s.at[t], t_s.at[t], t_send.at[n], t_recv.at[n], {"tp": lax.rem(t + n, 4)})

    def f_copy(n):
        return remote(f_s.at[f], f_s.at[f], f_send.at[n], f_recv.at[n], {"fsdp": lax.rem(f + n, 4)})

    def z_copy(n):
        return remote(z_s.at[me], z_s.at[me], z_send.at[n], z_recv.at[n], other(n))

    def c_copy(n):
        return remote(c_s.at[me], c_s.at[me], c_send.at[n], c_recv.at[n], other(n))

    for n in range(1, 4):
        t_copy(n).start()
        f_copy(n).start()
    for n in range(1, 16):
        z_copy(n).start()
    mixl.settle(2)
    mixl.trade(1)
    mixl.cross(3)
    swap(0).wait_recv()
    sm_s[1] = sm_s[0] + sm_r[0]
    swap(1).start()

    def lift(w):
        mixl.arrive(w)
        dft[w] = mixl.get(w)

    def leave(i):
        for r in range(WIN):
            home_o[i, (SHIFT + r) % WIN] = home_row(dft, row_tmp, i, r)

    mixl.hand(1)
    mixl.settle(3)
    home_in.go(1)
    mixl.trade(2)
    lift(0)
    swap(1).wait_recv()
    sm_s[2] = sm_s[1] + sm_r[1]
    swap(2).start()
    mixl.trade(3)
    mixl.hand(2)
    lift(1)
    leave(0)

    swap(2).wait_recv()
    sm = sm_s[2] + sm_r[2]

    def own_lanes(x, size):
        out = x[:, :size]
        for n in range(1, 4):
            out = jnp.where(f == n, x[:, n * size : (n + 1) * size], out)
        return out

    def own_units(row, count):
        all_lanes = count * HD
        at_lane = ints((count, all_lanes), 1)
        only = jnp.where(
            jnp.right_shift(at_lane, 5) == ints((count, all_lanes), 0),
            jnp.broadcast_to(row, (count, all_lanes)), 0.0,
        )
        pick = jnp.where(
            jnp.bitwise_and(ints((all_lanes, part_of), 0), HD - 1)
            == f * part_of + ints((all_lanes, part_of), 1),
            1.0, 0.0,
        )
        return only, pick

    gn = own_lanes(sm[0:6, :], shard)
    gh_new = [exact(*own_units(sm[8 + n : 9 + n, :width], heads), ((1,), (0,))) for n in range(2)]
    only, pick = own_units(sm[6:7, :], hidden // HD)
    gx = exact(pick, only, ((0,), (1,)))
    gt = sm[16 : 16 + heads, : w_table.shape[1]]
    gn_o[...] = gn
    gx_o[...] = gx
    gt_o[...] = gt
    small_sq = first_t * total_of(plain(gn, s_norm[...])[1] ** 2)
    for n in range(2):
        gh_o[:, n, :] = gh_new[n]
        small_sq = small_sq + total_of(plain(gh_new[n], s_heads[:, n, :])[1] ** 2)
    small_sq = small_sq + total_of(plain(gx, s_hidden[...])[1] ** 2)
    small_sq = small_sq + first_f * total_of(plain(gt, s_table[...])[1] ** 2)

    for n in range(1, 4):
        t_copy(n).wait_recv()
        f_copy(n).wait_recv()
    t_sum = t_s[0] + t_s[1] + t_s[2] + t_s[3]
    f_sum = f_s[0] + f_s[1] + f_s[2] + f_s[3]
    for n in range(1, 16):
        z_copy(n).wait_recv()
    z_sum = z_s[0]
    for n in range(1, 16):
        z_sum = z_sum + z_s[n]
    lane8 = ints((8, 128), 1)

    def scalar(n):
        return jnp.sum(jnp.where(lane8 == n, z_sum, 0.0)[0:1], axis=1, keepdims=True)

    def fresh(old, summed, count):
        return DECAY_RATE * old + keep * (summed / count + STAT_EPS)

    rq = fresh(row_qkv[...], t_sum[0:3, :], D)
    kq = fresh(col_qkv[...], f_sum[0:3, :width], D)
    rp = fresh(wide(row_proj), f_sum[3:4, :width], D)
    kp = fresh(wide(col_proj), t_sum[3:4, :], D)
    ru = fresh(wide(row_up), t_sum[4:5, :], ff)
    ku = fresh(wide(col_up), f_sum[4:5, :], D)
    rd = fresh(wide(row_down), f_sum[5:6, :], D)
    kd = fresh(wide(col_down), t_sum[5:6, :], ff)

    def mean_row(n, rows_all, cols_all):
        return (
            DECAY_RATE * scalar(6 + n) + keep * (scalar(n) / cols_all + rows_all * STAT_EPS)
        ) / rows_all

    means = [
        mean_row(0, D, D), mean_row(1, D, D), mean_row(2, D, D), mean_row(3, D, D),
        mean_row(4, D, ff), mean_row(5, ff, D),
    ]
    scales = update_scales(rq, kq, rp, kp, ru, ku, rd, kd, means)
    big_sq = small_sq
    grads = [gq_o[n] for n in range(3)] + [gp_o[...], gu_o[...], gd_o[...]]
    for grad, scale in zip(grads, scales):
        u = grad * scale
        big_sq = big_sq + total_of(u * u)
    c_s[me] = jnp.broadcast_to(big_sq, (8, 128))
    for n in range(1, 16):
        c_copy(n).start()
    rq_o[...] = rq
    kq_o[...] = kq
    for ref, row in ((rp_o, rp), (kp_o, kp), (ru_o, ru), (ku_o, ku), (rd_o, rd), (kd_o, kd)):
        put_wide(ref, row)
    mixl.hand(3)
    lift(2)
    lift(3)
    leave(1)

    counts = [3 * D * D, D * D, D * ff, ff * D] + [D] * 8 + [ff, RELP * HEADS]
    sizes = [jnp.sqrt(scalar(12 + n) / counts[n] + STAT_EPS) for n in range(14)]
    for n in range(1, 16):
        c_copy(n).wait_recv()
    all_sq = c_s[0]
    for n in range(1, 16):
        all_sq = all_sq + c_s[n]
    count_all = 4 * D * D + 2 * D * ff + 8 * D + ff + RELP * HEADS
    clip = jnp.sqrt(all_sq[0:1, 0:1] / count_all)
    factor = STEP_RATE / jnp.maximum(1.0, clip / CLIP_LEVEL)
    size_o[...] = lane_pack([size * factor for size in sizes] + [clip] + means)
    for i in range(images):
        home_in.wait(i)
    for n in range(3):
        swap(n).wait_send()
    for n in range(1, 4):
        t_copy(n).wait_send()
        f_copy(n).wait_send()
        proj_line(n).wait_send()
        for w in range(windows):
            ctx_copy(w, n).wait_send()
    for n in range(1, 16):
        z_copy(n).wait_send()
        c_copy(n).wait_send()
    for w in range(windows):
        mixl.drain(w)
        four.drain(w)
    for copy in halo_f:
        copy.wait_send()
    for copy in down_copies:
        copy.wait_send()
    for n in range(3):
        copy_of(n, 0, f, far).wait_send()
        copy_of(n, 1, f, near).wait_send()
        copy_of(n, 2, far, near).wait_send()
    for n in range(4):
        proj_copy(n, 0, f, far).wait_send()
        proj_copy(n, 1, f, near).wait_send()
        proj_copy(n, 2, far, near).wait_send()
    for member in (up, down, *qkv, proj, table):
        member.drain()
def finish_body(*refs):
    (
        (home_out, feat, home_in, og, gq, gp, g_up, g_down, gn, gh, gx, gt),
        (w_qkv, w_proj, w_up, w_down, w_norm, w_heads, w_hidden, w_table),
        (s_norm, s_heads, s_hidden, s_table),
        stats, (size,),
        (out_o, gin_o, gq_o, gp_o, gu_o, gd_o, gn_o, gh_o, gx_o, gt_o),
        (nq_o, np_o, nu_o, nd_o, nn_o, nh_o, nx_o, nt_o),
        (cq_o, cp_o, cu_o, cd_o),
        stats_o, (sn_o, sh_o, sx_o, st_o), (clip_o,),
    ) = take(refs, (12, 8, 4, 8, 1, 10, 8, 4, 8, 4, 1))
    lane8 = lax.broadcasted_iota(jnp.int32, (8, 128), 1)
    table = size[...]

    def step(n):
        return jnp.sum(jnp.where(lane8 == n, table, 0.0)[0:1], axis=1, keepdims=True)

    out_o[...] = feat[...].astype(F32) + home_out[...].astype(F32)
    gin_o[...] = og[...] + home_in[...].astype(F32)
    for src, dst in (
        (gq, gq_o), (gp, gp_o), (g_up, gu_o), (g_down, gd_o), (gn, gn_o), (gh, gh_o), (gx, gx_o),
        (gt, gt_o), *zip(stats, stats_o),
    ):
        dst[...] = src[...]
    rq, kq, *vecs = stats
    scales = update_scales(rq[...], kq[...], *map(wide, vecs), [step(15 + n) for n in range(6)])
    for n in range(3):
        new = w_qkv[n] - step(0) * (gq[n] * scales[n])
        nq_o[n] = new
        cq_o[n] = new.astype(BF)
    for n, (master, grad, new_o, low_o) in enumerate(
        ((w_proj, gp, np_o, cp_o), (w_up, g_up, nu_o, cu_o), (w_down, g_down, nd_o, cd_o))
    ):
        new = master[...] - step(1 + n) * (grad[...] * scales[3 + n])
        new_o[...] = new
        low_o[...] = new.astype(BF)
    sn, un = plain(gn[...], s_norm[...])
    sn_o[...] = sn
    for n in range(6):
        nn_o[n : n + 1, :] = w_norm[n : n + 1, :] - step(4 + n) * un[n : n + 1, :]
    for n in range(2):
        sh, uh = plain(gh[:, n, :], s_heads[:, n, :])
        sh_o[:, n, :] = sh
        nh_o[:, n, :] = w_heads[:, n, :] - step(10 + n) * uh
    sx, ux = plain(gx[...], s_hidden[...])
    sx_o[...] = sx
    nx_o[...] = w_hidden[...] - step(12) * ux
    st, ut = plain(gt[...], s_table[...])
    st_o[...] = st
    nt_o[...] = w_table[...] - step(13) * ut
    clip_o[...] = step(14)


def whole_step(feat, og, regions, rel_index, masters, stats, states):
    w_qkv, w_proj, w_up, w_down, w_norm, w_heads, w_hidden, w_table = masters
    images = feat.shape[0]
    windows = 2 * images
    shard, width = w_qkv.shape[1], w_qkv.shape[2]
    hidden = w_up.shape[1]
    heads = width // HD
    stats = [u if u.ndim == 2 else u.reshape(-1, 128) if u.shape[0] == D else u[None] for u in stats]
    like = lambda u: (u.shape, F32)
    mats = (w_qkv, w_proj, w_up, w_down)
    smalls = (w_norm, w_heads, w_hidden, w_table)
    vm, dma = pltpu.VMEM, pltpu.SemaphoreType.DMA
    flat = windows * TOK
    halves = (2 * windows, 2, ROWS, HALF)
    tokens = (windows, TOK, D)
    rows_of = (images, SHIFT, 24, D)
    outs = [
        (feat.shape, BF), (feat.shape, BF), *map(like, mats), *map(like, smalls),
        *map(like, stats), ((8, 128), F32),
    ]
    scratch = [
        vm((4, 16, shard), BF), vm((3, D, width), BF), vm((4, D, shard), BF), vm((D, D), BF),
        vm((D, hidden), BF), vm((D, hidden), BF), vm(rows_of, BF), vm(rows_of, BF), vm(rows_of, BF),
        vm((heads, TOK, 256), F32), vm((24, D), F32), vm((16, D), F32), vm((192, 256), jnp.int32),
        vm((8, 640), F32), vm((24, D), F32),
        vm(tokens, F32), vm(tokens, F32), vm((flat, D), BF), vm((windows, TOK, width), BF),
        vm((windows, TOK, width), BF), vm((windows, TOK, width), BF),
        vm((windows, heads, TOK, TOK), F32), vm((windows, 4, TOK, width), BF), vm(halves, F32),
        vm((flat, D), BF), vm((flat, hidden), BF), vm((flat, hidden), BF),
        vm(tokens, F32), vm((windows, TOK, 128), F32), vm(halves, BF), vm((D, hidden), F32),
        vm((D, hidden), F32), vm(tokens, F32), vm((flat, D), BF), vm(halves, F32),
        vm((3, flat, width), BF), vm((heads, 192, 256), F32), vm((heads, 24, 256), F32),
        vm(halves, BF),
        *LineSum.scratch(2 * windows), *LineSum.scratch(2 * windows),
        *ShardSum.scratch((shard, hidden)), *BandFirstSum.scratch((shard, hidden)),
        *[s for _ in range(3) for s in ShardSum.scratch((shard, width))], *ShardSum.scratch((width, shard)),
        *TableSum.scratch(heads),
        vm((3, 24, D), F32), vm((3, 24, D), F32), vm((4, 8, shard), F32), vm((4, 8, hidden), F32),
        vm((16, 8, 128), F32), vm((16, 8, 128), F32),
        vm(feat.shape, BF), vm(og.shape, F32), *[vm(u.shape, F32) for u in mats],
        vm(halves, BF), vm((windows, ROWS, HALF), BF), dma((windows,)), dma((windows,)), dma((6,)),
        dma((5,)), dma((5,)),
        dma((4, 3)), dma((4, 3)), dma((4, 3)), dma((4, 3)), dma((4,)), dma((4,)),
        dma((2 * images,)), dma((2 * images,)), *[dma((images,))] * 2,
        dma((windows, 4)), dma((windows, 4)),
        dma((3,)), dma((3,)), *[dma((4,))] * 4, *[dma((16,))] * 4,
    ]
    got = vmem_call(step_body, outs, scratch, "whole_step", 1, 6)(
        feat, og, *mats, regions, rel_index, *smalls, *stats, *states
    )
    home_out, home_in, g_qkv, g_proj, g_up, g_down, gn, gh, gx, gt, *rest = got
    new_stats, size = rest[:8], rest[8]
    outs = [
        like(og), like(og), *map(like, mats), *map(like, smalls), *map(like, masters),
        *[(u.shape, BF) for u in mats], *map(like, stats), *map(like, smalls), ((1, 1), F32),
    ]
    return vmem_call(finish_body, outs, [], "finish", None)(
        home_out, feat, home_in, og, g_qkv, g_proj, g_up, g_down, gn, gh, gx, gt,
        *masters, *states, *new_stats, size,
    )


def per_device_plain(
    features,
    out_grad,
    regions,
    rel_index,
    w_qkv,
    w_proj,
    w_up,
    w_down,
    norm_vecs,
    head_bias,
    hidden_bias,
    rel_table,
    row_qkv,
    col_qkv,
    row_proj,
    col_proj,
    row_up,
    col_up,
    row_down,
    col_down,
    state_norm,
    state_heads,
    state_hidden,
    state_table,
):
    images, band_rows, across, model_width = features.shape
    win_tokens = WIN * WIN
    fsdp_at = lax.axis_index("fsdp")
    ctx_at = lax.axis_index("ctx")
    tp_at = lax.axis_index("tp")
    first_fsdp = (fsdp_at == 0).astype(jnp.float32)
    first_ctx = (ctx_at == 0).astype(jnp.float32)
    first_tp = (tp_at == 0).astype(jnp.float32)
    weights_qkv, weights_proj, weights_up, weights_down, vec_copy, head_copy, hidden_copy = (
        lax.all_gather(w_qkv.astype(jnp.bfloat16), "fsdp", axis=1, tiled=True),
        lax.all_gather(w_proj.astype(jnp.bfloat16), "fsdp", axis=1, tiled=True),
        lax.all_gather(w_up.astype(jnp.bfloat16), "fsdp", axis=0, tiled=True),
        lax.all_gather(w_down.astype(jnp.bfloat16), "fsdp", axis=1, tiled=True),
        lax.all_gather(norm_vecs.astype(jnp.bfloat16), "fsdp", axis=1, tiled=True),
        lax.all_gather(head_bias.astype(jnp.bfloat16), "fsdp", axis=2, tiled=True),
        lax.all_gather(hidden_bias.astype(jnp.bfloat16), "fsdp", axis=1, tiled=True),
    )
    norm_rows = vec_copy.astype(jnp.float32)
    bias_query = head_copy[0].reshape(-1).astype(jnp.float32)
    bias_value = head_copy[1].reshape(-1).astype(jnp.float32)
    bias_hidden = hidden_copy.reshape(-1).astype(jnp.float32)
    table_copy = rel_table.astype(jnp.bfloat16)
    local_width = weights_qkv.shape[2]
    heads_here = local_width // HD

    def roll_in(home):
        received = passed_along(home[:, :SHIFT], "ctx", -1)
        return to_windows(enter_frame(home, received)).reshape(-1, model_width)

    def roll_out(rolled_flat):
        band = jnp.roll(
            from_windows(
                rolled_flat.reshape(-1, win_tokens, model_width), images, band_rows, across
            ),
            SHIFT,
            axis=2,
        )
        lower = passed_along(band[:, band_rows - SHIFT :], "ctx", 1)
        return jnp.concatenate([lower, band[:, : band_rows - SHIFT]], axis=1)

    flat_one = roll_in(features).astype(jnp.float32)
    grad_flat = roll_in(out_grad)
    win_count = flat_one.shape[0] // win_tokens
    normed_one, pull_one = jax.vjp(layer_norm, flat_one, norm_rows[0], norm_rows[1])
    normed_one_low = normed_one.astype(jnp.bfloat16)
    head_shape = (win_count, win_tokens, heads_here, HD)
    query_low, key_low, value_low = project_heads(
        normed_one_low, weights_qkv, bias_query, bias_value, head_shape
    )
    pos_bias = table_lookup(table_copy, rel_index)
    region_win = to_windows(regions[..., None])[..., 0]
    mask_add = jnp.where(region_win[:, :, None] == region_win[:, None, :], 0.0, MASK_FILL).astype(
        jnp.float32
    )
    scores = attention_scores(query_low, key_low, pos_bias, mask_add)
    top_score = jnp.max(scores, axis=-1, keepdims=True)
    lifted = jnp.exp(scores - top_score)
    prob_rows = lifted / jnp.sum(lifted, axis=-1, keepdims=True)
    prob_low = prob_rows.astype(jnp.bfloat16)
    context = jnp.einsum("whij,wjhc->wihc", prob_low, value_low, preferred_element_type=jnp.float32)
    context_low = context.astype(jnp.bfloat16).reshape(-1, local_width)
    branch_part = jnp.dot(context_low, weights_proj, preferred_element_type=jnp.float32)
    branch = lax.psum(branch_part.astype(jnp.bfloat16), "tp").astype(jnp.float32) + norm_rows[2]
    flat_two = flat_one + branch
    normed_two, pull_two = jax.vjp(layer_norm, flat_two, norm_rows[3], norm_rows[4])
    normed_two_low = normed_two.astype(jnp.bfloat16)
    pre_act = jnp.dot(normed_two_low, weights_up, preferred_element_type=jnp.float32) + bias_hidden
    hidden, pull_gelu = jax.vjp(exact_gelu, pre_act)
    hidden_low = hidden.astype(jnp.bfloat16)
    mixed_part = jnp.dot(hidden_low, weights_down, preferred_element_type=jnp.float32)
    mixed_whole = lax.psum(mixed_part.astype(jnp.bfloat16), "tp").astype(jnp.float32)
    block_out = features.astype(jnp.float32) + roll_out(
        (branch + mixed_whole + norm_rows[5]).astype(jnp.bfloat16)
    ).astype(jnp.float32)
    grad_low = grad_flat.astype(jnp.bfloat16)
    grad_down_full = jnp.einsum(
        "tf,td->fd", hidden_low, grad_low, preferred_element_type=jnp.float32
    )
    grad_down_bias = jnp.sum(grad_flat, axis=0)
    d_hidden = jnp.einsum("td,fd->tf", grad_low, weights_down, preferred_element_type=jnp.float32)
    d_pre = pull_gelu(d_hidden)[0]
    d_pre_low = d_pre.astype(jnp.bfloat16)
    grad_hidden_bias = jnp.sum(d_pre, axis=0)
    grad_up_full = jnp.einsum(
        "td,tf->df", normed_two_low, d_pre_low, preferred_element_type=jnp.float32
    )
    d_two_part = jnp.einsum("tf,df->td", d_pre_low, weights_up, preferred_element_type=jnp.float32)
    d_two = lax.psum(d_two_part.astype(jnp.bfloat16), "tp").astype(jnp.float32)
    d_flat_two, grad_gain_two, grad_offset_two = pull_two(d_two)
    d_resid = grad_flat + d_flat_two
    grad_proj_bias = jnp.sum(d_resid, axis=0)
    d_branch = d_resid.astype(jnp.bfloat16)
    grad_proj_full = jnp.einsum(
        "tc,td->cd", context_low, d_branch, preferred_element_type=jnp.float32
    )
    d_context = (
        jnp.einsum("td,cd->tc", d_branch, weights_proj, preferred_element_type=jnp.float32)
        .astype(jnp.bfloat16)
        .reshape(head_shape)
    )
    d_probs = jnp.einsum(
        "wihc,wjhc->whij", d_context, value_low, preferred_element_type=jnp.float32
    )
    d_value_low = jnp.einsum(
        "whij,wihc->wjhc", prob_low, d_context, preferred_element_type=jnp.float32
    ).astype(jnp.bfloat16)
    d_scores = prob_rows * (d_probs - jnp.sum(prob_rows * d_probs, axis=-1, keepdims=True))
    d_pos = jnp.sum(d_scores, axis=0)
    d_scaled = (d_scores * HD ** (-0.5)).astype(jnp.bfloat16)
    d_query_low = jnp.einsum(
        "whij,wjhc->wihc", d_scaled, key_low, preferred_element_type=jnp.float32
    ).astype(jnp.bfloat16)
    d_key_low = jnp.einsum(
        "whij,wihc->wjhc", d_scaled, query_low, preferred_element_type=jnp.float32
    ).astype(jnp.bfloat16)
    d_heads = jnp.stack([d_query_low, d_key_low, d_value_low]).reshape(3, -1, local_width)
    grad_qkv_full = jnp.einsum(
        "td,ktc->kdc", normed_one_low, d_heads, preferred_element_type=jnp.float32
    )
    grad_head_bias = jnp.stack(
        [
            jnp.sum(d_heads[0].astype(jnp.float32), axis=0),
            jnp.sum(d_heads[2].astype(jnp.float32), axis=0),
        ]
    ).reshape(2, heads_here, HD)
    d_one_part = jnp.einsum("ktc,kdc->td", d_heads, weights_qkv, preferred_element_type=jnp.float32)
    d_one = lax.psum(d_one_part.astype(jnp.bfloat16), "tp").astype(jnp.float32)
    d_flat_one, grad_gain_one, grad_offset_one = pull_one(d_one)
    grad_input = out_grad + roll_out((d_flat_two + d_flat_one).astype(jnp.bfloat16)).astype(
        jnp.float32
    )
    table_part = table_grad(d_pos, rel_index, rel_table.shape[0])
    grad_norm_full = jnp.stack(
        [
            grad_gain_one,
            grad_offset_one,
            grad_proj_bias,
            grad_gain_two,
            grad_offset_two,
            grad_down_bias,
        ]
    )
    grad_list = (
        grad_qkv_full,
        grad_proj_full,
        grad_up_full,
        grad_down_full,
        grad_norm_full,
        grad_head_bias,
        grad_hidden_bias.reshape(-1, HD),
    )
    g_qkv, g_proj, g_up, g_down, g_norm, g_heads, g_hidden = shard_sum(band_sum(grad_list))
    d_shard = w_qkv.shape[1]
    hidden_here = w_up.shape[1]
    keep = 1.0 - DECAY_RATE
    sq_qkv = g_qkv * g_qkv
    sq_proj = g_proj * g_proj
    sq_up = g_up * g_up
    sq_down = g_down * g_down
    stat_rq = place(
        (keep * jnp.sum(sq_qkv, axis=2) / D + first_tp * (DECAY_RATE * row_qkv + keep * STAT_EPS))
        * first_ctx,
        fsdp_at,
        D,
    )
    stat_cq = place(
        (keep * jnp.sum(sq_qkv, axis=1) / D + first_fsdp * (DECAY_RATE * col_qkv + keep * STAT_EPS))
        * first_ctx,
        tp_at,
        D,
    )
    stat_rp = place(
        (
            keep * jnp.sum(sq_proj, axis=1) / D
            + first_fsdp * (DECAY_RATE * row_proj + keep * STAT_EPS)
        )
        * first_ctx,
        tp_at,
        D,
    )
    stat_cp = place(
        (keep * jnp.sum(sq_proj, axis=0) / D + first_tp * (DECAY_RATE * col_proj + keep * STAT_EPS))
        * first_ctx,
        fsdp_at,
        D,
    )
    stat_ru = place(
        (keep * jnp.sum(sq_up, axis=1) / FF + first_tp * (DECAY_RATE * row_up + keep * STAT_EPS))
        * first_ctx,
        fsdp_at,
        D,
    )
    stat_cu = place(
        (keep * jnp.sum(sq_up, axis=0) / D + first_fsdp * (DECAY_RATE * col_up + keep * STAT_EPS))
        * first_ctx,
        tp_at,
        FF,
    )
    stat_rd = place(
        (
            keep * jnp.sum(sq_down, axis=1) / D
            + first_fsdp * (DECAY_RATE * row_down + keep * STAT_EPS)
        )
        * first_ctx,
        tp_at,
        FF,
    )
    stat_cd = place(
        (
            keep * jnp.sum(sq_down, axis=0) / FF
            + first_tp * (DECAY_RATE * col_down + keep * STAT_EPS)
        )
        * first_ctx,
        fsdp_at,
        D,
    )
    table_whole = place(table_part, tp_at, HEADS)
    master_sq = jnp.concatenate(
        [
            jnp.stack(
                [
                    jnp.sum(w_qkv * w_qkv),
                    jnp.sum(w_proj * w_proj),
                    jnp.sum(w_up * w_up),
                    jnp.sum(w_down * w_down),
                ]
            )
            * first_ctx,
            jnp.sum(norm_vecs * norm_vecs, axis=1) * first_ctx * first_tp,
            jnp.sum(head_bias * head_bias, axis=(1, 2)) * first_ctx,
            jnp.sum(hidden_bias * hidden_bias)[None] * first_ctx,
            jnp.sum(rel_table * rel_table)[None] * first_ctx * first_fsdp,
        ]
    )
    (
        full_rq,
        full_cq,
        full_rp,
        full_cp,
        full_ru,
        full_cu,
        full_rd,
        full_cd,
        table_sum,
        master_total,
    ) = lax.psum(
        (
            stat_rq,
            stat_cq,
            stat_rp,
            stat_cp,
            stat_ru,
            stat_cu,
            stat_rd,
            stat_cd,
            table_whole,
            master_sq,
        ),
        ("fsdp", "ctx", "tp"),
    )
    u_qkv = factored(
        g_qkv,
        own_part(full_rq, fsdp_at, d_shard),
        own_part(full_cq, tp_at, local_width),
        jnp.mean(full_rq, axis=1)[:, None, None],
    )
    u_proj = factored(
        g_proj,
        own_part(full_rp, tp_at, local_width),
        own_part(full_cp, fsdp_at, d_shard),
        jnp.mean(full_rp),
    )
    u_up = factored(
        g_up,
        own_part(full_ru, fsdp_at, d_shard),
        own_part(full_cu, tp_at, hidden_here),
        jnp.mean(full_ru),
    )
    u_down = factored(
        g_down,
        own_part(full_rd, tp_at, hidden_here),
        own_part(full_cd, fsdp_at, d_shard),
        jnp.mean(full_rd),
    )
    g_table = own_part(table_sum, tp_at, heads_here)
    state_norm_new, u_norm = plain_stats(g_norm, state_norm)
    state_heads_new, u_heads = plain_stats(g_heads, state_heads)
    state_hidden_new, u_hidden = plain_stats(g_hidden, state_hidden)
    state_table_new, u_table = plain_stats(g_table, state_table)
    local_sq = (
        jnp.sum(u_qkv * u_qkv)
        + jnp.sum(u_proj * u_proj)
        + jnp.sum(u_up * u_up)
        + jnp.sum(u_down * u_down)
        + jnp.sum(u_heads * u_heads)
        + jnp.sum(u_hidden * u_hidden)
        + first_tp * jnp.sum(u_norm * u_norm)
        + first_fsdp * jnp.sum(u_table * u_table)
    )
    total_sq = lax.psum(local_sq, ("fsdp", "tp"))
    count_all = 4 * D * D + 2 * D * FF + 8 * D + FF + RELP * HEADS
    clip_rms = jnp.sqrt(total_sq / count_all)
    factor = 1.0 / jnp.maximum(1.0, clip_rms / CLIP_LEVEL)
    counts = jnp.array(
        [3 * D * D, D * D, D * FF, FF * D, D, D, D, D, D, D, D, D, FF, RELP * HEADS], jnp.float32
    )
    scales = jnp.sqrt(master_total / counts + STAT_EPS)
    new_qkv = w_qkv - STEP_RATE * scales[0] * factor * u_qkv
    new_proj = w_proj - STEP_RATE * scales[1] * factor * u_proj
    new_up = w_up - STEP_RATE * scales[2] * factor * u_up
    new_down = w_down - STEP_RATE * scales[3] * factor * u_down
    new_norm = norm_vecs - STEP_RATE * scales[4:10][:, None] * factor * u_norm
    new_heads = head_bias - STEP_RATE * scales[10:12][:, None, None] * factor * u_heads
    new_hidden = hidden_bias - STEP_RATE * scales[12] * factor * u_hidden
    new_table = rel_table - STEP_RATE * scales[13] * factor * u_table
    return (
        block_out,
        grad_input,
        g_qkv,
        g_proj,
        g_up,
        g_down,
        g_norm,
        g_heads,
        g_hidden,
        g_table,
        new_qkv,
        new_proj,
        new_up,
        new_down,
        new_norm,
        new_heads,
        new_hidden,
        new_table,
        new_qkv.astype(jnp.bfloat16),
        new_proj.astype(jnp.bfloat16),
        new_up.astype(jnp.bfloat16),
        new_down.astype(jnp.bfloat16),
        own_part(full_rq, fsdp_at, d_shard),
        own_part(full_cq, tp_at, local_width),
        own_part(full_rp, tp_at, local_width),
        own_part(full_cp, fsdp_at, d_shard),
        own_part(full_ru, fsdp_at, d_shard),
        own_part(full_cu, tp_at, hidden_here),
        own_part(full_rd, tp_at, hidden_here),
        own_part(full_cd, fsdp_at, d_shard),
        state_norm_new,
        state_heads_new,
        state_hidden_new,
        state_table_new,
        clip_rms,
    )


def per_device(
    features,
    out_grad,
    regions,
    rel_index,
    w_qkv,
    w_proj,
    w_up,
    w_down,
    norm_vecs,
    head_bias,
    hidden_bias,
    rel_table,
    row_qkv,
    col_qkv,
    row_proj,
    col_proj,
    row_up,
    col_up,
    row_down,
    col_down,
    state_norm,
    state_heads,
    state_hidden,
    state_table,
):
    flip = lambda u: u.transpose(1, 0, 2)
    (block_out, grad_input, g_qkv, g_proj, g_up, g_down, g_norm, g_heads, g_hidden, g_table,
     new_qkv, new_proj, new_up, new_down, new_norm, new_heads, new_hidden, new_table,
     copy_qkv, copy_proj, copy_up, copy_down, *rest) = whole_step(
        features, out_grad, regions, rel_index,
        (w_qkv, w_proj, w_up, w_down.T, norm_vecs, flip(head_bias), hidden_bias.T, rel_table.T),
        (row_qkv, col_qkv, row_proj, col_proj, row_up, col_up, row_down, col_down),
        (state_norm, flip(state_heads), state_hidden.T, state_table.T))
    factors, states, clip_rms = rest[:8], rest[8:12], rest[12]
    factors = list(factors[:2]) + [u.reshape(-1) for u in factors[2:]]
    return (
        block_out, grad_input, g_qkv, g_proj, g_up, g_down.T, g_norm, flip(g_heads), g_hidden.T,
        g_table.T, new_qkv, new_proj, new_up, new_down.T, new_norm, flip(new_heads), new_hidden.T,
        new_table.T, copy_qkv, copy_proj, copy_up, copy_down.T, *factors,
        states[0], flip(states[1]), states[2].T, states[3].T, clip_rms[0, 0],
    )


def solution(mesh):
    line_of_four = mesh.shape["fsdp"] == 4 and mesh.shape["tp"] == 4 and mesh.shape["ctx"] == 2
    return jax.shard_map(
        per_device if line_of_four else per_device_plain,
        mesh=mesh,
        in_specs=(
            P("fsdp", "ctx", None, None),
            P("fsdp", "ctx", None, None),
            P("fsdp", "ctx", None),
            P(),
            P(None, "fsdp", "tp"),
            P("tp", "fsdp"),
            P("fsdp", "tp"),
            P("tp", "fsdp"),
            P(None, "fsdp"),
            P(None, "tp", "fsdp"),
            P("tp", "fsdp"),
            P(None, "tp"),
            P(None, "fsdp"),
            P(None, "tp"),
            P("tp"),
            P("fsdp"),
            P("fsdp"),
            P("tp"),
            P("tp"),
            P("fsdp"),
            P(None, "fsdp"),
            P(None, "tp", "fsdp"),
            P("tp", "fsdp"),
            P(None, "tp"),
        ),
        out_specs=(
            P("fsdp", "ctx", None, None),
            P("fsdp", "ctx", None, None),
            P(None, "fsdp", "tp"),
            P("tp", "fsdp"),
            P("fsdp", "tp"),
            P("tp", "fsdp"),
            P(None, "fsdp"),
            P(None, "tp", "fsdp"),
            P("tp", "fsdp"),
            P(None, "tp"),
            P(None, "fsdp", "tp"),
            P("tp", "fsdp"),
            P("fsdp", "tp"),
            P("tp", "fsdp"),
            P(None, "fsdp"),
            P(None, "tp", "fsdp"),
            P("tp", "fsdp"),
            P(None, "tp"),
            P(None, "fsdp", "tp"),
            P("tp", "fsdp"),
            P("fsdp", "tp"),
            P("tp", "fsdp"),
            P(None, "fsdp"),
            P(None, "tp"),
            P("tp"),
            P("fsdp"),
            P("fsdp"),
            P("tp"),
            P("tp"),
            P("fsdp"),
            P(None, "fsdp"),
            P(None, "tp", "fsdp"),
            P("tp", "fsdp"),
            P(None, "tp"),
            P(),
        ),
        check_vma=False,
    )
```

```python
import functools

import jax
import jax.numpy as jnp
from jax import lax
from jax.experimental import pallas as pl
from jax.experimental.pallas import tpu as pltpu
from jax.sharding import PartitionSpec as P


D = 768
HEADS = 24
HD = 32
FF = 3072
WIN = 12
SHIFT = 6
RELP = 529


DECAY_RATE = 0.5
STAT_EPS = 1e-06
NORM_EPS = 1e-05
MASK_FILL = -100.0
STEP_RATE = 1.0
CLIP_LEVEL = 0.25


def passed_along(x, axis, by):
    count = lax.axis_size(axis)
    return lax.ppermute(x, axis, [(i, (i + by) % count) for i in range(count)])


def layer_norm(values, gain_row, offset):
    mean_val = jnp.mean(values, axis=-1, keepdims=True)
    centred = values - mean_val
    var_val = jnp.mean(centred * centred, axis=-1, keepdims=True)
    return centred * lax.rsqrt(var_val + NORM_EPS) * gain_row + offset


def exact_gelu(values):
    return jax.nn.gelu(values, approximate=False)


def to_windows(values):
    image_count, row_count, col_count, channels = values.shape
    pieces = values.reshape(image_count, row_count // WIN, WIN, col_count // WIN, WIN, channels)
    return pieces.transpose(0, 1, 3, 2, 4, 5).reshape(-1, WIN * WIN, channels)


def from_windows(values, image_count, row_count, col_count):
    channels = values.shape[-1]
    pieces = values.reshape(image_count, row_count // WIN, col_count // WIN, WIN, WIN, channels)
    return pieces.transpose(0, 1, 3, 2, 4, 5).reshape(image_count, row_count, col_count, channels)


def enter_frame(own_rows, received):
    joined = jnp.concatenate([own_rows[:, SHIFT:], received], axis=1)
    return jnp.roll(joined, -SHIFT, axis=2)


def project_heads(normed_low, weights_qkv, bias_query, bias_value, head_shape):
    query_full = (
        jnp.dot(normed_low, weights_qkv[0], preferred_element_type=jnp.float32) + bias_query
    )
    key_full = jnp.dot(normed_low, weights_qkv[1], preferred_element_type=jnp.float32)
    value_full = (
        jnp.dot(normed_low, weights_qkv[2], preferred_element_type=jnp.float32) + bias_value
    )
    return tuple(
        (
            member.astype(jnp.bfloat16).reshape(head_shape)
            for member in (query_full, key_full, value_full)
        )
    )


def attention_scores(query_low, key_low, pos_bias, mask_add):
    products = jnp.einsum("wihc,wjhc->whij", query_low, key_low, preferred_element_type=jnp.float32)
    return products * query_low.shape[-1] ** (-0.5) + pos_bias[None] + mask_add[:, None]


def table_lookup(table_low, rel_index):
    win_tokens = rel_index.shape[0]
    code_ids = jnp.arange(table_low.shape[0], dtype=jnp.int32)
    index_blocks = rel_index.reshape(WIN, -1)

    def lookup(index_block):
        one_hot = (index_block[:, None] == code_ids[None, :]).astype(jnp.bfloat16)
        return jnp.dot(one_hot, table_low, preferred_element_type=jnp.float32)

    looked = lax.map(lookup, index_blocks)
    return looked.reshape(win_tokens, win_tokens, -1).transpose(2, 0, 1)


def table_grad(d_pos, rel_index, table_rows):
    heads_here = d_pos.shape[0]
    code_ids = jnp.arange(table_rows, dtype=jnp.int32)
    index_blocks = rel_index.reshape(WIN, -1)
    grad_blocks = d_pos.transpose(1, 2, 0).reshape(WIN, -1, heads_here)

    def accumulate(running, member):
        index_block, grad_block = member
        one_hot = (index_block[:, None] == code_ids[None, :]).astype(jnp.float32)
        added = lax.dot_general(
            one_hot,
            grad_block,
            (((0,), (0,)), ((), ())),
            precision=lax.Precision.HIGHEST,
            preferred_element_type=jnp.float32,
        )
        return (running + added, None)

    result_pair = lax.scan(
        accumulate, jnp.zeros((table_rows, heads_here), jnp.float32), (index_blocks, grad_blocks)
    )
    return result_pair[0]


def place(part_vec, index_at, whole_len):
    size_of = part_vec.shape[-1]
    base = jnp.zeros(part_vec.shape[:-1] + (whole_len,), jnp.float32)
    return lax.dynamic_update_slice_in_dim(base, part_vec, index_at * size_of, part_vec.ndim - 1)


def own_part(whole_vec, index_at, size_of):
    return lax.dynamic_slice_in_dim(whole_vec, index_at * size_of, size_of, whole_vec.ndim - 1)


def factored(grad, row_local, col_local, row_mean):
    return grad * lax.rsqrt(row_local[..., :, None] * col_local[..., None, :] / row_mean)


def plain_stats(grad, state_old):
    state_new = DECAY_RATE * state_old + (1.0 - DECAY_RATE) * (grad * grad + STAT_EPS)
    return (state_new, grad * lax.rsqrt(state_new))


def shard_sum(grad_list):
    return (
        lax.psum_scatter(grad_list[0], "fsdp", scatter_dimension=1, tiled=True),
        lax.psum_scatter(grad_list[1], "fsdp", scatter_dimension=1, tiled=True),
        lax.psum_scatter(grad_list[2], "fsdp", scatter_dimension=0, tiled=True),
        lax.psum_scatter(grad_list[3], "fsdp", scatter_dimension=1, tiled=True),
        lax.psum_scatter(grad_list[4], "fsdp", scatter_dimension=1, tiled=True),
        lax.psum_scatter(grad_list[5], "fsdp", scatter_dimension=2, tiled=True),
        lax.psum_scatter(grad_list[6], "fsdp", scatter_dimension=1, tiled=True),
    )


def band_sum(grad_list):
    return lax.psum(
        (
            grad_list[0],
            grad_list[1],
            grad_list[2],
            grad_list[3],
            grad_list[4],
            grad_list[5],
            grad_list[6],
        ),
        "ctx",
    )


BF = jnp.bfloat16
F32 = jnp.float32
MESH = pl.DeviceIdType.MESH
TOK = WIN * WIN
HALF = D // 2
ROWS = TOK // 2
VMEM_LIMIT = 67_043_328


def dot(a, b):
    return lax.dot_general(a, b, (((1,), (0,)), ((), ())), preferred_element_type=F32)


def dot_t(a, b):
    return lax.dot_general(a, b, (((1,), (1,)), ((), ())), preferred_element_type=F32)


def t_dot(a, b):
    return lax.dot_general(a, b, (((0,), (0,)), ((), ())), preferred_element_type=F32)


def row_mean(x):
    return jnp.sum(x, axis=-1, keepdims=True) * (1.0 / x.shape[-1])


def remote(src, dst, send, recv, where):
    return pltpu.make_async_remote_copy(
        src_ref=src, dst_ref=dst, send_sem=send, recv_sem=recv, device_id=where, device_id_type=MESH
    )


def greet(barrier, places):
    for place_of in places:
        pl.semaphore_signal(barrier, inc=1, device_id=place_of, device_id_type=MESH)


class LineSum:
    def __init__(self, part, send, from_outer, from_mid, total, sems):
        self.part, self.send, self.from_outer, self.from_mid, self.total = (
            part, send, from_outer, from_mid, total,
        )
        self.s_out, self.r_out, self.s_mid, self.r_mid, self.s_tot, self.r_tot, self.s_cross = sems
        z = lax.axis_index("tp")
        self.is_mid = jnp.logical_and(z > 0, z < 3)
        self.is_outer = jnp.logical_not(self.is_mid)
        self.outer = jnp.where(z < 2, 0, 3)
        self.mid = jnp.where(z < 2, 1, 2)
        self.other_mid = 3 - self.mid
        self.own = self.mid - 1
        self.other = 1 - self.own

    @staticmethod
    def scratch(count):
        return [
            pltpu.VMEM((count, 2, ROWS, HALF), BF),
            pltpu.VMEM((count, 2, ROWS, HALF), BF),
            pltpu.VMEM((count, ROWS, HALF), BF),
            pltpu.SemaphoreType.DMA((count, 2)),
            pltpu.SemaphoreType.DMA((count, 2)),
            pltpu.SemaphoreType.DMA((count,)),
            pltpu.SemaphoreType.DMA((count,)),
            pltpu.SemaphoreType.DMA((count, 2)),
            pltpu.SemaphoreType.DMA((count, 2)),
            pltpu.SemaphoreType.DMA((count,)),
        ]

    @staticmethod
    def build(part, refs, total):
        return LineSum(part, refs[0], refs[1], refs[2], total, refs[3:10])

    @staticmethod
    def peers():
        return 2

    def greet(self, barrier):
        pl.semaphore_signal(
            barrier, inc=1, device_id={"tp": jnp.where(self.is_mid, self.outer, self.mid)},
            device_id_type=MESH,
        )

        @pl.when(self.is_mid)
        def _():
            pl.semaphore_signal(
                barrier, inc=1, device_id={"tp": self.other_mid}, device_id_type=MESH
            )

    def greet_count(self):
        return jnp.where(self.is_mid, 2, 1)

    def _to_mid(self, w, h):
        return remote(self.send.at[w, h], self.from_outer.at[w, h], self.s_out.at[w, h],
                      self.r_out.at[w, h], {"tp": self.mid})

    def _across(self, w):
        return remote(self.send.at[w, self.other], self.from_mid.at[w], self.s_mid.at[w],
                      self.r_mid.at[w], {"tp": self.other_mid})

    def _total_across(self, w, h):
        return remote(self.total.at[w, h], self.total.at[w, h], self.s_cross.at[w],
                      self.r_tot.at[w, h], {"tp": self.other_mid})

    def _total_out(self, w, h):
        return remote(self.total.at[w, h], self.total.at[w, h], self.s_tot.at[w, h],
                      self.r_tot.at[w, h], {"tp": self.outer})

    def order(self, w):
        return (2 * w, 2 * w + 1)

    def put(self, w, value):
        for s in range(2):
            for h in range(2):
                self.part[2 * w + s, h] = value[s * ROWS : (s + 1) * ROWS, h * HALF : (h + 1) * HALF]

    def get(self, w):
        return jnp.concatenate(
            [
                jnp.concatenate([self.total[2 * w + s, h].astype(F32) for h in range(2)], axis=1)
                for s in range(2)
            ],
            axis=0,
        )

    def start(self, w):
        @pl.when(self.is_outer)
        def _():
            for h in (self.other, self.own):
                for j in self.order(w):
                    self.send[j, h] = self.part[j, h].astype(BF)
                    self._to_mid(j, h).start()

    def cross(self, w):
        @pl.when(self.is_mid)
        def _():
            for j in self.order(w):
                self._to_mid(j, self.other).wait_recv()
                self.send[j, self.other] = (
                    self.part[j, self.other] + self.from_outer[j, self.other].astype(F32)
                ).astype(BF)
                self._across(j).start()

    def settle(self, w):
        @pl.when(self.is_mid)
        def _():
            for j in (2 * w, 2 * w + 1):
                self._to_mid(j, self.own).wait_recv()
                self._across(j).wait_recv()
                self.total[j, self.own] = (
                    self.part[j, self.own]
                    + self.from_outer[j, self.own].astype(F32)
                    + self.from_mid[j].astype(F32)
                ).astype(BF)
                self._total_across(j, self.own).start()
                self._total_out(j, self.own).start()

    def hand(self, w):
        @pl.when(self.is_mid)
        def _():
            for j in (2 * w, 2 * w + 1):
                self._total_across(j, self.other).wait_recv()
                self._total_out(j, self.other).start()

    def arrive(self, w):
        @pl.when(self.is_outer)
        def _():
            for j in (2 * w, 2 * w + 1):
                self._total_out(j, 0).wait_recv()
                self._total_out(j, 1).wait_recv()

    def drain(self, w):
        @pl.when(self.is_outer)
        def _():
            for j in (2 * w, 2 * w + 1):
                self._to_mid(j, 0).wait_send()
                self._to_mid(j, 1).wait_send()

        @pl.when(self.is_mid)
        def _():
            for j in (2 * w, 2 * w + 1):
                self._across(j).wait_send()
                self._total_across(j, self.own).wait_send()
                self._total_out(j, 0).wait_send()
                self._total_out(j, 1).wait_send()


class TradeSum(LineSum):
    def __init__(self, base, away, sems):
        self.__dict__.update(base.__dict__)
        self.away, (self.s_ctx, self.r_ctx) = away, sems
        self.ctx = 1 - lax.axis_index("ctx")

    def order(self, w):
        return (2 * w + 1, 2 * w)

    def _trade(self, w):
        return remote(self.away.at[w], self.total.at[2 * w + 1, self.own], self.s_ctx.at[w],
                      self.r_ctx.at[w], {"ctx": self.ctx})

    def settle(self, w):
        @pl.when(self.is_mid)
        def _():
            for s, j in ((1, 2 * w + 1), (0, 2 * w)):
                self._to_mid(j, self.own).wait_recv()
                self._across(j).wait_recv()
                whole = (
                    self.part[j, self.own]
                    + self.from_outer[j, self.own].astype(F32)
                    + self.from_mid[j].astype(F32)
                ).astype(BF)
                if s == 1:
                    self.away[w] = whole
                    self._trade(w).start()
                else:
                    self.total[j, self.own] = whole
                    self._total_across(j, self.own).start()
                    self._total_out(j, self.own).start()

    def trade(self, w):
        @pl.when(self.is_mid)
        def _():
            j = 2 * w + 1
            self._trade(w).wait_recv()
            self._total_across(j, self.own).start()
            self._total_out(j, self.own).start()

    def drain(self, w):
        LineSum.drain(self, w)

        @pl.when(self.is_mid)
        def _():
            self._trade(w).wait_send()


class ShardSum:
    def __init__(self, block_of, out, refs):
        self.block_of, self.out = block_of, out
        self.snd1, self.rcv1, self.snd2, self.rcv2, self.snd3, self.rcv3, self.s, self.r = refs
        f = lax.axis_index("fsdp")
        core = lax.rem(f, 2)
        self.f, self.core = f, core
        self.near, self.far = f + 1 - 2 * core, lax.rem(f + 2, 4)
        self.ctx = 1 - lax.axis_index("ctx")

    @staticmethod
    def scratch(shape):
        return [
            pltpu.VMEM((2, *shape), BF), pltpu.VMEM((2, *shape), BF),
            pltpu.VMEM(shape, BF), pltpu.VMEM(shape, BF),
            pltpu.VMEM(shape, BF), pltpu.VMEM(shape, BF),
            pltpu.SemaphoreType.DMA((4,)), pltpu.SemaphoreType.DMA((4,)),
        ]

    def _near(self, x):
        return remote(self.snd1.at[x], self.rcv1.at[x], self.s.at[x], self.r.at[x], {"fsdp": self.near})

    def _far(self):
        return remote(self.snd2, self.rcv2, self.s.at[2], self.r.at[2], {"fsdp": self.far})

    def _ctx(self):
        return remote(self.snd3, self.rcv3, self.s.at[3], self.r.at[3], {"ctx": self.ctx})

    def start(self):
        for x in range(2):
            self.snd1[x] = self.block_of(2 * x + 1 - self.core).astype(BF)
            self._near(x).start()

    def pair(self):
        for x in range(2):
            self._near(x).wait_recv()
        other = lax.div(self.far, 2)
        self.snd2[...] = (self.block_of(self.far) + self.rcv1[other].astype(F32)).astype(BF)
        self._far().start()
        mine = lax.div(self.f, 2)
        self.out[...] = self.block_of(self.f) + self.rcv1[mine].astype(F32)

    def cross(self):
        self._far().wait_recv()
        self.snd3[...] = (self.out[...] + self.rcv2[...].astype(F32)).astype(BF)
        self._ctx().start()

    def finish(self):
        self._ctx().wait_recv()
        self.out[...] = self.snd3[...].astype(F32) + self.rcv3[...].astype(F32)

    def drain(self):
        for x in range(2):
            self._near(x).wait_send()
        self._far().wait_send()
        self._ctx().wait_send()


class BandFirstSum:
    def __init__(self, block_of, out, refs):
        self.block_of, self.out = block_of, out
        self.snd1, self.rcv1, self.sndy, self.rcvy, self.sndx, self.rcvx, self.sndf, self.rcvf = refs[:8]
        self.s, self.r = refs[8:]
        f = lax.axis_index("fsdp")
        self.f, self.core, self.x = f, lax.rem(f, 2), lax.div(f, 2)
        self.near, self.far = f + 1 - 2 * self.core, lax.rem(f + 2, 4)
        self.c = lax.axis_index("ctx")
        self.half = out.shape[0] // 2

    @staticmethod
    def scratch(shape):
        two = (2, *shape)
        half = (shape[0] // 2, shape[1])
        shapes = [two, two, (2, *half), (2, *half), half, half, half, half]
        return [*[pltpu.VMEM(u, BF) for u in shapes], pltpu.SemaphoreType.DMA((5,)),
                pltpu.SemaphoreType.DMA((5,))]

    def _near(self, x):
        return remote(self.snd1.at[x], self.rcv1.at[x], self.s.at[x], self.r.at[x], {"fsdp": self.near})

    def _copy(self, n):
        src, dst = ((self.sndy, self.rcvy), (self.sndx, self.rcvx), (self.sndf, self.rcvf))[n]
        where = {"fsdp": self.far} if n == 1 else {"ctx": 1 - self.c}
        return remote(src, dst, self.s.at[2 + n], self.r.at[2 + n], where)

    def _rows(self, c):
        return pl.ds(pl.multiple_of(c * self.half, self.half), self.half)

    def _sum(self, x, c):
        return self.block_of(2 * x + self.core, c * self.half, self.half) + self.rcv1[
            x, self._rows(c), :
        ].astype(F32)

    def start(self):
        for x in range(2):
            self.snd1[x] = self.block_of(2 * x + 1 - self.core, 0, 2 * self.half).astype(BF)
            self._near(x).start()

    def pair(self):
        for x in range(2):
            self._near(x).wait_recv()
            self.sndy[x] = self._sum(x, 1 - self.c).astype(BF)
        self._copy(0).start()

    def cross(self):
        self._copy(0).wait_recv()
        other = 1 - self.x
        self.sndx[...] = (self._sum(other, self.c) + self.rcvy[other].astype(F32)).astype(BF)
        self._copy(1).start()
        self.out[self._rows(self.c), :] = self._sum(self.x, self.c) + self.rcvy[self.x].astype(F32)

    def share(self):
        self._copy(1).wait_recv()
        self.sndf[...] = (self.out[self._rows(self.c), :] + self.rcvx[...].astype(F32)).astype(BF)
        self._copy(2).start()

    def finish(self):
        self._copy(2).wait_recv()
        self.out[self._rows(self.c), :] = self.sndf[...].astype(F32)
        self.out[self._rows(1 - self.c), :] = self.rcvf[...].astype(F32)

    def drain(self):
        for x in range(2):
            self._near(x).wait_send()
        for n in range(3):
            self._copy(n).wait_send()


def vmem_call(body, outs, scratch, name, collective_id, in_place, out_place):
    remote_kernel = {} if collective_id is None else dict(
        collective_id=collective_id, has_side_effects=True
    )
    anywhere = pl.BlockSpec(memory_space=pl.ANY)

    def call(*args):
        few_in = [pltpu.VMEM(u.shape, u.dtype) for u in args[in_place:]]
        few_out = [pltpu.VMEM(s, t) for s, t in outs[out_place:]]

        def whole(*refs):
            ins, results, own, vm_in, vm_out, sems = take(
                refs, (len(args), len(outs), len(scratch), len(few_in), len(few_out), 2)
            )
            fetch = [
                pltpu.make_async_copy(src, dst, sems[0].at[n])
                for n, (src, dst) in enumerate(zip(ins[in_place:], vm_in))
            ]
            for copy in fetch:
                copy.start()

            def ready():
                for copy in fetch:
                    copy.wait()

            body(ready, *ins[:in_place], *vm_in, *results[:out_place], *vm_out, *own)
            store = [
                pltpu.make_async_copy(src, dst, sems[1].at[n])
                for n, (src, dst) in enumerate(zip(vm_out, results[out_place:]))
            ]
            for copy in store:
                copy.start()
            for copy in store:
                copy.wait()

        return pl.pallas_call(
            whole,
            out_shape=[jax.ShapeDtypeStruct(s, t) for s, t in outs],
            in_specs=[anywhere] * len(args),
            out_specs=[anywhere] * len(outs),
            scratch_shapes=[
                *scratch, *few_in, *few_out,
                pltpu.SemaphoreType.DMA((len(few_in),)), pltpu.SemaphoreType.DMA((len(few_out),)),
            ],
            compiler_params=pltpu.CompilerParams(vmem_limit_bytes=VMEM_LIMIT, **remote_kernel),
            name=name,
        )(*args)

    return call


def take(refs, counts):
    groups, at = [], 0
    for n in counts:
        groups.append(refs[at : at + n])
        at += n
    return groups


def window_rows(row_of, row_tmp, image, dst):
    for r in range(WIN):
        row_tmp[...] = row_of(image, r).astype(F32)
        dst[2 * image, r * WIN : (r + 1) * WIN, :] = row_tmp[SHIFT : SHIFT + WIN, :]
        dst[2 * image + 1, r * WIN : r * WIN + SHIFT, :] = row_tmp[SHIFT + WIN :, :]
        dst[2 * image + 1, r * WIN + SHIFT : (r + 1) * WIN, :] = row_tmp[:SHIFT, :]


def home_row(delta, row_tmp, image, r):
    row_tmp[SHIFT : SHIFT + WIN, :] = delta[2 * image, r * WIN : (r + 1) * WIN, :]
    row_tmp[SHIFT + WIN :, :] = delta[2 * image + 1, r * WIN : r * WIN + SHIFT, :]
    row_tmp[:SHIFT, :] = delta[2 * image + 1, r * WIN + SHIFT : (r + 1) * WIN, :]
    return row_tmp[...].astype(BF)


class HomeRows:
    def __init__(self, delta, row_tmp, out, halo, send, recv):
        self.delta, self.row_tmp, self.out, self.halo, self.s, self.r = (
            delta, row_tmp, out, halo, send, recv,
        )

    def _copy(self, i):
        return remote(self.halo.at[i], self.out.at[i, 0:SHIFT], self.s.at[i], self.r.at[i],
                      {"ctx": 1 - lax.axis_index("ctx")})

    def go(self, i):
        for r in range(SHIFT, WIN):
            self.halo[i, r - SHIFT] = home_row(self.delta, self.row_tmp, i, r)
        self._copy(i).start()
        for r in range(SHIFT):
            self.out[i, SHIFT + r] = home_row(self.delta, self.row_tmp, i, r)

    def wait(self, i):
        self._copy(i).wait_recv()
        self._copy(i).wait_send()


class TableSum:
    def __init__(self, part, refs):
        self.part = part
        self.snd1, self.rcv1, self.snd2, self.rcv2, self.snd3, self.rcv3, self.s, self.r = refs
        f = lax.axis_index("fsdp")
        self.core, self.x, self.c = lax.rem(f, 2), lax.div(f, 2), lax.axis_index("ctx")
        self.near, self.far = f + 1 - 2 * self.core, lax.rem(f + 2, 4)

    @staticmethod
    def scratch(heads):
        shapes = [(heads, 2, 2, 24, 256)] * 2 + [(heads, 2, 24, 256)] * 2 + [(heads, 24, 256)] * 2
        return [*[pltpu.VMEM(s, BF) for s in shapes], pltpu.SemaphoreType.DMA((3,)),
                pltpu.SemaphoreType.DMA((3,))]

    def _copy(self, n):
        src, dst = ((self.snd1, self.rcv1), (self.snd2, self.rcv2), (self.snd3, self.rcv3))[n]
        where = ({"fsdp": self.near}, {"fsdp": self.far}, {"ctx": 1 - self.c})[n]
        return remote(src, dst, self.s.at[n], self.r.at[n], where)

    def rows(self, core, x, c):
        return pl.ds(pl.multiple_of(core * 96 + x * 48 + c * 24, 8), 24)

    def start(self):
        for x in range(2):
            for c in range(2):
                self.snd1[:, x, c] = self.part[:, self.rows(1 - self.core, x, c), :].astype(BF)
        self._copy(0).start()

    def pair(self):
        self._copy(0).wait_recv()
        x = 1 - self.x
        for c in range(2):
            self.snd2[:, c] = (
                self.part[:, self.rows(self.core, x, c), :] + self.rcv1[:, x, c].astype(F32)
            ).astype(BF)
        self._copy(1).start()

    def cross(self):
        self._copy(1).wait_recv()
        c = 1 - self.c
        self.snd3[...] = (
            self.part[:, self.rows(self.core, self.x, c), :] + self.rcv1[:, self.x, c].astype(F32)
            + self.rcv2[:, c].astype(F32)
        ).astype(BF)
        self._copy(2).start()

    def finish(self, out):
        self._copy(2).wait_recv()
        out[...] = (
            self.part[:, self.rows(self.core, self.x, self.c), :]
            + self.rcv1[:, self.x, self.c].astype(F32)
            + self.rcv2[:, self.c].astype(F32) + self.rcv3[...].astype(F32)
        )

    def first_row(self):
        return self.core * 96 + self.x * 48 + self.c * 24

    def drain(self):
        for n in range(3):
            self._copy(n).wait_send()


def total_of(x):
    return jnp.sum(jnp.sum(x, axis=1, keepdims=True), axis=0, keepdims=True)


def exact(a, b, dims):
    return lax.dot_general(
        a, b, (dims, ((), ())), precision=lax.Precision.HIGHEST, preferred_element_type=F32
    )


def lane_sums(squares):
    return exact(jnp.ones((8, squares.shape[1]), F32), squares, ((1,), (1,)))[0:1]


def as_column(row):
    n = row.shape[1]
    step = 64
    eye = lax.broadcasted_iota(jnp.int32, (step, step), 0) == lax.broadcasted_iota(
        jnp.int32, (step, step), 1
    )
    return jnp.concatenate(
        [
            jnp.sum(
                jnp.where(eye, jnp.broadcast_to(row[:, at : at + step], (step, step)), 0.0),
                axis=1, keepdims=True,
            )
            for at in range(0, n, step)
        ],
        axis=0,
    )


def lane_pack(values):
    lane = lax.broadcasted_iota(jnp.int32, (8, 128), 1)
    packed = jnp.zeros((8, 128), F32)
    for n, value in enumerate(values):
        packed = packed + jnp.where(lane == n, jnp.broadcast_to(value, (8, 128)), 0.0)
    return packed


def wide(ref):
    if ref.shape[1] != 128:
        return ref[...]
    return jnp.concatenate([ref[n : n + 1, :] for n in range(ref.shape[0])], axis=1)


def put_wide(ref, row):
    if ref.shape[1] != 128:
        ref[...] = row
    else:
        for n in range(ref.shape[0]):
            ref[n : n + 1, :] = row[:, n * 128 : (n + 1) * 128]


def plain(grad, state):
    new = DECAY_RATE * state + (1.0 - DECAY_RATE) * (grad * grad + STAT_EPS)
    return new, grad * lax.rsqrt(new)


def update_scales(rq, kq, rp, kp, ru, ku, rd, kd, means):
    def outer(first, second):
        return as_column(lax.rsqrt(first)) * lax.rsqrt(second)

    return [
        *[outer(rq[n : n + 1, :] / means[n], kq[n : n + 1, :]) for n in range(3)],
        outer(rp / means[3], kp), outer(ru / means[4], ku), outer(kd, rd / means[5]),
    ]


def step_body(ready, *refs):
    (
        big_inputs,
        (regions, ridx_m, w_norm, w_heads, w_hidden, w_table),
        (row_qkv, col_qkv, row_proj, col_proj, row_up, col_up, row_down, col_down),
        (s_norm, s_heads, s_hidden, s_table),
        big_outputs, (gn_o, gh_o, gx_o, gt_o),
        (rq_o, kq_o, rp_o, kp_o, ru_o, ku_o, rd_o, kd_o, size_o),
        (sm_g, wq, wp_g, wp, wu, wd, fh, gh, og_low, bias_s, row_tmp, rows, ridx, table_t, small),
        (xw, ogw, n1, q, k, v, probs, ctx, part),
        (n2_s, hid_s, dpl_s, xhat_s, rstd_s, tot_two, gu, gd, dft, dbr, mix),
        (dh_s, dpos_s, chunk_s, tot_four),
        ls_two, ls_four, up_refs, down_refs, qkv_refs, proj_refs, table_refs,
        (sm_s, sm_r, t_s, f_s, z_s, c_s),
        (feat, og, w_qkv, w_proj, w_up, w_down), (tot_mix, away, y_send, y_recv, i_sem, d_send, d_recv),
        (home_o, gin_o, gq_o, gp_o, gu_o, gd_o, o_sem),
        (w_send, w_recv, p_send, p_recv, v_send, v_recv, h_send, h_recv, a_send, a_recv,
         x_send, x_recv),
        (sm_send, sm_recv, t_send, t_recv, f_send, f_recv, z_send, z_recv, c_send, c_recv),
    ) = take(refs, (6, 6, 8, 4, 6, 4, 9, 15, 9, 11, 4, 10, 10, 8, 10, 24, 8, 8, 6, 6, 7, 7, 12, 10))
    windows, heads = probs.shape[0], probs.shape[1]
    images = windows // 2
    width = q.shape[2]
    shard = w_qkv.shape[1]
    hidden = w_up.shape[1]
    ff = 4 * hidden
    f, c, t = lax.axis_index("fsdp"), lax.axis_index("ctx"), lax.axis_index("tp")
    near, far = f + 1 - 2 * lax.rem(f, 2), lax.rem(f + 2, 4)
    me = f * 4 + t
    two = LineSum.build(part, ls_two, tot_two)
    four = LineSum.build(part, ls_four, tot_four)
    mixl = TradeSum(LineSum.build(mix, ls_two, tot_mix), away, (y_send, y_recv))

    def block(at):
        return pl.ds(pl.multiple_of(at * shard, shard), shard)

    def band(at):
        return pl.ds(pl.multiple_of(at * width, width), width)

    def other(n):
        at = lax.rem(me + n, 16)
        return {"fsdp": lax.div(at, 4), "tp": lax.rem(at, 4)}

    up = ShardSum(lambda at: gu[block(at), :], gu_o, up_refs)
    down = BandFirstSum(
        lambda at, first, size: gd[pl.ds(pl.multiple_of(at * shard + first, 32), size), :], gd_o, down_refs
    )
    qkv = [
        ShardSum(
            lambda at, n=n: gu[block(at), n * 256 : n * 256 + width], gq_o.at[n], qkv_refs[8 * n : 8 * n + 8]
        )
        for n in range(3)
    ]
    proj = ShardSum(lambda at: gd[block(at), :shard], gp_o, proj_refs)
    table = TableSum(dpos_s, table_refs)
    barrier = pltpu.get_barrier_semaphore()
    greet(barrier, [{"ctx": 1 - c}] + [other(n) for n in range(1, 16)])
    fetch = [
        pltpu.make_async_copy(src, dst, i_sem.at[n])
        for n, (src, dst) in enumerate(zip(big_inputs, (feat, og, w_qkv, w_proj, w_up, w_down)))
    ]
    for n in (2, 3, 0, 4, 5, 1):
        fetch[n].start()

    store = [
        pltpu.make_async_copy(src, dst, o_sem.at[n])
        for n, (src, dst) in enumerate(zip((home_o, gin_o, gq_o, gp_o, gu_o, gd_o), big_outputs))
    ]

    ready()

    part_of = HD // 4

    def ints(shape, axis):
        return lax.broadcasted_iota(jnp.int32, shape, axis)

    def ones_where(cond):
        return jnp.where(cond, 1.0, 0.0).astype(BF)

    def flat_units(values, count):
        lanes = count * part_of
        spread = dot(values, ones_where(jnp.bitwise_and(ints((part_of, lanes), 1), 7) == ints((part_of, lanes), 0)))
        return jnp.sum(
            jnp.where(jnp.right_shift(ints((count, lanes), 1), 3) == ints((count, lanes), 0), spread, 0.0),
            axis=0, keepdims=True,
        )

    units = hidden // HD
    lanes = units * part_of
    spread = dot(
        w_hidden[...].astype(BF),
        ones_where(jnp.right_shift(ints((units, lanes), 1), 3) == ints((units, lanes), 0)),
    )
    hidden_row = jnp.sum(
        jnp.where(jnp.bitwise_and(ints((8, lanes), 1), 7) == ints((8, lanes), 0), spread, 0.0),
        axis=0, keepdims=True,
    )
    own = jnp.concatenate([w_norm[...], jnp.zeros((2, shard), F32), hidden_row, jnp.zeros((7, shard), F32)], axis=0)
    small[0:16, :shard] = own
    small[0:16, shard:] = jnp.zeros((16, D - shard), F32)
    for n in range(2):
        small[9 + n : 10 + n, : heads * part_of] = flat_units(w_heads[:, n, :].astype(BF), heads)
    sm_g[f] = small[0:16, :shard].astype(BF)
    fetch[2].wait()
    wq[:, block(f), :] = w_qkv[...].astype(BF)
    fetch[3].wait()
    wp_g[f, band(t), :] = w_proj[...].astype(BF)
    fetch[0].wait()
    fetch[4].wait()
    wu[block(f), :] = w_up[...].astype(BF)
    fetch[5].wait()
    wd[block(f), :] = w_down[...].astype(BF)
    fetch[1].wait()
    for i in range(images):
        og_low[i] = og[i, 0:SHIFT].astype(BF)
    pl.semaphore_wait(barrier, 16)

    items = [
        lambda at: sm_g.at[at],
        lambda at: wq.at[:, block(at), :],
    ]
    half = shard // 2

    def split_copies(full, k):
        def piece(n, at, cc, where):
            ref = full.at[block(at), :] if cc is None else full.at[
                pl.ds(pl.multiple_of(at * shard + cc * half, half), half), :
            ]
            return remote(ref, ref, d_send.at[k, n], d_recv.at[k, n], where)

        return (
            piece(0, f, c, {"fsdp": far}), piece(1, f, None, {"fsdp": near}),
            piece(2, far, c, {"ctx": 1 - c}), piece(3, far, c, {"fsdp": near}),
            piece(4, far, 1 - c, {"fsdp": near}),
        )

    down_copies = split_copies(wd, 0)
    up_copies = split_copies(wu, 1)

    def copy_of(n, kind, at, where):
        ref = items[n](at)
        return remote(ref, ref, w_send.at[n, kind], w_recv.at[n, kind], {"fsdp": where})

    def proj_copy(n, kind, at, where):
        ref = wp_g.at[at, band(lax.rem(t - n + 4, 4))]
        return remote(ref, ref, p_send.at[n, kind], p_recv.at[n, kind], {"fsdp": where})

    def proj_line(n):
        ref = wp_g.at[f, band(t)]
        return remote(ref, ref, v_send.at[n], v_recv.at[n], {"tp": lax.rem(t + n, 4)})

    halo_f = [
        remote(feat.at[i, 0:SHIFT], fh.at[i], h_send.at[i], h_recv.at[i], {"ctx": 1 - c})
        for i in range(images)
    ]
    halo_g = [
        remote(og_low.at[i], gh.at[i], h_send.at[images + i], h_recv.at[images + i], {"ctx": 1 - c})
        for i in range(images)
    ]

    def send_both(n):
        copy_of(n, 0, f, far).start()
        copy_of(n, 1, f, near).start()

    def proj_both(n):
        proj_copy(n, 0, f, far).start()
        proj_copy(n, 1, f, near).start()

    send_both(0)
    for copy in halo_f:
        copy.start()
    for n in range(1, 4):
        proj_line(n).start()
    send_both(1)
    proj_both(0)
    down_copies[0].start()
    up_copies[0].start()
    halo_g[0].start()
    down_copies[1].start()
    up_copies[1].start()

    def relay(n):
        copy_of(n, 0, f, far).wait_recv()
        copy_of(n, 2, far, near).start()

    def gathered(n):
        copy_of(n, 1, f, near).wait_recv()
        copy_of(n, 2, far, near).wait_recv()

    ridx[...] = jnp.zeros_like(ridx)
    ridx[:TOK, :TOK] = ridx_m[...]
    table_t[...] = jnp.zeros_like(table_t)
    table_t[:heads, : w_table.shape[1]] = w_table[...].astype(BF).astype(F32)

    def bias_rows(step, carry):
        rows_at = pl.ds(pl.multiple_of(step * 8, 8), 8)
        for half in range(2):
            lanes_at = slice(half * 128, (half + 1) * 128)
            idx = ridx[rows_at, lanes_at]
            low = jnp.bitwise_and(idx, 127)
            high = jnp.right_shift(idx, 7)
            picks = [high == n for n in range(5)]
            for h in range(heads):
                found = jnp.zeros((8, 128), F32)
                for n in range(5):
                    tab = jnp.broadcast_to(table_t[h : h + 1, n * 128 : (n + 1) * 128], (8, 128))
                    got = jnp.take_along_axis(tab, low, axis=1, mode="promise_in_bounds")
                    found = jnp.where(picks[n], got, found)
                bias_s[h, rows_at, lanes_at] = found
        return carry

    lax.fori_loop(0, TOK // 8, bias_rows, 0)
    relay(0)
    dpos_s[...] = jnp.zeros_like(dpos_s)
    for n in range(1, 4):
        proj_line(n).wait_recv()
        proj_both(n)
    gathered(0)
    rows[...] = jnp.concatenate([sm_g[n].astype(F32) for n in range(4)], axis=1)
    unit = ints((shard, D), 0)
    lane = ints((shard, D), 1)
    biases = jnp.zeros((16, D), F32)
    for n in range(4):
        same = jnp.logical_and(
            jnp.right_shift(lane, 5) == jnp.right_shift(unit, 3),
            jnp.bitwise_and(lane, 31) == jnp.bitwise_and(unit, 7) + n * 8,
        )
        biases = biases + dot(sm_g[n], ones_where(same))
    rows[8:16, :] = biases[8:16, :]
    small[...] = jnp.zeros_like(small)
    relay(1)

    def enter(i):
        halo_f[i].wait_recv()
        window_rows(
            lambda im, r: feat[im, SHIFT + r] if r < SHIFT else fh[im, r - SHIFT], row_tmp, i, xw
        )

    enter(0)
    gain_one, offset_one = rows[0:1, :], rows[1:2, :]
    bias_proj, gain_two, offset_two = rows[2:3, :], rows[3:4, :], rows[4:5, :]
    bias_hidden = rows[8:9, :]
    bias_q, bias_v = rows[9:10, :width], rows[10:11, :width]
    head_of = jnp.right_shift(ints((1, width), 1), 5)
    picks_of = [ones_where(head_of == h) for h in range(heads)]

    def over(p):
        return jnp.right_shift(p * 171, 11)

    def region_forms(w):
        i, j = lax.div(w, 2), lax.rem(w, 2)
        both = jnp.where(i == 0, regions[:, 0, :], regions[:, 1, :]).astype(F32)
        square = jnp.where(j == 0, both[:, :WIN], both[:, WIN:]).astype(BF)
        p_row, r_row = ints((WIN, TOK), 1), ints((WIN, TOK), 0)
        spread_row = dot(square, ones_where(p_row - WIN * over(p_row) == r_row))
        row = jnp.sum(jnp.where(over(p_row) == r_row, spread_row, 0.0), axis=0, keepdims=True)
        p_col, r_col = ints((TOK, WIN), 0), ints((TOK, WIN), 1)
        spread_col = dot(ones_where(over(p_col) == r_col), square)
        col = jnp.sum(
            jnp.where(p_col - WIN * over(p_col) == r_col, spread_col, 0.0), axis=1, keepdims=True
        )
        return row, col

    def spot(w):
        return pl.ds(pl.multiple_of(w * TOK, TOK), TOK)

    def add_rows(n, term):
        small[n : n + 1, : term.shape[1]] = small[n : n + 1, : term.shape[1]] + jnp.sum(
            term, axis=0, keepdims=True
        )

    def ctx_copy(p, kind, at, where):
        ref = ctx.at[p, at]
        return remote(ref, ref, x_send.at[p, kind], x_recv.at[p, at], {"tp": where})

    other_outer = 3 - two.outer

    def ctx_wait(p, at):
        ctx_copy(p, 0, at, two.mid).wait_recv()

    def pass_in(p):
        ctx_wait(p, two.outer)
        ctx_copy(p, 2, two.outer, two.other_mid).start()
        ctx_wait(p, two.other_mid)
        ctx_copy(p, 3, two.other_mid, two.outer).start()

    def pass_out(p):
        ctx_wait(p, other_outer)
        ctx_copy(p, 4, other_outer, two.outer).start()

    gathered(1)

    def forward(w, carry):
        @pl.when(w == 2)
        def _():
            enter(1)

        x = xw[w]
        centred = x - row_mean(x)
        xhat = centred * lax.rsqrt(row_mean(centred * centred) + NORM_EPS)
        normed = (xhat * gain_one + offset_one).astype(BF)
        n1[spot(w), :] = normed
        q_w = (dot(normed, wq[0]) + bias_q).astype(BF)
        k_w = dot(normed, wq[1]).astype(BF)
        v_w = (dot(normed, wq[2]) + bias_v).astype(BF)
        q[w] = q_w
        k[w] = k_w
        v[w] = v_w
        reg_row, reg_col = region_forms(w)
        mask = jnp.where(reg_col == reg_row, 0.0, MASK_FILL)
        context = jnp.zeros((TOK, width), F32)
        for h in range(heads):
            scores = dot_t(q_w * picks_of[h], k_w) * HD ** (-0.5) + bias_s[h, :, :TOK] + mask
            lifted = jnp.exp(scores - jnp.max(scores, axis=-1, keepdims=True))
            p = lifted / jnp.sum(lifted, axis=-1, keepdims=True)
            probs[w, h] = p
            context = context + dot(p.astype(BF), v_w * picks_of[h])
        low = context.astype(BF)
        p_at = lax.div(w, 2)

        @pl.when(lax.rem(w, 2) == 0)
        def _():
            ctx[p_at, t, :, :width] = low

        @pl.when(lax.rem(w, 2) == 1)
        def _():
            ctx[p_at, t, :, width:] = low
            ctx_copy(p_at, 0, t, jnp.where(two.is_mid, two.outer, two.mid)).start()

            @pl.when(two.is_mid)
            def _():
                ctx_copy(p_at, 1, t, two.other_mid).start()

        return carry

    lax.fori_loop(0, windows, forward, 0)
    for copies in (down_copies, up_copies):
        copies[0].wait_recv()
        copies[2].start()
        copies[3].start()
    for copy in halo_g[1:]:
        copy.start()

    @pl.when(two.is_mid)
    def _():
        pass_in(0)

    for n in range(4):
        proj_copy(n, 0, f, far).wait_recv()
        proj_copy(n, 2, far, near).start()

    @pl.when(two.is_mid)
    def _():
        pass_out(0)
        pass_in(1)

    down_copies[2].wait_recv()
    down_copies[4].start()

    for n in range(4):
        proj_copy(n, 1, f, near).wait_recv()
        proj_copy(n, 2, far, near).wait_recv()
    wp[...] = jnp.concatenate([wp_g[n] for n in range(4)], axis=1)
    up_copies[2].wait_recv()
    up_copies[4].start()
    for n in (1, 3, 4):
        down_copies[n].wait_recv()
        up_copies[n].wait_recv()

    def middle(w, carry):
        p_at, odd = lax.div(w, 2), lax.rem(w, 2) == 1

        @pl.when(jnp.logical_and(two.is_outer, jnp.logical_not(odd)))
        def _():
            for at in (two.mid, two.other_mid, other_outer):
                ctx_wait(p_at, at)

        branch = jnp.zeros((TOK, D), F32) + bias_proj
        for n in range(4):
            both = ctx[p_at, n]
            low = jnp.where(odd, both[:, width:], both[:, :width])
            branch = branch + dot(low, wp[n * width : (n + 1) * width, :])
        resid = xw[w] + branch
        centred = resid - row_mean(resid)
        rstd = lax.rsqrt(row_mean(centred * centred) + NORM_EPS)
        xhat = centred * rstd
        xhat_s[w] = xhat
        rstd_s[w] = jnp.broadcast_to(rstd, (TOK, 128))
        normed = (xhat * gain_two + offset_two).astype(BF)
        n2_s[spot(w), :] = normed
        pre = dot(normed, wu[...]) + bias_hidden
        cdf = 0.5 * (1.0 + lax.erf(pre * 0.7071067811865476))
        slope = cdf + pre * (jnp.exp(-0.5 * (pre * pre)) * 0.3989422804014327)
        hid = (pre * cdf).astype(BF)
        hid_s[spot(w), :] = hid

        for n in range(images):

            @pl.when(w == 2 * n)
            def _():
                halo_g[n].wait_recv()
                window_rows(
                    lambda im, r: og[im, SHIFT + r] if r < SHIFT else gh[im, r - SHIFT],
                    row_tmp, n, ogw,
                )

        @pl.when(jnp.logical_and(two.is_mid, w == 0))
        def _():
            pass_out(1)

        @pl.when(w >= 3)
        def _():
            two.hand(w - 3)

        @pl.when(w >= 2)
        def _():
            two.settle(w - 2)

        @pl.when(w >= 1)
        def _():
            two.cross(w - 1)

        low = ogw[w].astype(BF)
        d_pre = dot(low, wd[...]) * slope
        add_rows(6, d_pre)
        dpl = d_pre.astype(BF)
        dpl_s[spot(w), :] = dpl
        two.put(w, dot_t(dpl, wu[...]))
        two.start(w)
        mixl.put(w, dot_t(hid, wd[...]))

        @pl.when(two.is_mid)
        def _():
            whole = branch + rows[5:6, :]
            for s in range(2):
                for h in range(2):

                    @pl.when(two.own == h)
                    def _():
                        mix[2 * w + s, h] = (
                            mix[2 * w + s, h]
                            + whole[s * ROWS : (s + 1) * ROWS, h * HALF : (h + 1) * HALF]
                        )

        return carry

    lax.fori_loop(0, windows, middle, 0)
    two.cross(windows - 1)

    def grad_chunk(m, carry):
        chunk = pl.ds(pl.multiple_of(m * 256, 256), 256)
        low = jnp.concatenate([ogw[w, :, chunk] for w in range(windows)], axis=0).astype(BF)
        gd[chunk, :] = t_dot(low, hid_s[...])
        gu[chunk, :] = t_dot(n2_s[:, chunk], dpl_s[...])
        return carry

    two.hand(windows - 3)
    two.settle(windows - 2)
    lax.fori_loop(0, D // 256, grad_chunk, 0)
    down.start()
    up.start()

    def backward(w, carry):
        two.arrive(w)
        d_two = two.get(w)
        xhat = xhat_s[w]
        e = d_two * gain_two
        d_flat = (e - row_mean(e) - xhat * row_mean(e * xhat)) * rstd_s[w, :, 0:1]
        og_w = ogw[w]
        d_resid = og_w + d_flat
        dft[w] = d_flat
        d_branch = d_resid.astype(BF)
        dbr[spot(w), :] = d_branch
        for n, term in ((2, d_resid), (3, d_two * xhat), (4, d_two), (5, og_w)):
            add_rows(n, term)
        d_ctx = dot_t(d_branch, wp[band(t), :]).astype(BF)
        q_w, k_w, v_w = q[w], k[w], v[w]
        d_q = jnp.zeros((TOK, width), F32)
        d_k = jnp.zeros((TOK, width), F32)
        d_v = jnp.zeros((TOK, width), F32)
        for h in range(heads):
            d_ctx_h = d_ctx * picks_of[h]
            p = probs[w, h]
            d_p = dot_t(d_ctx_h, v_w)
            d_v = d_v + t_dot(p.astype(BF), d_ctx_h)
            d_s = p * (d_p - jnp.sum(p * d_p, axis=-1, keepdims=True))
            dpos_s[h, :TOK, :TOK] = dpos_s[h, :TOK, :TOK] + d_s
            d_l = (d_s * HD ** (-0.5)).astype(BF)
            d_q = d_q + dot(d_l, k_w * picks_of[h])
            d_k = d_k + t_dot(d_l, q_w * picks_of[h])
        partial = jnp.zeros((TOK, D), F32)
        for n, d_n in enumerate((d_q, d_k, d_v)):
            low = d_n.astype(BF)
            dh_s[n, spot(w), :] = low
            partial = partial + dot_t(low, wq[n])
            if n != 1:
                add_rows(8 + n // 2, low.astype(F32))
        four.put(w, partial)
        four.start(w)

        @pl.when(w == 0)
        def _():
            down.pair()
            up.pair()
            two.settle(windows - 1)
            two.hand(windows - 2)

        @pl.when(w == 1)
        def _():
            two.hand(windows - 1)

        @pl.when(w >= 2)
        def _():
            four.cross(w - 2)

        @pl.when(w == 2)
        def _():
            down.cross()

        @pl.when(w == 3)
        def _():
            up.cross()

        return carry

    lax.fori_loop(0, windows, backward, 0)
    table.start()
    for n in range(3):
        gu[:, n * 256 : n * 256 + width] = t_dot(n1[...], dh_s[n])
        qkv[n].start()
    four.settle(0)
    ctx_own = jnp.concatenate(
        [ctx[w // 2, t, :, (w % 2) * width : (w % 2 + 1) * width] for w in range(windows)], axis=0
    )
    gp = t_dot(ctx_own, dbr[...])
    for n in range(4):
        gd[n * width : (n + 1) * width, :shard] = gp[:, n * shard : (n + 1) * shard]
    proj.start()
    for w in range(windows):
        two.drain(w)
        mixl.start(w)
    table.pair()
    down.share()
    four.cross(2)
    four.settle(1)
    for member in (*qkv, proj):
        member.pair()
    four.hand(0)
    four.cross(3)
    table.cross()
    four.hand(1)
    four.settle(2)
    qkv[0].cross()

    keep = 1.0 - DECAY_RATE
    first_f = jnp.where(f == 0, 1.0, 0.0)
    first_t = jnp.where(t == 0, 1.0, 0.0)
    old_rows = [
        first_t * jnp.sum(row_qkv[0:1, :], axis=1, keepdims=True),
        first_t * jnp.sum(row_qkv[1:2, :], axis=1, keepdims=True),
        first_t * jnp.sum(row_qkv[2:3, :], axis=1, keepdims=True),
        first_f * total_of(row_proj[...]),
        first_t * total_of(row_up[...]),
        first_f * total_of(row_down[...]),
    ]
    masters = [
        sum(total_of(w_qkv[n] * w_qkv[n]) for n in range(3)),
        total_of(w_proj[...] * w_proj[...]),
        total_of(w_up[...] * w_up[...]),
        total_of(w_down[...] * w_down[...]),
        *[
            first_t * jnp.sum(w_norm[n : n + 1, :] * w_norm[n : n + 1, :], axis=1, keepdims=True)
            for n in range(6)
        ],
        *[total_of(w_heads[:, n, :] * w_heads[:, n, :]) for n in range(2)],
        total_of(w_hidden[...] * w_hidden[...]),
        first_f * total_of(w_table[...] * w_table[...]),
    ]
    four.settle(3)

    for copy in halo_g:
        copy.wait_send()
    home_in = HomeRows(xhat_s, row_tmp, gin_o, og_low, a_send, a_recv)

    def back(w):
        four.arrive(w)
        x = xw[w]
        centred = x - row_mean(x)
        rstd = lax.rsqrt(row_mean(centred * centred) + NORM_EPS)
        xhat = centred * rstd
        d_one = four.get(w)
        e = d_one * gain_one
        xhat_s[w] = dft[w] + (e - row_mean(e) - xhat * row_mean(e * xhat)) * rstd
        for n, term in ((0, d_one * xhat), (1, d_one)):
            add_rows(n, term)

    back(0)
    mixl.cross(0)
    four.hand(2)
    qkv[1].cross()
    qkv[2].cross()
    back(1)
    four.hand(3)
    proj.cross()
    mixl.settle(0)
    mixl.cross(1)
    down.finish()
    up.finish()
    store[4].start()
    store[5].start()
    t_s[t] = jnp.zeros((8, shard), F32)
    f_s[f] = jnp.zeros((8, hidden), F32)
    sq_up = gu_o[...] * gu_o[...]
    sq_down = gd_o[...] * gd_o[...]
    t_s[t, 4:5, :] = lane_sums(sq_up)
    t_s[t, 5:6, :] = lane_sums(sq_down)
    f_s[f, 4:5, :] = jnp.sum(sq_up, axis=0, keepdims=True)
    f_s[f, 5:6, :] = jnp.sum(sq_down, axis=0, keepdims=True)
    tot_up, tot_down = total_of(sq_up), total_of(sq_down)
    table.finish(chunk_s)
    first = table.first_row()
    ident = ints((640, TOK), 0)

    def bin_row(step, acc):
        for n in range(4):
            i = step * 4 + n
            hot = ones_where(ident == ridx[pl.ds(first + i, 1), :TOK])
            vals = jnp.concatenate(
                [chunk_s[h, pl.ds(i, 1), :TOK] for h in range(heads)]
                + [jnp.zeros((8 - heads, TOK), F32)],
                axis=0,
            )
            high = vals.astype(BF)
            low = (vals - high.astype(F32)).astype(BF)
            acc = acc + dot_t(jnp.concatenate([high, low], axis=0), hot)
        return acc

    hist = lax.fori_loop(0, 3, bin_row, jnp.zeros((16, 640), F32))
    mixl.settle(1)
    back(2)
    mixl.trade(0)
    hist = lax.fori_loop(3, 6, bin_row, hist)
    small[16:24, :640] = hist[0:8] + hist[8:16]
    mixl.cross(2)
    home_in.go(0)
    back(3)
    sm_s[0] = small[...]

    def swap(n):
        where = ({"fsdp": near}, {"fsdp": far}, {"ctx": 1 - c})[n]
        return remote(sm_s.at[n], sm_r.at[n], sm_send.at[n], sm_recv.at[n], where)

    swap(0).start()
    mixl.hand(0)
    for member in (*qkv, proj):
        member.finish()
    store[2].start()
    store[3].start()

    tot_q = []
    for n in range(3):
        sq = gq_o[n] * gq_o[n]
        t_s[t, n : n + 1, :] = lane_sums(sq)
        f_s[f, n : n + 1, :width] = jnp.sum(sq, axis=0, keepdims=True)
        tot_q.append(total_of(sq))
    sq = gp_o[...] * gp_o[...]
    f_s[f, 3:4, :shard] = lane_sums(sq)
    t_s[t, 3:4, :] = jnp.sum(sq, axis=0, keepdims=True)
    z_s[me] = lane_pack([*tot_q, total_of(sq), tot_up, tot_down, *old_rows, *masters])

    def t_copy(n):
        return remote(t_s.at[t], t_s.at[t], t_send.at[n], t_recv.at[n], {"tp": lax.rem(t + n, 4)})

    def f_copy(n):
        return remote(f_s.at[f], f_s.at[f], f_send.at[n], f_recv.at[n], {"fsdp": lax.rem(f + n, 4)})

    def z_copy(n):
        return remote(z_s.at[me], z_s.at[me], z_send.at[n], z_recv.at[n], other(n))

    def c_copy(n):
        return remote(c_s.at[me], c_s.at[me], c_send.at[n], c_recv.at[n], other(n))

    for n in range(1, 4):
        t_copy(n).start()
        f_copy(n).start()
    for n in range(1, 16):
        z_copy(n).start()
    mixl.settle(2)
    mixl.trade(1)
    mixl.cross(3)
    swap(0).wait_recv()
    sm_s[1] = sm_s[0] + sm_r[0]
    swap(1).start()

    def lift(w):
        mixl.arrive(w)
        dft[w] = mixl.get(w)

    def leave(i):
        for r in range(WIN):
            home_o[i, (SHIFT + r) % WIN] = home_row(dft, row_tmp, i, r)

    mixl.hand(1)
    mixl.settle(3)
    home_in.go(1)
    mixl.trade(2)
    lift(0)
    swap(1).wait_recv()
    sm_s[2] = sm_s[1] + sm_r[1]
    swap(2).start()
    mixl.trade(3)
    mixl.hand(2)
    lift(1)
    leave(0)

    swap(2).wait_recv()
    sm = sm_s[2] + sm_r[2]

    def own_lanes(x, size):
        out = x[:, :size]
        for n in range(1, 4):
            out = jnp.where(f == n, x[:, n * size : (n + 1) * size], out)
        return out

    def own_units(row, count):
        all_lanes = count * HD
        at_lane = ints((count, all_lanes), 1)
        only = jnp.where(
            jnp.right_shift(at_lane, 5) == ints((count, all_lanes), 0),
            jnp.broadcast_to(row, (count, all_lanes)), 0.0,
        )
        pick = jnp.where(
            jnp.bitwise_and(ints((all_lanes, part_of), 0), HD - 1)
            == f * part_of + ints((all_lanes, part_of), 1),
            1.0, 0.0,
        )
        return only, pick

    gn = own_lanes(sm[0:6, :], shard)
    gh_new = [exact(*own_units(sm[8 + n : 9 + n, :width], heads), ((1,), (0,))) for n in range(2)]
    only, pick = own_units(sm[6:7, :], hidden // HD)
    gx = exact(pick, only, ((0,), (1,)))
    gt = sm[16 : 16 + heads, : w_table.shape[1]]
    gn_o[...] = gn
    gx_o[...] = gx
    gt_o[...] = gt
    small_sq = first_t * total_of(plain(gn, s_norm[...])[1] ** 2)
    for n in range(2):
        gh_o[:, n, :] = gh_new[n]
        small_sq = small_sq + total_of(plain(gh_new[n], s_heads[:, n, :])[1] ** 2)
    small_sq = small_sq + total_of(plain(gx, s_hidden[...])[1] ** 2)
    small_sq = small_sq + first_f * total_of(plain(gt, s_table[...])[1] ** 2)

    for n in range(1, 4):
        t_copy(n).wait_recv()
        f_copy(n).wait_recv()
    t_sum = t_s[0] + t_s[1] + t_s[2] + t_s[3]
    f_sum = f_s[0] + f_s[1] + f_s[2] + f_s[3]
    for n in range(1, 16):
        z_copy(n).wait_recv()
    z_sum = z_s[0]
    for n in range(1, 16):
        z_sum = z_sum + z_s[n]
    lane8 = ints((8, 128), 1)

    def scalar(n):
        return jnp.sum(jnp.where(lane8 == n, z_sum, 0.0)[0:1], axis=1, keepdims=True)

    def fresh(old, summed, count):
        return DECAY_RATE * old + keep * (summed / count + STAT_EPS)

    rq = fresh(row_qkv[...], t_sum[0:3, :], D)
    kq = fresh(col_qkv[...], f_sum[0:3, :width], D)
    rp = fresh(wide(row_proj), f_sum[3:4, :width], D)
    kp = fresh(wide(col_proj), t_sum[3:4, :], D)
    ru = fresh(wide(row_up), t_sum[4:5, :], ff)
    ku = fresh(wide(col_up), f_sum[4:5, :], D)
    rd = fresh(wide(row_down), f_sum[5:6, :], D)
    kd = fresh(wide(col_down), t_sum[5:6, :], ff)

    def mean_row(n, rows_all, cols_all):
        return (
            DECAY_RATE * scalar(6 + n) + keep * (scalar(n) / cols_all + rows_all * STAT_EPS)
        ) / rows_all

    means = [
        mean_row(0, D, D), mean_row(1, D, D), mean_row(2, D, D), mean_row(3, D, D),
        mean_row(4, D, ff), mean_row(5, ff, D),
    ]
    scales = update_scales(rq, kq, rp, kp, ru, ku, rd, kd, means)
    big_sq = small_sq
    grads = [gq_o[n] for n in range(3)] + [gp_o[...], gu_o[...], gd_o[...]]
    for grad, scale in zip(grads, scales):
        u = grad * scale
        big_sq = big_sq + total_of(u * u)
    c_s[me] = jnp.broadcast_to(big_sq, (8, 128))
    for n in range(1, 16):
        c_copy(n).start()
    rq_o[...] = rq
    kq_o[...] = kq
    for ref, row in ((rp_o, rp), (kp_o, kp), (ru_o, ru), (ku_o, ku), (rd_o, rd), (kd_o, kd)):
        put_wide(ref, row)
    mixl.hand(3)
    lift(2)
    lift(3)
    leave(1)
    store[0].start()
    for i in range(images):
        home_in.wait(i)
    store[1].start()

    counts = [3 * D * D, D * D, D * ff, ff * D] + [D] * 8 + [ff, RELP * HEADS]
    sizes = [jnp.sqrt(scalar(12 + n) / counts[n] + STAT_EPS) for n in range(14)]
    for n in range(1, 16):
        c_copy(n).wait_recv()
    all_sq = c_s[0]
    for n in range(1, 16):
        all_sq = all_sq + c_s[n]
    count_all = 4 * D * D + 2 * D * ff + 8 * D + ff + RELP * HEADS
    clip = jnp.sqrt(all_sq[0:1, 0:1] / count_all)
    factor = STEP_RATE / jnp.maximum(1.0, clip / CLIP_LEVEL)
    size_o[...] = lane_pack([size * factor for size in sizes] + [clip] + means)
    for n in range(3):
        swap(n).wait_send()
    for n in range(1, 4):
        t_copy(n).wait_send()
        f_copy(n).wait_send()
        proj_line(n).wait_send()
    for p in range(windows // 2):
        ctx_copy(p, 0, t, two.mid).wait_send()

        @pl.when(two.is_mid)
        def _():
            for kind in range(1, 5):
                ctx_copy(p, kind, t, two.mid).wait_send()

    for n in range(1, 16):
        z_copy(n).wait_send()
        c_copy(n).wait_send()
    for w in range(windows):
        mixl.drain(w)
        four.drain(w)
    for copy in halo_f:
        copy.wait_send()
    for copy in (*down_copies, *up_copies):
        copy.wait_send()
    for n in range(2):
        copy_of(n, 0, f, far).wait_send()
        copy_of(n, 1, f, near).wait_send()
        copy_of(n, 2, far, near).wait_send()
    for n in range(4):
        proj_copy(n, 0, f, far).wait_send()
        proj_copy(n, 1, f, near).wait_send()
        proj_copy(n, 2, far, near).wait_send()
    for member in (up, down, *qkv, proj, table):
        member.drain()
    for copy in store:
        copy.wait()
def finish_body(ready, *refs):
    (
        big_in, (gn, gh, gx, gt), (w_norm, w_heads, w_hidden, w_table),
        (s_norm, s_heads, s_hidden, s_table), stats, (size,),
        big_out, (gn_o, gh_o, gx_o, gt_o), (nn_o, nh_o, nx_o, nt_o), stats_o,
        (sn_o, sh_o, sx_o, st_o), (clip_o,), held, made, (i_sem, o_sem),
    ) = take(refs, (12, 4, 4, 4, 8, 1, 14, 4, 4, 8, 4, 1, 12, 10, 2))
    home_out, feat, home_in, og = held[:4]
    grads, masters = held[4:8], held[8:12]
    fetch = [
        pltpu.make_async_copy(src, dst, i_sem.at[n]) for n, (src, dst) in enumerate(zip(big_in, held))
    ]
    for n in (4, 8, 5, 9, 6, 10, 7, 11, 0, 1, 2, 3):
        fetch[n].start()
    sources = [*made[:2], *grads, *made[2:]]
    store = [
        pltpu.make_async_copy(src, dst, o_sem.at[n]) for n, (src, dst) in enumerate(zip(sources, big_out))
    ]
    ready()
    lane8 = lax.broadcasted_iota(jnp.int32, (8, 128), 1)
    table = size[...]

    def step(n):
        return jnp.sum(jnp.where(lane8 == n, table, 0.0)[0:1], axis=1, keepdims=True)

    rq, kq, *vecs = stats
    scales = update_scales(rq[...], kq[...], *map(wide, vecs), [step(15 + n) for n in range(6)])
    for n in range(4):
        fetch[4 + n].wait()
        store[2 + n].start()
        fetch[8 + n].wait()
        new_o, low_o = made[2 + n], made[6 + n]
        if n == 0:
            for m in range(3):
                new = masters[0][m] - step(0) * (grads[0][m] * scales[m])
                new_o[m] = new
                low_o[m] = new.astype(BF)
        else:
            new = masters[n][...] - step(n) * (grads[n][...] * scales[2 + n])
            new_o[...] = new
            low_o[...] = new.astype(BF)
        store[6 + n].start()
        store[10 + n].start()
    for n in (0, 1):
        fetch[n].wait()
    made[0][...] = feat[...].astype(F32) + home_out[...].astype(F32)
    store[0].start()
    for n in (2, 3):
        fetch[n].wait()
    made[1][...] = og[...] + home_in[...].astype(F32)
    store[1].start()
    for src, dst in ((gn, gn_o), (gh, gh_o), (gx, gx_o), (gt, gt_o), *zip(stats, stats_o)):
        dst[...] = src[...]
    sn, un = plain(gn[...], s_norm[...])
    sn_o[...] = sn
    for n in range(6):
        nn_o[n : n + 1, :] = w_norm[n : n + 1, :] - step(4 + n) * un[n : n + 1, :]
    for n in range(2):
        sh, uh = plain(gh[:, n, :], s_heads[:, n, :])
        sh_o[:, n, :] = sh
        nh_o[:, n, :] = w_heads[:, n, :] - step(10 + n) * uh
    sx, ux = plain(gx[...], s_hidden[...])
    sx_o[...] = sx
    nx_o[...] = w_hidden[...] - step(12) * ux
    st, ut = plain(gt[...], s_table[...])
    st_o[...] = st
    nt_o[...] = w_table[...] - step(13) * ut
    clip_o[...] = step(14)
    for copy in store:
        copy.wait()


def whole_step(feat, og, regions, rel_index, masters, stats, states):
    w_qkv, w_proj, w_up, w_down, w_norm, w_heads, w_hidden, w_table = masters
    images = feat.shape[0]
    windows = 2 * images
    shard, width = w_qkv.shape[1], w_qkv.shape[2]
    hidden = w_up.shape[1]
    heads = width // HD
    stats = [u if u.ndim == 2 else u.reshape(-1, 128) if u.shape[0] == D else u[None] for u in stats]
    like = lambda u: (u.shape, F32)
    mats = (w_qkv, w_proj, w_up, w_down)
    smalls = (w_norm, w_heads, w_hidden, w_table)
    vm, dma = pltpu.VMEM, pltpu.SemaphoreType.DMA
    flat = windows * TOK
    halves = (2 * windows, 2, ROWS, HALF)
    tokens = (windows, TOK, D)
    rows_of = (images, SHIFT, 24, D)
    outs = [
        (feat.shape, BF), (feat.shape, BF), *map(like, mats), *map(like, smalls),
        *map(like, stats), ((8, 128), F32),
    ]
    scratch = [
        vm((4, 16, shard), BF), vm((3, D, width), BF), vm((4, D, shard), BF), vm((D, D), BF),
        vm((D, hidden), BF), vm((D, hidden), BF), vm(rows_of, BF), vm(rows_of, BF), vm(rows_of, BF),
        vm((heads, TOK, 256), F32), vm((24, D), F32), vm((16, D), F32), vm((192, 256), jnp.int32),
        vm((8, 640), F32), vm((24, D), F32),
        vm(tokens, F32), vm(tokens, F32), vm((flat, D), BF), vm((windows, TOK, width), BF),
        vm((windows, TOK, width), BF), vm((windows, TOK, width), BF),
        vm((windows, heads, TOK, TOK), F32), vm((windows // 2, 4, TOK, 2 * width), BF), vm(halves, F32),
        vm((flat, D), BF), vm((flat, hidden), BF), vm((flat, hidden), BF),
        vm(tokens, F32), vm((windows, TOK, 128), F32), vm(halves, BF), vm((D, hidden), F32),
        vm((D, hidden), F32), vm(tokens, F32), vm((flat, D), BF), vm(halves, F32),
        vm((3, flat, width), BF), vm((heads, 192, 256), F32), vm((heads, 24, 256), F32),
        vm(halves, BF),
        *LineSum.scratch(2 * windows), *LineSum.scratch(2 * windows),
        *ShardSum.scratch((shard, hidden)), *BandFirstSum.scratch((shard, hidden)),
        *[s for _ in range(3) for s in ShardSum.scratch((shard, width))], *ShardSum.scratch((width, shard)),
        *TableSum.scratch(heads),
        vm((3, 24, D), F32), vm((3, 24, D), F32), vm((4, 8, shard), F32), vm((4, 8, hidden), F32),
        vm((16, 8, 128), F32), vm((16, 8, 128), F32),
        vm(feat.shape, BF), vm(og.shape, F32), *[vm(u.shape, F32) for u in mats],
        vm(halves, BF), vm((windows, ROWS, HALF), BF), dma((windows,)), dma((windows,)), dma((6,)),
        dma((2, 5)), dma((2, 5)),
        vm(feat.shape, BF), vm(feat.shape, BF), *[vm(u.shape, F32) for u in mats], dma((6,)),
        dma((2, 3)), dma((2, 3)), dma((4, 3)), dma((4, 3)), dma((4,)), dma((4,)),
        dma((2 * images,)), dma((2 * images,)), *[dma((images,))] * 2,
        dma((windows // 2, 5)), dma((windows // 2, 4)),
        dma((3,)), dma((3,)), *[dma((4,))] * 4, *[dma((16,))] * 4,
    ]
    got = vmem_call(step_body, outs, scratch, "whole_step", 1, 6, 6)(
        feat, og, *mats, regions, rel_index, *smalls, *stats, *states
    )
    home_out, home_in, g_qkv, g_proj, g_up, g_down, gn, gh, gx, gt, *rest = got
    new_stats, size = rest[:8], rest[8]
    outs = [
        like(og), like(og), *map(like, mats), *map(like, mats), *[(u.shape, BF) for u in mats],
        *map(like, smalls), *map(like, smalls), *map(like, stats), *map(like, smalls), ((1, 1), F32),
    ]
    scratch = [
        vm(feat.shape, BF), vm(feat.shape, BF), vm(feat.shape, BF), vm(og.shape, F32),
        *[vm(u.shape, F32) for u in mats], *[vm(u.shape, F32) for u in mats],
        vm(og.shape, F32), vm(og.shape, F32), *[vm(u.shape, F32) for u in mats],
        *[vm(u.shape, BF) for u in mats], dma((12,)), dma((14,)),
    ]
    return vmem_call(finish_body, outs, scratch, "finish", None, 12, 14)(
        home_out, feat, home_in, og, g_qkv, g_proj, g_up, g_down, *mats, gn, gh, gx, gt,
        *smalls, *states, *new_stats, size,
    )


def per_device_plain(
    features,
    out_grad,
    regions,
    rel_index,
    w_qkv,
    w_proj,
    w_up,
    w_down,
    norm_vecs,
    head_bias,
    hidden_bias,
    rel_table,
    row_qkv,
    col_qkv,
    row_proj,
    col_proj,
    row_up,
    col_up,
    row_down,
    col_down,
    state_norm,
    state_heads,
    state_hidden,
    state_table,
):
    images, band_rows, across, model_width = features.shape
    win_tokens = WIN * WIN
    fsdp_at = lax.axis_index("fsdp")
    ctx_at = lax.axis_index("ctx")
    tp_at = lax.axis_index("tp")
    first_fsdp = (fsdp_at == 0).astype(jnp.float32)
    first_ctx = (ctx_at == 0).astype(jnp.float32)
    first_tp = (tp_at == 0).astype(jnp.float32)
    weights_qkv, weights_proj, weights_up, weights_down, vec_copy, head_copy, hidden_copy = (
        lax.all_gather(w_qkv.astype(jnp.bfloat16), "fsdp", axis=1, tiled=True),
        lax.all_gather(w_proj.astype(jnp.bfloat16), "fsdp", axis=1, tiled=True),
        lax.all_gather(w_up.astype(jnp.bfloat16), "fsdp", axis=0, tiled=True),
        lax.all_gather(w_down.astype(jnp.bfloat16), "fsdp", axis=1, tiled=True),
        lax.all_gather(norm_vecs.astype(jnp.bfloat16), "fsdp", axis=1, tiled=True),
        lax.all_gather(head_bias.astype(jnp.bfloat16), "fsdp", axis=2, tiled=True),
        lax.all_gather(hidden_bias.astype(jnp.bfloat16), "fsdp", axis=1, tiled=True),
    )
    norm_rows = vec_copy.astype(jnp.float32)
    bias_query = head_copy[0].reshape(-1).astype(jnp.float32)
    bias_value = head_copy[1].reshape(-1).astype(jnp.float32)
    bias_hidden = hidden_copy.reshape(-1).astype(jnp.float32)
    table_copy = rel_table.astype(jnp.bfloat16)
    local_width = weights_qkv.shape[2]
    heads_here = local_width // HD

    def roll_in(home):
        received = passed_along(home[:, :SHIFT], "ctx", -1)
        return to_windows(enter_frame(home, received)).reshape(-1, model_width)

    def roll_out(rolled_flat):
        band = jnp.roll(
            from_windows(
                rolled_flat.reshape(-1, win_tokens, model_width), images, band_rows, across
            ),
            SHIFT,
            axis=2,
        )
        lower = passed_along(band[:, band_rows - SHIFT :], "ctx", 1)
        return jnp.concatenate([lower, band[:, : band_rows - SHIFT]], axis=1)

    flat_one = roll_in(features).astype(jnp.float32)
    grad_flat = roll_in(out_grad)
    win_count = flat_one.shape[0] // win_tokens
    normed_one, pull_one = jax.vjp(layer_norm, flat_one, norm_rows[0], norm_rows[1])
    normed_one_low = normed_one.astype(jnp.bfloat16)
    head_shape = (win_count, win_tokens, heads_here, HD)
    query_low, key_low, value_low = project_heads(
        normed_one_low, weights_qkv, bias_query, bias_value, head_shape
    )
    pos_bias = table_lookup(table_copy, rel_index)
    region_win = to_windows(regions[..., None])[..., 0]
    mask_add = jnp.where(region_win[:, :, None] == region_win[:, None, :], 0.0, MASK_FILL).astype(
        jnp.float32
    )
    scores = attention_scores(query_low, key_low, pos_bias, mask_add)
    top_score = jnp.max(scores, axis=-1, keepdims=True)
    lifted = jnp.exp(scores - top_score)
    prob_rows = lifted / jnp.sum(lifted, axis=-1, keepdims=True)
    prob_low = prob_rows.astype(jnp.bfloat16)
    context = jnp.einsum("whij,wjhc->wihc", prob_low, value_low, preferred_element_type=jnp.float32)
    context_low = context.astype(jnp.bfloat16).reshape(-1, local_width)
    branch_part = jnp.dot(context_low, weights_proj, preferred_element_type=jnp.float32)
    branch = lax.psum(branch_part.astype(jnp.bfloat16), "tp").astype(jnp.float32) + norm_rows[2]
    flat_two = flat_one + branch
    normed_two, pull_two = jax.vjp(layer_norm, flat_two, norm_rows[3], norm_rows[4])
    normed_two_low = normed_two.astype(jnp.bfloat16)
    pre_act = jnp.dot(normed_two_low, weights_up, preferred_element_type=jnp.float32) + bias_hidden
    hidden, pull_gelu = jax.vjp(exact_gelu, pre_act)
    hidden_low = hidden.astype(jnp.bfloat16)
    mixed_part = jnp.dot(hidden_low, weights_down, preferred_element_type=jnp.float32)
    mixed_whole = lax.psum(mixed_part.astype(jnp.bfloat16), "tp").astype(jnp.float32)
    block_out = features.astype(jnp.float32) + roll_out(
        (branch + mixed_whole + norm_rows[5]).astype(jnp.bfloat16)
    ).astype(jnp.float32)
    grad_low = grad_flat.astype(jnp.bfloat16)
    grad_down_full = jnp.einsum(
        "tf,td->fd", hidden_low, grad_low, preferred_element_type=jnp.float32
    )
    grad_down_bias = jnp.sum(grad_flat, axis=0)
    d_hidden = jnp.einsum("td,fd->tf", grad_low, weights_down, preferred_element_type=jnp.float32)
    d_pre = pull_gelu(d_hidden)[0]
    d_pre_low = d_pre.astype(jnp.bfloat16)
    grad_hidden_bias = jnp.sum(d_pre, axis=0)
    grad_up_full = jnp.einsum(
        "td,tf->df", normed_two_low, d_pre_low, preferred_element_type=jnp.float32
    )
    d_two_part = jnp.einsum("tf,df->td", d_pre_low, weights_up, preferred_element_type=jnp.float32)
    d_two = lax.psum(d_two_part.astype(jnp.bfloat16), "tp").astype(jnp.float32)
    d_flat_two, grad_gain_two, grad_offset_two = pull_two(d_two)
    d_resid = grad_flat + d_flat_two
    grad_proj_bias = jnp.sum(d_resid, axis=0)
    d_branch = d_resid.astype(jnp.bfloat16)
    grad_proj_full = jnp.einsum(
        "tc,td->cd", context_low, d_branch, preferred_element_type=jnp.float32
    )
    d_context = (
        jnp.einsum("td,cd->tc", d_branch, weights_proj, preferred_element_type=jnp.float32)
        .astype(jnp.bfloat16)
        .reshape(head_shape)
    )
    d_probs = jnp.einsum(
        "wihc,wjhc->whij", d_context, value_low, preferred_element_type=jnp.float32
    )
    d_value_low = jnp.einsum(
        "whij,wihc->wjhc", prob_low, d_context, preferred_element_type=jnp.float32
    ).astype(jnp.bfloat16)
    d_scores = prob_rows * (d_probs - jnp.sum(prob_rows * d_probs, axis=-1, keepdims=True))
    d_pos = jnp.sum(d_scores, axis=0)
    d_scaled = (d_scores * HD ** (-0.5)).astype(jnp.bfloat16)
    d_query_low = jnp.einsum(
        "whij,wjhc->wihc", d_scaled, key_low, preferred_element_type=jnp.float32
    ).astype(jnp.bfloat16)
    d_key_low = jnp.einsum(
        "whij,wihc->wjhc", d_scaled, query_low, preferred_element_type=jnp.float32
    ).astype(jnp.bfloat16)
    d_heads = jnp.stack([d_query_low, d_key_low, d_value_low]).reshape(3, -1, local_width)
    grad_qkv_full = jnp.einsum(
        "td,ktc->kdc", normed_one_low, d_heads, preferred_element_type=jnp.float32
    )
    grad_head_bias = jnp.stack(
        [
            jnp.sum(d_heads[0].astype(jnp.float32), axis=0),
            jnp.sum(d_heads[2].astype(jnp.float32), axis=0),
        ]
    ).reshape(2, heads_here, HD)
    d_one_part = jnp.einsum("ktc,kdc->td", d_heads, weights_qkv, preferred_element_type=jnp.float32)
    d_one = lax.psum(d_one_part.astype(jnp.bfloat16), "tp").astype(jnp.float32)
    d_flat_one, grad_gain_one, grad_offset_one = pull_one(d_one)
    grad_input = out_grad + roll_out((d_flat_two + d_flat_one).astype(jnp.bfloat16)).astype(
        jnp.float32
    )
    table_part = table_grad(d_pos, rel_index, rel_table.shape[0])
    grad_norm_full = jnp.stack(
        [
            grad_gain_one,
            grad_offset_one,
            grad_proj_bias,
            grad_gain_two,
            grad_offset_two,
            grad_down_bias,
        ]
    )
    grad_list = (
        grad_qkv_full,
        grad_proj_full,
        grad_up_full,
        grad_down_full,
        grad_norm_full,
        grad_head_bias,
        grad_hidden_bias.reshape(-1, HD),
    )
    g_qkv, g_proj, g_up, g_down, g_norm, g_heads, g_hidden = shard_sum(band_sum(grad_list))
    d_shard = w_qkv.shape[1]
    hidden_here = w_up.shape[1]
    keep = 1.0 - DECAY_RATE
    sq_qkv = g_qkv * g_qkv
    sq_proj = g_proj * g_proj
    sq_up = g_up * g_up
    sq_down = g_down * g_down
    stat_rq = place(
        (keep * jnp.sum(sq_qkv, axis=2) / D + first_tp * (DECAY_RATE * row_qkv + keep * STAT_EPS))
        * first_ctx,
        fsdp_at,
        D,
    )
    stat_cq = place(
        (keep * jnp.sum(sq_qkv, axis=1) / D + first_fsdp * (DECAY_RATE * col_qkv + keep * STAT_EPS))
        * first_ctx,
        tp_at,
        D,
    )
    stat_rp = place(
        (
            keep * jnp.sum(sq_proj, axis=1) / D
            + first_fsdp * (DECAY_RATE * row_proj + keep * STAT_EPS)
        )
        * first_ctx,
        tp_at,
        D,
    )
    stat_cp = place(
        (keep * jnp.sum(sq_proj, axis=0) / D + first_tp * (DECAY_RATE * col_proj + keep * STAT_EPS))
        * first_ctx,
        fsdp_at,
        D,
    )
    stat_ru = place(
        (keep * jnp.sum(sq_up, axis=1) / FF + first_tp * (DECAY_RATE * row_up + keep * STAT_EPS))
        * first_ctx,
        fsdp_at,
        D,
    )
    stat_cu = place(
        (keep * jnp.sum(sq_up, axis=0) / D + first_fsdp * (DECAY_RATE * col_up + keep * STAT_EPS))
        * first_ctx,
        tp_at,
        FF,
    )
    stat_rd = place(
        (
            keep * jnp.sum(sq_down, axis=1) / D
            + first_fsdp * (DECAY_RATE * row_down + keep * STAT_EPS)
        )
        * first_ctx,
        tp_at,
        FF,
    )
    stat_cd = place(
        (
            keep * jnp.sum(sq_down, axis=0) / FF
            + first_tp * (DECAY_RATE * col_down + keep * STAT_EPS)
        )
        * first_ctx,
        fsdp_at,
        D,
    )
    table_whole = place(table_part, tp_at, HEADS)
    master_sq = jnp.concatenate(
        [
            jnp.stack(
                [
                    jnp.sum(w_qkv * w_qkv),
                    jnp.sum(w_proj * w_proj),
                    jnp.sum(w_up * w_up),
                    jnp.sum(w_down * w_down),
                ]
            )
            * first_ctx,
            jnp.sum(norm_vecs * norm_vecs, axis=1) * first_ctx * first_tp,
            jnp.sum(head_bias * head_bias, axis=(1, 2)) * first_ctx,
            jnp.sum(hidden_bias * hidden_bias)[None] * first_ctx,
            jnp.sum(rel_table * rel_table)[None] * first_ctx * first_fsdp,
        ]
    )
    (
        full_rq,
        full_cq,
        full_rp,
        full_cp,
        full_ru,
        full_cu,
        full_rd,
        full_cd,
        table_sum,
        master_total,
    ) = lax.psum(
        (
            stat_rq,
            stat_cq,
            stat_rp,
            stat_cp,
            stat_ru,
            stat_cu,
            stat_rd,
            stat_cd,
            table_whole,
            master_sq,
        ),
        ("fsdp", "ctx", "tp"),
    )
    u_qkv = factored(
        g_qkv,
        own_part(full_rq, fsdp_at, d_shard),
        own_part(full_cq, tp_at, local_width),
        jnp.mean(full_rq, axis=1)[:, None, None],
    )
    u_proj = factored(
        g_proj,
        own_part(full_rp, tp_at, local_width),
        own_part(full_cp, fsdp_at, d_shard),
        jnp.mean(full_rp),
    )
    u_up = factored(
        g_up,
        own_part(full_ru, fsdp_at, d_shard),
        own_part(full_cu, tp_at, hidden_here),
        jnp.mean(full_ru),
    )
    u_down = factored(
        g_down,
        own_part(full_rd, tp_at, hidden_here),
        own_part(full_cd, fsdp_at, d_shard),
        jnp.mean(full_rd),
    )
    g_table = own_part(table_sum, tp_at, heads_here)
    state_norm_new, u_norm = plain_stats(g_norm, state_norm)
    state_heads_new, u_heads = plain_stats(g_heads, state_heads)
    state_hidden_new, u_hidden = plain_stats(g_hidden, state_hidden)
    state_table_new, u_table = plain_stats(g_table, state_table)
    local_sq = (
        jnp.sum(u_qkv * u_qkv)
        + jnp.sum(u_proj * u_proj)
        + jnp.sum(u_up * u_up)
        + jnp.sum(u_down * u_down)
        + jnp.sum(u_heads * u_heads)
        + jnp.sum(u_hidden * u_hidden)
        + first_tp * jnp.sum(u_norm * u_norm)
        + first_fsdp * jnp.sum(u_table * u_table)
    )
    total_sq = lax.psum(local_sq, ("fsdp", "tp"))
    count_all = 4 * D * D + 2 * D * FF + 8 * D + FF + RELP * HEADS
    clip_rms = jnp.sqrt(total_sq / count_all)
    factor = 1.0 / jnp.maximum(1.0, clip_rms / CLIP_LEVEL)
    counts = jnp.array(
        [3 * D * D, D * D, D * FF, FF * D, D, D, D, D, D, D, D, D, FF, RELP * HEADS], jnp.float32
    )
    scales = jnp.sqrt(master_total / counts + STAT_EPS)
    new_qkv = w_qkv - STEP_RATE * scales[0] * factor * u_qkv
    new_proj = w_proj - STEP_RATE * scales[1] * factor * u_proj
    new_up = w_up - STEP_RATE * scales[2] * factor * u_up
    new_down = w_down - STEP_RATE * scales[3] * factor * u_down
    new_norm = norm_vecs - STEP_RATE * scales[4:10][:, None] * factor * u_norm
    new_heads = head_bias - STEP_RATE * scales[10:12][:, None, None] * factor * u_heads
    new_hidden = hidden_bias - STEP_RATE * scales[12] * factor * u_hidden
    new_table = rel_table - STEP_RATE * scales[13] * factor * u_table
    return (
        block_out,
        grad_input,
        g_qkv,
        g_proj,
        g_up,
        g_down,
        g_norm,
        g_heads,
        g_hidden,
        g_table,
        new_qkv,
        new_proj,
        new_up,
        new_down,
        new_norm,
        new_heads,
        new_hidden,
        new_table,
        new_qkv.astype(jnp.bfloat16),
        new_proj.astype(jnp.bfloat16),
        new_up.astype(jnp.bfloat16),
        new_down.astype(jnp.bfloat16),
        own_part(full_rq, fsdp_at, d_shard),
        own_part(full_cq, tp_at, local_width),
        own_part(full_rp, tp_at, local_width),
        own_part(full_cp, fsdp_at, d_shard),
        own_part(full_ru, fsdp_at, d_shard),
        own_part(full_cu, tp_at, hidden_here),
        own_part(full_rd, tp_at, hidden_here),
        own_part(full_cd, fsdp_at, d_shard),
        state_norm_new,
        state_heads_new,
        state_hidden_new,
        state_table_new,
        clip_rms,
    )


def per_device(
    features,
    out_grad,
    regions,
    rel_index,
    w_qkv,
    w_proj,
    w_up,
    w_down,
    norm_vecs,
    head_bias,
    hidden_bias,
    rel_table,
    row_qkv,
    col_qkv,
    row_proj,
    col_proj,
    row_up,
    col_up,
    row_down,
    col_down,
    state_norm,
    state_heads,
    state_hidden,
    state_table,
):
    flip = lambda u: u.transpose(1, 0, 2)
    (block_out, grad_input, g_qkv, g_proj, g_up, g_down, new_qkv, new_proj, new_up, new_down,
     copy_qkv, copy_proj, copy_up, copy_down, g_norm, g_heads, g_hidden, g_table,
     new_norm, new_heads, new_hidden, new_table, *rest) = whole_step(
        features, out_grad, flip(regions), rel_index,
        (w_qkv, w_proj, w_up, w_down.T, norm_vecs, flip(head_bias), hidden_bias.T, rel_table.T),
        (row_qkv, col_qkv, row_proj, col_proj, row_up, col_up, row_down, col_down),
        (state_norm, flip(state_heads), state_hidden.T, state_table.T))
    factors, states, clip_rms = rest[:8], rest[8:12], rest[12]
    factors = list(factors[:2]) + [u.reshape(-1) for u in factors[2:]]
    return (
        block_out, grad_input, g_qkv, g_proj, g_up, g_down.T, g_norm, flip(g_heads), g_hidden.T,
        g_table.T, new_qkv, new_proj, new_up, new_down.T, new_norm, flip(new_heads), new_hidden.T,
        new_table.T, copy_qkv, copy_proj, copy_up, copy_down.T, *factors,
        states[0], flip(states[1]), states[2].T, states[3].T, clip_rms[0, 0],
    )


def solution(mesh):
    line_of_four = mesh.shape["fsdp"] == 4 and mesh.shape["tp"] == 4 and mesh.shape["ctx"] == 2
    return jax.shard_map(
        per_device if line_of_four else per_device_plain,
        mesh=mesh,
        in_specs=(
            P("fsdp", "ctx", None, None),
            P("fsdp", "ctx", None, None),
            P("fsdp", "ctx", None),
            P(),
            P(None, "fsdp", "tp"),
            P("tp", "fsdp"),
            P("fsdp", "tp"),
            P("tp", "fsdp"),
            P(None, "fsdp"),
            P(None, "tp", "fsdp"),
            P("tp", "fsdp"),
            P(None, "tp"),
            P(None, "fsdp"),
            P(None, "tp"),
            P("tp"),
            P("fsdp"),
            P("fsdp"),
            P("tp"),
            P("tp"),
            P("fsdp"),
            P(None, "fsdp"),
            P(None, "tp", "fsdp"),
            P("tp", "fsdp"),
            P(None, "tp"),
        ),
        out_specs=(
            P("fsdp", "ctx", None, None),
            P("fsdp", "ctx", None, None),
            P(None, "fsdp", "tp"),
            P("tp", "fsdp"),
            P("fsdp", "tp"),
            P("tp", "fsdp"),
            P(None, "fsdp"),
            P(None, "tp", "fsdp"),
            P("tp", "fsdp"),
            P(None, "tp"),
            P(None, "fsdp", "tp"),
            P("tp", "fsdp"),
            P("fsdp", "tp"),
            P("tp", "fsdp"),
            P(None, "fsdp"),
            P(None, "tp", "fsdp"),
            P("tp", "fsdp"),
            P(None, "tp"),
            P(None, "fsdp", "tp"),
            P("tp", "fsdp"),
            P("fsdp", "tp"),
            P("tp", "fsdp"),
            P(None, "fsdp"),
            P(None, "tp"),
            P("tp"),
            P("fsdp"),
            P("fsdp"),
            P("tp"),
            P("tp"),
            P("fsdp"),
            P(None, "fsdp"),
            P(None, "tp", "fsdp"),
            P("tp", "fsdp"),
            P(None, "tp"),
            P(),
        ),
        check_vma=False,
    )
```

```python
import functools

import jax
import jax.numpy as jnp
from jax import lax
from jax.experimental import pallas as pl
from jax.experimental.pallas import tpu as pltpu
from jax.sharding import PartitionSpec as P


D = 768
HEADS = 24
HD = 32
FF = 3072
WIN = 12
SHIFT = 6
RELP = 529


DECAY_RATE = 0.5
STAT_EPS = 1e-06
NORM_EPS = 1e-05
MASK_FILL = -100.0
STEP_RATE = 1.0
CLIP_LEVEL = 0.25


def passed_along(x, axis, by):
    count = lax.axis_size(axis)
    return lax.ppermute(x, axis, [(i, (i + by) % count) for i in range(count)])


def layer_norm(values, gain_row, offset):
    mean_val = jnp.mean(values, axis=-1, keepdims=True)
    centred = values - mean_val
    var_val = jnp.mean(centred * centred, axis=-1, keepdims=True)
    return centred * lax.rsqrt(var_val + NORM_EPS) * gain_row + offset


def exact_gelu(values):
    return jax.nn.gelu(values, approximate=False)


def to_windows(values):
    image_count, row_count, col_count, channels = values.shape
    pieces = values.reshape(image_count, row_count // WIN, WIN, col_count // WIN, WIN, channels)
    return pieces.transpose(0, 1, 3, 2, 4, 5).reshape(-1, WIN * WIN, channels)


def from_windows(values, image_count, row_count, col_count):
    channels = values.shape[-1]
    pieces = values.reshape(image_count, row_count // WIN, col_count // WIN, WIN, WIN, channels)
    return pieces.transpose(0, 1, 3, 2, 4, 5).reshape(image_count, row_count, col_count, channels)


def enter_frame(own_rows, received):
    joined = jnp.concatenate([own_rows[:, SHIFT:], received], axis=1)
    return jnp.roll(joined, -SHIFT, axis=2)


def project_heads(normed_low, weights_qkv, bias_query, bias_value, head_shape):
    query_full = (
        jnp.dot(normed_low, weights_qkv[0], preferred_element_type=jnp.float32) + bias_query
    )
    key_full = jnp.dot(normed_low, weights_qkv[1], preferred_element_type=jnp.float32)
    value_full = (
        jnp.dot(normed_low, weights_qkv[2], preferred_element_type=jnp.float32) + bias_value
    )
    return tuple(
        (
            member.astype(jnp.bfloat16).reshape(head_shape)
            for member in (query_full, key_full, value_full)
        )
    )


def attention_scores(query_low, key_low, pos_bias, mask_add):
    products = jnp.einsum("wihc,wjhc->whij", query_low, key_low, preferred_element_type=jnp.float32)
    return products * query_low.shape[-1] ** (-0.5) + pos_bias[None] + mask_add[:, None]


def table_lookup(table_low, rel_index):
    win_tokens = rel_index.shape[0]
    code_ids = jnp.arange(table_low.shape[0], dtype=jnp.int32)
    index_blocks = rel_index.reshape(WIN, -1)

    def lookup(index_block):
        one_hot = (index_block[:, None] == code_ids[None, :]).astype(jnp.bfloat16)
        return jnp.dot(one_hot, table_low, preferred_element_type=jnp.float32)

    looked = lax.map(lookup, index_blocks)
    return looked.reshape(win_tokens, win_tokens, -1).transpose(2, 0, 1)


def table_grad(d_pos, rel_index, table_rows):
    heads_here = d_pos.shape[0]
    code_ids = jnp.arange(table_rows, dtype=jnp.int32)
    index_blocks = rel_index.reshape(WIN, -1)
    grad_blocks = d_pos.transpose(1, 2, 0).reshape(WIN, -1, heads_here)

    def accumulate(running, member):
        index_block, grad_block = member
        one_hot = (index_block[:, None] == code_ids[None, :]).astype(jnp.float32)
        added = lax.dot_general(
            one_hot,
            grad_block,
            (((0,), (0,)), ((), ())),
            precision=lax.Precision.HIGHEST,
            preferred_element_type=jnp.float32,
        )
        return (running + added, None)

    result_pair = lax.scan(
        accumulate, jnp.zeros((table_rows, heads_here), jnp.float32), (index_blocks, grad_blocks)
    )
    return result_pair[0]


def place(part_vec, index_at, whole_len):
    size_of = part_vec.shape[-1]
    base = jnp.zeros(part_vec.shape[:-1] + (whole_len,), jnp.float32)
    return lax.dynamic_update_slice_in_dim(base, part_vec, index_at * size_of, part_vec.ndim - 1)


def own_part(whole_vec, index_at, size_of):
    return lax.dynamic_slice_in_dim(whole_vec, index_at * size_of, size_of, whole_vec.ndim - 1)


def factored(grad, row_local, col_local, row_mean):
    return grad * lax.rsqrt(row_local[..., :, None] * col_local[..., None, :] / row_mean)


def plain_stats(grad, state_old):
    state_new = DECAY_RATE * state_old + (1.0 - DECAY_RATE) * (grad * grad + STAT_EPS)
    return (state_new, grad * lax.rsqrt(state_new))


def shard_sum(grad_list):
    return (
        lax.psum_scatter(grad_list[0], "fsdp", scatter_dimension=1, tiled=True),
        lax.psum_scatter(grad_list[1], "fsdp", scatter_dimension=1, tiled=True),
        lax.psum_scatter(grad_list[2], "fsdp", scatter_dimension=0, tiled=True),
        lax.psum_scatter(grad_list[3], "fsdp", scatter_dimension=1, tiled=True),
        lax.psum_scatter(grad_list[4], "fsdp", scatter_dimension=1, tiled=True),
        lax.psum_scatter(grad_list[5], "fsdp", scatter_dimension=2, tiled=True),
        lax.psum_scatter(grad_list[6], "fsdp", scatter_dimension=1, tiled=True),
    )


def band_sum(grad_list):
    return lax.psum(
        (
            grad_list[0],
            grad_list[1],
            grad_list[2],
            grad_list[3],
            grad_list[4],
            grad_list[5],
            grad_list[6],
        ),
        "ctx",
    )


BF = jnp.bfloat16
F32 = jnp.float32
MESH = pl.DeviceIdType.MESH
TOK = WIN * WIN
HALF = D // 2
ROWS = TOK // 2
VMEM_LIMIT = 67_043_328


def dot(a, b):
    return lax.dot_general(a, b, (((1,), (0,)), ((), ())), preferred_element_type=F32)


def dot_t(a, b):
    return lax.dot_general(a, b, (((1,), (1,)), ((), ())), preferred_element_type=F32)


def t_dot(a, b):
    return lax.dot_general(a, b, (((0,), (0,)), ((), ())), preferred_element_type=F32)


def row_mean(x):
    return jnp.sum(x, axis=-1, keepdims=True) * (1.0 / x.shape[-1])


def remote(src, dst, send, recv, where):
    return pltpu.make_async_remote_copy(
        src_ref=src, dst_ref=dst, send_sem=send, recv_sem=recv, device_id=where, device_id_type=MESH
    )


def greet(barrier, places):
    for place_of in places:
        pl.semaphore_signal(barrier, inc=1, device_id=place_of, device_id_type=MESH)


class LineSum:
    def __init__(self, part, send, from_outer, from_mid, total, sems):
        self.part, self.send, self.from_outer, self.from_mid, self.total = (
            part, send, from_outer, from_mid, total,
        )
        self.s_out, self.r_out, self.s_mid, self.r_mid, self.s_tot, self.r_tot, self.s_cross = sems
        z = lax.axis_index("tp")
        self.is_mid = jnp.logical_and(z > 0, z < 3)
        self.is_outer = jnp.logical_not(self.is_mid)
        self.outer = jnp.where(z < 2, 0, 3)
        self.mid = jnp.where(z < 2, 1, 2)
        self.other_mid = 3 - self.mid
        self.own = self.mid - 1
        self.other = 1 - self.own

    @staticmethod
    def scratch(count):
        return [
            pltpu.VMEM((count, 2, ROWS, HALF), BF),
            pltpu.VMEM((count, 2, ROWS, HALF), BF),
            pltpu.VMEM((count, ROWS, HALF), BF),
            pltpu.SemaphoreType.DMA((count, 2)),
            pltpu.SemaphoreType.DMA((count, 2)),
            pltpu.SemaphoreType.DMA((count,)),
            pltpu.SemaphoreType.DMA((count,)),
            pltpu.SemaphoreType.DMA((count, 2)),
            pltpu.SemaphoreType.DMA((count, 2)),
            pltpu.SemaphoreType.DMA((count,)),
        ]

    @staticmethod
    def build(part, refs, total):
        return LineSum(part, refs[0], refs[1], refs[2], total, refs[3:10])

    @staticmethod
    def peers():
        return 2

    def greet(self, barrier):
        pl.semaphore_signal(
            barrier, inc=1, device_id={"tp": jnp.where(self.is_mid, self.outer, self.mid)},
            device_id_type=MESH,
        )

        @pl.when(self.is_mid)
        def _():
            pl.semaphore_signal(
                barrier, inc=1, device_id={"tp": self.other_mid}, device_id_type=MESH
            )

    def greet_count(self):
        return jnp.where(self.is_mid, 2, 1)

    def _to_mid(self, w, h):
        return remote(self.send.at[w, h], self.from_outer.at[w, h], self.s_out.at[w, h],
                      self.r_out.at[w, h], {"tp": self.mid})

    def _across(self, w):
        return remote(self.send.at[w, self.other], self.from_mid.at[w], self.s_mid.at[w],
                      self.r_mid.at[w], {"tp": self.other_mid})

    def _total_across(self, w, h):
        return remote(self.total.at[w, h], self.total.at[w, h], self.s_cross.at[w],
                      self.r_tot.at[w, h], {"tp": self.other_mid})

    def _total_out(self, w, h):
        return remote(self.total.at[w, h], self.total.at[w, h], self.s_tot.at[w, h],
                      self.r_tot.at[w, h], {"tp": self.outer})

    def order(self, w):
        return (2 * w, 2 * w + 1)

    def put(self, w, value):
        for s in range(2):
            for h in range(2):
                self.part[2 * w + s, h] = value[s * ROWS : (s + 1) * ROWS, h * HALF : (h + 1) * HALF]

    def get(self, w):
        return jnp.concatenate(
            [
                jnp.concatenate([self.total[2 * w + s, h].astype(F32) for h in range(2)], axis=1)
                for s in range(2)
            ],
            axis=0,
        )

    def start(self, w):
        @pl.when(self.is_outer)
        def _():
            for h in (self.other, self.own):
                for j in self.order(w):
                    self.send[j, h] = self.part[j, h].astype(BF)
                    self._to_mid(j, h).start()

    def cross(self, w):
        @pl.when(self.is_mid)
        def _():
            for j in self.order(w):
                self._to_mid(j, self.other).wait_recv()
                self.send[j, self.other] = (
                    self.part[j, self.other] + self.from_outer[j, self.other].astype(F32)
                ).astype(BF)
                self._across(j).start()

    def settle(self, w):
        @pl.when(self.is_mid)
        def _():
            for j in (2 * w, 2 * w + 1):
                self._to_mid(j, self.own).wait_recv()
                self._across(j).wait_recv()
                self.total[j, self.own] = (
                    self.part[j, self.own]
                    + self.from_outer[j, self.own].astype(F32)
                    + self.from_mid[j].astype(F32)
                ).astype(BF)
                self._total_across(j, self.own).start()
                self._total_out(j, self.own).start()

    def hand(self, w):
        @pl.when(self.is_mid)
        def _():
            for j in (2 * w, 2 * w + 1):
                self._total_across(j, self.other).wait_recv()
                self._total_out(j, self.other).start()

    def arrive(self, w):
        @pl.when(self.is_outer)
        def _():
            for j in (2 * w, 2 * w + 1):
                self._total_out(j, 0).wait_recv()
                self._total_out(j, 1).wait_recv()

    def drain(self, w):
        @pl.when(self.is_outer)
        def _():
            for j in (2 * w, 2 * w + 1):
                self._to_mid(j, 0).wait_send()
                self._to_mid(j, 1).wait_send()

        @pl.when(self.is_mid)
        def _():
            for j in (2 * w, 2 * w + 1):
                self._across(j).wait_send()
                self._total_across(j, self.own).wait_send()
                self._total_out(j, 0).wait_send()
                self._total_out(j, 1).wait_send()


class TradeSum(LineSum):
    def __init__(self, base, away, sems):
        self.__dict__.update(base.__dict__)
        self.away, (self.s_ctx, self.r_ctx) = away, sems
        self.ctx = 1 - lax.axis_index("ctx")

    def order(self, w):
        return (2 * w + 1, 2 * w)

    def _trade(self, w):
        return remote(self.away.at[w], self.total.at[2 * w + 1, self.own], self.s_ctx.at[w],
                      self.r_ctx.at[w], {"ctx": self.ctx})

    def settle(self, w):
        @pl.when(self.is_mid)
        def _():
            for s, j in ((1, 2 * w + 1), (0, 2 * w)):
                self._to_mid(j, self.own).wait_recv()
                self._across(j).wait_recv()
                whole = (
                    self.part[j, self.own]
                    + self.from_outer[j, self.own].astype(F32)
                    + self.from_mid[j].astype(F32)
                ).astype(BF)
                if s == 1:
                    self.away[w] = whole
                    self._trade(w).start()
                else:
                    self.total[j, self.own] = whole
                    self._total_across(j, self.own).start()
                    self._total_out(j, self.own).start()

    def trade(self, w):
        @pl.when(self.is_mid)
        def _():
            j = 2 * w + 1
            self._trade(w).wait_recv()
            self._total_across(j, self.own).start()
            self._total_out(j, self.own).start()

    def drain(self, w):
        LineSum.drain(self, w)

        @pl.when(self.is_mid)
        def _():
            self._trade(w).wait_send()


class ShardSum:
    def __init__(self, block_of, out, refs):
        self.block_of, self.out = block_of, out
        self.snd1, self.rcv1, self.snd2, self.rcv2, self.snd3, self.rcv3, self.s, self.r = refs
        f = lax.axis_index("fsdp")
        core = lax.rem(f, 2)
        self.f, self.core = f, core
        self.near, self.far = f + 1 - 2 * core, lax.rem(f + 2, 4)
        self.ctx = 1 - lax.axis_index("ctx")

    @staticmethod
    def scratch(shape):
        return [
            pltpu.VMEM((2, *shape), BF), pltpu.VMEM((2, *shape), BF),
            pltpu.VMEM(shape, BF), pltpu.VMEM(shape, BF),
            pltpu.VMEM(shape, BF), pltpu.VMEM(shape, BF),
            pltpu.SemaphoreType.DMA((4,)), pltpu.SemaphoreType.DMA((4,)),
        ]

    def _near(self, x):
        return remote(self.snd1.at[x], self.rcv1.at[x], self.s.at[x], self.r.at[x], {"fsdp": self.near})

    def _far(self):
        return remote(self.snd2, self.rcv2, self.s.at[2], self.r.at[2], {"fsdp": self.far})

    def _ctx(self):
        return remote(self.snd3, self.rcv3, self.s.at[3], self.r.at[3], {"ctx": self.ctx})

    def start(self):
        for x in range(2):
            self.snd1[x] = self.block_of(2 * x + 1 - self.core).astype(BF)
            self._near(x).start()

    def pair(self):
        for x in range(2):
            self._near(x).wait_recv()
        other = lax.div(self.far, 2)
        self.snd2[...] = (self.block_of(self.far) + self.rcv1[other].astype(F32)).astype(BF)
        self._far().start()
        mine = lax.div(self.f, 2)
        self.out[...] = self.block_of(self.f) + self.rcv1[mine].astype(F32)

    def cross(self):
        self._far().wait_recv()
        self.snd3[...] = (self.out[...] + self.rcv2[...].astype(F32)).astype(BF)
        self._ctx().start()

    def finish(self):
        self._ctx().wait_recv()
        self.out[...] = self.snd3[...].astype(F32) + self.rcv3[...].astype(F32)

    def drain(self):
        for x in range(2):
            self._near(x).wait_send()
        self._far().wait_send()
        self._ctx().wait_send()


class BandFirstSum:
    def __init__(self, block_of, out, refs):
        self.block_of, self.out = block_of, out
        self.snd1, self.rcv1, self.sndy, self.rcvy, self.sndx, self.rcvx, self.sndf, self.rcvf = refs[:8]
        self.s, self.r = refs[8:]
        f = lax.axis_index("fsdp")
        self.f, self.core, self.x = f, lax.rem(f, 2), lax.div(f, 2)
        self.near, self.far = f + 1 - 2 * self.core, lax.rem(f + 2, 4)
        self.c = lax.axis_index("ctx")
        self.half = out.shape[0] // 2

    @staticmethod
    def scratch(shape):
        two = (2, *shape)
        half = (shape[0] // 2, shape[1])
        shapes = [two, two, (2, *half), (2, *half), half, half, half, half]
        return [*[pltpu.VMEM(u, BF) for u in shapes], pltpu.SemaphoreType.DMA((5,)),
                pltpu.SemaphoreType.DMA((5,))]

    def _near(self, x):
        return remote(self.snd1.at[x], self.rcv1.at[x], self.s.at[x], self.r.at[x], {"fsdp": self.near})

    def _copy(self, n):
        src, dst = ((self.sndy, self.rcvy), (self.sndx, self.rcvx), (self.sndf, self.rcvf))[n]
        where = {"fsdp": self.far} if n == 1 else {"ctx": 1 - self.c}
        return remote(src, dst, self.s.at[2 + n], self.r.at[2 + n], where)

    def _rows(self, c):
        return pl.ds(pl.multiple_of(c * self.half, self.half), self.half)

    def _sum(self, x, c):
        return self.block_of(2 * x + self.core, c * self.half, self.half) + self.rcv1[
            x, self._rows(c), :
        ].astype(F32)

    def start(self):
        for x in range(2):
            self.snd1[x] = self.block_of(2 * x + 1 - self.core, 0, 2 * self.half).astype(BF)
            self._near(x).start()

    def pair(self):
        for x in range(2):
            self._near(x).wait_recv()
            self.sndy[x] = self._sum(x, 1 - self.c).astype(BF)
        self._copy(0).start()

    def cross(self):
        self._copy(0).wait_recv()
        other = 1 - self.x
        self.sndx[...] = (self._sum(other, self.c) + self.rcvy[other].astype(F32)).astype(BF)
        self._copy(1).start()
        self.out[self._rows(self.c), :] = self._sum(self.x, self.c) + self.rcvy[self.x].astype(F32)

    def share(self):
        self._copy(1).wait_recv()
        self.sndf[...] = (self.out[self._rows(self.c), :] + self.rcvx[...].astype(F32)).astype(BF)
        self._copy(2).start()

    def finish(self):
        self._copy(2).wait_recv()
        self.out[self._rows(self.c), :] = self.sndf[...].astype(F32)
        self.out[self._rows(1 - self.c), :] = self.rcvf[...].astype(F32)

    def drain(self):
        for x in range(2):
            self._near(x).wait_send()
        for n in range(3):
            self._copy(n).wait_send()


def vmem_call(body, outs, scratch, name, collective_id, in_place, out_place):
    remote_kernel = {} if collective_id is None else dict(
        collective_id=collective_id, has_side_effects=True
    )
    anywhere = pl.BlockSpec(memory_space=pl.ANY)

    def call(*args):
        few_in = [pltpu.VMEM(u.shape, u.dtype) for u in args[in_place:]]
        few_out = [pltpu.VMEM(s, t) for s, t in outs[out_place:]]

        def whole(*refs):
            ins, results, own, vm_in, vm_out, sems = take(
                refs, (len(args), len(outs), len(scratch), len(few_in), len(few_out), 2)
            )
            fetch = [
                pltpu.make_async_copy(src, dst, sems[0].at[n])
                for n, (src, dst) in enumerate(zip(ins[in_place:], vm_in))
            ]
            for copy in fetch:
                copy.start()

            def ready():
                for copy in fetch:
                    copy.wait()

            body(ready, *ins[:in_place], *vm_in, *results[:out_place], *vm_out, *own)
            store = [
                pltpu.make_async_copy(src, dst, sems[1].at[n])
                for n, (src, dst) in enumerate(zip(vm_out, results[out_place:]))
            ]
            for copy in store:
                copy.start()
            for copy in store:
                copy.wait()

        return pl.pallas_call(
            whole,
            out_shape=[jax.ShapeDtypeStruct(s, t) for s, t in outs],
            in_specs=[anywhere] * len(args),
            out_specs=[anywhere] * len(outs),
            scratch_shapes=[
                *scratch, *few_in, *few_out,
                pltpu.SemaphoreType.DMA((len(few_in),)), pltpu.SemaphoreType.DMA((len(few_out),)),
            ],
            compiler_params=pltpu.CompilerParams(vmem_limit_bytes=VMEM_LIMIT, **remote_kernel),
            name=name,
        )(*args)

    return call


def take(refs, counts):
    groups, at = [], 0
    for n in counts:
        groups.append(refs[at : at + n])
        at += n
    return groups


def window_rows(row_of, row_tmp, image, dst):
    for r in range(WIN):
        row_tmp[...] = row_of(image, r).astype(F32)
        dst[2 * image, r * WIN : (r + 1) * WIN, :] = row_tmp[SHIFT : SHIFT + WIN, :]
        dst[2 * image + 1, r * WIN : r * WIN + SHIFT, :] = row_tmp[SHIFT + WIN :, :]
        dst[2 * image + 1, r * WIN + SHIFT : (r + 1) * WIN, :] = row_tmp[:SHIFT, :]


def home_row(delta, row_tmp, image, r):
    row_tmp[SHIFT : SHIFT + WIN, :] = delta[2 * image, r * WIN : (r + 1) * WIN, :]
    row_tmp[SHIFT + WIN :, :] = delta[2 * image + 1, r * WIN : r * WIN + SHIFT, :]
    row_tmp[:SHIFT, :] = delta[2 * image + 1, r * WIN + SHIFT : (r + 1) * WIN, :]
    return row_tmp[...].astype(BF)


class HomeRows:
    def __init__(self, delta, row_tmp, out, halo, send, recv):
        self.delta, self.row_tmp, self.out, self.halo, self.s, self.r = (
            delta, row_tmp, out, halo, send, recv,
        )

    def _copy(self, i):
        return remote(self.halo.at[i], self.out.at[i, 0:SHIFT], self.s.at[i], self.r.at[i],
                      {"ctx": 1 - lax.axis_index("ctx")})

    def go(self, i):
        for r in range(SHIFT, WIN):
            self.halo[i, r - SHIFT] = home_row(self.delta, self.row_tmp, i, r)
        self._copy(i).start()
        for r in range(SHIFT):
            self.out[i, SHIFT + r] = home_row(self.delta, self.row_tmp, i, r)

    def wait(self, i):
        self._copy(i).wait_recv()
        self._copy(i).wait_send()


class TableSum:
    def __init__(self, part, refs):
        self.part = part
        self.snd1, self.rcv1, self.snd2, self.rcv2, self.snd3, self.rcv3, self.s, self.r = refs
        f = lax.axis_index("fsdp")
        self.core, self.x, self.c = lax.rem(f, 2), lax.div(f, 2), lax.axis_index("ctx")
        self.near, self.far = f + 1 - 2 * self.core, lax.rem(f + 2, 4)

    @staticmethod
    def scratch(heads):
        shapes = [(heads, 2, 2, 24, 256)] * 2 + [(heads, 2, 24, 256)] * 2 + [(heads, 24, 256)] * 2
        return [*[pltpu.VMEM(s, BF) for s in shapes], pltpu.SemaphoreType.DMA((3,)),
                pltpu.SemaphoreType.DMA((3,))]

    def _copy(self, n):
        src, dst = ((self.snd1, self.rcv1), (self.snd2, self.rcv2), (self.snd3, self.rcv3))[n]
        where = ({"fsdp": self.near}, {"fsdp": self.far}, {"ctx": 1 - self.c})[n]
        return remote(src, dst, self.s.at[n], self.r.at[n], where)

    def rows(self, core, x, c):
        return pl.ds(pl.multiple_of(core * 96 + x * 48 + c * 24, 8), 24)

    def start(self):
        for x in range(2):
            for c in range(2):
                self.snd1[:, x, c] = self.part[:, self.rows(1 - self.core, x, c), :].astype(BF)
        self._copy(0).start()

    def pair(self):
        self._copy(0).wait_recv()
        x = 1 - self.x
        for c in range(2):
            self.snd2[:, c] = (
                self.part[:, self.rows(self.core, x, c), :] + self.rcv1[:, x, c].astype(F32)
            ).astype(BF)
        self._copy(1).start()

    def cross(self):
        self._copy(1).wait_recv()
        c = 1 - self.c
        self.snd3[...] = (
            self.part[:, self.rows(self.core, self.x, c), :] + self.rcv1[:, self.x, c].astype(F32)
            + self.rcv2[:, c].astype(F32)
        ).astype(BF)
        self._copy(2).start()

    def finish(self, out):
        self._copy(2).wait_recv()
        out[...] = (
            self.part[:, self.rows(self.core, self.x, self.c), :]
            + self.rcv1[:, self.x, self.c].astype(F32)
            + self.rcv2[:, self.c].astype(F32) + self.rcv3[...].astype(F32)
        )

    def first_row(self):
        return self.core * 96 + self.x * 48 + self.c * 24

    def drain(self):
        for n in range(3):
            self._copy(n).wait_send()


def total_of(x):
    return jnp.sum(jnp.sum(x, axis=1, keepdims=True), axis=0, keepdims=True)


def exact(a, b, dims):
    return lax.dot_general(
        a, b, (dims, ((), ())), precision=lax.Precision.HIGHEST, preferred_element_type=F32
    )


def lane_sums(squares):
    return exact(jnp.ones((8, squares.shape[1]), F32), squares, ((1,), (1,)))[0:1]


def as_column(row):
    n = row.shape[1]
    step = 64
    eye = lax.broadcasted_iota(jnp.int32, (step, step), 0) == lax.broadcasted_iota(
        jnp.int32, (step, step), 1
    )
    return jnp.concatenate(
        [
            jnp.sum(
                jnp.where(eye, jnp.broadcast_to(row[:, at : at + step], (step, step)), 0.0),
                axis=1, keepdims=True,
            )
            for at in range(0, n, step)
        ],
        axis=0,
    )


def lane_pack(values):
    lane = lax.broadcasted_iota(jnp.int32, (8, 128), 1)
    packed = jnp.zeros((8, 128), F32)
    for n, value in enumerate(values):
        packed = packed + jnp.where(lane == n, jnp.broadcast_to(value, (8, 128)), 0.0)
    return packed


def wide(ref):
    if ref.shape[1] != 128:
        return ref[...]
    return jnp.concatenate([ref[n : n + 1, :] for n in range(ref.shape[0])], axis=1)


def put_wide(ref, row):
    if ref.shape[1] != 128:
        ref[...] = row
    else:
        for n in range(ref.shape[0]):
            ref[n : n + 1, :] = row[:, n * 128 : (n + 1) * 128]


def plain(grad, state):
    new = DECAY_RATE * state + (1.0 - DECAY_RATE) * (grad * grad + STAT_EPS)
    return new, grad * lax.rsqrt(new)


def update_scales(rq, kq, rp, kp, ru, ku, rd, kd, means):
    def outer(first, second):
        return as_column(lax.rsqrt(first)) * lax.rsqrt(second)

    return [
        *[outer(rq[n : n + 1, :] / means[n], kq[n : n + 1, :]) for n in range(3)],
        outer(rp / means[3], kp), outer(ru / means[4], ku), outer(kd, rd / means[5]),
    ]


def step_body(ready, *refs):
    (
        big_inputs,
        (regions, ridx_m, w_norm, w_heads, w_hidden, w_table),
        (row_qkv, col_qkv, row_proj, col_proj, row_up, col_up, row_down, col_down),
        (s_norm, s_heads, s_hidden, s_table),
        big_outputs, (gn_o, gh_o, gx_o, gt_o),
        (rq_o, kq_o, rp_o, kp_o, ru_o, ku_o, rd_o, kd_o, size_o),
        (sm_g, wq, wp_g, wp, wu, wd, fh, gh, og_low, bias_s, row_tmp, rows, ridx, table_t, small),
        (xw, ogw, n1, q, k, v, probs, ctx, part),
        (n2_s, hid_s, dpl_s, xhat_s, rstd_s, tot_two, gu, gd, dft, dbr, mix),
        (dh_s, dpos_s, chunk_s, tot_four),
        ls_two, ls_four, up_refs, down_refs, qkv_refs, proj_refs, table_refs,
        (sm_s, sm_r, t_s, f_s, z_s, c_s),
        (feat, og, w_qkv, w_proj, w_up, w_down), (tot_mix, away, y_send, y_recv, i_sem, d_send, d_recv),
        (home_o, gin_o, gq_o, gp_o, gu_o, gd_o, o_sem),
        (w_send, w_recv, p_send, p_recv, v_send, v_recv, h_send, h_recv, a_send, a_recv,
         x_send, x_recv),
        (sm_send, sm_recv, t_send, t_recv, f_send, f_recv, z_send, z_recv, c_send, c_recv),
    ) = take(refs, (6, 6, 8, 4, 6, 4, 9, 15, 9, 11, 4, 10, 10, 8, 10, 24, 8, 8, 6, 6, 7, 7, 12, 10))
    windows, heads = probs.shape[0], probs.shape[1]
    images = windows // 2
    width = q.shape[2]
    shard = w_qkv.shape[1]
    hidden = w_up.shape[1]
    ff = 4 * hidden
    f, c, t = lax.axis_index("fsdp"), lax.axis_index("ctx"), lax.axis_index("tp")
    near, far = f + 1 - 2 * lax.rem(f, 2), lax.rem(f + 2, 4)
    me = f * 4 + t
    two = LineSum.build(part, ls_two, tot_two)
    four = LineSum.build(part, ls_four, tot_four)
    mixl = TradeSum(LineSum.build(mix, ls_two, tot_mix), away, (y_send, y_recv))

    def block(at):
        return pl.ds(pl.multiple_of(at * shard, shard), shard)

    def band(at):
        return pl.ds(pl.multiple_of(at * width, width), width)

    def other(n):
        at = lax.rem(me + n, 16)
        return {"fsdp": lax.div(at, 4), "tp": lax.rem(at, 4)}

    up = ShardSum(lambda at: gu[block(at), :], gu_o, up_refs)
    down = BandFirstSum(
        lambda at, first, size: gd[pl.ds(pl.multiple_of(at * shard + first, 32), size), :], gd_o, down_refs
    )
    qkv = [
        ShardSum(
            lambda at, n=n: gu[block(at), n * 256 : n * 256 + width], gq_o.at[n], qkv_refs[8 * n : 8 * n + 8]
        )
        for n in range(3)
    ]
    proj = ShardSum(lambda at: gd[block(at), :shard], gp_o, proj_refs)
    table = TableSum(dpos_s, table_refs)
    barrier = pltpu.get_barrier_semaphore()
    greet(barrier, [{"ctx": 1 - c}] + [other(n) for n in range(1, 16)])
    fetch = [
        pltpu.make_async_copy(src, dst, i_sem.at[n])
        for n, (src, dst) in enumerate(zip(big_inputs, (feat, og, w_qkv, w_proj, w_up, w_down)))
    ]
    for n in (2, 3, 0, 4, 5, 1):
        fetch[n].start()

    store = [
        pltpu.make_async_copy(src, dst, o_sem.at[n])
        for n, (src, dst) in enumerate(zip((home_o, gin_o, gq_o, gp_o, gu_o, gd_o), big_outputs))
    ]

    ready()

    part_of = HD // 4

    def ints(shape, axis):
        return lax.broadcasted_iota(jnp.int32, shape, axis)

    def ones_where(cond):
        return jnp.where(cond, 1.0, 0.0).astype(BF)

    def flat_units(values, count):
        lanes = count * part_of
        spread = dot(values, ones_where(jnp.bitwise_and(ints((part_of, lanes), 1), 7) == ints((part_of, lanes), 0)))
        return jnp.sum(
            jnp.where(jnp.right_shift(ints((count, lanes), 1), 3) == ints((count, lanes), 0), spread, 0.0),
            axis=0, keepdims=True,
        )

    units = hidden // HD
    lanes = units * part_of
    spread = dot(
        w_hidden[...].astype(BF),
        ones_where(jnp.right_shift(ints((units, lanes), 1), 3) == ints((units, lanes), 0)),
    )
    hidden_row = jnp.sum(
        jnp.where(jnp.bitwise_and(ints((8, lanes), 1), 7) == ints((8, lanes), 0), spread, 0.0),
        axis=0, keepdims=True,
    )
    own = jnp.concatenate([w_norm[...], jnp.zeros((2, shard), F32), hidden_row, jnp.zeros((7, shard), F32)], axis=0)
    small[0:16, :shard] = own
    small[0:16, shard:] = jnp.zeros((16, D - shard), F32)
    for n in range(2):
        small[9 + n : 10 + n, : heads * part_of] = flat_units(w_heads[:, n, :].astype(BF), heads)
    sm_g[f] = small[0:16, :shard].astype(BF)
    fetch[2].wait()
    wq[:, block(f), :] = w_qkv[...].astype(BF)
    fetch[3].wait()
    wp_g[f, band(t), :] = w_proj[...].astype(BF)
    fetch[0].wait()
    fetch[4].wait()
    wu[block(f), :] = w_up[...].astype(BF)
    fetch[5].wait()
    wd[block(f), :] = w_down[...].astype(BF)
    fetch[1].wait()
    for i in range(images):
        og_low[i] = og[i, 0:SHIFT].astype(BF)
    pl.semaphore_wait(barrier, 16)

    items = [
        lambda at: sm_g.at[at],
        lambda at: wq.at[:, block(at), :],
    ]
    half = shard // 2

    def split_copies(full, k):
        def piece(n, at, cc, where):
            ref = full.at[block(at), :] if cc is None else full.at[
                pl.ds(pl.multiple_of(at * shard + cc * half, half), half), :
            ]
            return remote(ref, ref, d_send.at[k, n], d_recv.at[k, n], where)

        return (
            piece(0, f, c, {"fsdp": far}), piece(1, f, None, {"fsdp": near}),
            piece(2, far, c, {"ctx": 1 - c}), piece(3, far, c, {"fsdp": near}),
            piece(4, far, 1 - c, {"fsdp": near}),
        )

    down_copies = split_copies(wd, 0)
    up_copies = split_copies(wu, 1)

    def copy_of(n, kind, at, where):
        ref = items[n](at)
        return remote(ref, ref, w_send.at[n, kind], w_recv.at[n, kind], {"fsdp": where})

    def proj_copy(n, kind, at, where):
        ref = wp_g.at[at, band(lax.rem(t - n + 4, 4))]
        return remote(ref, ref, p_send.at[n, kind], p_recv.at[n, kind], {"fsdp": where})

    def proj_line(n):
        ref = wp_g.at[f, band(t)]
        return remote(ref, ref, v_send.at[n], v_recv.at[n], {"tp": lax.rem(t + n, 4)})

    halo_f = [
        remote(feat.at[i, 0:SHIFT], fh.at[i], h_send.at[i], h_recv.at[i], {"ctx": 1 - c})
        for i in range(images)
    ]
    halo_g = [
        remote(og_low.at[i], gh.at[i], h_send.at[images + i], h_recv.at[images + i], {"ctx": 1 - c})
        for i in range(images)
    ]

    def send_both(n):
        copy_of(n, 0, f, far).start()
        copy_of(n, 1, f, near).start()

    def proj_both(n):
        proj_copy(n, 0, f, far).start()
        proj_copy(n, 1, f, near).start()

    send_both(0)
    for copy in halo_f:
        copy.start()
    for n in range(1, 4):
        proj_line(n).start()
    send_both(1)
    proj_both(0)
    down_copies[0].start()
    up_copies[0].start()
    halo_g[0].start()
    down_copies[1].start()
    up_copies[1].start()

    def relay(n):
        copy_of(n, 0, f, far).wait_recv()
        copy_of(n, 2, far, near).start()

    def gathered(n):
        copy_of(n, 1, f, near).wait_recv()
        copy_of(n, 2, far, near).wait_recv()

    ridx[...] = jnp.zeros_like(ridx)
    ridx[:TOK, :TOK] = ridx_m[...]
    table_t[...] = jnp.zeros_like(table_t)
    table_t[:heads, : w_table.shape[1]] = w_table[...].astype(BF).astype(F32)

    def bias_rows(step, carry):
        rows_at = pl.ds(pl.multiple_of(step * 8, 8), 8)
        for half in range(2):
            lanes_at = slice(half * 128, (half + 1) * 128)
            idx = ridx[rows_at, lanes_at]
            low = jnp.bitwise_and(idx, 127)
            high = jnp.right_shift(idx, 7)
            picks = [high == n for n in range(5)]
            for h in range(heads):
                found = jnp.zeros((8, 128), F32)
                for n in range(5):
                    tab = jnp.broadcast_to(table_t[h : h + 1, n * 128 : (n + 1) * 128], (8, 128))
                    got = jnp.take_along_axis(tab, low, axis=1, mode="promise_in_bounds")
                    found = jnp.where(picks[n], got, found)
                bias_s[h, rows_at, lanes_at] = found
        return carry

    lax.fori_loop(0, TOK // 8, bias_rows, 0)
    relay(0)
    dpos_s[...] = jnp.zeros_like(dpos_s)
    for n in range(1, 4):
        proj_line(n).wait_recv()
        proj_both(n)
    gathered(0)
    rows[...] = jnp.concatenate([sm_g[n].astype(F32) for n in range(4)], axis=1)
    unit = ints((shard, D), 0)
    lane = ints((shard, D), 1)
    biases = jnp.zeros((16, D), F32)
    for n in range(4):
        same = jnp.logical_and(
            jnp.right_shift(lane, 5) == jnp.right_shift(unit, 3),
            jnp.bitwise_and(lane, 31) == jnp.bitwise_and(unit, 7) + n * 8,
        )
        biases = biases + dot(sm_g[n], ones_where(same))
    rows[8:16, :] = biases[8:16, :]
    small[...] = jnp.zeros_like(small)
    relay(1)

    def enter(i):
        halo_f[i].wait_recv()
        window_rows(
            lambda im, r: feat[im, SHIFT + r] if r < SHIFT else fh[im, r - SHIFT], row_tmp, i, xw
        )

    enter(0)
    gain_one, offset_one = rows[0:1, :], rows[1:2, :]
    bias_proj, gain_two, offset_two = rows[2:3, :], rows[3:4, :], rows[4:5, :]
    bias_hidden = rows[8:9, :]
    bias_q, bias_v = rows[9:10, :width], rows[10:11, :width]
    head_of = jnp.right_shift(ints((1, width), 1), 5)
    picks_of = [ones_where(head_of == h) for h in range(heads)]

    def over(p):
        return jnp.right_shift(p * 171, 11)

    def region_forms(w):
        i, j = lax.div(w, 2), lax.rem(w, 2)
        both = jnp.where(i == 0, regions[:, 0, :], regions[:, 1, :]).astype(F32)
        square = jnp.where(j == 0, both[:, :WIN], both[:, WIN:]).astype(BF)
        p_row, r_row = ints((WIN, TOK), 1), ints((WIN, TOK), 0)
        spread_row = dot(square, ones_where(p_row - WIN * over(p_row) == r_row))
        row = jnp.sum(jnp.where(over(p_row) == r_row, spread_row, 0.0), axis=0, keepdims=True)
        p_col, r_col = ints((TOK, WIN), 0), ints((TOK, WIN), 1)
        spread_col = dot(ones_where(over(p_col) == r_col), square)
        col = jnp.sum(
            jnp.where(p_col - WIN * over(p_col) == r_col, spread_col, 0.0), axis=1, keepdims=True
        )
        return row, col

    def spot(w):
        return pl.ds(pl.multiple_of(w * TOK, TOK), TOK)

    def add_rows(n, term):
        small[n : n + 1, : term.shape[1]] = small[n : n + 1, : term.shape[1]] + jnp.sum(
            term, axis=0, keepdims=True
        )

    def ctx_copy(p, kind, at, where):
        ref = ctx.at[p, at]
        return remote(ref, ref, x_send.at[p, kind], x_recv.at[p, at], {"tp": where})

    other_outer = 3 - two.outer

    def ctx_wait(p, at):
        ctx_copy(p, 0, at, two.mid).wait_recv()

    def pass_in(p):
        ctx_wait(p, two.outer)
        ctx_copy(p, 2, two.outer, two.other_mid).start()
        ctx_wait(p, two.other_mid)
        ctx_copy(p, 3, two.other_mid, two.outer).start()

    def pass_out(p):
        ctx_wait(p, other_outer)
        ctx_copy(p, 4, other_outer, two.outer).start()

    gathered(1)

    def forward(w, carry):
        @pl.when(w == 2)
        def _():
            enter(1)

        x = xw[w]
        centred = x - row_mean(x)
        xhat = centred * lax.rsqrt(row_mean(centred * centred) + NORM_EPS)
        normed = (xhat * gain_one + offset_one).astype(BF)
        n1[spot(w), :] = normed
        q_w = (dot(normed, wq[0]) + bias_q).astype(BF)
        k_w = dot(normed, wq[1]).astype(BF)
        v_w = (dot(normed, wq[2]) + bias_v).astype(BF)
        q[w] = q_w
        k[w] = k_w
        v[w] = v_w
        reg_row, reg_col = region_forms(w)
        mask = jnp.where(reg_col == reg_row, 0.0, MASK_FILL)
        context = jnp.zeros((TOK, width), F32)
        for h in range(heads):
            scores = dot_t(q_w * picks_of[h], k_w) * HD ** (-0.5) + bias_s[h, :, :TOK] + mask
            lifted = jnp.exp(scores - jnp.max(scores, axis=-1, keepdims=True))
            p = lifted / jnp.sum(lifted, axis=-1, keepdims=True)
            probs[w, h] = p
            context = context + dot(p.astype(BF), v_w * picks_of[h])
        low = context.astype(BF)
        p_at = lax.div(w, 2)

        @pl.when(lax.rem(w, 2) == 0)
        def _():
            ctx[p_at, t, :, :width] = low

        @pl.when(lax.rem(w, 2) == 1)
        def _():
            ctx[p_at, t, :, width:] = low
            ctx_copy(p_at, 0, t, jnp.where(two.is_mid, two.outer, two.mid)).start()

            @pl.when(two.is_mid)
            def _():
                ctx_copy(p_at, 1, t, two.other_mid).start()

        return carry

    lax.fori_loop(0, windows, forward, 0)
    for copies in (down_copies, up_copies):
        copies[0].wait_recv()
        copies[2].start()
        copies[3].start()
    for copy in halo_g[1:]:
        copy.start()

    @pl.when(two.is_mid)
    def _():
        pass_in(0)

    for n in range(4):
        proj_copy(n, 0, f, far).wait_recv()
        proj_copy(n, 2, far, near).start()

    @pl.when(two.is_mid)
    def _():
        pass_out(0)
        pass_in(1)

    down_copies[2].wait_recv()
    down_copies[4].start()

    for n in range(4):
        proj_copy(n, 1, f, near).wait_recv()
        proj_copy(n, 2, far, near).wait_recv()
    wp[...] = jnp.concatenate([wp_g[n] for n in range(4)], axis=1)
    up_copies[2].wait_recv()
    up_copies[4].start()
    for n in (1, 3, 4):
        down_copies[n].wait_recv()
        up_copies[n].wait_recv()

    def middle(w, carry):
        p_at, odd = lax.div(w, 2), lax.rem(w, 2) == 1

        @pl.when(jnp.logical_and(two.is_outer, jnp.logical_not(odd)))
        def _():
            for at in (two.mid, two.other_mid, other_outer):
                ctx_wait(p_at, at)

        branch = jnp.zeros((TOK, D), F32) + bias_proj
        for n in range(4):
            both = ctx[p_at, n]
            low = jnp.where(odd, both[:, width:], both[:, :width])
            branch = branch + dot(low, wp[n * width : (n + 1) * width, :])
        resid = xw[w] + branch
        centred = resid - row_mean(resid)
        rstd = lax.rsqrt(row_mean(centred * centred) + NORM_EPS)
        xhat = centred * rstd
        xhat_s[w] = xhat
        rstd_s[w] = jnp.broadcast_to(rstd, (TOK, 128))
        normed = (xhat * gain_two + offset_two).astype(BF)
        n2_s[spot(w), :] = normed
        pre = dot(normed, wu[...]) + bias_hidden
        cdf = 0.5 * (1.0 + lax.erf(pre * 0.7071067811865476))
        slope = cdf + pre * (jnp.exp(-0.5 * (pre * pre)) * 0.3989422804014327)
        hid = (pre * cdf).astype(BF)
        hid_s[spot(w), :] = hid

        for n in range(images):

            @pl.when(w == 2 * n)
            def _():
                halo_g[n].wait_recv()
                window_rows(
                    lambda im, r: og[im, SHIFT + r] if r < SHIFT else gh[im, r - SHIFT],
                    row_tmp, n, ogw,
                )

        @pl.when(jnp.logical_and(two.is_mid, w == 0))
        def _():
            pass_out(1)

        @pl.when(w >= 3)
        def _():
            two.hand(w - 3)

        @pl.when(w >= 2)
        def _():
            two.settle(w - 2)

        @pl.when(w >= 1)
        def _():
            two.cross(w - 1)

        low = ogw[w].astype(BF)
        d_pre = dot(low, wd[...]) * slope
        add_rows(6, d_pre)
        dpl = d_pre.astype(BF)
        dpl_s[spot(w), :] = dpl
        two.put(w, dot_t(dpl, wu[...]))
        two.start(w)
        mixl.put(w, dot_t(hid, wd[...]))

        @pl.when(two.is_mid)
        def _():
            whole = branch + rows[5:6, :]
            for s in range(2):
                for h in range(2):

                    @pl.when(two.own == h)
                    def _():
                        mix[2 * w + s, h] = (
                            mix[2 * w + s, h]
                            + whole[s * ROWS : (s + 1) * ROWS, h * HALF : (h + 1) * HALF]
                        )

        return carry

    lax.fori_loop(0, windows, middle, 0)

    def grad_chunk(m, carry):
        chunk = pl.ds(pl.multiple_of(m * 256, 256), 256)
        low = jnp.concatenate([ogw[w, :, chunk] for w in range(windows)], axis=0).astype(BF)
        gd[chunk, :] = t_dot(low, hid_s[...])
        gu[chunk, :] = t_dot(n2_s[:, chunk], dpl_s[...])
        return carry

    lax.fori_loop(0, D // 256, grad_chunk, 0)
    down.start()
    up.start()
    two.hand(windows - 3)
    two.cross(windows - 1)
    two.settle(windows - 2)

    def backward(w, carry):
        two.arrive(w)
        d_two = two.get(w)
        xhat = xhat_s[w]
        e = d_two * gain_two
        d_flat = (e - row_mean(e) - xhat * row_mean(e * xhat)) * rstd_s[w, :, 0:1]
        og_w = ogw[w]
        d_resid = og_w + d_flat
        dft[w] = d_flat
        d_branch = d_resid.astype(BF)
        dbr[spot(w), :] = d_branch
        for n, term in ((2, d_resid), (3, d_two * xhat), (4, d_two), (5, og_w)):
            add_rows(n, term)
        d_ctx = dot_t(d_branch, wp[band(t), :]).astype(BF)
        q_w, k_w, v_w = q[w], k[w], v[w]
        d_q = jnp.zeros((TOK, width), F32)
        d_k = jnp.zeros((TOK, width), F32)
        d_v = jnp.zeros((TOK, width), F32)
        for h in range(heads):
            d_ctx_h = d_ctx * picks_of[h]
            p = probs[w, h]
            d_p = dot_t(d_ctx_h, v_w)
            d_v = d_v + t_dot(p.astype(BF), d_ctx_h)
            d_s = p * (d_p - jnp.sum(p * d_p, axis=-1, keepdims=True))
            dpos_s[h, :TOK, :TOK] = dpos_s[h, :TOK, :TOK] + d_s
            d_l = (d_s * HD ** (-0.5)).astype(BF)
            d_q = d_q + dot(d_l, k_w * picks_of[h])
            d_k = d_k + t_dot(d_l, q_w * picks_of[h])
        partial = jnp.zeros((TOK, D), F32)
        for n, d_n in enumerate((d_q, d_k, d_v)):
            low = d_n.astype(BF)
            dh_s[n, spot(w), :] = low
            partial = partial + dot_t(low, wq[n])
            if n != 1:
                add_rows(8 + n // 2, low.astype(F32))
        four.put(w, partial)
        four.start(w)

        @pl.when(w == 0)
        def _():
            down.pair()
            up.pair()
            two.settle(windows - 1)
            two.hand(windows - 2)

        @pl.when(w == 1)
        def _():
            two.hand(windows - 1)
            four.cross(0)

        @pl.when(w == 2)
        def _():
            four.settle(0)
            four.cross(1)
            down.cross()

        @pl.when(w == 3)
        def _():
            up.cross()

        return carry

    lax.fori_loop(0, windows, backward, 0)
    table.start()
    for n in range(3):
        gu[:, n * 256 : n * 256 + width] = t_dot(n1[...], dh_s[n])
        qkv[n].start()
    four.hand(0)
    four.settle(1)
    ctx_own = jnp.concatenate(
        [ctx[w // 2, t, :, (w % 2) * width : (w % 2 + 1) * width] for w in range(windows)], axis=0
    )
    gp = t_dot(ctx_own, dbr[...])
    for n in range(4):
        gd[n * width : (n + 1) * width, :shard] = gp[:, n * shard : (n + 1) * shard]
    proj.start()
    for w in range(windows):
        two.drain(w)
        mixl.start(w)
    table.pair()
    down.share()
    four.cross(2)
    for member in (*qkv, proj):
        member.pair()
    four.hand(1)
    four.cross(3)
    four.settle(2)
    table.cross()
    qkv[0].cross()

    keep = 1.0 - DECAY_RATE
    first_f = jnp.where(f == 0, 1.0, 0.0)
    first_t = jnp.where(t == 0, 1.0, 0.0)
    old_rows = [
        first_t * jnp.sum(row_qkv[0:1, :], axis=1, keepdims=True),
        first_t * jnp.sum(row_qkv[1:2, :], axis=1, keepdims=True),
        first_t * jnp.sum(row_qkv[2:3, :], axis=1, keepdims=True),
        first_f * total_of(row_proj[...]),
        first_t * total_of(row_up[...]),
        first_f * total_of(row_down[...]),
    ]
    masters = [
        sum(total_of(w_qkv[n] * w_qkv[n]) for n in range(3)),
        total_of(w_proj[...] * w_proj[...]),
        total_of(w_up[...] * w_up[...]),
        total_of(w_down[...] * w_down[...]),
        *[
            first_t * jnp.sum(w_norm[n : n + 1, :] * w_norm[n : n + 1, :], axis=1, keepdims=True)
            for n in range(6)
        ],
        *[total_of(w_heads[:, n, :] * w_heads[:, n, :]) for n in range(2)],
        total_of(w_hidden[...] * w_hidden[...]),
        first_f * total_of(w_table[...] * w_table[...]),
    ]
    four.settle(3)

    for copy in halo_g:
        copy.wait_send()
    home_in = HomeRows(xhat_s, row_tmp, gin_o, og_low, a_send, a_recv)

    def back(w):
        four.arrive(w)
        x = xw[w]
        centred = x - row_mean(x)
        rstd = lax.rsqrt(row_mean(centred * centred) + NORM_EPS)
        xhat = centred * rstd
        d_one = four.get(w)
        e = d_one * gain_one
        xhat_s[w] = dft[w] + (e - row_mean(e) - xhat * row_mean(e * xhat)) * rstd
        for n, term in ((0, d_one * xhat), (1, d_one)):
            add_rows(n, term)

    back(0)
    four.hand(2)
    qkv[1].cross()
    mixl.cross(0)
    qkv[2].cross()
    back(1)
    four.hand(3)
    mixl.cross(1)
    mixl.settle(0)
    proj.cross()
    down.finish()
    up.finish()
    store[4].start()
    store[5].start()
    t_s[t] = jnp.zeros((8, shard), F32)
    f_s[f] = jnp.zeros((8, hidden), F32)
    sq_up = gu_o[...] * gu_o[...]
    sq_down = gd_o[...] * gd_o[...]
    t_s[t, 4:5, :] = lane_sums(sq_up)
    t_s[t, 5:6, :] = lane_sums(sq_down)
    f_s[f, 4:5, :] = jnp.sum(sq_up, axis=0, keepdims=True)
    f_s[f, 5:6, :] = jnp.sum(sq_down, axis=0, keepdims=True)
    tot_up, tot_down = total_of(sq_up), total_of(sq_down)
    table.finish(chunk_s)
    first = table.first_row()
    ident = ints((640, TOK), 0)

    def bin_row(step, acc):
        for n in range(4):
            i = step * 4 + n
            hot = ones_where(ident == ridx[pl.ds(first + i, 1), :TOK])
            vals = jnp.concatenate(
                [chunk_s[h, pl.ds(i, 1), :TOK] for h in range(heads)]
                + [jnp.zeros((8 - heads, TOK), F32)],
                axis=0,
            )
            high = vals.astype(BF)
            low = (vals - high.astype(F32)).astype(BF)
            acc = acc + dot_t(jnp.concatenate([high, low], axis=0), hot)
        return acc

    hist = lax.fori_loop(0, 3, bin_row, jnp.zeros((16, 640), F32))
    mixl.cross(2)
    mixl.settle(1)
    mixl.trade(0)
    hist = lax.fori_loop(3, 6, bin_row, hist)
    small[16:24, :640] = hist[0:8] + hist[8:16]
    back(2)
    back(3)
    sm_s[0] = small[...]

    def swap(n):
        where = ({"fsdp": near}, {"fsdp": far}, {"ctx": 1 - c})[n]
        return remote(sm_s.at[n], sm_r.at[n], sm_send.at[n], sm_recv.at[n], where)

    swap(0).start()
    mixl.cross(3)
    mixl.settle(2)
    mixl.hand(0)
    mixl.trade(1)
    for member in (*qkv, proj):
        member.finish()
    store[2].start()
    store[3].start()

    tot_q = []
    for n in range(3):
        sq = gq_o[n] * gq_o[n]
        t_s[t, n : n + 1, :] = lane_sums(sq)
        f_s[f, n : n + 1, :width] = jnp.sum(sq, axis=0, keepdims=True)
        tot_q.append(total_of(sq))
    sq = gp_o[...] * gp_o[...]
    f_s[f, 3:4, :shard] = lane_sums(sq)
    t_s[t, 3:4, :] = jnp.sum(sq, axis=0, keepdims=True)
    z_s[me] = lane_pack([*tot_q, total_of(sq), tot_up, tot_down, *old_rows, *masters])

    def t_copy(n):
        return remote(t_s.at[t], t_s.at[t], t_send.at[n], t_recv.at[n], {"tp": lax.rem(t + n, 4)})

    def f_copy(n):
        return remote(f_s.at[f], f_s.at[f], f_send.at[n], f_recv.at[n], {"fsdp": lax.rem(f + n, 4)})

    def z_copy(n):
        return remote(z_s.at[me], z_s.at[me], z_send.at[n], z_recv.at[n], other(n))

    def c_copy(n):
        return remote(c_s.at[me], c_s.at[me], c_send.at[n], c_recv.at[n], other(n))

    for n in range(1, 4):
        t_copy(n).start()
        f_copy(n).start()
    for n in range(1, 16):
        z_copy(n).start()
    mixl.settle(3)
    home_in.go(0)
    home_in.go(1)
    mixl.hand(1)
    mixl.trade(2)
    swap(0).wait_recv()
    sm_s[1] = sm_s[0] + sm_r[0]
    swap(1).start()

    def lift(w):
        mixl.arrive(w)
        dft[w] = mixl.get(w)

    def leave(i):
        for r in range(WIN):
            home_o[i, (SHIFT + r) % WIN] = home_row(dft, row_tmp, i, r)

    lift(0)
    swap(1).wait_recv()
    sm_s[2] = sm_s[1] + sm_r[1]
    swap(2).start()
    mixl.trade(3)
    mixl.hand(2)
    lift(1)
    leave(0)

    swap(2).wait_recv()
    sm = sm_s[2] + sm_r[2]

    def own_lanes(x, size):
        out = x[:, :size]
        for n in range(1, 4):
            out = jnp.where(f == n, x[:, n * size : (n + 1) * size], out)
        return out

    def own_units(row, count):
        all_lanes = count * HD
        at_lane = ints((count, all_lanes), 1)
        only = jnp.where(
            jnp.right_shift(at_lane, 5) == ints((count, all_lanes), 0),
            jnp.broadcast_to(row, (count, all_lanes)), 0.0,
        )
        pick = jnp.where(
            jnp.bitwise_and(ints((all_lanes, part_of), 0), HD - 1)
            == f * part_of + ints((all_lanes, part_of), 1),
            1.0, 0.0,
        )
        return only, pick

    gn = own_lanes(sm[0:6, :], shard)
    gh_new = [exact(*own_units(sm[8 + n : 9 + n, :width], heads), ((1,), (0,))) for n in range(2)]
    only, pick = own_units(sm[6:7, :], hidden // HD)
    gx = exact(pick, only, ((0,), (1,)))
    gt = sm[16 : 16 + heads, : w_table.shape[1]]
    gn_o[...] = gn
    gx_o[...] = gx
    gt_o[...] = gt
    small_sq = first_t * total_of(plain(gn, s_norm[...])[1] ** 2)
    for n in range(2):
        gh_o[:, n, :] = gh_new[n]
        small_sq = small_sq + total_of(plain(gh_new[n], s_heads[:, n, :])[1] ** 2)
    small_sq = small_sq + total_of(plain(gx, s_hidden[...])[1] ** 2)
    small_sq = small_sq + first_f * total_of(plain(gt, s_table[...])[1] ** 2)

    for n in range(1, 4):
        t_copy(n).wait_recv()
        f_copy(n).wait_recv()
    t_sum = t_s[0] + t_s[1] + t_s[2] + t_s[3]
    f_sum = f_s[0] + f_s[1] + f_s[2] + f_s[3]
    for n in range(1, 16):
        z_copy(n).wait_recv()
    z_sum = z_s[0]
    for n in range(1, 16):
        z_sum = z_sum + z_s[n]
    lane8 = ints((8, 128), 1)

    def scalar(n):
        return jnp.sum(jnp.where(lane8 == n, z_sum, 0.0)[0:1], axis=1, keepdims=True)

    def fresh(old, summed, count):
        return DECAY_RATE * old + keep * (summed / count + STAT_EPS)

    rq = fresh(row_qkv[...], t_sum[0:3, :], D)
    kq = fresh(col_qkv[...], f_sum[0:3, :width], D)
    rp = fresh(wide(row_proj), f_sum[3:4, :width], D)
    kp = fresh(wide(col_proj), t_sum[3:4, :], D)
    ru = fresh(wide(row_up), t_sum[4:5, :], ff)
    ku = fresh(wide(col_up), f_sum[4:5, :], D)
    rd = fresh(wide(row_down), f_sum[5:6, :], D)
    kd = fresh(wide(col_down), t_sum[5:6, :], ff)

    def mean_row(n, rows_all, cols_all):
        return (
            DECAY_RATE * scalar(6 + n) + keep * (scalar(n) / cols_all + rows_all * STAT_EPS)
        ) / rows_all

    means = [
        mean_row(0, D, D), mean_row(1, D, D), mean_row(2, D, D), mean_row(3, D, D),
        mean_row(4, D, ff), mean_row(5, ff, D),
    ]
    scales = update_scales(rq, kq, rp, kp, ru, ku, rd, kd, means)
    big_sq = small_sq
    grads = [gq_o[n] for n in range(3)] + [gp_o[...], gu_o[...], gd_o[...]]
    for grad, scale in zip(grads, scales):
        u = grad * scale
        big_sq = big_sq + total_of(u * u)
    c_s[me] = jnp.broadcast_to(big_sq, (8, 128))
    for n in range(1, 16):
        c_copy(n).start()
    rq_o[...] = rq
    kq_o[...] = kq
    for ref, row in ((rp_o, rp), (kp_o, kp), (ru_o, ru), (ku_o, ku), (rd_o, rd), (kd_o, kd)):
        put_wide(ref, row)
    mixl.hand(3)
    lift(2)
    lift(3)
    leave(1)
    store[0].start()
    for i in range(images):
        home_in.wait(i)
    store[1].start()

    counts = [3 * D * D, D * D, D * ff, ff * D] + [D] * 8 + [ff, RELP * HEADS]
    sizes = [jnp.sqrt(scalar(12 + n) / counts[n] + STAT_EPS) for n in range(14)]
    for n in range(1, 16):
        c_copy(n).wait_recv()
    all_sq = c_s[0]
    for n in range(1, 16):
        all_sq = all_sq + c_s[n]
    count_all = 4 * D * D + 2 * D * ff + 8 * D + ff + RELP * HEADS
    clip = jnp.sqrt(all_sq[0:1, 0:1] / count_all)
    factor = STEP_RATE / jnp.maximum(1.0, clip / CLIP_LEVEL)
    size_o[...] = lane_pack([size * factor for size in sizes] + [clip] + means)
    for n in range(3):
        swap(n).wait_send()
    for n in range(1, 4):
        t_copy(n).wait_send()
        f_copy(n).wait_send()
        proj_line(n).wait_send()
    for p in range(windows // 2):
        ctx_copy(p, 0, t, two.mid).wait_send()

        @pl.when(two.is_mid)
        def _():
            for kind in range(1, 5):
                ctx_copy(p, kind, t, two.mid).wait_send()

    for n in range(1, 16):
        z_copy(n).wait_send()
        c_copy(n).wait_send()
    for w in range(windows):
        mixl.drain(w)
        four.drain(w)
    for copy in halo_f:
        copy.wait_send()
    for copy in (*down_copies, *up_copies):
        copy.wait_send()
    for n in range(2):
        copy_of(n, 0, f, far).wait_send()
        copy_of(n, 1, f, near).wait_send()
        copy_of(n, 2, far, near).wait_send()
    for n in range(4):
        proj_copy(n, 0, f, far).wait_send()
        proj_copy(n, 1, f, near).wait_send()
        proj_copy(n, 2, far, near).wait_send()
    for member in (up, down, *qkv, proj, table):
        member.drain()
    for copy in store:
        copy.wait()
def finish_body(ready, *refs):
    (
        big_in, (gn, gh, gx, gt), (w_norm, w_heads, w_hidden, w_table),
        (s_norm, s_heads, s_hidden, s_table), stats, (size,),
        big_out, (gn_o, gh_o, gx_o, gt_o), (nn_o, nh_o, nx_o, nt_o), stats_o,
        (sn_o, sh_o, sx_o, st_o), (clip_o,), held, made, (i_sem, o_sem),
    ) = take(refs, (12, 4, 4, 4, 8, 1, 14, 4, 4, 8, 4, 1, 12, 10, 2))
    home_out, feat, home_in, og = held[:4]
    grads, masters = held[4:8], held[8:12]
    fetch = [
        pltpu.make_async_copy(src, dst, i_sem.at[n]) for n, (src, dst) in enumerate(zip(big_in, held))
    ]
    for n in (4, 5, 6, 7, 1, 0, 3, 2, 8, 9, 10, 11):
        fetch[n].start()
    sources = [*made[:2], *grads, *made[2:]]
    store = [
        pltpu.make_async_copy(src, dst, o_sem.at[n]) for n, (src, dst) in enumerate(zip(sources, big_out))
    ]
    for n in range(4):
        fetch[4 + n].wait()
        store[2 + n].start()
    for n in (0, 1):
        fetch[n].wait()
    made[0][...] = feat[...].astype(F32) + home_out[...].astype(F32)
    store[0].start()
    for n in (2, 3):
        fetch[n].wait()
    made[1][...] = og[...] + home_in[...].astype(F32)
    store[1].start()
    ready()
    lane8 = lax.broadcasted_iota(jnp.int32, (8, 128), 1)
    table = size[...]

    def step(n):
        return jnp.sum(jnp.where(lane8 == n, table, 0.0)[0:1], axis=1, keepdims=True)

    rq, kq, *vecs = stats
    scales = update_scales(rq[...], kq[...], *map(wide, vecs), [step(15 + n) for n in range(6)])
    for n in range(4):
        fetch[8 + n].wait()
        new_o, low_o = made[2 + n], made[6 + n]
        if n == 0:
            for m in range(3):
                new = masters[0][m] - step(0) * (grads[0][m] * scales[m])
                new_o[m] = new
                low_o[m] = new.astype(BF)
        else:
            new = masters[n][...] - step(n) * (grads[n][...] * scales[2 + n])
            new_o[...] = new
            low_o[...] = new.astype(BF)
        store[6 + n].start()
        store[10 + n].start()
    for src, dst in ((gn, gn_o), (gh, gh_o), (gx, gx_o), (gt, gt_o), *zip(stats, stats_o)):
        dst[...] = src[...]
    sn, un = plain(gn[...], s_norm[...])
    sn_o[...] = sn
    for n in range(6):
        nn_o[n : n + 1, :] = w_norm[n : n + 1, :] - step(4 + n) * un[n : n + 1, :]
    for n in range(2):
        sh, uh = plain(gh[:, n, :], s_heads[:, n, :])
        sh_o[:, n, :] = sh
        nh_o[:, n, :] = w_heads[:, n, :] - step(10 + n) * uh
    sx, ux = plain(gx[...], s_hidden[...])
    sx_o[...] = sx
    nx_o[...] = w_hidden[...] - step(12) * ux
    st, ut = plain(gt[...], s_table[...])
    st_o[...] = st
    nt_o[...] = w_table[...] - step(13) * ut
    clip_o[...] = step(14)
    for copy in store:
        copy.wait()


def whole_step(feat, og, regions, rel_index, masters, stats, states):
    w_qkv, w_proj, w_up, w_down, w_norm, w_heads, w_hidden, w_table = masters
    images = feat.shape[0]
    windows = 2 * images
    shard, width = w_qkv.shape[1], w_qkv.shape[2]
    hidden = w_up.shape[1]
    heads = width // HD
    stats = [u if u.ndim == 2 else u.reshape(-1, 128) if u.shape[0] == D else u[None] for u in stats]
    like = lambda u: (u.shape, F32)
    mats = (w_qkv, w_proj, w_up, w_down)
    smalls = (w_norm, w_heads, w_hidden, w_table)
    vm, dma = pltpu.VMEM, pltpu.SemaphoreType.DMA
    flat = windows * TOK
    halves = (2 * windows, 2, ROWS, HALF)
    tokens = (windows, TOK, D)
    rows_of = (images, SHIFT, 24, D)
    outs = [
        (feat.shape, BF), (feat.shape, BF), *map(like, mats), *map(like, smalls),
        *map(like, stats), ((8, 128), F32),
    ]
    scratch = [
        vm((4, 16, shard), BF), vm((3, D, width), BF), vm((4, D, shard), BF), vm((D, D), BF),
        vm((D, hidden), BF), vm((D, hidden), BF), vm(rows_of, BF), vm(rows_of, BF), vm(rows_of, BF),
        vm((heads, TOK, 256), F32), vm((24, D), F32), vm((16, D), F32), vm((192, 256), jnp.int32),
        vm((8, 640), F32), vm((24, D), F32),
        vm(tokens, F32), vm(tokens, F32), vm((flat, D), BF), vm((windows, TOK, width), BF),
        vm((windows, TOK, width), BF), vm((windows, TOK, width), BF),
        vm((windows, heads, TOK, TOK), F32), vm((windows // 2, 4, TOK, 2 * width), BF), vm(halves, F32),
        vm((flat, D), BF), vm((flat, hidden), BF), vm((flat, hidden), BF),
        vm(tokens, F32), vm((windows, TOK, 128), F32), vm(halves, BF), vm((D, hidden), F32),
        vm((D, hidden), F32), vm(tokens, F32), vm((flat, D), BF), vm(halves, F32),
        vm((3, flat, width), BF), vm((heads, 192, 256), F32), vm((heads, 24, 256), F32),
        vm(halves, BF),
        *LineSum.scratch(2 * windows), *LineSum.scratch(2 * windows),
        *ShardSum.scratch((shard, hidden)), *BandFirstSum.scratch((shard, hidden)),
        *[s for _ in range(3) for s in ShardSum.scratch((shard, width))], *ShardSum.scratch((width, shard)),
        *TableSum.scratch(heads),
        vm((3, 24, D), F32), vm((3, 24, D), F32), vm((4, 8, shard), F32), vm((4, 8, hidden), F32),
        vm((16, 8, 128), F32), vm((16, 8, 128), F32),
        vm(feat.shape, BF), vm(og.shape, F32), *[vm(u.shape, F32) for u in mats],
        vm(halves, BF), vm((windows, ROWS, HALF), BF), dma((windows,)), dma((windows,)), dma((6,)),
        dma((2, 5)), dma((2, 5)),
        vm(feat.shape, BF), vm(feat.shape, BF), *[vm(u.shape, F32) for u in mats], dma((6,)),
        dma((2, 3)), dma((2, 3)), dma((4, 3)), dma((4, 3)), dma((4,)), dma((4,)),
        dma((2 * images,)), dma((2 * images,)), *[dma((images,))] * 2,
        dma((windows // 2, 5)), dma((windows // 2, 4)),
        dma((3,)), dma((3,)), *[dma((4,))] * 4, *[dma((16,))] * 4,
    ]
    got = vmem_call(step_body, outs, scratch, "whole_step", 1, 6, 6)(
        feat, og, *mats, regions, rel_index, *smalls, *stats, *states
    )
    home_out, home_in, g_qkv, g_proj, g_up, g_down, gn, gh, gx, gt, *rest = got
    new_stats, size = rest[:8], rest[8]
    outs = [
        like(og), like(og), *map(like, mats), *map(like, mats), *[(u.shape, BF) for u in mats],
        *map(like, smalls), *map(like, smalls), *map(like, stats), *map(like, smalls), ((1, 1), F32),
    ]
    scratch = [
        vm(feat.shape, BF), vm(feat.shape, BF), vm(feat.shape, BF), vm(og.shape, F32),
        *[vm(u.shape, F32) for u in mats], *[vm(u.shape, F32) for u in mats],
        vm(og.shape, F32), vm(og.shape, F32), *[vm(u.shape, F32) for u in mats],
        *[vm(u.shape, BF) for u in mats], dma((12,)), dma((14,)),
    ]
    return vmem_call(finish_body, outs, scratch, "finish", None, 12, 14)(
        home_out, feat, home_in, og, g_qkv, g_proj, g_up, g_down, *mats, gn, gh, gx, gt,
        *smalls, *states, *new_stats, size,
    )


def per_device_plain(
    features,
    out_grad,
    regions,
    rel_index,
    w_qkv,
    w_proj,
    w_up,
    w_down,
    norm_vecs,
    head_bias,
    hidden_bias,
    rel_table,
    row_qkv,
    col_qkv,
    row_proj,
    col_proj,
    row_up,
    col_up,
    row_down,
    col_down,
    state_norm,
    state_heads,
    state_hidden,
    state_table,
):
    images, band_rows, across, model_width = features.shape
    win_tokens = WIN * WIN
    fsdp_at = lax.axis_index("fsdp")
    ctx_at = lax.axis_index("ctx")
    tp_at = lax.axis_index("tp")
    first_fsdp = (fsdp_at == 0).astype(jnp.float32)
    first_ctx = (ctx_at == 0).astype(jnp.float32)
    first_tp = (tp_at == 0).astype(jnp.float32)
    weights_qkv, weights_proj, weights_up, weights_down, vec_copy, head_copy, hidden_copy = (
        lax.all_gather(w_qkv.astype(jnp.bfloat16), "fsdp", axis=1, tiled=True),
        lax.all_gather(w_proj.astype(jnp.bfloat16), "fsdp", axis=1, tiled=True),
        lax.all_gather(w_up.astype(jnp.bfloat16), "fsdp", axis=0, tiled=True),
        lax.all_gather(w_down.astype(jnp.bfloat16), "fsdp", axis=1, tiled=True),
        lax.all_gather(norm_vecs.astype(jnp.bfloat16), "fsdp", axis=1, tiled=True),
        lax.all_gather(head_bias.astype(jnp.bfloat16), "fsdp", axis=2, tiled=True),
        lax.all_gather(hidden_bias.astype(jnp.bfloat16), "fsdp", axis=1, tiled=True),
    )
    norm_rows = vec_copy.astype(jnp.float32)
    bias_query = head_copy[0].reshape(-1).astype(jnp.float32)
    bias_value = head_copy[1].reshape(-1).astype(jnp.float32)
    bias_hidden = hidden_copy.reshape(-1).astype(jnp.float32)
    table_copy = rel_table.astype(jnp.bfloat16)
    local_width = weights_qkv.shape[2]
    heads_here = local_width // HD

    def roll_in(home):
        received = passed_along(home[:, :SHIFT], "ctx", -1)
        return to_windows(enter_frame(home, received)).reshape(-1, model_width)

    def roll_out(rolled_flat):
        band = jnp.roll(
            from_windows(
                rolled_flat.reshape(-1, win_tokens, model_width), images, band_rows, across
            ),
            SHIFT,
            axis=2,
        )
        lower = passed_along(band[:, band_rows - SHIFT :], "ctx", 1)
        return jnp.concatenate([lower, band[:, : band_rows - SHIFT]], axis=1)

    flat_one = roll_in(features).astype(jnp.float32)
    grad_flat = roll_in(out_grad)
    win_count = flat_one.shape[0] // win_tokens
    normed_one, pull_one = jax.vjp(layer_norm, flat_one, norm_rows[0], norm_rows[1])
    normed_one_low = normed_one.astype(jnp.bfloat16)
    head_shape = (win_count, win_tokens, heads_here, HD)
    query_low, key_low, value_low = project_heads(
        normed_one_low, weights_qkv, bias_query, bias_value, head_shape
    )
    pos_bias = table_lookup(table_copy, rel_index)
    region_win = to_windows(regions[..., None])[..., 0]
    mask_add = jnp.where(region_win[:, :, None] == region_win[:, None, :], 0.0, MASK_FILL).astype(
        jnp.float32
    )
    scores = attention_scores(query_low, key_low, pos_bias, mask_add)
    top_score = jnp.max(scores, axis=-1, keepdims=True)
    lifted = jnp.exp(scores - top_score)
    prob_rows = lifted / jnp.sum(lifted, axis=-1, keepdims=True)
    prob_low = prob_rows.astype(jnp.bfloat16)
    context = jnp.einsum("whij,wjhc->wihc", prob_low, value_low, preferred_element_type=jnp.float32)
    context_low = context.astype(jnp.bfloat16).reshape(-1, local_width)
    branch_part = jnp.dot(context_low, weights_proj, preferred_element_type=jnp.float32)
    branch = lax.psum(branch_part.astype(jnp.bfloat16), "tp").astype(jnp.float32) + norm_rows[2]
    flat_two = flat_one + branch
    normed_two, pull_two = jax.vjp(layer_norm, flat_two, norm_rows[3], norm_rows[4])
    normed_two_low = normed_two.astype(jnp.bfloat16)
    pre_act = jnp.dot(normed_two_low, weights_up, preferred_element_type=jnp.float32) + bias_hidden
    hidden, pull_gelu = jax.vjp(exact_gelu, pre_act)
    hidden_low = hidden.astype(jnp.bfloat16)
    mixed_part = jnp.dot(hidden_low, weights_down, preferred_element_type=jnp.float32)
    mixed_whole = lax.psum(mixed_part.astype(jnp.bfloat16), "tp").astype(jnp.float32)
    block_out = features.astype(jnp.float32) + roll_out(
        (branch + mixed_whole + norm_rows[5]).astype(jnp.bfloat16)
    ).astype(jnp.float32)
    grad_low = grad_flat.astype(jnp.bfloat16)
    grad_down_full = jnp.einsum(
        "tf,td->fd", hidden_low, grad_low, preferred_element_type=jnp.float32
    )
    grad_down_bias = jnp.sum(grad_flat, axis=0)
    d_hidden = jnp.einsum("td,fd->tf", grad_low, weights_down, preferred_element_type=jnp.float32)
    d_pre = pull_gelu(d_hidden)[0]
    d_pre_low = d_pre.astype(jnp.bfloat16)
    grad_hidden_bias = jnp.sum(d_pre, axis=0)
    grad_up_full = jnp.einsum(
        "td,tf->df", normed_two_low, d_pre_low, preferred_element_type=jnp.float32
    )
    d_two_part = jnp.einsum("tf,df->td", d_pre_low, weights_up, preferred_element_type=jnp.float32)
    d_two = lax.psum(d_two_part.astype(jnp.bfloat16), "tp").astype(jnp.float32)
    d_flat_two, grad_gain_two, grad_offset_two = pull_two(d_two)
    d_resid = grad_flat + d_flat_two
    grad_proj_bias = jnp.sum(d_resid, axis=0)
    d_branch = d_resid.astype(jnp.bfloat16)
    grad_proj_full = jnp.einsum(
        "tc,td->cd", context_low, d_branch, preferred_element_type=jnp.float32
    )
    d_context = (
        jnp.einsum("td,cd->tc", d_branch, weights_proj, preferred_element_type=jnp.float32)
        .astype(jnp.bfloat16)
        .reshape(head_shape)
    )
    d_probs = jnp.einsum(
        "wihc,wjhc->whij", d_context, value_low, preferred_element_type=jnp.float32
    )
    d_value_low = jnp.einsum(
        "whij,wihc->wjhc", prob_low, d_context, preferred_element_type=jnp.float32
    ).astype(jnp.bfloat16)
    d_scores = prob_rows * (d_probs - jnp.sum(prob_rows * d_probs, axis=-1, keepdims=True))
    d_pos = jnp.sum(d_scores, axis=0)
    d_scaled = (d_scores * HD ** (-0.5)).astype(jnp.bfloat16)
    d_query_low = jnp.einsum(
        "whij,wjhc->wihc", d_scaled, key_low, preferred_element_type=jnp.float32
    ).astype(jnp.bfloat16)
    d_key_low = jnp.einsum(
        "whij,wihc->wjhc", d_scaled, query_low, preferred_element_type=jnp.float32
    ).astype(jnp.bfloat16)
    d_heads = jnp.stack([d_query_low, d_key_low, d_value_low]).reshape(3, -1, local_width)
    grad_qkv_full = jnp.einsum(
        "td,ktc->kdc", normed_one_low, d_heads, preferred_element_type=jnp.float32
    )
    grad_head_bias = jnp.stack(
        [
            jnp.sum(d_heads[0].astype(jnp.float32), axis=0),
            jnp.sum(d_heads[2].astype(jnp.float32), axis=0),
        ]
    ).reshape(2, heads_here, HD)
    d_one_part = jnp.einsum("ktc,kdc->td", d_heads, weights_qkv, preferred_element_type=jnp.float32)
    d_one = lax.psum(d_one_part.astype(jnp.bfloat16), "tp").astype(jnp.float32)
    d_flat_one, grad_gain_one, grad_offset_one = pull_one(d_one)
    grad_input = out_grad + roll_out((d_flat_two + d_flat_one).astype(jnp.bfloat16)).astype(
        jnp.float32
    )
    table_part = table_grad(d_pos, rel_index, rel_table.shape[0])
    grad_norm_full = jnp.stack(
        [
            grad_gain_one,
            grad_offset_one,
            grad_proj_bias,
            grad_gain_two,
            grad_offset_two,
            grad_down_bias,
        ]
    )
    grad_list = (
        grad_qkv_full,
        grad_proj_full,
        grad_up_full,
        grad_down_full,
        grad_norm_full,
        grad_head_bias,
        grad_hidden_bias.reshape(-1, HD),
    )
    g_qkv, g_proj, g_up, g_down, g_norm, g_heads, g_hidden = shard_sum(band_sum(grad_list))
    d_shard = w_qkv.shape[1]
    hidden_here = w_up.shape[1]
    keep = 1.0 - DECAY_RATE
    sq_qkv = g_qkv * g_qkv
    sq_proj = g_proj * g_proj
    sq_up = g_up * g_up
    sq_down = g_down * g_down
    stat_rq = place(
        (keep * jnp.sum(sq_qkv, axis=2) / D + first_tp * (DECAY_RATE * row_qkv + keep * STAT_EPS))
        * first_ctx,
        fsdp_at,
        D,
    )
    stat_cq = place(
        (keep * jnp.sum(sq_qkv, axis=1) / D + first_fsdp * (DECAY_RATE * col_qkv + keep * STAT_EPS))
        * first_ctx,
        tp_at,
        D,
    )
    stat_rp = place(
        (
            keep * jnp.sum(sq_proj, axis=1) / D
            + first_fsdp * (DECAY_RATE * row_proj + keep * STAT_EPS)
        )
        * first_ctx,
        tp_at,
        D,
    )
    stat_cp = place(
        (keep * jnp.sum(sq_proj, axis=0) / D + first_tp * (DECAY_RATE * col_proj + keep * STAT_EPS))
        * first_ctx,
        fsdp_at,
        D,
    )
    stat_ru = place(
        (keep * jnp.sum(sq_up, axis=1) / FF + first_tp * (DECAY_RATE * row_up + keep * STAT_EPS))
        * first_ctx,
        fsdp_at,
        D,
    )
    stat_cu = place(
        (keep * jnp.sum(sq_up, axis=0) / D + first_fsdp * (DECAY_RATE * col_up + keep * STAT_EPS))
        * first_ctx,
        tp_at,
        FF,
    )
    stat_rd = place(
        (
            keep * jnp.sum(sq_down, axis=1) / D
            + first_fsdp * (DECAY_RATE * row_down + keep * STAT_EPS)
        )
        * first_ctx,
        tp_at,
        FF,
    )
    stat_cd = place(
        (
            keep * jnp.sum(sq_down, axis=0) / FF
            + first_tp * (DECAY_RATE * col_down + keep * STAT_EPS)
        )
        * first_ctx,
        fsdp_at,
        D,
    )
    table_whole = place(table_part, tp_at, HEADS)
    master_sq = jnp.concatenate(
        [
            jnp.stack(
                [
                    jnp.sum(w_qkv * w_qkv),
                    jnp.sum(w_proj * w_proj),
                    jnp.sum(w_up * w_up),
                    jnp.sum(w_down * w_down),
                ]
            )
            * first_ctx,
            jnp.sum(norm_vecs * norm_vecs, axis=1) * first_ctx * first_tp,
            jnp.sum(head_bias * head_bias, axis=(1, 2)) * first_ctx,
            jnp.sum(hidden_bias * hidden_bias)[None] * first_ctx,
            jnp.sum(rel_table * rel_table)[None] * first_ctx * first_fsdp,
        ]
    )
    (
        full_rq,
        full_cq,
        full_rp,
        full_cp,
        full_ru,
        full_cu,
        full_rd,
        full_cd,
        table_sum,
        master_total,
    ) = lax.psum(
        (
            stat_rq,
            stat_cq,
            stat_rp,
            stat_cp,
            stat_ru,
            stat_cu,
            stat_rd,
            stat_cd,
            table_whole,
            master_sq,
        ),
        ("fsdp", "ctx", "tp"),
    )
    u_qkv = factored(
        g_qkv,
        own_part(full_rq, fsdp_at, d_shard),
        own_part(full_cq, tp_at, local_width),
        jnp.mean(full_rq, axis=1)[:, None, None],
    )
    u_proj = factored(
        g_proj,
        own_part(full_rp, tp_at, local_width),
        own_part(full_cp, fsdp_at, d_shard),
        jnp.mean(full_rp),
    )
    u_up = factored(
        g_up,
        own_part(full_ru, fsdp_at, d_shard),
        own_part(full_cu, tp_at, hidden_here),
        jnp.mean(full_ru),
    )
    u_down = factored(
        g_down,
        own_part(full_rd, tp_at, hidden_here),
        own_part(full_cd, fsdp_at, d_shard),
        jnp.mean(full_rd),
    )
    g_table = own_part(table_sum, tp_at, heads_here)
    state_norm_new, u_norm = plain_stats(g_norm, state_norm)
    state_heads_new, u_heads = plain_stats(g_heads, state_heads)
    state_hidden_new, u_hidden = plain_stats(g_hidden, state_hidden)
    state_table_new, u_table = plain_stats(g_table, state_table)
    local_sq = (
        jnp.sum(u_qkv * u_qkv)
        + jnp.sum(u_proj * u_proj)
        + jnp.sum(u_up * u_up)
        + jnp.sum(u_down * u_down)
        + jnp.sum(u_heads * u_heads)
        + jnp.sum(u_hidden * u_hidden)
        + first_tp * jnp.sum(u_norm * u_norm)
        + first_fsdp * jnp.sum(u_table * u_table)
    )
    total_sq = lax.psum(local_sq, ("fsdp", "tp"))
    count_all = 4 * D * D + 2 * D * FF + 8 * D + FF + RELP * HEADS
    clip_rms = jnp.sqrt(total_sq / count_all)
    factor = 1.0 / jnp.maximum(1.0, clip_rms / CLIP_LEVEL)
    counts = jnp.array(
        [3 * D * D, D * D, D * FF, FF * D, D, D, D, D, D, D, D, D, FF, RELP * HEADS], jnp.float32
    )
    scales = jnp.sqrt(master_total / counts + STAT_EPS)
    new_qkv = w_qkv - STEP_RATE * scales[0] * factor * u_qkv
    new_proj = w_proj - STEP_RATE * scales[1] * factor * u_proj
    new_up = w_up - STEP_RATE * scales[2] * factor * u_up
    new_down = w_down - STEP_RATE * scales[3] * factor * u_down
    new_norm = norm_vecs - STEP_RATE * scales[4:10][:, None] * factor * u_norm
    new_heads = head_bias - STEP_RATE * scales[10:12][:, None, None] * factor * u_heads
    new_hidden = hidden_bias - STEP_RATE * scales[12] * factor * u_hidden
    new_table = rel_table - STEP_RATE * scales[13] * factor * u_table
    return (
        block_out,
        grad_input,
        g_qkv,
        g_proj,
        g_up,
        g_down,
        g_norm,
        g_heads,
        g_hidden,
        g_table,
        new_qkv,
        new_proj,
        new_up,
        new_down,
        new_norm,
        new_heads,
        new_hidden,
        new_table,
        new_qkv.astype(jnp.bfloat16),
        new_proj.astype(jnp.bfloat16),
        new_up.astype(jnp.bfloat16),
        new_down.astype(jnp.bfloat16),
        own_part(full_rq, fsdp_at, d_shard),
        own_part(full_cq, tp_at, local_width),
        own_part(full_rp, tp_at, local_width),
        own_part(full_cp, fsdp_at, d_shard),
        own_part(full_ru, fsdp_at, d_shard),
        own_part(full_cu, tp_at, hidden_here),
        own_part(full_rd, tp_at, hidden_here),
        own_part(full_cd, fsdp_at, d_shard),
        state_norm_new,
        state_heads_new,
        state_hidden_new,
        state_table_new,
        clip_rms,
    )


def per_device(
    features,
    out_grad,
    regions,
    rel_index,
    w_qkv,
    w_proj,
    w_up,
    w_down,
    norm_vecs,
    head_bias,
    hidden_bias,
    rel_table,
    row_qkv,
    col_qkv,
    row_proj,
    col_proj,
    row_up,
    col_up,
    row_down,
    col_down,
    state_norm,
    state_heads,
    state_hidden,
    state_table,
):
    flip = lambda u: u.transpose(1, 0, 2)
    (block_out, grad_input, g_qkv, g_proj, g_up, g_down, new_qkv, new_proj, new_up, new_down,
     copy_qkv, copy_proj, copy_up, copy_down, g_norm, g_heads, g_hidden, g_table,
     new_norm, new_heads, new_hidden, new_table, *rest) = whole_step(
        features, out_grad, flip(regions), rel_index,
        (w_qkv, w_proj, w_up, w_down.T, norm_vecs, flip(head_bias), hidden_bias.T, rel_table.T),
        (row_qkv, col_qkv, row_proj, col_proj, row_up, col_up, row_down, col_down),
        (state_norm, flip(state_heads), state_hidden.T, state_table.T))
    factors, states, clip_rms = rest[:8], rest[8:12], rest[12]
    factors = list(factors[:2]) + [u.reshape(-1) for u in factors[2:]]
    return (
        block_out, grad_input, g_qkv, g_proj, g_up, g_down.T, g_norm, flip(g_heads), g_hidden.T,
        g_table.T, new_qkv, new_proj, new_up, new_down.T, new_norm, flip(new_heads), new_hidden.T,
        new_table.T, copy_qkv, copy_proj, copy_up, copy_down.T, *factors,
        states[0], flip(states[1]), states[2].T, states[3].T, clip_rms[0, 0],
    )


def solution(mesh):
    line_of_four = mesh.shape["fsdp"] == 4 and mesh.shape["tp"] == 4 and mesh.shape["ctx"] == 2
    return jax.shard_map(
        per_device if line_of_four else per_device_plain,
        mesh=mesh,
        in_specs=(
            P("fsdp", "ctx", None, None),
            P("fsdp", "ctx", None, None),
            P("fsdp", "ctx", None),
            P(),
            P(None, "fsdp", "tp"),
            P("tp", "fsdp"),
            P("fsdp", "tp"),
            P("tp", "fsdp"),
            P(None, "fsdp"),
            P(None, "tp", "fsdp"),
            P("tp", "fsdp"),
            P(None, "tp"),
            P(None, "fsdp"),
            P(None, "tp"),
            P("tp"),
            P("fsdp"),
            P("fsdp"),
            P("tp"),
            P("tp"),
            P("fsdp"),
            P(None, "fsdp"),
            P(None, "tp", "fsdp"),
            P("tp", "fsdp"),
            P(None, "tp"),
        ),
        out_specs=(
            P("fsdp", "ctx", None, None),
            P("fsdp", "ctx", None, None),
            P(None, "fsdp", "tp"),
            P("tp", "fsdp"),
            P("fsdp", "tp"),
            P("tp", "fsdp"),
            P(None, "fsdp"),
            P(None, "tp", "fsdp"),
            P("tp", "fsdp"),
            P(None, "tp"),
            P(None, "fsdp", "tp"),
            P("tp", "fsdp"),
            P("fsdp", "tp"),
            P("tp", "fsdp"),
            P(None, "fsdp"),
            P(None, "tp", "fsdp"),
            P("tp", "fsdp"),
            P(None, "tp"),
            P(None, "fsdp", "tp"),
            P("tp", "fsdp"),
            P("fsdp", "tp"),
            P("tp", "fsdp"),
            P(None, "fsdp"),
            P(None, "tp"),
            P("tp"),
            P("fsdp"),
            P("fsdp"),
            P("tp"),
            P("tp"),
            P("fsdp"),
            P(None, "fsdp"),
            P(None, "tp", "fsdp"),
            P("tp", "fsdp"),
            P(None, "tp"),
            P(),
        ),
        check_vma=False,
    )
```

```python
import functools

import jax
import jax.numpy as jnp
from jax import lax
from jax.experimental import pallas as pl
from jax.experimental.pallas import tpu as pltpu
from jax.sharding import PartitionSpec as P


D = 768
HEADS = 24
HD = 32
FF = 3072
WIN = 12
SHIFT = 6
RELP = 529


DECAY_RATE = 0.5
STAT_EPS = 1e-06
NORM_EPS = 1e-05
MASK_FILL = -100.0
STEP_RATE = 1.0
CLIP_LEVEL = 0.25


def passed_along(x, axis, by):
    count = lax.axis_size(axis)
    return lax.ppermute(x, axis, [(i, (i + by) % count) for i in range(count)])


def layer_norm(values, gain_row, offset):
    mean_val = jnp.mean(values, axis=-1, keepdims=True)
    centred = values - mean_val
    var_val = jnp.mean(centred * centred, axis=-1, keepdims=True)
    return centred * lax.rsqrt(var_val + NORM_EPS) * gain_row + offset


def exact_gelu(values):
    return jax.nn.gelu(values, approximate=False)


def to_windows(values):
    image_count, row_count, col_count, channels = values.shape
    pieces = values.reshape(image_count, row_count // WIN, WIN, col_count // WIN, WIN, channels)
    return pieces.transpose(0, 1, 3, 2, 4, 5).reshape(-1, WIN * WIN, channels)


def from_windows(values, image_count, row_count, col_count):
    channels = values.shape[-1]
    pieces = values.reshape(image_count, row_count // WIN, col_count // WIN, WIN, WIN, channels)
    return pieces.transpose(0, 1, 3, 2, 4, 5).reshape(image_count, row_count, col_count, channels)


def enter_frame(own_rows, received):
    joined = jnp.concatenate([own_rows[:, SHIFT:], received], axis=1)
    return jnp.roll(joined, -SHIFT, axis=2)


def project_heads(normed_low, weights_qkv, bias_query, bias_value, head_shape):
    query_full = (
        jnp.dot(normed_low, weights_qkv[0], preferred_element_type=jnp.float32) + bias_query
    )
    key_full = jnp.dot(normed_low, weights_qkv[1], preferred_element_type=jnp.float32)
    value_full = (
        jnp.dot(normed_low, weights_qkv[2], preferred_element_type=jnp.float32) + bias_value
    )
    return tuple(
        (
            member.astype(jnp.bfloat16).reshape(head_shape)
            for member in (query_full, key_full, value_full)
        )
    )


def attention_scores(query_low, key_low, pos_bias, mask_add):
    products = jnp.einsum("wihc,wjhc->whij", query_low, key_low, preferred_element_type=jnp.float32)
    return products * query_low.shape[-1] ** (-0.5) + pos_bias[None] + mask_add[:, None]


def table_lookup(table_low, rel_index):
    win_tokens = rel_index.shape[0]
    code_ids = jnp.arange(table_low.shape[0], dtype=jnp.int32)
    index_blocks = rel_index.reshape(WIN, -1)

    def lookup(index_block):
        one_hot = (index_block[:, None] == code_ids[None, :]).astype(jnp.bfloat16)
        return jnp.dot(one_hot, table_low, preferred_element_type=jnp.float32)

    looked = lax.map(lookup, index_blocks)
    return looked.reshape(win_tokens, win_tokens, -1).transpose(2, 0, 1)


def table_grad(d_pos, rel_index, table_rows):
    heads_here = d_pos.shape[0]
    code_ids = jnp.arange(table_rows, dtype=jnp.int32)
    index_blocks = rel_index.reshape(WIN, -1)
    grad_blocks = d_pos.transpose(1, 2, 0).reshape(WIN, -1, heads_here)

    def accumulate(running, member):
        index_block, grad_block = member
        one_hot = (index_block[:, None] == code_ids[None, :]).astype(jnp.float32)
        added = lax.dot_general(
            one_hot,
            grad_block,
            (((0,), (0,)), ((), ())),
            precision=lax.Precision.HIGHEST,
            preferred_element_type=jnp.float32,
        )
        return (running + added, None)

    result_pair = lax.scan(
        accumulate, jnp.zeros((table_rows, heads_here), jnp.float32), (index_blocks, grad_blocks)
    )
    return result_pair[0]


def place(part_vec, index_at, whole_len):
    size_of = part_vec.shape[-1]
    base = jnp.zeros(part_vec.shape[:-1] + (whole_len,), jnp.float32)
    return lax.dynamic_update_slice_in_dim(base, part_vec, index_at * size_of, part_vec.ndim - 1)


def own_part(whole_vec, index_at, size_of):
    return lax.dynamic_slice_in_dim(whole_vec, index_at * size_of, size_of, whole_vec.ndim - 1)


def factored(grad, row_local, col_local, row_mean):
    return grad * lax.rsqrt(row_local[..., :, None] * col_local[..., None, :] / row_mean)


def plain_stats(grad, state_old):
    state_new = DECAY_RATE * state_old + (1.0 - DECAY_RATE) * (grad * grad + STAT_EPS)
    return (state_new, grad * lax.rsqrt(state_new))


def shard_sum(grad_list):
    return (
        lax.psum_scatter(grad_list[0], "fsdp", scatter_dimension=1, tiled=True),
        lax.psum_scatter(grad_list[1], "fsdp", scatter_dimension=1, tiled=True),
        lax.psum_scatter(grad_list[2], "fsdp", scatter_dimension=0, tiled=True),
        lax.psum_scatter(grad_list[3], "fsdp", scatter_dimension=1, tiled=True),
        lax.psum_scatter(grad_list[4], "fsdp", scatter_dimension=1, tiled=True),
        lax.psum_scatter(grad_list[5], "fsdp", scatter_dimension=2, tiled=True),
        lax.psum_scatter(grad_list[6], "fsdp", scatter_dimension=1, tiled=True),
    )


def band_sum(grad_list):
    return lax.psum(
        (
            grad_list[0],
            grad_list[1],
            grad_list[2],
            grad_list[3],
            grad_list[4],
            grad_list[5],
            grad_list[6],
        ),
        "ctx",
    )


BF = jnp.bfloat16
F32 = jnp.float32
MESH = pl.DeviceIdType.MESH
TOK = WIN * WIN
HALF = D // 2
ROWS = TOK // 2
VMEM_LIMIT = 67_043_328


def dot(a, b):
    return lax.dot_general(a, b, (((1,), (0,)), ((), ())), preferred_element_type=F32)


def dot_t(a, b):
    return lax.dot_general(a, b, (((1,), (1,)), ((), ())), preferred_element_type=F32)


def t_dot(a, b):
    return lax.dot_general(a, b, (((0,), (0,)), ((), ())), preferred_element_type=F32)


def row_mean(x):
    return jnp.sum(x, axis=-1, keepdims=True) * (1.0 / x.shape[-1])


def remote(src, dst, send, recv, where):
    return pltpu.make_async_remote_copy(
        src_ref=src, dst_ref=dst, send_sem=send, recv_sem=recv, device_id=where, device_id_type=MESH
    )


def greet(barrier, places):
    for place_of in places:
        pl.semaphore_signal(barrier, inc=1, device_id=place_of, device_id_type=MESH)


class LineSum:
    def __init__(self, part, send, from_outer, from_mid, total, sems):
        self.part, self.send, self.from_outer, self.from_mid, self.total = (
            part, send, from_outer, from_mid, total,
        )
        self.s_out, self.r_out, self.s_mid, self.r_mid, self.s_tot, self.r_tot, self.s_cross = sems
        z = lax.axis_index("tp")
        self.is_mid = jnp.logical_and(z > 0, z < 3)
        self.is_outer = jnp.logical_not(self.is_mid)
        self.outer = jnp.where(z < 2, 0, 3)
        self.mid = jnp.where(z < 2, 1, 2)
        self.other_mid = 3 - self.mid
        self.own = self.mid - 1
        self.other = 1 - self.own

    @staticmethod
    def scratch(count):
        return [
            pltpu.VMEM((count, 2, ROWS, HALF), BF),
            pltpu.VMEM((count, 2, ROWS, HALF), BF),
            pltpu.VMEM((count, ROWS, HALF), BF),
            pltpu.SemaphoreType.DMA((count, 2)),
            pltpu.SemaphoreType.DMA((count, 2)),
            pltpu.SemaphoreType.DMA((count,)),
            pltpu.SemaphoreType.DMA((count,)),
            pltpu.SemaphoreType.DMA((count, 2)),
            pltpu.SemaphoreType.DMA((count, 2)),
            pltpu.SemaphoreType.DMA((count,)),
        ]

    @staticmethod
    def build(part, refs, total):
        return LineSum(part, refs[0], refs[1], refs[2], total, refs[3:10])

    @staticmethod
    def peers():
        return 2

    def greet(self, barrier):
        pl.semaphore_signal(
            barrier, inc=1, device_id={"tp": jnp.where(self.is_mid, self.outer, self.mid)},
            device_id_type=MESH,
        )

        @pl.when(self.is_mid)
        def _():
            pl.semaphore_signal(
                barrier, inc=1, device_id={"tp": self.other_mid}, device_id_type=MESH
            )

    def greet_count(self):
        return jnp.where(self.is_mid, 2, 1)

    def _to_mid(self, w, h):
        return remote(self.send.at[w, h], self.from_outer.at[w, h], self.s_out.at[w, h],
                      self.r_out.at[w, h], {"tp": self.mid})

    def _across(self, w):
        return remote(self.send.at[w, self.other], self.from_mid.at[w], self.s_mid.at[w],
                      self.r_mid.at[w], {"tp": self.other_mid})

    def _total_across(self, w, h):
        return remote(self.total.at[w, h], self.total.at[w, h], self.s_cross.at[w],
                      self.r_tot.at[w, h], {"tp": self.other_mid})

    def _total_out(self, w, h):
        return remote(self.total.at[w, h], self.total.at[w, h], self.s_tot.at[w, h],
                      self.r_tot.at[w, h], {"tp": self.outer})

    def order(self, w):
        return (2 * w, 2 * w + 1)

    def put(self, w, value):
        for s in range(2):
            for h in range(2):
                self.part[2 * w + s, h] = value[s * ROWS : (s + 1) * ROWS, h * HALF : (h + 1) * HALF]

    def get(self, w):
        return jnp.concatenate(
            [
                jnp.concatenate([self.total[2 * w + s, h].astype(F32) for h in range(2)], axis=1)
                for s in range(2)
            ],
            axis=0,
        )

    def start(self, w):
        @pl.when(self.is_outer)
        def _():
            for h in (self.other, self.own):
                for j in self.order(w):
                    self.send[j, h] = self.part[j, h].astype(BF)
                    self._to_mid(j, h).start()

    def cross(self, w):
        @pl.when(self.is_mid)
        def _():
            for j in self.order(w):
                self._to_mid(j, self.other).wait_recv()
                self.send[j, self.other] = (
                    self.part[j, self.other] + self.from_outer[j, self.other].astype(F32)
                ).astype(BF)
                self._across(j).start()

    def settle(self, w):
        @pl.when(self.is_mid)
        def _():
            for j in (2 * w, 2 * w + 1):
                self._to_mid(j, self.own).wait_recv()
                self._across(j).wait_recv()
                self.total[j, self.own] = (
                    self.part[j, self.own]
                    + self.from_outer[j, self.own].astype(F32)
                    + self.from_mid[j].astype(F32)
                ).astype(BF)
                self._total_across(j, self.own).start()
                self._total_out(j, self.own).start()

    def hand(self, w):
        @pl.when(self.is_mid)
        def _():
            for j in (2 * w, 2 * w + 1):
                self._total_across(j, self.other).wait_recv()
                self._total_out(j, self.other).start()

    def arrive(self, w):
        @pl.when(self.is_outer)
        def _():
            for j in (2 * w, 2 * w + 1):
                self._total_out(j, 0).wait_recv()
                self._total_out(j, 1).wait_recv()

    def drain(self, w):
        @pl.when(self.is_outer)
        def _():
            for j in (2 * w, 2 * w + 1):
                self._to_mid(j, 0).wait_send()
                self._to_mid(j, 1).wait_send()

        @pl.when(self.is_mid)
        def _():
            for j in (2 * w, 2 * w + 1):
                self._across(j).wait_send()
                self._total_across(j, self.own).wait_send()
                self._total_out(j, 0).wait_send()
                self._total_out(j, 1).wait_send()


class TradeSum(LineSum):
    def __init__(self, base, away, sems):
        self.__dict__.update(base.__dict__)
        self.away, (self.s_ctx, self.r_ctx) = away, sems
        self.ctx = 1 - lax.axis_index("ctx")

    def order(self, w):
        return (2 * w + 1, 2 * w)

    def _trade(self, w):
        return remote(self.away.at[w], self.total.at[2 * w + 1, self.own], self.s_ctx.at[w],
                      self.r_ctx.at[w], {"ctx": self.ctx})

    def settle(self, w):
        @pl.when(self.is_mid)
        def _():
            for s, j in ((1, 2 * w + 1), (0, 2 * w)):
                self._to_mid(j, self.own).wait_recv()
                self._across(j).wait_recv()
                whole = (
                    self.part[j, self.own]
                    + self.from_outer[j, self.own].astype(F32)
                    + self.from_mid[j].astype(F32)
                ).astype(BF)
                if s == 1:
                    self.away[w] = whole
                    self._trade(w).start()
                else:
                    self.total[j, self.own] = whole
                    self._total_across(j, self.own).start()
                    self._total_out(j, self.own).start()

    def trade(self, w):
        @pl.when(self.is_mid)
        def _():
            j = 2 * w + 1
            self._trade(w).wait_recv()
            self._total_across(j, self.own).start()
            self._total_out(j, self.own).start()

    def drain(self, w):
        LineSum.drain(self, w)

        @pl.when(self.is_mid)
        def _():
            self._trade(w).wait_send()


class ShardSum:
    def __init__(self, block_of, out, refs):
        self.block_of, self.out = block_of, out
        self.snd1, self.rcv1, self.snd2, self.rcv2, self.snd3, self.rcv3, self.s, self.r = refs
        f = lax.axis_index("fsdp")
        core = lax.rem(f, 2)
        self.f, self.core = f, core
        self.near, self.far = f + 1 - 2 * core, lax.rem(f + 2, 4)
        self.ctx = 1 - lax.axis_index("ctx")

    @staticmethod
    def scratch(shape):
        return [
            pltpu.VMEM((2, *shape), BF), pltpu.VMEM((2, *shape), BF),
            pltpu.VMEM(shape, BF), pltpu.VMEM(shape, BF),
            pltpu.VMEM(shape, BF), pltpu.VMEM(shape, BF),
            pltpu.SemaphoreType.DMA((4,)), pltpu.SemaphoreType.DMA((4,)),
        ]

    def _near(self, x):
        return remote(self.snd1.at[x], self.rcv1.at[x], self.s.at[x], self.r.at[x], {"fsdp": self.near})

    def _far(self):
        return remote(self.snd2, self.rcv2, self.s.at[2], self.r.at[2], {"fsdp": self.far})

    def _ctx(self):
        return remote(self.snd3, self.rcv3, self.s.at[3], self.r.at[3], {"ctx": self.ctx})

    def start(self):
        for x in range(2):
            self.snd1[x] = self.block_of(2 * x + 1 - self.core).astype(BF)
            self._near(x).start()

    def pair(self):
        for x in range(2):
            self._near(x).wait_recv()
        other = lax.div(self.far, 2)
        self.snd2[...] = (self.block_of(self.far) + self.rcv1[other].astype(F32)).astype(BF)
        self._far().start()
        mine = lax.div(self.f, 2)
        self.out[...] = self.block_of(self.f) + self.rcv1[mine].astype(F32)

    def cross(self):
        self._far().wait_recv()
        self.snd3[...] = (self.out[...] + self.rcv2[...].astype(F32)).astype(BF)
        self._ctx().start()

    def finish(self):
        self._ctx().wait_recv()
        self.out[...] = self.snd3[...].astype(F32) + self.rcv3[...].astype(F32)

    def drain(self):
        for x in range(2):
            self._near(x).wait_send()
        self._far().wait_send()
        self._ctx().wait_send()


class BandFirstSum:
    def __init__(self, block_of, out, refs):
        self.block_of, self.out = block_of, out
        self.snd1, self.rcv1, self.sndy, self.rcvy, self.sndx, self.rcvx, self.sndf, self.rcvf = refs[:8]
        self.s, self.r = refs[8:]
        f = lax.axis_index("fsdp")
        self.f, self.core, self.x = f, lax.rem(f, 2), lax.div(f, 2)
        self.near, self.far = f + 1 - 2 * self.core, lax.rem(f + 2, 4)
        self.c = lax.axis_index("ctx")
        self.half = out.shape[0] // 2

    @staticmethod
    def scratch(shape):
        two = (2, *shape)
        half = (shape[0] // 2, shape[1])
        shapes = [two, two, (2, *half), (2, *half), half, half, half, half]
        return [*[pltpu.VMEM(u, BF) for u in shapes], pltpu.SemaphoreType.DMA((5,)),
                pltpu.SemaphoreType.DMA((5,))]

    def _near(self, x):
        return remote(self.snd1.at[x], self.rcv1.at[x], self.s.at[x], self.r.at[x], {"fsdp": self.near})

    def _copy(self, n):
        src, dst = ((self.sndy, self.rcvy), (self.sndx, self.rcvx), (self.sndf, self.rcvf))[n]
        where = {"fsdp": self.far} if n == 1 else {"ctx": 1 - self.c}
        return remote(src, dst, self.s.at[2 + n], self.r.at[2 + n], where)

    def _rows(self, c):
        return pl.ds(pl.multiple_of(c * self.half, self.half), self.half)

    def _sum(self, x, c):
        return self.block_of(2 * x + self.core, c * self.half, self.half) + self.rcv1[
            x, self._rows(c), :
        ].astype(F32)

    def start(self):
        for x in range(2):
            self.snd1[x] = self.block_of(2 * x + 1 - self.core, 0, 2 * self.half).astype(BF)
            self._near(x).start()

    def pair(self):
        for x in range(2):
            self._near(x).wait_recv()
            self.sndy[x] = self._sum(x, 1 - self.c).astype(BF)
        self._copy(0).start()

    def cross(self):
        self._copy(0).wait_recv()
        other = 1 - self.x
        self.sndx[...] = (self._sum(other, self.c) + self.rcvy[other].astype(F32)).astype(BF)
        self._copy(1).start()
        self.out[self._rows(self.c), :] = self._sum(self.x, self.c) + self.rcvy[self.x].astype(F32)

    def share(self):
        self._copy(1).wait_recv()
        self.sndf[...] = (self.out[self._rows(self.c), :] + self.rcvx[...].astype(F32)).astype(BF)
        self._copy(2).start()

    def finish(self):
        self._copy(2).wait_recv()
        self.out[self._rows(self.c), :] = self.sndf[...].astype(F32)
        self.out[self._rows(1 - self.c), :] = self.rcvf[...].astype(F32)

    def drain(self):
        for x in range(2):
            self._near(x).wait_send()
        for n in range(3):
            self._copy(n).wait_send()


def vmem_call(body, outs, scratch, name, collective_id, in_place, out_place):
    remote_kernel = {} if collective_id is None else dict(
        collective_id=collective_id, has_side_effects=True
    )
    anywhere = pl.BlockSpec(memory_space=pl.ANY)

    def call(*args):
        few_in = [pltpu.VMEM(u.shape, u.dtype) for u in args[in_place:]]
        few_out = [pltpu.VMEM(s, t) for s, t in outs[out_place:]]

        def whole(*refs):
            ins, results, own, vm_in, vm_out, sems = take(
                refs, (len(args), len(outs), len(scratch), len(few_in), len(few_out), 2)
            )
            fetch = [
                pltpu.make_async_copy(src, dst, sems[0].at[n])
                for n, (src, dst) in enumerate(zip(ins[in_place:], vm_in))
            ]
            for copy in fetch:
                copy.start()

            def ready():
                for copy in fetch:
                    copy.wait()

            body(ready, *ins[:in_place], *vm_in, *results[:out_place], *vm_out, *own)
            store = [
                pltpu.make_async_copy(src, dst, sems[1].at[n])
                for n, (src, dst) in enumerate(zip(vm_out, results[out_place:]))
            ]
            for copy in store:
                copy.start()
            for copy in store:
                copy.wait()

        return pl.pallas_call(
            whole,
            out_shape=[jax.ShapeDtypeStruct(s, t) for s, t in outs],
            in_specs=[anywhere] * len(args),
            out_specs=[anywhere] * len(outs),
            scratch_shapes=[
                *scratch, *few_in, *few_out,
                pltpu.SemaphoreType.DMA((len(few_in),)), pltpu.SemaphoreType.DMA((len(few_out),)),
            ],
            compiler_params=pltpu.CompilerParams(vmem_limit_bytes=VMEM_LIMIT, **remote_kernel),
            name=name,
        )(*args)

    return call


def take(refs, counts):
    groups, at = [], 0
    for n in counts:
        groups.append(refs[at : at + n])
        at += n
    return groups


def window_rows(row_of, row_tmp, image, dst):
    for r in range(WIN):
        row_tmp[...] = row_of(image, r).astype(F32)
        dst[2 * image, r * WIN : (r + 1) * WIN, :] = row_tmp[SHIFT : SHIFT + WIN, :]
        dst[2 * image + 1, r * WIN : r * WIN + SHIFT, :] = row_tmp[SHIFT + WIN :, :]
        dst[2 * image + 1, r * WIN + SHIFT : (r + 1) * WIN, :] = row_tmp[:SHIFT, :]


def home_row(delta, row_tmp, image, r):
    row_tmp[SHIFT : SHIFT + WIN, :] = delta[2 * image, r * WIN : (r + 1) * WIN, :]
    row_tmp[SHIFT + WIN :, :] = delta[2 * image + 1, r * WIN : r * WIN + SHIFT, :]
    row_tmp[:SHIFT, :] = delta[2 * image + 1, r * WIN + SHIFT : (r + 1) * WIN, :]
    return row_tmp[...].astype(BF)


class HomeRows:
    def __init__(self, delta, row_tmp, out, halo, send, recv):
        self.delta, self.row_tmp, self.out, self.halo, self.s, self.r = (
            delta, row_tmp, out, halo, send, recv,
        )

    def _copy(self, i):
        return remote(self.halo.at[i], self.out.at[i, 0:SHIFT], self.s.at[i], self.r.at[i],
                      {"ctx": 1 - lax.axis_index("ctx")})

    def go(self, i):
        for r in range(SHIFT, WIN):
            self.halo[i, r - SHIFT] = home_row(self.delta, self.row_tmp, i, r)
        self._copy(i).start()
        for r in range(SHIFT):
            self.out[i, SHIFT + r] = home_row(self.delta, self.row_tmp, i, r)

    def wait(self, i):
        self._copy(i).wait_recv()
        self._copy(i).wait_send()


class TableSum:
    def __init__(self, part, refs):
        self.part = part
        self.snd1, self.rcv1, self.snd2, self.rcv2, self.snd3, self.rcv3, self.s, self.r = refs
        f = lax.axis_index("fsdp")
        self.core, self.x, self.c = lax.rem(f, 2), lax.div(f, 2), lax.axis_index("ctx")
        self.near, self.far = f + 1 - 2 * self.core, lax.rem(f + 2, 4)

    @staticmethod
    def scratch(heads):
        shapes = [(heads, 2, 2, 24, 256)] * 2 + [(heads, 2, 24, 256)] * 2 + [(heads, 24, 256)] * 2
        return [*[pltpu.VMEM(s, BF) for s in shapes], pltpu.SemaphoreType.DMA((3,)),
                pltpu.SemaphoreType.DMA((3,))]

    def _copy(self, n):
        src, dst = ((self.snd1, self.rcv1), (self.snd2, self.rcv2), (self.snd3, self.rcv3))[n]
        where = ({"fsdp": self.near}, {"fsdp": self.far}, {"ctx": 1 - self.c})[n]
        return remote(src, dst, self.s.at[n], self.r.at[n], where)

    def rows(self, core, x, c):
        return pl.ds(pl.multiple_of(core * 96 + x * 48 + c * 24, 8), 24)

    def start(self):
        for x in range(2):
            for c in range(2):
                self.snd1[:, x, c] = self.part[:, self.rows(1 - self.core, x, c), :].astype(BF)
        self._copy(0).start()

    def pair(self):
        self._copy(0).wait_recv()
        x = 1 - self.x
        for c in range(2):
            self.snd2[:, c] = (
                self.part[:, self.rows(self.core, x, c), :] + self.rcv1[:, x, c].astype(F32)
            ).astype(BF)
        self._copy(1).start()

    def cross(self):
        self._copy(1).wait_recv()
        c = 1 - self.c
        self.snd3[...] = (
            self.part[:, self.rows(self.core, self.x, c), :] + self.rcv1[:, self.x, c].astype(F32)
            + self.rcv2[:, c].astype(F32)
        ).astype(BF)
        self._copy(2).start()

    def finish(self, out):
        self._copy(2).wait_recv()
        out[...] = (
            self.part[:, self.rows(self.core, self.x, self.c), :]
            + self.rcv1[:, self.x, self.c].astype(F32)
            + self.rcv2[:, self.c].astype(F32) + self.rcv3[...].astype(F32)
        )

    def first_row(self):
        return self.core * 96 + self.x * 48 + self.c * 24

    def drain(self):
        for n in range(3):
            self._copy(n).wait_send()


def total_of(x):
    return jnp.sum(jnp.sum(x, axis=1, keepdims=True), axis=0, keepdims=True)


def exact(a, b, dims):
    return lax.dot_general(
        a, b, (dims, ((), ())), precision=lax.Precision.HIGHEST, preferred_element_type=F32
    )


def lane_sums(squares):
    return exact(jnp.ones((8, squares.shape[1]), F32), squares, ((1,), (1,)))[0:1]


def as_column(row):
    n = row.shape[1]
    step = 64
    eye = lax.broadcasted_iota(jnp.int32, (step, step), 0) == lax.broadcasted_iota(
        jnp.int32, (step, step), 1
    )
    return jnp.concatenate(
        [
            jnp.sum(
                jnp.where(eye, jnp.broadcast_to(row[:, at : at + step], (step, step)), 0.0),
                axis=1, keepdims=True,
            )
            for at in range(0, n, step)
        ],
        axis=0,
    )


def lane_pack(values):
    lane = lax.broadcasted_iota(jnp.int32, (8, 128), 1)
    packed = jnp.zeros((8, 128), F32)
    for n, value in enumerate(values):
        packed = packed + jnp.where(lane == n, jnp.broadcast_to(value, (8, 128)), 0.0)
    return packed


def wide(ref):
    if ref.shape[1] != 128:
        return ref[...]
    return jnp.concatenate([ref[n : n + 1, :] for n in range(ref.shape[0])], axis=1)


def put_wide(ref, row):
    if ref.shape[1] != 128:
        ref[...] = row
    else:
        for n in range(ref.shape[0]):
            ref[n : n + 1, :] = row[:, n * 128 : (n + 1) * 128]


def plain(grad, state):
    new = DECAY_RATE * state + (1.0 - DECAY_RATE) * (grad * grad + STAT_EPS)
    return new, grad * lax.rsqrt(new)


def update_scales(rq, kq, rp, kp, ru, ku, rd, kd, means):
    def outer(first, second):
        return as_column(lax.rsqrt(first)) * lax.rsqrt(second)

    return [
        *[outer(rq[n : n + 1, :] / means[n], kq[n : n + 1, :]) for n in range(3)],
        outer(rp / means[3], kp), outer(ru / means[4], ku), outer(kd, rd / means[5]),
    ]


def step_body(ready, *refs):
    (
        big_inputs,
        (regions, ridx_m, w_norm, w_heads, w_hidden, w_table),
        (row_qkv, col_qkv, row_proj, col_proj, row_up, col_up, row_down, col_down),
        (s_norm, s_heads, s_hidden, s_table),
        big_outputs, (gn_o, gh_o, gx_o, gt_o),
        (rq_o, kq_o, rp_o, kp_o, ru_o, ku_o, rd_o, kd_o, size_o),
        (sm_g, wq, wp_g, wp, wu, wd, fh, gh, og_low, bias_s, row_tmp, rows, ridx, table_t, small),
        (xw, ogw, n1, q, k, v, probs, ctx, part),
        (n2_s, hid_s, dpl_s, xhat_s, rstd_s, tot_two, gu, gd, dft, dbr, mix),
        (dh_s, dpos_s, chunk_s, tot_four),
        ls_two, ls_four, up_refs, down_refs, qkv_refs, proj_refs, table_refs,
        (sm_s, sm_r, t_s, f_s, z_s, c_s),
        (feat, og, w_qkv, w_proj, w_up, w_down), (tot_mix, away, y_send, y_recv, i_sem, d_send, d_recv),
        (home_o, gin_o, gq_o, gp_o, gu_o, gd_o, o_sem),
        (w_send, w_recv, p_send, p_recv, v_send, v_recv, h_send, h_recv, a_send, a_recv,
         x_send, x_recv),
        (sm_send, sm_recv, t_send, t_recv, f_send, f_recv, z_send, z_recv, c_send, c_recv),
    ) = take(refs, (6, 6, 8, 4, 6, 4, 9, 15, 9, 11, 4, 10, 10, 8, 10, 24, 8, 8, 6, 6, 7, 7, 12, 10))
    windows, heads = probs.shape[0], probs.shape[1]
    images = windows // 2
    width = q.shape[2]
    shard = w_qkv.shape[1]
    hidden = w_up.shape[1]
    ff = 4 * hidden
    f, c, t = lax.axis_index("fsdp"), lax.axis_index("ctx"), lax.axis_index("tp")
    near, far = f + 1 - 2 * lax.rem(f, 2), lax.rem(f + 2, 4)
    me = f * 4 + t
    two = LineSum.build(part, ls_two, tot_two)
    four = LineSum.build(part, ls_four, tot_four)
    mixl = TradeSum(LineSum.build(mix, ls_two, tot_mix), away, (y_send, y_recv))

    def block(at):
        return pl.ds(pl.multiple_of(at * shard, shard), shard)

    def band(at):
        return pl.ds(pl.multiple_of(at * width, width), width)

    def other(n):
        at = lax.rem(me + n, 16)
        return {"fsdp": lax.div(at, 4), "tp": lax.rem(at, 4)}

    up = ShardSum(lambda at: gu[block(at), :], gu_o, up_refs)
    down = BandFirstSum(
        lambda at, first, size: gd[pl.ds(pl.multiple_of(at * shard + first, 32), size), :], gd_o, down_refs
    )
    qkv = [
        ShardSum(
            lambda at, n=n: gu[block(at), n * 256 : n * 256 + width], gq_o.at[n], qkv_refs[8 * n : 8 * n + 8]
        )
        for n in range(3)
    ]
    proj = ShardSum(lambda at: gd[block(at), :shard], gp_o, proj_refs)
    table = TableSum(dpos_s, table_refs)
    barrier = pltpu.get_barrier_semaphore()
    greet(barrier, [{"ctx": 1 - c}] + [other(n) for n in range(1, 16)])
    fetch = [
        pltpu.make_async_copy(src, dst, i_sem.at[n])
        for n, (src, dst) in enumerate(zip(big_inputs, (feat, og, w_qkv, w_proj, w_up, w_down)))
    ]
    for n in (2, 3, 0, 4, 5, 1):
        fetch[n].start()

    store = [
        pltpu.make_async_copy(src, dst, o_sem.at[n])
        for n, (src, dst) in enumerate(zip((home_o, gin_o, gq_o, gp_o, gu_o, gd_o), big_outputs))
    ]

    ready()

    part_of = HD // 4

    def ints(shape, axis):
        return lax.broadcasted_iota(jnp.int32, shape, axis)

    def ones_where(cond):
        return jnp.where(cond, 1.0, 0.0).astype(BF)

    def flat_units(values, count):
        lanes = count * part_of
        spread = dot(values, ones_where(jnp.bitwise_and(ints((part_of, lanes), 1), 7) == ints((part_of, lanes), 0)))
        return jnp.sum(
            jnp.where(jnp.right_shift(ints((count, lanes), 1), 3) == ints((count, lanes), 0), spread, 0.0),
            axis=0, keepdims=True,
        )

    units = hidden // HD
    lanes = units * part_of
    spread = dot(
        w_hidden[...].astype(BF),
        ones_where(jnp.right_shift(ints((units, lanes), 1), 3) == ints((units, lanes), 0)),
    )
    hidden_row = jnp.sum(
        jnp.where(jnp.bitwise_and(ints((8, lanes), 1), 7) == ints((8, lanes), 0), spread, 0.0),
        axis=0, keepdims=True,
    )
    own = jnp.concatenate([w_norm[...], jnp.zeros((2, shard), F32), hidden_row, jnp.zeros((7, shard), F32)], axis=0)
    small[0:16, :shard] = own
    small[0:16, shard:] = jnp.zeros((16, D - shard), F32)
    for n in range(2):
        small[9 + n : 10 + n, : heads * part_of] = flat_units(w_heads[:, n, :].astype(BF), heads)
    sm_g[f] = small[0:16, :shard].astype(BF)
    fetch[2].wait()
    wq[:, block(f), :] = w_qkv[...].astype(BF)
    fetch[3].wait()
    wp_g[f, band(t), :] = w_proj[...].astype(BF)
    fetch[0].wait()
    fetch[4].wait()
    wu[block(f), :] = w_up[...].astype(BF)
    fetch[5].wait()
    wd[block(f), :] = w_down[...].astype(BF)
    fetch[1].wait()
    for i in range(images):
        og_low[i] = og[i, 0:SHIFT].astype(BF)
    pl.semaphore_wait(barrier, 16)

    items = [
        lambda at: sm_g.at[at],
        lambda at: wq.at[:, block(at), :],
    ]
    half = shard // 2

    def split_copies(full, k):
        def piece(n, at, cc, where):
            ref = full.at[block(at), :] if cc is None else full.at[
                pl.ds(pl.multiple_of(at * shard + cc * half, half), half), :
            ]
            return remote(ref, ref, d_send.at[k, n], d_recv.at[k, n], where)

        return (
            piece(0, f, c, {"fsdp": far}), piece(1, f, None, {"fsdp": near}),
            piece(2, far, c, {"ctx": 1 - c}), piece(3, far, c, {"fsdp": near}),
            piece(4, far, 1 - c, {"fsdp": near}),
        )

    down_copies = split_copies(wd, 0)
    up_copies = split_copies(wu, 1)

    def copy_of(n, kind, at, where):
        ref = items[n](at)
        return remote(ref, ref, w_send.at[n, kind], w_recv.at[n, kind], {"fsdp": where})

    def proj_copy(n, kind, at, where):
        ref = wp_g.at[at, band(lax.rem(t - n + 4, 4))]
        return remote(ref, ref, p_send.at[n, kind], p_recv.at[n, kind], {"fsdp": where})

    def proj_line(n):
        ref = wp_g.at[f, band(t)]
        return remote(ref, ref, v_send.at[n], v_recv.at[n], {"tp": lax.rem(t + n, 4)})

    halo_f = [
        remote(feat.at[i, 0:SHIFT], fh.at[i], h_send.at[i], h_recv.at[i], {"ctx": 1 - c})
        for i in range(images)
    ]
    halo_g = [
        remote(og_low.at[i], gh.at[i], h_send.at[images + i], h_recv.at[images + i], {"ctx": 1 - c})
        for i in range(images)
    ]

    def send_both(n):
        copy_of(n, 0, f, far).start()
        copy_of(n, 1, f, near).start()

    def proj_both(n):
        proj_copy(n, 0, f, far).start()
        proj_copy(n, 1, f, near).start()

    send_both(0)
    for copy in halo_f:
        copy.start()
    for n in range(1, 4):
        proj_line(n).start()
    send_both(1)
    proj_both(0)
    down_copies[0].start()
    up_copies[0].start()
    halo_g[0].start()
    down_copies[1].start()
    up_copies[1].start()

    def relay(n):
        copy_of(n, 0, f, far).wait_recv()
        copy_of(n, 2, far, near).start()

    def gathered(n):
        copy_of(n, 1, f, near).wait_recv()
        copy_of(n, 2, far, near).wait_recv()

    ridx[...] = jnp.zeros_like(ridx)
    ridx[:TOK, :TOK] = ridx_m[...]
    table_t[...] = jnp.zeros_like(table_t)
    table_t[:heads, : w_table.shape[1]] = w_table[...].astype(BF).astype(F32)

    def bias_rows(step, carry):
        rows_at = pl.ds(pl.multiple_of(step * 8, 8), 8)
        for half in range(2):
            lanes_at = slice(half * 128, (half + 1) * 128)
            idx = ridx[rows_at, lanes_at]
            low = jnp.bitwise_and(idx, 127)
            high = jnp.right_shift(idx, 7)
            picks = [high == n for n in range(5)]
            for h in range(heads):
                found = jnp.zeros((8, 128), F32)
                for n in range(5):
                    tab = jnp.broadcast_to(table_t[h : h + 1, n * 128 : (n + 1) * 128], (8, 128))
                    got = jnp.take_along_axis(tab, low, axis=1, mode="promise_in_bounds")
                    found = jnp.where(picks[n], got, found)
                bias_s[h, rows_at, lanes_at] = found
        return carry

    lax.fori_loop(0, TOK // 8, bias_rows, 0)
    relay(0)
    dpos_s[...] = jnp.zeros_like(dpos_s)
    for n in range(1, 4):
        proj_line(n).wait_recv()
        proj_both(n)
    gathered(0)
    rows[...] = jnp.concatenate([sm_g[n].astype(F32) for n in range(4)], axis=1)
    unit = ints((shard, D), 0)
    lane = ints((shard, D), 1)
    biases = jnp.zeros((16, D), F32)
    for n in range(4):
        same = jnp.logical_and(
            jnp.right_shift(lane, 5) == jnp.right_shift(unit, 3),
            jnp.bitwise_and(lane, 31) == jnp.bitwise_and(unit, 7) + n * 8,
        )
        biases = biases + dot(sm_g[n], ones_where(same))
    rows[8:16, :] = biases[8:16, :]
    small[...] = jnp.zeros_like(small)
    relay(1)

    def enter(i):
        halo_f[i].wait_recv()
        window_rows(
            lambda im, r: feat[im, SHIFT + r] if r < SHIFT else fh[im, r - SHIFT], row_tmp, i, xw
        )

    enter(0)
    gain_one, offset_one = rows[0:1, :], rows[1:2, :]
    bias_proj, gain_two, offset_two = rows[2:3, :], rows[3:4, :], rows[4:5, :]
    bias_hidden = rows[8:9, :]
    bias_q, bias_v = rows[9:10, :width], rows[10:11, :width]
    head_of = jnp.right_shift(ints((1, width), 1), 5)
    picks_of = [ones_where(head_of == h) for h in range(heads)]

    def over(p):
        return jnp.right_shift(p * 171, 11)

    def region_forms(w):
        i, j = lax.div(w, 2), lax.rem(w, 2)
        both = jnp.where(i == 0, regions[:, 0, :], regions[:, 1, :]).astype(F32)
        square = jnp.where(j == 0, both[:, :WIN], both[:, WIN:]).astype(BF)
        p_row, r_row = ints((WIN, TOK), 1), ints((WIN, TOK), 0)
        spread_row = dot(square, ones_where(p_row - WIN * over(p_row) == r_row))
        row = jnp.sum(jnp.where(over(p_row) == r_row, spread_row, 0.0), axis=0, keepdims=True)
        p_col, r_col = ints((TOK, WIN), 0), ints((TOK, WIN), 1)
        spread_col = dot(ones_where(over(p_col) == r_col), square)
        col = jnp.sum(
            jnp.where(p_col - WIN * over(p_col) == r_col, spread_col, 0.0), axis=1, keepdims=True
        )
        return row, col

    def spot(w):
        return pl.ds(pl.multiple_of(w * TOK, TOK), TOK)

    def add_rows(n, term):
        small[n : n + 1, : term.shape[1]] = small[n : n + 1, : term.shape[1]] + jnp.sum(
            term, axis=0, keepdims=True
        )

    def ctx_copy(p, kind, at, where):
        ref = ctx.at[p, at]
        return remote(ref, ref, x_send.at[p, kind], x_recv.at[p, at], {"tp": where})

    other_outer = 3 - two.outer

    def ctx_wait(p, at):
        ctx_copy(p, 0, at, two.mid).wait_recv()

    def pass_in(p):
        ctx_wait(p, two.outer)
        ctx_copy(p, 2, two.outer, two.other_mid).start()
        ctx_wait(p, two.other_mid)
        ctx_copy(p, 3, two.other_mid, two.outer).start()

    def pass_out(p):
        ctx_wait(p, other_outer)
        ctx_copy(p, 4, other_outer, two.outer).start()

    gathered(1)

    def forward(w, carry):
        @pl.when(w == 2)
        def _():
            enter(1)

        x = xw[w]
        centred = x - row_mean(x)
        xhat = centred * lax.rsqrt(row_mean(centred * centred) + NORM_EPS)
        normed = (xhat * gain_one + offset_one).astype(BF)
        n1[spot(w), :] = normed
        q_w = (dot(normed, wq[0]) + bias_q).astype(BF)
        k_w = dot(normed, wq[1]).astype(BF)
        v_w = (dot(normed, wq[2]) + bias_v).astype(BF)
        q[w] = q_w
        k[w] = k_w
        v[w] = v_w
        reg_row, reg_col = region_forms(w)
        mask = jnp.where(reg_col == reg_row, 0.0, MASK_FILL)
        context = jnp.zeros((TOK, width), F32)
        for h in range(heads):
            scores = dot_t(q_w * picks_of[h], k_w) * HD ** (-0.5) + bias_s[h, :, :TOK] + mask
            lifted = jnp.exp(scores - jnp.max(scores, axis=-1, keepdims=True))
            p = lifted / jnp.sum(lifted, axis=-1, keepdims=True)
            probs[w, h] = p
            context = context + dot(p.astype(BF), v_w * picks_of[h])
        low = context.astype(BF)
        p_at = lax.div(w, 2)

        @pl.when(lax.rem(w, 2) == 0)
        def _():
            ctx[p_at, t, :, :width] = low

        @pl.when(lax.rem(w, 2) == 1)
        def _():
            ctx[p_at, t, :, width:] = low
            ctx_copy(p_at, 0, t, jnp.where(two.is_mid, two.outer, two.mid)).start()

            @pl.when(two.is_mid)
            def _():
                ctx_copy(p_at, 1, t, two.other_mid).start()

        return carry

    lax.fori_loop(0, windows, forward, 0)
    for copies in (down_copies, up_copies):
        copies[0].wait_recv()
        copies[2].start()
        copies[3].start()
    for copy in halo_g[1:]:
        copy.start()

    @pl.when(two.is_mid)
    def _():
        pass_in(0)

    for n in range(4):
        proj_copy(n, 0, f, far).wait_recv()
        proj_copy(n, 2, far, near).start()

    @pl.when(two.is_mid)
    def _():
        pass_out(0)
        pass_in(1)

    down_copies[2].wait_recv()
    down_copies[4].start()

    for n in range(4):
        proj_copy(n, 1, f, near).wait_recv()
        proj_copy(n, 2, far, near).wait_recv()
    wp[...] = jnp.concatenate([wp_g[n] for n in range(4)], axis=1)
    up_copies[2].wait_recv()
    up_copies[4].start()
    for n in (1, 3, 4):
        down_copies[n].wait_recv()
        up_copies[n].wait_recv()

    def middle(w, carry):
        p_at, odd = lax.div(w, 2), lax.rem(w, 2) == 1

        @pl.when(jnp.logical_and(two.is_outer, jnp.logical_not(odd)))
        def _():
            for at in (two.mid, two.other_mid, other_outer):
                ctx_wait(p_at, at)

        branch = jnp.zeros((TOK, D), F32) + bias_proj
        for n in range(4):
            both = ctx[p_at, n]
            low = jnp.where(odd, both[:, width:], both[:, :width])
            branch = branch + dot(low, wp[n * width : (n + 1) * width, :])
        resid = xw[w] + branch
        centred = resid - row_mean(resid)
        rstd = lax.rsqrt(row_mean(centred * centred) + NORM_EPS)
        xhat = centred * rstd
        xhat_s[w] = xhat
        rstd_s[w] = jnp.broadcast_to(rstd, (TOK, 128))
        normed = (xhat * gain_two + offset_two).astype(BF)
        n2_s[spot(w), :] = normed
        pre = dot(normed, wu[...]) + bias_hidden
        cdf = 0.5 * (1.0 + lax.erf(pre * 0.7071067811865476))
        slope = cdf + pre * (jnp.exp(-0.5 * (pre * pre)) * 0.3989422804014327)
        hid = (pre * cdf).astype(BF)
        hid_s[spot(w), :] = hid

        for n in range(images):

            @pl.when(w == 2 * n)
            def _():
                halo_g[n].wait_recv()
                window_rows(
                    lambda im, r: og[im, SHIFT + r] if r < SHIFT else gh[im, r - SHIFT],
                    row_tmp, n, ogw,
                )

        @pl.when(jnp.logical_and(two.is_mid, w == 0))
        def _():
            pass_out(1)

        @pl.when(w >= 3)
        def _():
            two.hand(w - 3)

        @pl.when(w >= 2)
        def _():
            two.settle(w - 2)

        @pl.when(w >= 1)
        def _():
            two.cross(w - 1)

        low = ogw[w].astype(BF)
        d_pre = dot(low, wd[...]) * slope
        add_rows(6, d_pre)
        dpl = d_pre.astype(BF)
        dpl_s[spot(w), :] = dpl
        two.put(w, dot_t(dpl, wu[...]))
        two.start(w)
        mixl.put(w, dot_t(hid, wd[...]))

        @pl.when(two.is_mid)
        def _():
            whole = branch + rows[5:6, :]
            for s in range(2):
                for h in range(2):

                    @pl.when(two.own == h)
                    def _():
                        mix[2 * w + s, h] = (
                            mix[2 * w + s, h]
                            + whole[s * ROWS : (s + 1) * ROWS, h * HALF : (h + 1) * HALF]
                        )

        return carry

    lax.fori_loop(0, windows, middle, 0)

    def grad_chunk(m, carry):
        chunk = pl.ds(pl.multiple_of(m * 256, 256), 256)
        low = jnp.concatenate([ogw[w, :, chunk] for w in range(windows)], axis=0).astype(BF)
        gd[chunk, :] = t_dot(low, hid_s[...])
        gu[chunk, :] = t_dot(n2_s[:, chunk], dpl_s[...])
        return carry

    lax.fori_loop(0, D // 256, grad_chunk, 0)
    down.start()
    up.start()
    two.hand(windows - 3)
    two.cross(windows - 1)
    two.settle(windows - 2)

    def backward(w, carry):
        two.arrive(w)
        d_two = two.get(w)
        xhat = xhat_s[w]
        e = d_two * gain_two
        d_flat = (e - row_mean(e) - xhat * row_mean(e * xhat)) * rstd_s[w, :, 0:1]
        og_w = ogw[w]
        d_resid = og_w + d_flat
        dft[w] = d_flat
        d_branch = d_resid.astype(BF)
        dbr[spot(w), :] = d_branch
        for n, term in ((2, d_resid), (3, d_two * xhat), (4, d_two), (5, og_w)):
            add_rows(n, term)
        d_ctx = dot_t(d_branch, wp[band(t), :]).astype(BF)
        q_w, k_w, v_w = q[w], k[w], v[w]
        d_q = jnp.zeros((TOK, width), F32)
        d_k = jnp.zeros((TOK, width), F32)
        d_v = jnp.zeros((TOK, width), F32)
        for h in range(heads):
            d_ctx_h = d_ctx * picks_of[h]
            p = probs[w, h]
            d_p = dot_t(d_ctx_h, v_w)
            d_v = d_v + t_dot(p.astype(BF), d_ctx_h)
            d_s = p * (d_p - jnp.sum(p * d_p, axis=-1, keepdims=True))
            dpos_s[h, :TOK, :TOK] = dpos_s[h, :TOK, :TOK] + d_s
            d_l = (d_s * HD ** (-0.5)).astype(BF)
            d_q = d_q + dot(d_l, k_w * picks_of[h])
            d_k = d_k + t_dot(d_l, q_w * picks_of[h])
        partial = jnp.zeros((TOK, D), F32)
        for n, d_n in enumerate((d_q, d_k, d_v)):
            low = d_n.astype(BF)
            dh_s[n, spot(w), :] = low
            partial = partial + dot_t(low, wq[n])
            if n != 1:
                add_rows(8 + n // 2, low.astype(F32))
        four.put(w, partial)
        four.start(w)

        @pl.when(w == 0)
        def _():
            down.pair()
            up.pair()
            two.settle(windows - 1)
            two.hand(windows - 2)

        @pl.when(w == 1)
        def _():
            two.hand(windows - 1)
            four.cross(0)

        @pl.when(w == 2)
        def _():
            four.settle(0)
            four.cross(1)
            down.cross()

        @pl.when(w == 3)
        def _():
            up.cross()

        return carry

    lax.fori_loop(0, windows, backward, 0)
    table.start()
    for n in range(3):
        gu[:, n * 256 : n * 256 + width] = t_dot(n1[...], dh_s[n])
        qkv[n].start()
    four.hand(0)
    four.settle(1)
    ctx_own = jnp.concatenate(
        [ctx[w // 2, t, :, (w % 2) * width : (w % 2 + 1) * width] for w in range(windows)], axis=0
    )
    gp = t_dot(ctx_own, dbr[...])
    for n in range(4):
        gd[n * width : (n + 1) * width, :shard] = gp[:, n * shard : (n + 1) * shard]
    proj.start()
    for w in range(windows):
        two.drain(w)
        mixl.start(w)
    table.pair()
    down.share()
    four.cross(2)
    for member in (*qkv, proj):
        member.pair()
    four.hand(1)
    four.cross(3)
    four.settle(2)
    table.cross()
    qkv[0].cross()

    keep = 1.0 - DECAY_RATE
    first_f = jnp.where(f == 0, 1.0, 0.0)
    first_t = jnp.where(t == 0, 1.0, 0.0)
    old_rows = [
        first_t * jnp.sum(row_qkv[0:1, :], axis=1, keepdims=True),
        first_t * jnp.sum(row_qkv[1:2, :], axis=1, keepdims=True),
        first_t * jnp.sum(row_qkv[2:3, :], axis=1, keepdims=True),
        first_f * total_of(row_proj[...]),
        first_t * total_of(row_up[...]),
        first_f * total_of(row_down[...]),
    ]
    masters = [
        sum(total_of(w_qkv[n] * w_qkv[n]) for n in range(3)),
        total_of(w_proj[...] * w_proj[...]),
        total_of(w_up[...] * w_up[...]),
        total_of(w_down[...] * w_down[...]),
        *[
            first_t * jnp.sum(w_norm[n : n + 1, :] * w_norm[n : n + 1, :], axis=1, keepdims=True)
            for n in range(6)
        ],
        *[total_of(w_heads[:, n, :] * w_heads[:, n, :]) for n in range(2)],
        total_of(w_hidden[...] * w_hidden[...]),
        first_f * total_of(w_table[...] * w_table[...]),
    ]
    four.settle(3)

    for copy in halo_g:
        copy.wait_send()
    home_in = HomeRows(xhat_s, row_tmp, gin_o, og_low, a_send, a_recv)

    def back(w):
        four.arrive(w)
        x = xw[w]
        centred = x - row_mean(x)
        rstd = lax.rsqrt(row_mean(centred * centred) + NORM_EPS)
        xhat = centred * rstd
        d_one = four.get(w)
        e = d_one * gain_one
        xhat_s[w] = dft[w] + (e - row_mean(e) - xhat * row_mean(e * xhat)) * rstd
        for n, term in ((0, d_one * xhat), (1, d_one)):
            add_rows(n, term)

    back(0)
    four.hand(2)
    qkv[1].cross()
    mixl.cross(0)
    qkv[2].cross()
    back(1)
    four.hand(3)
    mixl.cross(1)
    mixl.settle(0)
    proj.cross()
    down.finish()
    up.finish()
    store[4].start()
    store[5].start()
    t_s[t] = jnp.zeros((8, shard), F32)
    f_s[f] = jnp.zeros((8, hidden), F32)
    sq_up = gu_o[...] * gu_o[...]
    sq_down = gd_o[...] * gd_o[...]
    t_s[t, 4:5, :] = lane_sums(sq_up)
    t_s[t, 5:6, :] = lane_sums(sq_down)
    f_s[f, 4:5, :] = jnp.sum(sq_up, axis=0, keepdims=True)
    f_s[f, 5:6, :] = jnp.sum(sq_down, axis=0, keepdims=True)
    tot_up, tot_down = total_of(sq_up), total_of(sq_down)
    table.finish(chunk_s)
    first = table.first_row()
    ident = ints((640, TOK), 0)

    def bin_row(step, acc):
        for n in range(4):
            i = step * 4 + n
            hot = ones_where(ident == ridx[pl.ds(first + i, 1), :TOK])
            vals = jnp.concatenate(
                [chunk_s[h, pl.ds(i, 1), :TOK] for h in range(heads)]
                + [jnp.zeros((8 - heads, TOK), F32)],
                axis=0,
            )
            high = vals.astype(BF)
            low = (vals - high.astype(F32)).astype(BF)
            acc = acc + dot_t(jnp.concatenate([high, low], axis=0), hot)
        return acc

    hist = lax.fori_loop(0, 3, bin_row, jnp.zeros((16, 640), F32))
    mixl.cross(2)
    mixl.settle(1)
    mixl.trade(0)
    hist = lax.fori_loop(3, 6, bin_row, hist)
    small[16:24, :640] = hist[0:8] + hist[8:16]
    back(2)
    back(3)
    sm_s[0] = small[...]

    def swap(n):
        where = ({"fsdp": near}, {"fsdp": far}, {"ctx": 1 - c})[n]
        return remote(sm_s.at[n], sm_r.at[n], sm_send.at[n], sm_recv.at[n], where)

    swap(0).start()
    mixl.cross(3)
    mixl.settle(2)
    mixl.hand(0)
    mixl.trade(1)
    swap(0).wait_recv()
    sm_s[1] = sm_s[0] + sm_r[0]
    swap(1).start()
    for member in (*qkv, proj):
        member.finish()
    store[2].start()
    store[3].start()

    tot_q = []
    for n in range(3):
        sq = gq_o[n] * gq_o[n]
        t_s[t, n : n + 1, :] = lane_sums(sq)
        f_s[f, n : n + 1, :width] = jnp.sum(sq, axis=0, keepdims=True)
        tot_q.append(total_of(sq))
    sq = gp_o[...] * gp_o[...]
    f_s[f, 3:4, :shard] = lane_sums(sq)
    t_s[t, 3:4, :] = jnp.sum(sq, axis=0, keepdims=True)
    z_s[me] = lane_pack([*tot_q, total_of(sq), tot_up, tot_down, *old_rows, *masters])

    def t_copy(n):
        return remote(t_s.at[t], t_s.at[t], t_send.at[n], t_recv.at[n], {"tp": lax.rem(t + n, 4)})

    def f_copy(n):
        return remote(f_s.at[f], f_s.at[f], f_send.at[n], f_recv.at[n], {"fsdp": lax.rem(f + n, 4)})

    def z_copy(n):
        return remote(z_s.at[me], z_s.at[me], z_send.at[n], z_recv.at[n], other(n))

    def c_copy(n):
        return remote(c_s.at[me], c_s.at[me], c_send.at[n], c_recv.at[n], other(n))

    for n in range(1, 4):
        t_copy(n).start()
        f_copy(n).start()
    for n in range(1, 16):
        z_copy(n).start()
    mixl.settle(3)
    mixl.hand(1)
    swap(1).wait_recv()
    sm_s[2] = sm_s[1] + sm_r[1]
    swap(2).start()
    home_in.go(0)
    home_in.go(1)
    mixl.trade(2)

    def lift(w):
        mixl.arrive(w)
        dft[w] = mixl.get(w)

    def leave(i):
        for r in range(WIN):
            home_o[i, (SHIFT + r) % WIN] = home_row(dft, row_tmp, i, r)

    lift(0)
    mixl.trade(3)
    mixl.hand(2)
    lift(1)
    leave(0)

    swap(2).wait_recv()
    sm = sm_s[2] + sm_r[2]

    def own_lanes(x, size):
        out = x[:, :size]
        for n in range(1, 4):
            out = jnp.where(f == n, x[:, n * size : (n + 1) * size], out)
        return out

    def own_units(row, count):
        all_lanes = count * HD
        at_lane = ints((count, all_lanes), 1)
        only = jnp.where(
            jnp.right_shift(at_lane, 5) == ints((count, all_lanes), 0),
            jnp.broadcast_to(row, (count, all_lanes)), 0.0,
        )
        pick = jnp.where(
            jnp.bitwise_and(ints((all_lanes, part_of), 0), HD - 1)
            == f * part_of + ints((all_lanes, part_of), 1),
            1.0, 0.0,
        )
        return only, pick

    gn = own_lanes(sm[0:6, :], shard)
    gh_new = [exact(*own_units(sm[8 + n : 9 + n, :width], heads), ((1,), (0,))) for n in range(2)]
    only, pick = own_units(sm[6:7, :], hidden // HD)
    gx = exact(pick, only, ((0,), (1,)))
    gt = sm[16 : 16 + heads, : w_table.shape[1]]
    gn_o[...] = gn
    gx_o[...] = gx
    gt_o[...] = gt
    small_sq = first_t * total_of(plain(gn, s_norm[...])[1] ** 2)
    for n in range(2):
        gh_o[:, n, :] = gh_new[n]
        small_sq = small_sq + total_of(plain(gh_new[n], s_heads[:, n, :])[1] ** 2)
    small_sq = small_sq + total_of(plain(gx, s_hidden[...])[1] ** 2)
    small_sq = small_sq + first_f * total_of(plain(gt, s_table[...])[1] ** 2)

    for n in range(1, 4):
        t_copy(n).wait_recv()
        f_copy(n).wait_recv()
    t_sum = t_s[0] + t_s[1] + t_s[2] + t_s[3]
    f_sum = f_s[0] + f_s[1] + f_s[2] + f_s[3]
    for n in range(1, 16):
        z_copy(n).wait_recv()
    z_sum = z_s[0]
    for n in range(1, 16):
        z_sum = z_sum + z_s[n]
    lane8 = ints((8, 128), 1)

    def scalar(n):
        return jnp.sum(jnp.where(lane8 == n, z_sum, 0.0)[0:1], axis=1, keepdims=True)

    def fresh(old, summed, count):
        return DECAY_RATE * old + keep * (summed / count + STAT_EPS)

    rq = fresh(row_qkv[...], t_sum[0:3, :], D)
    kq = fresh(col_qkv[...], f_sum[0:3, :width], D)
    rp = fresh(wide(row_proj), f_sum[3:4, :width], D)
    kp = fresh(wide(col_proj), t_sum[3:4, :], D)
    ru = fresh(wide(row_up), t_sum[4:5, :], ff)
    ku = fresh(wide(col_up), f_sum[4:5, :], D)
    rd = fresh(wide(row_down), f_sum[5:6, :], D)
    kd = fresh(wide(col_down), t_sum[5:6, :], ff)

    def mean_row(n, rows_all, cols_all):
        return (
            DECAY_RATE * scalar(6 + n) + keep * (scalar(n) / cols_all + rows_all * STAT_EPS)
        ) / rows_all

    means = [
        mean_row(0, D, D), mean_row(1, D, D), mean_row(2, D, D), mean_row(3, D, D),
        mean_row(4, D, ff), mean_row(5, ff, D),
    ]
    scales = update_scales(rq, kq, rp, kp, ru, ku, rd, kd, means)
    big_sq = small_sq
    grads = [gq_o[n] for n in range(3)] + [gp_o[...], gu_o[...], gd_o[...]]
    for grad, scale in zip(grads, scales):
        u = grad * scale
        big_sq = big_sq + total_of(u * u)
    c_s[me] = jnp.broadcast_to(big_sq, (8, 128))
    for n in range(1, 16):
        c_copy(n).start()
    rq_o[...] = rq
    kq_o[...] = kq
    for ref, row in ((rp_o, rp), (kp_o, kp), (ru_o, ru), (ku_o, ku), (rd_o, rd), (kd_o, kd)):
        put_wide(ref, row)
    mixl.hand(3)
    lift(2)
    lift(3)
    leave(1)
    store[0].start()
    for i in range(images):
        home_in.wait(i)
    store[1].start()

    counts = [3 * D * D, D * D, D * ff, ff * D] + [D] * 8 + [ff, RELP * HEADS]
    sizes = [jnp.sqrt(scalar(12 + n) / counts[n] + STAT_EPS) for n in range(14)]
    for n in range(1, 16):
        c_copy(n).wait_recv()
    all_sq = c_s[0]
    for n in range(1, 16):
        all_sq = all_sq + c_s[n]
    count_all = 4 * D * D + 2 * D * ff + 8 * D + ff + RELP * HEADS
    clip = jnp.sqrt(all_sq[0:1, 0:1] / count_all)
    factor = STEP_RATE / jnp.maximum(1.0, clip / CLIP_LEVEL)
    size_o[...] = lane_pack([size * factor for size in sizes] + [clip] + means)
    for n in range(3):
        swap(n).wait_send()
    for n in range(1, 4):
        t_copy(n).wait_send()
        f_copy(n).wait_send()
        proj_line(n).wait_send()
    for p in range(windows // 2):
        ctx_copy(p, 0, t, two.mid).wait_send()

        @pl.when(two.is_mid)
        def _():
            for kind in range(1, 5):
                ctx_copy(p, kind, t, two.mid).wait_send()

    for n in range(1, 16):
        z_copy(n).wait_send()
        c_copy(n).wait_send()
    for w in range(windows):
        mixl.drain(w)
        four.drain(w)
    for copy in halo_f:
        copy.wait_send()
    for copy in (*down_copies, *up_copies):
        copy.wait_send()
    for n in range(2):
        copy_of(n, 0, f, far).wait_send()
        copy_of(n, 1, f, near).wait_send()
        copy_of(n, 2, far, near).wait_send()
    for n in range(4):
        proj_copy(n, 0, f, far).wait_send()
        proj_copy(n, 1, f, near).wait_send()
        proj_copy(n, 2, far, near).wait_send()
    for member in (up, down, *qkv, proj, table):
        member.drain()
    for copy in store:
        copy.wait()
def finish_body(ready, *refs):
    (
        big_in, (gn, gh, gx, gt), (w_norm, w_heads, w_hidden, w_table),
        (s_norm, s_heads, s_hidden, s_table), stats, (size,),
        big_out, (gn_o, gh_o, gx_o, gt_o), (nn_o, nh_o, nx_o, nt_o), stats_o,
        (sn_o, sh_o, sx_o, st_o), (clip_o,), held, made, (i_sem, o_sem),
    ) = take(refs, (12, 4, 4, 4, 8, 1, 14, 4, 4, 8, 4, 1, 12, 10, 2))
    home_out, feat, home_in, og = held[:4]
    grads, masters = held[4:8], held[8:12]
    fetch = [
        pltpu.make_async_copy(src, dst, i_sem.at[n]) for n, (src, dst) in enumerate(zip(big_in, held))
    ]
    for n in (4, 5, 6, 7, 1, 0, 3, 2, 8, 9, 10, 11):
        fetch[n].start()
    sources = [*made[:2], *grads, *made[2:]]
    store = [
        pltpu.make_async_copy(src, dst, o_sem.at[n]) for n, (src, dst) in enumerate(zip(sources, big_out))
    ]
    for n in range(4):
        fetch[4 + n].wait()
        store[2 + n].start()
    for n in (0, 1):
        fetch[n].wait()
    made[0][...] = feat[...].astype(F32) + home_out[...].astype(F32)
    store[0].start()
    for n in (2, 3):
        fetch[n].wait()
    made[1][...] = og[...] + home_in[...].astype(F32)
    store[1].start()
    ready()
    lane8 = lax.broadcasted_iota(jnp.int32, (8, 128), 1)
    table = size[...]

    def step(n):
        return jnp.sum(jnp.where(lane8 == n, table, 0.0)[0:1], axis=1, keepdims=True)

    rq, kq, *vecs = stats
    scales = update_scales(rq[...], kq[...], *map(wide, vecs), [step(15 + n) for n in range(6)])
    for n in range(4):
        fetch[8 + n].wait()
        new_o, low_o = made[2 + n], made[6 + n]
        if n == 0:
            for m in range(3):
                new = masters[0][m] - step(0) * (grads[0][m] * scales[m])
                new_o[m] = new
                low_o[m] = new.astype(BF)
        else:
            new = masters[n][...] - step(n) * (grads[n][...] * scales[2 + n])
            new_o[...] = new
            low_o[...] = new.astype(BF)
        store[6 + n].start()
        store[10 + n].start()
    for src, dst in ((gn, gn_o), (gh, gh_o), (gx, gx_o), (gt, gt_o), *zip(stats, stats_o)):
        dst[...] = src[...]
    sn, un = plain(gn[...], s_norm[...])
    sn_o[...] = sn
    for n in range(6):
        nn_o[n : n + 1, :] = w_norm[n : n + 1, :] - step(4 + n) * un[n : n + 1, :]
    for n in range(2):
        sh, uh = plain(gh[:, n, :], s_heads[:, n, :])
        sh_o[:, n, :] = sh
        nh_o[:, n, :] = w_heads[:, n, :] - step(10 + n) * uh
    sx, ux = plain(gx[...], s_hidden[...])
    sx_o[...] = sx
    nx_o[...] = w_hidden[...] - step(12) * ux
    st, ut = plain(gt[...], s_table[...])
    st_o[...] = st
    nt_o[...] = w_table[...] - step(13) * ut
    clip_o[...] = step(14)
    for copy in store:
        copy.wait()


def whole_step(feat, og, regions, rel_index, masters, stats, states):
    w_qkv, w_proj, w_up, w_down, w_norm, w_heads, w_hidden, w_table = masters
    images = feat.shape[0]
    windows = 2 * images
    shard, width = w_qkv.shape[1], w_qkv.shape[2]
    hidden = w_up.shape[1]
    heads = width // HD
    stats = [u if u.ndim == 2 else u.reshape(-1, 128) if u.shape[0] == D else u[None] for u in stats]
    like = lambda u: (u.shape, F32)
    mats = (w_qkv, w_proj, w_up, w_down)
    smalls = (w_norm, w_heads, w_hidden, w_table)
    vm, dma = pltpu.VMEM, pltpu.SemaphoreType.DMA
    flat = windows * TOK
    halves = (2 * windows, 2, ROWS, HALF)
    tokens = (windows, TOK, D)
    rows_of = (images, SHIFT, 24, D)
    outs = [
        (feat.shape, BF), (feat.shape, BF), *map(like, mats), *map(like, smalls),
        *map(like, stats), ((8, 128), F32),
    ]
    scratch = [
        vm((4, 16, shard), BF), vm((3, D, width), BF), vm((4, D, shard), BF), vm((D, D), BF),
        vm((D, hidden), BF), vm((D, hidden), BF), vm(rows_of, BF), vm(rows_of, BF), vm(rows_of, BF),
        vm((heads, TOK, 256), F32), vm((24, D), F32), vm((16, D), F32), vm((192, 256), jnp.int32),
        vm((8, 640), F32), vm((24, D), F32),
        vm(tokens, F32), vm(tokens, F32), vm((flat, D), BF), vm((windows, TOK, width), BF),
        vm((windows, TOK, width), BF), vm((windows, TOK, width), BF),
        vm((windows, heads, TOK, TOK), F32), vm((windows // 2, 4, TOK, 2 * width), BF), vm(halves, F32),
        vm((flat, D), BF), vm((flat, hidden), BF), vm((flat, hidden), BF),
        vm(tokens, F32), vm((windows, TOK, 128), F32), vm(halves, BF), vm((D, hidden), F32),
        vm((D, hidden), F32), vm(tokens, F32), vm((flat, D), BF), vm(halves, F32),
        vm((3, flat, width), BF), vm((heads, 192, 256), F32), vm((heads, 24, 256), F32),
        vm(halves, BF),
        *LineSum.scratch(2 * windows), *LineSum.scratch(2 * windows),
        *ShardSum.scratch((shard, hidden)), *BandFirstSum.scratch((shard, hidden)),
        *[s for _ in range(3) for s in ShardSum.scratch((shard, width))], *ShardSum.scratch((width, shard)),
        *TableSum.scratch(heads),
        vm((3, 24, D), F32), vm((3, 24, D), F32), vm((4, 8, shard), F32), vm((4, 8, hidden), F32),
        vm((16, 8, 128), F32), vm((16, 8, 128), F32),
        vm(feat.shape, BF), vm(og.shape, F32), *[vm(u.shape, F32) for u in mats],
        vm(halves, BF), vm((windows, ROWS, HALF), BF), dma((windows,)), dma((windows,)), dma((6,)),
        dma((2, 5)), dma((2, 5)),
        vm(feat.shape, BF), vm(feat.shape, BF), *[vm(u.shape, F32) for u in mats], dma((6,)),
        dma((2, 3)), dma((2, 3)), dma((4, 3)), dma((4, 3)), dma((4,)), dma((4,)),
        dma((2 * images,)), dma((2 * images,)), *[dma((images,))] * 2,
        dma((windows // 2, 5)), dma((windows // 2, 4)),
        dma((3,)), dma((3,)), *[dma((4,))] * 4, *[dma((16,))] * 4,
    ]
    got = vmem_call(step_body, outs, scratch, "whole_step", 1, 6, 6)(
        feat, og, *mats, regions, rel_index, *smalls, *stats, *states
    )
    home_out, home_in, g_qkv, g_proj, g_up, g_down, gn, gh, gx, gt, *rest = got
    new_stats, size = rest[:8], rest[8]
    outs = [
        like(og), like(og), *map(like, mats), *map(like, mats), *[(u.shape, BF) for u in mats],
        *map(like, smalls), *map(like, smalls), *map(like, stats), *map(like, smalls), ((1, 1), F32),
    ]
    scratch = [
        vm(feat.shape, BF), vm(feat.shape, BF), vm(feat.shape, BF), vm(og.shape, F32),
        *[vm(u.shape, F32) for u in mats], *[vm(u.shape, F32) for u in mats],
        vm(og.shape, F32), vm(og.shape, F32), *[vm(u.shape, F32) for u in mats],
        *[vm(u.shape, BF) for u in mats], dma((12,)), dma((14,)),
    ]
    return vmem_call(finish_body, outs, scratch, "finish", None, 12, 14)(
        home_out, feat, home_in, og, g_qkv, g_proj, g_up, g_down, *mats, gn, gh, gx, gt,
        *smalls, *states, *new_stats, size,
    )


def per_device_plain(
    features,
    out_grad,
    regions,
    rel_index,
    w_qkv,
    w_proj,
    w_up,
    w_down,
    norm_vecs,
    head_bias,
    hidden_bias,
    rel_table,
    row_qkv,
    col_qkv,
    row_proj,
    col_proj,
    row_up,
    col_up,
    row_down,
    col_down,
    state_norm,
    state_heads,
    state_hidden,
    state_table,
):
    images, band_rows, across, model_width = features.shape
    win_tokens = WIN * WIN
    fsdp_at = lax.axis_index("fsdp")
    ctx_at = lax.axis_index("ctx")
    tp_at = lax.axis_index("tp")
    first_fsdp = (fsdp_at == 0).astype(jnp.float32)
    first_ctx = (ctx_at == 0).astype(jnp.float32)
    first_tp = (tp_at == 0).astype(jnp.float32)
    weights_qkv, weights_proj, weights_up, weights_down, vec_copy, head_copy, hidden_copy = (
        lax.all_gather(w_qkv.astype(jnp.bfloat16), "fsdp", axis=1, tiled=True),
        lax.all_gather(w_proj.astype(jnp.bfloat16), "fsdp", axis=1, tiled=True),
        lax.all_gather(w_up.astype(jnp.bfloat16), "fsdp", axis=0, tiled=True),
        lax.all_gather(w_down.astype(jnp.bfloat16), "fsdp", axis=1, tiled=True),
        lax.all_gather(norm_vecs.astype(jnp.bfloat16), "fsdp", axis=1, tiled=True),
        lax.all_gather(head_bias.astype(jnp.bfloat16), "fsdp", axis=2, tiled=True),
        lax.all_gather(hidden_bias.astype(jnp.bfloat16), "fsdp", axis=1, tiled=True),
    )
    norm_rows = vec_copy.astype(jnp.float32)
    bias_query = head_copy[0].reshape(-1).astype(jnp.float32)
    bias_value = head_copy[1].reshape(-1).astype(jnp.float32)
    bias_hidden = hidden_copy.reshape(-1).astype(jnp.float32)
    table_copy = rel_table.astype(jnp.bfloat16)
    local_width = weights_qkv.shape[2]
    heads_here = local_width // HD

    def roll_in(home):
        received = passed_along(home[:, :SHIFT], "ctx", -1)
        return to_windows(enter_frame(home, received)).reshape(-1, model_width)

    def roll_out(rolled_flat):
        band = jnp.roll(
            from_windows(
                rolled_flat.reshape(-1, win_tokens, model_width), images, band_rows, across
            ),
            SHIFT,
            axis=2,
        )
        lower = passed_along(band[:, band_rows - SHIFT :], "ctx", 1)
        return jnp.concatenate([lower, band[:, : band_rows - SHIFT]], axis=1)

    flat_one = roll_in(features).astype(jnp.float32)
    grad_flat = roll_in(out_grad)
    win_count = flat_one.shape[0] // win_tokens
    normed_one, pull_one = jax.vjp(layer_norm, flat_one, norm_rows[0], norm_rows[1])
    normed_one_low = normed_one.astype(jnp.bfloat16)
    head_shape = (win_count, win_tokens, heads_here, HD)
    query_low, key_low, value_low = project_heads(
        normed_one_low, weights_qkv, bias_query, bias_value, head_shape
    )
    pos_bias = table_lookup(table_copy, rel_index)
    region_win = to_windows(regions[..., None])[..., 0]
    mask_add = jnp.where(region_win[:, :, None] == region_win[:, None, :], 0.0, MASK_FILL).astype(
        jnp.float32
    )
    scores = attention_scores(query_low, key_low, pos_bias, mask_add)
    top_score = jnp.max(scores, axis=-1, keepdims=True)
    lifted = jnp.exp(scores - top_score)
    prob_rows = lifted / jnp.sum(lifted, axis=-1, keepdims=True)
    prob_low = prob_rows.astype(jnp.bfloat16)
    context = jnp.einsum("whij,wjhc->wihc", prob_low, value_low, preferred_element_type=jnp.float32)
    context_low = context.astype(jnp.bfloat16).reshape(-1, local_width)
    branch_part = jnp.dot(context_low, weights_proj, preferred_element_type=jnp.float32)
    branch = lax.psum(branch_part.astype(jnp.bfloat16), "tp").astype(jnp.float32) + norm_rows[2]
    flat_two = flat_one + branch
    normed_two, pull_two = jax.vjp(layer_norm, flat_two, norm_rows[3], norm_rows[4])
    normed_two_low = normed_two.astype(jnp.bfloat16)
    pre_act = jnp.dot(normed_two_low, weights_up, preferred_element_type=jnp.float32) + bias_hidden
    hidden, pull_gelu = jax.vjp(exact_gelu, pre_act)
    hidden_low = hidden.astype(jnp.bfloat16)
    mixed_part = jnp.dot(hidden_low, weights_down, preferred_element_type=jnp.float32)
    mixed_whole = lax.psum(mixed_part.astype(jnp.bfloat16), "tp").astype(jnp.float32)
    block_out = features.astype(jnp.float32) + roll_out(
        (branch + mixed_whole + norm_rows[5]).astype(jnp.bfloat16)
    ).astype(jnp.float32)
    grad_low = grad_flat.astype(jnp.bfloat16)
    grad_down_full = jnp.einsum(
        "tf,td->fd", hidden_low, grad_low, preferred_element_type=jnp.float32
    )
    grad_down_bias = jnp.sum(grad_flat, axis=0)
    d_hidden = jnp.einsum("td,fd->tf", grad_low, weights_down, preferred_element_type=jnp.float32)
    d_pre = pull_gelu(d_hidden)[0]
    d_pre_low = d_pre.astype(jnp.bfloat16)
    grad_hidden_bias = jnp.sum(d_pre, axis=0)
    grad_up_full = jnp.einsum(
        "td,tf->df", normed_two_low, d_pre_low, preferred_element_type=jnp.float32
    )
    d_two_part = jnp.einsum("tf,df->td", d_pre_low, weights_up, preferred_element_type=jnp.float32)
    d_two = lax.psum(d_two_part.astype(jnp.bfloat16), "tp").astype(jnp.float32)
    d_flat_two, grad_gain_two, grad_offset_two = pull_two(d_two)
    d_resid = grad_flat + d_flat_two
    grad_proj_bias = jnp.sum(d_resid, axis=0)
    d_branch = d_resid.astype(jnp.bfloat16)
    grad_proj_full = jnp.einsum(
        "tc,td->cd", context_low, d_branch, preferred_element_type=jnp.float32
    )
    d_context = (
        jnp.einsum("td,cd->tc", d_branch, weights_proj, preferred_element_type=jnp.float32)
        .astype(jnp.bfloat16)
        .reshape(head_shape)
    )
    d_probs = jnp.einsum(
        "wihc,wjhc->whij", d_context, value_low, preferred_element_type=jnp.float32
    )
    d_value_low = jnp.einsum(
        "whij,wihc->wjhc", prob_low, d_context, preferred_element_type=jnp.float32
    ).astype(jnp.bfloat16)
    d_scores = prob_rows * (d_probs - jnp.sum(prob_rows * d_probs, axis=-1, keepdims=True))
    d_pos = jnp.sum(d_scores, axis=0)
    d_scaled = (d_scores * HD ** (-0.5)).astype(jnp.bfloat16)
    d_query_low = jnp.einsum(
        "whij,wjhc->wihc", d_scaled, key_low, preferred_element_type=jnp.float32
    ).astype(jnp.bfloat16)
    d_key_low = jnp.einsum(
        "whij,wihc->wjhc", d_scaled, query_low, preferred_element_type=jnp.float32
    ).astype(jnp.bfloat16)
    d_heads = jnp.stack([d_query_low, d_key_low, d_value_low]).reshape(3, -1, local_width)
    grad_qkv_full = jnp.einsum(
        "td,ktc->kdc", normed_one_low, d_heads, preferred_element_type=jnp.float32
    )
    grad_head_bias = jnp.stack(
        [
            jnp.sum(d_heads[0].astype(jnp.float32), axis=0),
            jnp.sum(d_heads[2].astype(jnp.float32), axis=0),
        ]
    ).reshape(2, heads_here, HD)
    d_one_part = jnp.einsum("ktc,kdc->td", d_heads, weights_qkv, preferred_element_type=jnp.float32)
    d_one = lax.psum(d_one_part.astype(jnp.bfloat16), "tp").astype(jnp.float32)
    d_flat_one, grad_gain_one, grad_offset_one = pull_one(d_one)
    grad_input = out_grad + roll_out((d_flat_two + d_flat_one).astype(jnp.bfloat16)).astype(
        jnp.float32
    )
    table_part = table_grad(d_pos, rel_index, rel_table.shape[0])
    grad_norm_full = jnp.stack(
        [
            grad_gain_one,
            grad_offset_one,
            grad_proj_bias,
            grad_gain_two,
            grad_offset_two,
            grad_down_bias,
        ]
    )
    grad_list = (
        grad_qkv_full,
        grad_proj_full,
        grad_up_full,
        grad_down_full,
        grad_norm_full,
        grad_head_bias,
        grad_hidden_bias.reshape(-1, HD),
    )
    g_qkv, g_proj, g_up, g_down, g_norm, g_heads, g_hidden = shard_sum(band_sum(grad_list))
    d_shard = w_qkv.shape[1]
    hidden_here = w_up.shape[1]
    keep = 1.0 - DECAY_RATE
    sq_qkv = g_qkv * g_qkv
    sq_proj = g_proj * g_proj
    sq_up = g_up * g_up
    sq_down = g_down * g_down
    stat_rq = place(
        (keep * jnp.sum(sq_qkv, axis=2) / D + first_tp * (DECAY_RATE * row_qkv + keep * STAT_EPS))
        * first_ctx,
        fsdp_at,
        D,
    )
    stat_cq = place(
        (keep * jnp.sum(sq_qkv, axis=1) / D + first_fsdp * (DECAY_RATE * col_qkv + keep * STAT_EPS))
        * first_ctx,
        tp_at,
        D,
    )
    stat_rp = place(
        (
            keep * jnp.sum(sq_proj, axis=1) / D
            + first_fsdp * (DECAY_RATE * row_proj + keep * STAT_EPS)
        )
        * first_ctx,
        tp_at,
        D,
    )
    stat_cp = place(
        (keep * jnp.sum(sq_proj, axis=0) / D + first_tp * (DECAY_RATE * col_proj + keep * STAT_EPS))
        * first_ctx,
        fsdp_at,
        D,
    )
    stat_ru = place(
        (keep * jnp.sum(sq_up, axis=1) / FF + first_tp * (DECAY_RATE * row_up + keep * STAT_EPS))
        * first_ctx,
        fsdp_at,
        D,
    )
    stat_cu = place(
        (keep * jnp.sum(sq_up, axis=0) / D + first_fsdp * (DECAY_RATE * col_up + keep * STAT_EPS))
        * first_ctx,
        tp_at,
        FF,
    )
    stat_rd = place(
        (
            keep * jnp.sum(sq_down, axis=1) / D
            + first_fsdp * (DECAY_RATE * row_down + keep * STAT_EPS)
        )
        * first_ctx,
        tp_at,
        FF,
    )
    stat_cd = place(
        (
            keep * jnp.sum(sq_down, axis=0) / FF
            + first_tp * (DECAY_RATE * col_down + keep * STAT_EPS)
        )
        * first_ctx,
        fsdp_at,
        D,
    )
    table_whole = place(table_part, tp_at, HEADS)
    master_sq = jnp.concatenate(
        [
            jnp.stack(
                [
                    jnp.sum(w_qkv * w_qkv),
                    jnp.sum(w_proj * w_proj),
                    jnp.sum(w_up * w_up),
                    jnp.sum(w_down * w_down),
                ]
            )
            * first_ctx,
            jnp.sum(norm_vecs * norm_vecs, axis=1) * first_ctx * first_tp,
            jnp.sum(head_bias * head_bias, axis=(1, 2)) * first_ctx,
            jnp.sum(hidden_bias * hidden_bias)[None] * first_ctx,
            jnp.sum(rel_table * rel_table)[None] * first_ctx * first_fsdp,
        ]
    )
    (
        full_rq,
        full_cq,
        full_rp,
        full_cp,
        full_ru,
        full_cu,
        full_rd,
        full_cd,
        table_sum,
        master_total,
    ) = lax.psum(
        (
            stat_rq,
            stat_cq,
            stat_rp,
            stat_cp,
            stat_ru,
            stat_cu,
            stat_rd,
            stat_cd,
            table_whole,
            master_sq,
        ),
        ("fsdp", "ctx", "tp"),
    )
    u_qkv = factored(
        g_qkv,
        own_part(full_rq, fsdp_at, d_shard),
        own_part(full_cq, tp_at, local_width),
        jnp.mean(full_rq, axis=1)[:, None, None],
    )
    u_proj = factored(
        g_proj,
        own_part(full_rp, tp_at, local_width),
        own_part(full_cp, fsdp_at, d_shard),
        jnp.mean(full_rp),
    )
    u_up = factored(
        g_up,
        own_part(full_ru, fsdp_at, d_shard),
        own_part(full_cu, tp_at, hidden_here),
        jnp.mean(full_ru),
    )
    u_down = factored(
        g_down,
        own_part(full_rd, tp_at, hidden_here),
        own_part(full_cd, fsdp_at, d_shard),
        jnp.mean(full_rd),
    )
    g_table = own_part(table_sum, tp_at, heads_here)
    state_norm_new, u_norm = plain_stats(g_norm, state_norm)
    state_heads_new, u_heads = plain_stats(g_heads, state_heads)
    state_hidden_new, u_hidden = plain_stats(g_hidden, state_hidden)
    state_table_new, u_table = plain_stats(g_table, state_table)
    local_sq = (
        jnp.sum(u_qkv * u_qkv)
        + jnp.sum(u_proj * u_proj)
        + jnp.sum(u_up * u_up)
        + jnp.sum(u_down * u_down)
        + jnp.sum(u_heads * u_heads)
        + jnp.sum(u_hidden * u_hidden)
        + first_tp * jnp.sum(u_norm * u_norm)
        + first_fsdp * jnp.sum(u_table * u_table)
    )
    total_sq = lax.psum(local_sq, ("fsdp", "tp"))
    count_all = 4 * D * D + 2 * D * FF + 8 * D + FF + RELP * HEADS
    clip_rms = jnp.sqrt(total_sq / count_all)
    factor = 1.0 / jnp.maximum(1.0, clip_rms / CLIP_LEVEL)
    counts = jnp.array(
        [3 * D * D, D * D, D * FF, FF * D, D, D, D, D, D, D, D, D, FF, RELP * HEADS], jnp.float32
    )
    scales = jnp.sqrt(master_total / counts + STAT_EPS)
    new_qkv = w_qkv - STEP_RATE * scales[0] * factor * u_qkv
    new_proj = w_proj - STEP_RATE * scales[1] * factor * u_proj
    new_up = w_up - STEP_RATE * scales[2] * factor * u_up
    new_down = w_down - STEP_RATE * scales[3] * factor * u_down
    new_norm = norm_vecs - STEP_RATE * scales[4:10][:, None] * factor * u_norm
    new_heads = head_bias - STEP_RATE * scales[10:12][:, None, None] * factor * u_heads
    new_hidden = hidden_bias - STEP_RATE * scales[12] * factor * u_hidden
    new_table = rel_table - STEP_RATE * scales[13] * factor * u_table
    return (
        block_out,
        grad_input,
        g_qkv,
        g_proj,
        g_up,
        g_down,
        g_norm,
        g_heads,
        g_hidden,
        g_table,
        new_qkv,
        new_proj,
        new_up,
        new_down,
        new_norm,
        new_heads,
        new_hidden,
        new_table,
        new_qkv.astype(jnp.bfloat16),
        new_proj.astype(jnp.bfloat16),
        new_up.astype(jnp.bfloat16),
        new_down.astype(jnp.bfloat16),
        own_part(full_rq, fsdp_at, d_shard),
        own_part(full_cq, tp_at, local_width),
        own_part(full_rp, tp_at, local_width),
        own_part(full_cp, fsdp_at, d_shard),
        own_part(full_ru, fsdp_at, d_shard),
        own_part(full_cu, tp_at, hidden_here),
        own_part(full_rd, tp_at, hidden_here),
        own_part(full_cd, fsdp_at, d_shard),
        state_norm_new,
        state_heads_new,
        state_hidden_new,
        state_table_new,
        clip_rms,
    )


def per_device(
    features,
    out_grad,
    regions,
    rel_index,
    w_qkv,
    w_proj,
    w_up,
    w_down,
    norm_vecs,
    head_bias,
    hidden_bias,
    rel_table,
    row_qkv,
    col_qkv,
    row_proj,
    col_proj,
    row_up,
    col_up,
    row_down,
    col_down,
    state_norm,
    state_heads,
    state_hidden,
    state_table,
):
    flip = lambda u: u.transpose(1, 0, 2)
    (block_out, grad_input, g_qkv, g_proj, g_up, g_down, new_qkv, new_proj, new_up, new_down,
     copy_qkv, copy_proj, copy_up, copy_down, g_norm, g_heads, g_hidden, g_table,
     new_norm, new_heads, new_hidden, new_table, *rest) = whole_step(
        features, out_grad, flip(regions), rel_index,
        (w_qkv, w_proj, w_up, w_down.T, norm_vecs, flip(head_bias), hidden_bias.T, rel_table.T),
        (row_qkv, col_qkv, row_proj, col_proj, row_up, col_up, row_down, col_down),
        (state_norm, flip(state_heads), state_hidden.T, state_table.T))
    factors, states, clip_rms = rest[:8], rest[8:12], rest[12]
    factors = list(factors[:2]) + [u.reshape(-1) for u in factors[2:]]
    return (
        block_out, grad_input, g_qkv, g_proj, g_up, g_down.T, g_norm, flip(g_heads), g_hidden.T,
        g_table.T, new_qkv, new_proj, new_up, new_down.T, new_norm, flip(new_heads), new_hidden.T,
        new_table.T, copy_qkv, copy_proj, copy_up, copy_down.T, *factors,
        states[0], flip(states[1]), states[2].T, states[3].T, clip_rms[0, 0],
    )


def solution(mesh):
    line_of_four = mesh.shape["fsdp"] == 4 and mesh.shape["tp"] == 4 and mesh.shape["ctx"] == 2
    return jax.shard_map(
        per_device if line_of_four else per_device_plain,
        mesh=mesh,
        in_specs=(
            P("fsdp", "ctx", None, None),
            P("fsdp", "ctx", None, None),
            P("fsdp", "ctx", None),
            P(),
            P(None, "fsdp", "tp"),
            P("tp", "fsdp"),
            P("fsdp", "tp"),
            P("tp", "fsdp"),
            P(None, "fsdp"),
            P(None, "tp", "fsdp"),
            P("tp", "fsdp"),
            P(None, "tp"),
            P(None, "fsdp"),
            P(None, "tp"),
            P("tp"),
            P("fsdp"),
            P("fsdp"),
            P("tp"),
            P("tp"),
            P("fsdp"),
            P(None, "fsdp"),
            P(None, "tp", "fsdp"),
            P("tp", "fsdp"),
            P(None, "tp"),
        ),
        out_specs=(
            P("fsdp", "ctx", None, None),
            P("fsdp", "ctx", None, None),
            P(None, "fsdp", "tp"),
            P("tp", "fsdp"),
            P("fsdp", "tp"),
            P("tp", "fsdp"),
            P(None, "fsdp"),
            P(None, "tp", "fsdp"),
            P("tp", "fsdp"),
            P(None, "tp"),
            P(None, "fsdp", "tp"),
            P("tp", "fsdp"),
            P("fsdp", "tp"),
            P("tp", "fsdp"),
            P(None, "fsdp"),
            P(None, "tp", "fsdp"),
            P("tp", "fsdp"),
            P(None, "tp"),
            P(None, "fsdp", "tp"),
            P("tp", "fsdp"),
            P("fsdp", "tp"),
            P("tp", "fsdp"),
            P(None, "fsdp"),
            P(None, "tp"),
            P("tp"),
            P("fsdp"),
            P("fsdp"),
            P("tp"),
            P("tp"),
            P("fsdp"),
            P(None, "fsdp"),
            P(None, "tp", "fsdp"),
            P("tp", "fsdp"),
            P(None, "tp"),
            P(),
        ),
        check_vma=False,
    )
```
